32 devices in a mesh: model: 4 (over z), data: 8 (over y, x, core).
Axes of the slice: x: 2, y: 2, z: 4, core: 2. Of those that a mesh axis runs over, the one named last changes fastest.
Arguments:
- x_in: bfloat16 [8, 2048, 1024], P('data')
- cot_out: bfloat16 [8, 2048, 1024], P('data')
- step_emb: bfloat16 [2, 1024], replicated
- w_q: bfloat16 [1024, 1024], P(None, 'model')
- w_k: bfloat16 [1024, 1024], P(None, 'model')
- w_v: bfloat16 [1024, 1024], P(None, 'model')
- w_o: bfloat16 [1024, 1024], P('model')
- w_1: bfloat16 [1024, 4096], P(None, 'model')
- w_2: bfloat16 [4096, 1024], P('model')
Outputs:
- output 1: float32 [1024, 1024], P(None, 'model')
- output 2: float32 [1024, 1024], P(None, 'model')
- output 3: float32 [1024, 1024], P(None, 'model')
- output 4: float32 [1024, 1024], P('model')
- output 5: float32 [1024, 4096], P(None, 'model')
- output 6: float32 [4096, 1024], P('model')
- output 7: bfloat16 [8, 2048, 1024], P('data')
All inputs are finite; a program needn't handle non-finite values.
Results may differ from the reference program's by a relative error of at most 0.0150261.
Values are sent between devices in bfloat16 or wider.
A program may use at most 1 GiB of HBM per device.

```python
import jax
import jax.numpy as jnp
from jax import lax

BATCH = 8
SEQ = 2048
D = 1024
HEADS = 16
FF = 4096
LAYERS = 2


def normal_weight(key, rows, cols):
    return (jax.random.normal(key, (rows, cols), jnp.float32) * rows ** -0.5).astype(jnp.bfloat16)


def setup_inputs(seed: int = 0) -> dict:
    key_list = jax.random.split(jax.random.key(seed), 9)
    x_in = jax.random.normal(key_list[0], (BATCH, SEQ, D), jnp.float32).astype(jnp.bfloat16)
    cot_out = jax.random.normal(key_list[1], (BATCH, SEQ, D), jnp.float32).astype(jnp.bfloat16)
    step_emb = (0.5 * jax.random.normal(key_list[2], (LAYERS, D), jnp.float32)).astype(jnp.bfloat16)
    return dict(x_in=x_in, cot_out=cot_out, step_emb=step_emb,
                w_q=normal_weight(key_list[3], D, D), w_k=normal_weight(key_list[4], D, D),
                w_v=normal_weight(key_list[5], D, D), w_o=normal_weight(key_list[6], D, D),
                w_1=normal_weight(key_list[7], D, FF), w_2=normal_weight(key_list[8], FF, D))


def rms_norm(values):
    return values * lax.rsqrt(jnp.mean(values * values, axis=-1, keepdims=True) + 1e-6)


def attend_one(qkv_seq):
    q_seq, k_seq, v_seq = qkv_seq
    head_dim = q_seq.shape[-1]
    scores = jnp.einsum('qhe,khe->hqk', q_seq, k_seq) * (head_dim ** -0.5)
    prob_mat = jax.nn.softmax(scores, axis=-1).astype(jnp.bfloat16).astype(jnp.float32)
    return jnp.einsum('hqk,khe->qhe', prob_mat, v_seq).astype(jnp.bfloat16)


def shared_block(x_cur, step_vec, weights32):
    w_q, w_k, w_v, w_o, w_1, w_2 = weights32
    batch_size, seq_len, width_model = x_cur.shape
    head_shape = (batch_size, seq_len, HEADS, width_model // HEADS)
    x_f = x_cur.astype(jnp.float32) + step_vec.astype(jnp.float32)
    u_f = rms_norm(x_f).astype(jnp.bfloat16).astype(jnp.float32)
    q_all = jnp.einsum('bsd,de->bse', u_f, w_q).astype(jnp.bfloat16).astype(jnp.float32).reshape(head_shape)
    k_all = jnp.einsum('bsd,de->bse', u_f, w_k).astype(jnp.bfloat16).astype(jnp.float32).reshape(head_shape)
    v_all = jnp.einsum('bsd,de->bse', u_f, w_v).astype(jnp.bfloat16).astype(jnp.float32).reshape(head_shape)
    context = lax.map(jax.checkpoint(attend_one), (q_all, k_all, v_all))
    context_f = context.reshape(batch_size, seq_len, width_model).astype(jnp.float32)
    h_f = (x_f + jnp.einsum('bse,ed->bsd', context_f, w_o)).astype(jnp.bfloat16).astype(jnp.float32)
    m_f = rms_norm(h_f).astype(jnp.bfloat16).astype(jnp.float32)
    z_b = jnp.einsum('bsd,df->bsf', m_f, w_1).astype(jnp.bfloat16)
    g_f = jax.nn.gelu(z_b.astype(jnp.float32)).astype(jnp.bfloat16).astype(jnp.float32)
    return (h_f + jnp.einsum('bsf,fd->bsd', g_f, w_2)).astype(jnp.bfloat16)


def reference(x_in, cot_out, step_emb, w_q, w_k, w_v, w_o, w_1, w_2):
    weights32 = tuple(weight.astype(jnp.float32) for weight in (w_q, w_k, w_v, w_o, w_1, w_2))

    def forward(x_start, weight_set):
        def scan_body(x_cur, step_vec):
            return jax.checkpoint(shared_block)(x_cur, step_vec, weight_set), None
        x_last, _ = lax.scan(scan_body, x_start, step_emb)
        return x_last

    _, pull_back = jax.vjp(forward, x_in, weights32)
    d_x, d_w = pull_back(cot_out)
    return (d_w[0], d_w[1], d_w[2], d_w[3], d_w[4], d_w[5], d_x)
```

```python
import functools
import math

import jax
import jax.numpy as jnp
from jax import lax
from jax.experimental import pallas as pl
from jax.experimental.pallas import tpu as pltpu
from jax.sharding import PartitionSpec as P

HEAD_DIM = 64
EPS_NORM = 1e-6
SCALE = HEAD_DIM ** -0.5
EXP2_SCALE = SCALE * math.log2(math.e)
PAIR = 2 * HEAD_DIM
BLOCK_Q = 256
INTERPRET = False
AXES = ('model', 'data')
BF16 = jnp.bfloat16
F32 = jnp.float32


def rms_norm(values):
    return values * lax.rsqrt(jnp.mean(values * values, axis=-1, keepdims=True) + EPS_NORM)


def dot_nt(a, b):
    return lax.dot_general(a, b, (((1,), (1,)), ((), ())), preferred_element_type=F32)


def dot_nn(a, b):
    return lax.dot_general(a, b, (((1,), (0,)), ((), ())), preferred_element_type=F32)


def dot_tn(a, b):
    return lax.dot_general(a, b, (((0,), (0,)), ((), ())), preferred_element_type=F32)


def attn_fwd_kernel(q_ref, k_ref, v_ref, o_ref, lse_ref, vt_ref):
    @pl.when(pl.program_id(1) == 0)
    def _():
        vt_ref[...] = v_ref[...].T

    lane = lax.broadcasted_iota(jnp.int32, q_ref.shape, 1)
    outs = []
    for head in range(2):
        q_head = jnp.where(lane // HEAD_DIM == head, q_ref[...], jnp.zeros_like(q_ref))
        scores = dot_nt(k_ref[...], q_head)
        top = jnp.max(scores, axis=0, keepdims=True) * EXP2_SCALE
        weights = jnp.exp2(scores * EXP2_SCALE - top)
        total = jnp.sum(weights, axis=0, keepdims=True)
        probs = (weights * (1.0 / total)).astype(BF16)
        lse_ref[0, head:head + 1, :] = top + jnp.log2(total)
        outs.append(dot_nn(vt_ref[head * HEAD_DIM:(head + 1) * HEAD_DIM, :], probs))
    o_ref[...] = jnp.concatenate(outs, axis=0).T.astype(BF16)


def attn_fwd(qkv):
    seq, width = qkv.shape[0], qkv.shape[1] // 3
    pairs = width // PAIR
    grid = (pairs, seq // BLOCK_Q)
    return pl.pallas_call(
        attn_fwd_kernel,
        grid=grid,
        in_specs=[
            pl.BlockSpec((BLOCK_Q, PAIR), lambda p, i: (i, p)),
            pl.BlockSpec((seq, PAIR), lambda p, i: (0, pairs + p)),
            pl.BlockSpec((seq, PAIR), lambda p, i: (0, 2 * pairs + p)),
        ],
        out_specs=[
            pl.BlockSpec((BLOCK_Q, PAIR), lambda p, i: (i, p)),
            pl.BlockSpec((1, 2, BLOCK_Q), lambda p, i: (p, 0, i)),
        ],
        out_shape=[
            jax.ShapeDtypeStruct((seq, width), BF16),
            jax.ShapeDtypeStruct((pairs, 2, seq), F32),
        ],
        scratch_shapes=[pltpu.VMEM((PAIR, seq), BF16)],
        compiler_params=pltpu.CompilerParams(vmem_limit_bytes=60 << 20),
        cost_estimate=pl.CostEstimate(
            flops=16 * seq * seq * width, bytes_accessed=8 * seq * width, transcendentals=seq * seq * 2 * pairs),
        interpret=INTERPRET,
        name="attn_fwd",
    )(qkv, qkv, qkv)


def attn_bwd_kernel(q_ref, k_ref, v_ref, do_ref, lse_ref, dq_ref, dk_ref, dv_ref,
                    kt_ref, dk_acc, dv_acc, p_cat, ds_cat):
    step = pl.program_id(1)

    @pl.when(step == 0)
    def _():
        kt_ref[...] = k_ref[...].T
        dk_acc[...] = jnp.zeros_like(dk_acc)
        dv_acc[...] = jnp.zeros_like(dv_acc)

    block = q_ref.shape[0]
    lane = lax.broadcasted_iota(jnp.int32, q_ref.shape, 1)
    q_heads, do_heads, dqs = [], [], []
    for head in range(2):
        mine = lane // HEAD_DIM == head
        q_head = jnp.where(mine, q_ref[...], jnp.zeros_like(q_ref))
        do_head = jnp.where(mine, do_ref[...], jnp.zeros_like(do_ref))
        scores = dot_nt(k_ref[...], q_head)
        probs = jnp.exp2(scores * EXP2_SCALE - lse_ref[0, head:head + 1, :])
        d_probs = dot_nt(v_ref[...], do_head).astype(BF16).astype(F32)
        inner = jnp.sum(probs * d_probs, axis=0, keepdims=True)
        cols = slice(head * block, (head + 1) * block)
        p_cat[:, cols] = probs.astype(BF16)
        ds_cat[:, cols] = (probs * (d_probs - inner)).astype(BF16)
        dqs.append(dot_nn(kt_ref[head * HEAD_DIM:(head + 1) * HEAD_DIM, :], ds_cat[:, cols]))
        q_heads.append(q_head)
        do_heads.append(do_head)
    dv_acc[...] += dot_nn(p_cat[...], jnp.concatenate(do_heads, axis=0))
    dk_acc[...] += dot_nn(ds_cat[...], jnp.concatenate(q_heads, axis=0))
    dq_ref[...] = (jnp.concatenate(dqs, axis=0).T * SCALE).astype(BF16)

    @pl.when(step == pl.num_programs(1) - 1)
    def _():
        dk_ref[...] = (dk_acc[...] * SCALE).astype(BF16)
        dv_ref[...] = dv_acc[...].astype(BF16)


def attn_bwd(qkv, d_context, lse):
    seq, width = d_context.shape
    pairs = width // PAIR
    full = lambda offset: pl.BlockSpec((seq, PAIR), lambda p, i: (0, offset + p))
    rows = pl.BlockSpec((BLOCK_Q, PAIR), lambda p, i: (i, p))
    return pl.pallas_call(
        attn_bwd_kernel,
        grid=(pairs, seq // BLOCK_Q),
        in_specs=[rows, full(pairs), full(2 * pairs), rows, pl.BlockSpec((1, 2, BLOCK_Q), lambda p, i: (p, 0, i))],
        out_specs=[rows, full(0), full(0)],
        out_shape=[jax.ShapeDtypeStruct((seq, width), BF16)] * 3,
        scratch_shapes=[
            pltpu.VMEM((PAIR, seq), BF16),
            pltpu.VMEM((seq, PAIR), F32),
            pltpu.VMEM((seq, PAIR), F32),
            pltpu.VMEM((seq, 2 * BLOCK_Q), BF16),
            pltpu.VMEM((seq, 2 * BLOCK_Q), BF16),
        ],
        compiler_params=pltpu.CompilerParams(vmem_limit_bytes=60 << 20),
        cost_estimate=pl.CostEstimate(
            flops=40 * seq * seq * width, bytes_accessed=14 * seq * width, transcendentals=seq * seq * 2 * pairs),
        interpret=INTERPRET,
        name="attn_bwd",
    )(qkv, qkv, qkv, d_context, lse)


def lin(z, y, x, c):
    return z * 8 + y * 4 + x * 2 + c


def send(value, to):
    pairs = []
    for z in range(4):
        for y in range(2):
            for x in range(2):
                for c in range(2):
                    dst = to(z, y, x, c)
                    if dst is not None:
                        pairs.append((lin(z, y, x, c), lin(*dst)))
    return lax.ppermute(value, AXES, pairs)


def role_of(z, c):
    return (z % 2) * 2 + c


def in_group(k):
    def to(z, y, x, c):
        role = role_of(z, c) ^ k
        return (z // 2 * 2 + role // 2, y, x, role % 2)
    return to


def to_group(k):
    def to(z, y, x, c):
        role = z ^ k
        return (2 * c + role // 2, y, x, role % 2)
    return to


def to_planes(k):
    def to(z, y, x, c):
        return (role_of(z, c) ^ k, y, x, z // 2)
    return to


def unscramble(parts, role):
    odd, high = role % 2 == 1, role // 2 == 1
    a = [jnp.where(odd, parts[i ^ 1], parts[i]) for i in range(4)]
    return [jnp.where(high, a[i ^ 2], a[i]) for i in range(4)]


def rows_of(value, index, count):
    return lax.dynamic_slice_in_dim(value, index * count, count, axis=0)


def solution(mesh):
    spec_col = P(None, 'model')
    spec_row = P('model', None)
    spec_act = P('data', None, None)
    spec_rep = P(None, None)

    def device_step(x_in, cot_out, step_emb, w_q, w_k, w_v, w_o, w_1, w_2):
        seq, d_model = x_in.shape[1:]
        head_cols = w_q.shape[1]
        ff_cols = w_1.shape[1]
        blk = seq // 4
        piece = d_model // 8
        z = lax.axis_index('model')
        d = lax.axis_index('data')
        y, x, core = d // 4, d // 2 % 2, d % 2
        group = z // 2
        role = z % 2 * 2 + core
        owner = core == group
        emb = step_emb.astype(F32)

        def gather(shard):
            part = rows_of(shard, d, piece)
            part = lax.all_gather(part, 'model', axis=1, tiled=True)
            return lax.all_gather(part, 'data', axis=0, tiled=True)

        w_qkv_own = jnp.concatenate([w_q, w_k, w_v], axis=1)
        wo_t = gather(w_o.T)
        w1 = gather(w_1)
        w2_t = gather(w_2.T)
        w_qkv = gather(w_qkv_own)
        w_qkv_role = lax.dynamic_slice_in_dim(w_qkv, role * 3 * head_cols, 3 * head_cols, axis=1)

        def to_partner(value):
            return send(value, lambda z, y, x, c: (z, y, x, 1 - c))

        def from_owner(value):
            got = send(value, lambda z, y, x, c: (z, y, x, 1 - c) if c == z // 2 else None)
            return jnp.where(owner, value, got)

        x_seq = from_owner(x_in[0])
        x_1 = rows_of(x_seq, role, blk)
        cot = from_owner(jnp.where(owner, rows_of(cot_out[0], z % 2 * 2 + 1 - core, blk), 0))
        cot = jnp.where(owner, rows_of(cot_out[0], role, blk), cot)

        def exchange(parts):
            swapped = unscramble(parts, role)
            got = [swapped[0]] + [send(swapped[k], in_group(k)) for k in (1, 2, 3)]
            return unscramble(got, role)

        def mlp_forward(x_f, context):
            h = (x_f + dot_nt(context, wo_t)).astype(BF16)
            m = rms_norm(h.astype(F32)).astype(BF16)
            up = dot_nn(m, w1).astype(BF16)
            act = jax.nn.gelu(up.astype(F32)).astype(BF16)
            return h, m, up, act

        u_nat = rms_norm(x_in[0].astype(F32) + emb[0]).astype(BF16)
        c_nat, lse_nat = attn_fwd(dot_nn(u_nat, w_qkv_own).astype(BF16))
        got = [send(rows_of(c_nat, z ^ k, blk), to_group(k)) for k in range(4)]
        c_1 = jnp.concatenate(unscramble(got, role), axis=1)
        lse_1 = send(lse_nat, lambda z, y, x, c: (2 * c + z // 2, y, x, z % 2))
        s_1 = x_1.astype(F32) + emb[0]
        h_1, m_1, up_1, act_1 = mlp_forward(s_1, c_1)
        x_2 = (h_1.astype(F32) + dot_nt(act_1, w2_t)).astype(BF16)

        side = to_partner(x_2)
        over = send(x_2, in_group(2))
        x_2_seq = jnp.concatenate(unscramble([x_2, side, over, to_partner(over)], role), axis=0)
        u_2_seq = rms_norm(x_2_seq.astype(F32) + emb[1]).astype(BF16)
        qkv_2 = dot_nn(u_2_seq, w_qkv_role).astype(BF16)
        c_2_heads, lse_2 = attn_fwd(qkv_2)
        c_2 = jnp.concatenate(exchange([c_2_heads[i * blk:(i + 1) * blk] for i in range(4)]), axis=1)
        s_2 = x_2.astype(F32) + emb[1]
        h_2, m_2, up_2, act_2 = mlp_forward(s_2, c_2)

        def mlp_backward(d_next, h, up):
            d_act = dot_nn(d_next, w2_t).astype(BF16)
            d_up = jax.vjp(jax.nn.gelu, up.astype(F32))[1](d_act.astype(F32))[0].astype(BF16)
            d_m = dot_nt(d_up, w1).astype(BF16)
            d_h = jax.vjp(rms_norm, h.astype(F32))[1](d_m.astype(F32))[0]
            return d_up, (d_next.astype(F32) + d_h).astype(BF16)

        def attn_backward(d_mid, qkv, lse, s_f):
            d_c = dot_nn(d_mid, wo_t).astype(BF16)
            d_c_heads = jnp.concatenate(
                exchange([d_c[:, i * head_cols:(i + 1) * head_cols] for i in range(4)]), axis=0)
            d_qkv = jnp.concatenate(attn_bwd(qkv, d_c_heads, lse), axis=1)
            d_qkv = jnp.concatenate(exchange([d_qkv[i * blk:(i + 1) * blk] for i in range(4)]), axis=1)
            d_u = dot_nt(d_qkv, w_qkv).astype(BF16)
            d_s = jax.vjp(rms_norm, s_f)[1](d_u.astype(F32))[0]
            return d_qkv, (d_mid.astype(F32) + d_s).astype(BF16)

        d_up_2, d_mid_2 = mlp_backward(cot, h_2, up_2)
        d_qkv_2, d_2 = attn_backward(d_mid_2, qkv_2, lse_2, s_2)

        u_1_seq = rms_norm(x_seq.astype(F32) + emb[0]).astype(BF16)
        qkv_1 = dot_nn(u_1_seq, w_qkv_role).astype(BF16)
        d_up_1, d_mid_1 = mlp_backward(d_2, h_1, up_1)

        def gathered_rows(value):
            own = value.reshape(blk, 4, 2, piece)
            mine = lax.dynamic_index_in_dim(own, core, axis=2, keepdims=False)
            other = to_partner(lax.dynamic_index_in_dim(own, 1 - core, axis=2, keepdims=False))
            return mine, other

        first, second = jnp.where(core == 0, x, y), jnp.where(core == 0, y, x)

        def at(i, j):
            return jnp.where(core == 0, j * 2 + i, i * 2 + j)

        def swap_first(value):
            return send(value, lambda z, y, x, c: (z, y, 1 - x, c) if c == 0 else (z, 1 - y, x, c))

        def swap_second(value):
            return send(value, lambda z, y, x, c: (z, 1 - y, x, c) if c == 0 else (z, y, 1 - x, c))

        def weight_grad(sides):
            lefts, rights = [], []
            for left, right in sides:
                lefts += list(gathered_rows(left))
                rights += [right, to_partner(right)]
            left = jnp.concatenate(lefts, axis=0)
            right = jnp.concatenate(rights, axis=0)

            def product(i, j):
                return dot_tn(lax.dynamic_index_in_dim(left, at(i, j), axis=1, keepdims=False), right)

            away = swap_first(jnp.stack([product(1 - first, second), product(1 - first, 1 - second)]))
            mid = swap_second(product(first, 1 - second) + away[1])
            total = product(first, second) + away[0] + mid
            total = total.reshape(piece, 2, 2, -1)
            near = lax.dynamic_index_in_dim(total, 1 - z % 2, axis=2, keepdims=False)
            near = send(near, lambda z, y, x, c: (z ^ 1, y, x, c))
            total = lax.dynamic_index_in_dim(total, z % 2, axis=2, keepdims=False) + near
            far = lax.dynamic_index_in_dim(total, 1 - z // 2, axis=1, keepdims=False)
            far = send(far, lambda z, y, x, c: (z ^ 2, y, x, c))
            total = lax.dynamic_index_in_dim(total, z // 2, axis=1, keepdims=False) + far
            return lax.all_gather(total, 'data', axis=0, tiled=True)

        g_w2 = weight_grad([(cot, act_2), (d_2, act_1)]).T
        g_w1 = weight_grad([(m_2, d_up_2), (m_1, d_up_1)])
        g_wo = weight_grad([(d_mid_2, c_2), (d_mid_1, c_1)]).T
        d_qkv_1, d_1 = attn_backward(d_mid_1, qkv_1, lse_1, s_1)
        u_1 = rows_of(u_1_seq, role, blk)
        u_2 = rms_norm(s_2).astype(BF16)
        g_qkv = weight_grad([(u_2, d_qkv_2), (u_1, d_qkv_1)])

        d_x = [send(d_1, to_planes(k)) for k in range(4)]
        d_x = jnp.concatenate(unscramble(d_x, z), axis=0)[None]
        return (g_qkv[:, :head_cols], g_qkv[:, head_cols:2 * head_cols], g_qkv[:, 2 * head_cols:],
                g_wo, g_w1, g_w2, d_x)

    return jax.shard_map(device_step, mesh=mesh,
                         in_specs=(spec_act, spec_act, spec_rep, spec_col, spec_col, spec_col, spec_row, spec_col, spec_row),
                         out_specs=(spec_col, spec_col, spec_col, spec_row, spec_col, spec_row, spec_act),
                         check_vma=False)
```

```python
import math

import jax
import jax.numpy as jnp
from jax import lax
from jax.experimental import pallas as pl
from jax.experimental.pallas import tpu as pltpu
from jax.sharding import PartitionSpec as P


HEAD_DIM = 64
EPS_NORM = 1e-6
SCALE = HEAD_DIM ** -0.5
EXP2_SCALE = SCALE * math.log2(math.e)
PAIR = 2 * HEAD_DIM
FWD_ROWS = 512
BWD_ROWS = 256
KEYS = 256
GRAD_COLS = 512
INTERPRET = False
AXES = ('model', 'data')
BF16 = jnp.bfloat16
F32 = jnp.float32


def rms_norm(values):
    return values * lax.rsqrt(jnp.mean(values * values, axis=-1, keepdims=True) + EPS_NORM)


def dot_nt(a, b):
    return lax.dot_general(a, b, (((1,), (1,)), ((), ())), preferred_element_type=F32)


def dot_nn(a, b):
    return lax.dot_general(a, b, (((1,), (0,)), ((), ())), preferred_element_type=F32)


def dot_tn(a, b):
    return lax.dot_general(a, b, (((0,), (0,)), ((), ())), preferred_element_type=F32)


def attn_fwd_kernel(q_ref, k_ref, v_ref, o_ref, lse_ref, vt_ref, *e_refs):
    @pl.when(pl.program_id(0) == 0)
    def _():
        vt_ref[...] = v_ref[...].T

    count = k_ref.shape[0] // KEYS
    lane = lax.broadcasted_iota(jnp.int32, q_ref.shape, 1)
    q_heads = [jnp.where(lane // HEAD_DIM == head, q_ref[...], jnp.zeros_like(q_ref)) for head in range(2)]
    tops, run, total, outs = [[], []], [None, None], [None, None], []
    for j in range(count):
        keys = slice(j * KEYS, (j + 1) * KEYS)
        for head in range(2):
            scores = dot_nt(k_ref[keys, :], q_heads[head])
            top = jnp.max(scores, axis=0, keepdims=True) * EXP2_SCALE
            if j:
                top = jnp.maximum(top, run[head])
            weights = jnp.exp2(scores * EXP2_SCALE - top)
            part = jnp.sum(weights, axis=0, keepdims=True)
            total[head] = total[head] * jnp.exp2(run[head] - top) + part if j else part
            run[head] = top
            tops[head].append(top)
            e_refs[head][keys, :] = weights
    for head in range(2):
        inverse = 1.0 / total[head]
        out = None
        for j in range(count):
            keys = slice(j * KEYS, (j + 1) * KEYS)
            factor = inverse * jnp.exp2(tops[head][j] - run[head])
            probs = (e_refs[head][keys, :] * factor).astype(BF16)
            part = dot_nn(vt_ref[head * HEAD_DIM:(head + 1) * HEAD_DIM, keys], probs)
            out = out + part if j else part
        lse_ref[head:head + 1, :] = run[head] + jnp.log2(total[head])
        outs.append(out)
    o_ref[...] = jnp.concatenate(outs, axis=0).T.astype(BF16)


def attn_fwd(qkv, pair):
    seq = qkv.shape[0]
    rows = min(FWD_ROWS, seq)
    return pl.pallas_call(
        attn_fwd_kernel,
        grid=(seq // rows,),
        in_specs=[
            pl.BlockSpec((rows, PAIR), lambda i: (i, 3 * pair)),
            pl.BlockSpec((seq, PAIR), lambda i: (0, 3 * pair + 1)),
            pl.BlockSpec((seq, PAIR), lambda i: (0, 3 * pair + 2)),
        ],
        out_specs=[
            pl.BlockSpec((rows, PAIR), lambda i: (i, 0)),
            pl.BlockSpec((2, rows), lambda i: (0, i)),
        ],
        out_shape=[jax.ShapeDtypeStruct((seq, PAIR), BF16), jax.ShapeDtypeStruct((2, seq), F32)],
        scratch_shapes=[pltpu.VMEM((PAIR, seq), BF16)] + [pltpu.VMEM((seq, rows), F32)] * 2,
        compiler_params=pltpu.CompilerParams(vmem_limit_bytes=60 << 20),
        cost_estimate=pl.CostEstimate(
            flops=16 * seq * seq * PAIR, bytes_accessed=8 * seq * PAIR, transcendentals=seq * seq * 2),
        interpret=INTERPRET,
        name="attn_fwd",
    )(qkv, qkv, qkv)


def attn_bwd_kernel(q_ref, k_ref, v_ref, do_ref, lse_ref, out_ref,
                    kt_ref, dk_acc, dv_acc, p_cat, ds_cat):
    step = pl.program_id(0)

    @pl.when(step == 0)
    def _():
        kt_ref[...] = k_ref[...].T
        dk_acc[...] = jnp.zeros_like(dk_acc)
        dv_acc[...] = jnp.zeros_like(dv_acc)

    block = q_ref.shape[0]
    lane = lax.broadcasted_iota(jnp.int32, q_ref.shape, 1)
    q_heads, do_heads, dqs = [], [], []
    for head in range(2):
        mine = lane // HEAD_DIM == head
        q_head = jnp.where(mine, q_ref[...], jnp.zeros_like(q_ref))
        do_head = jnp.where(mine, do_ref[...], jnp.zeros_like(do_ref))
        scores = dot_nt(k_ref[...], q_head)
        probs = jnp.exp2(scores * EXP2_SCALE - lse_ref[head:head + 1, :])
        d_probs = dot_nt(v_ref[...], do_head).astype(BF16).astype(F32)
        inner = jnp.sum(probs * d_probs, axis=0, keepdims=True)
        cols = slice(head * block, (head + 1) * block)
        p_cat[:, cols] = probs.astype(BF16)
        ds_cat[:, cols] = (probs * (d_probs - inner)).astype(BF16)
        dqs.append(dot_nn(kt_ref[head * HEAD_DIM:(head + 1) * HEAD_DIM, :], ds_cat[:, cols]))
        q_heads.append(q_head)
        do_heads.append(do_head)
    dv_acc[...] += dot_nn(p_cat[...], jnp.concatenate(do_heads, axis=0))
    dk_acc[...] += dot_nn(ds_cat[...], jnp.concatenate(q_heads, axis=0))
    out_ref[pl.ds(pl.multiple_of(step * block, block), block), :PAIR] = (jnp.concatenate(dqs, axis=0).T * SCALE).astype(BF16)

    @pl.when(step == pl.num_programs(0) - 1)
    def _():
        out_ref[:, PAIR:2 * PAIR] = (dk_acc[...] * SCALE).astype(BF16)
        out_ref[:, 2 * PAIR:] = dv_acc[...].astype(BF16)


def attn_bwd(qkv, d_context, lse, pair):
    seq = qkv.shape[0]
    full = lambda column: pl.BlockSpec((seq, PAIR), lambda i: (0, column))
    rows = lambda column: pl.BlockSpec((BWD_ROWS, PAIR), lambda i: (i, column))
    return pl.pallas_call(
        attn_bwd_kernel,
        grid=(seq // BWD_ROWS,),
        in_specs=[rows(3 * pair), full(3 * pair + 1), full(3 * pair + 2), rows(0), pl.BlockSpec((2, BWD_ROWS), lambda i: (0, i))],
        out_specs=pl.BlockSpec((seq, 3 * PAIR), lambda i: (0, 0)),
        out_shape=jax.ShapeDtypeStruct((seq, 3 * PAIR), BF16),
        scratch_shapes=[
            pltpu.VMEM((PAIR, seq), BF16),
            pltpu.VMEM((seq, PAIR), F32),
            pltpu.VMEM((seq, PAIR), F32),
            pltpu.VMEM((seq, 2 * BWD_ROWS), BF16),
            pltpu.VMEM((seq, 2 * BWD_ROWS), BF16),
        ],
        compiler_params=pltpu.CompilerParams(vmem_limit_bytes=60 << 20),
        cost_estimate=pl.CostEstimate(
            flops=40 * seq * seq * PAIR, bytes_accessed=14 * seq * PAIR, transcendentals=seq * seq * 2),
        interpret=INTERPRET,
        name="attn_bwd",
    )(qkv, qkv, qkv, d_context, lse)


def grad_kernel(_, *refs):
    lefts, rights, (away_ref, mid_ref, keep_ref, left_t) = refs[:16], refs[16:20], refs[20:]
    count, piece = lefts[0].shape

    @pl.when(pl.program_id(0) == 0)
    def _():
        for i in range(16):
            left_t[i % 4 * piece:(i % 4 + 1) * piece, i // 4 * count:(i // 4 + 1) * count] = lefts[i][...].T

    total = dot_nn(left_t[:, :count], rights[0][...])
    for i in range(1, 4):
        total += dot_nn(left_t[:, i * count:(i + 1) * count], rights[i][...])
    away_ref[...] = total[:2 * piece]
    mid_ref[...] = total[2 * piece:3 * piece]
    keep_ref[...] = total[3 * piece:]


def grad_products(order, lefts, rights):
    count, cols = rights[0].shape
    piece = lefts[0].shape[1] // 8
    tile = min(GRAD_COLS, cols)
    left_spec = lambda n: pl.BlockSpec((count, piece), lambda i, order: (0, order[n]))
    return pl.pallas_call(
        grad_kernel,
        grid_spec=pltpu.PrefetchScalarGridSpec(
            num_scalar_prefetch=1,
            grid=(cols // tile,),
            in_specs=[left_spec(n) for _ in range(4) for n in range(4)]
            + [pl.BlockSpec((count, tile), lambda i, order: (0, i))] * 4,
            out_specs=[pl.BlockSpec((n * piece, tile), lambda i, order: (0, i)) for n in (2, 1, 1)],
            scratch_shapes=[pltpu.VMEM((4 * piece, 4 * count), BF16)],
        ),
        out_shape=[jax.ShapeDtypeStruct((n * piece, cols), F32) for n in (2, 1, 1)],
        compiler_params=pltpu.CompilerParams(vmem_limit_bytes=60 << 20),
        cost_estimate=pl.CostEstimate(
            flops=32 * count * piece * cols, bytes_accessed=8 * count * (4 * piece + cols) + 16 * piece * cols,
            transcendentals=0),
        interpret=INTERPRET,
        name="grad",
    )(order, *[left for left in lefts for _ in range(4)], *rights)


def lin(z, y, x, c):
    return z * 8 + y * 4 + x * 2 + c


def send(value, to):
    pairs = []
    for z in range(4):
        for y in range(2):
            for x in range(2):
                for c in range(2):
                    dst = to(z, y, x, c)
                    if dst is not None:
                        pairs.append((lin(z, y, x, c), lin(*dst)))
    return lax.ppermute(value, AXES, pairs)


def role_of(z, c):
    return (z % 2) * 2 + c


def in_group(k):
    def to(z, y, x, c):
        role = role_of(z, c) ^ k
        return (z // 2 * 2 + role // 2, y, x, role % 2)

    return to


def to_group(k):
    def to(z, y, x, c):
        role = z ^ k
        return (2 * c + role // 2, y, x, role % 2)

    return to


def other_core(z, y, x, c):
    return (z, y, x, 1 - c)


def swap_first(z, y, x, c):
    return (z, y, 1 - x, c) if c == 0 else (z, 1 - y, x, c)


def swap_second(z, y, x, c):
    return (z, 1 - y, x, c) if c == 0 else (z, y, 1 - x, c)


def unscramble(parts, role):
    odd, high = role % 2 == 1, role // 2 == 1
    a = [jnp.where(odd, parts[i ^ 1], parts[i]) for i in range(4)]
    return [jnp.where(high, a[i ^ 2], a[i]) for i in range(4)]


def rows_of(value, index, count):
    return lax.dynamic_slice_in_dim(value, index * count, count, axis=0)


def pick(value, index, axis):
    return lax.dynamic_index_in_dim(value, index, axis=axis, keepdims=False)


def solution(mesh):
    spec_col = P(None, 'model')
    spec_row = P('model', None)
    spec_act = P('data', None, None)
    spec_rep = P(None, None)

    def device_step(x_in, cot_out, step_emb, w_q, w_k, w_v, w_o, w_1, w_2):
        seq, d_model = x_in.shape[1:]
        head_cols = w_q.shape[1]
        blk = seq // 4
        piece = d_model // 8
        z = lax.axis_index('model')
        d = lax.axis_index('data')
        y, x, core = d // 4, d // 2 % 2, d % 2
        role = z % 2 * 2 + core
        owner = core == z // 2
        emb = step_emb.astype(F32)

        def by_pair(q, k, v):
            return jnp.concatenate([w[:, j * PAIR:(j + 1) * PAIR] for j in range(2) for w in (q, k, v)], axis=1)

        w_qkv_own = by_pair(w_q, w_k, w_v)
        widths = [w_o.shape[0], w_1.shape[1], w_2.shape[0], 3 * head_cols]
        own = [rows_of(w, d, piece) for w in (w_o.T, w_1, w_2.T, w_qkv_own)]
        planes = lax.all_gather(jnp.concatenate(own, axis=1), 'model', axis=0)
        full, at_col = [], 0
        for width in widths:
            part = planes[:, :, at_col:at_col + width].transpose(1, 0, 2).reshape(piece, 4 * width)
            full.append(lax.all_gather(part, 'data', axis=0, tiled=True))
            at_col += width
        wo_t, w1, w2_t, w_qkv = full
        w_qkv_role = lax.dynamic_slice_in_dim(w_qkv, role * 3 * head_cols, 3 * head_cols, axis=1)

        def from_owner(value):
            got = send(value, lambda z, y, x, c: (z, y, x, 1 - c) if c == z // 2 else None)
            return jnp.where(owner, value, got)

        x_seq = from_owner(x_in[0])
        x_1 = rows_of(x_seq, role, blk)
        cot = from_owner(jnp.where(owner, rows_of(cot_out[0], z % 2 * 2 + 1 - core, blk), 0))
        cot = jnp.where(owner, rows_of(cot_out[0], role, blk), cot)

        def exchange(parts):
            swapped = unscramble(parts, role)
            got = [swapped[0]] + [send(swapped[k], in_group(k)) for k in (1, 2, 3)]
            return unscramble(got, role)

        def mlp_forward(x_f, context):
            h = (x_f + dot_nt(context, wo_t)).astype(BF16)
            m = rms_norm(h.astype(F32)).astype(BF16)
            up = dot_nn(m, w1).astype(BF16)
            act = jax.nn.gelu(up.astype(F32)).astype(BF16)
            return h, m, up, act

        def interleave(pairs):
            return jnp.concatenate([pairs[j][i] for i in range(4) for j in range(2)], axis=1)

        u_nat = rms_norm(x_in[0].astype(F32) + emb[0]).astype(BF16)
        qkv_nat = dot_nn(u_nat, w_qkv_own).astype(BF16)
        got, lses = [], []
        for j in range(2):
            c_nat, lse_nat = attn_fwd(qkv_nat, j)
            got.append(unscramble([send(rows_of(c_nat, z ^ k, blk), to_group(k)) for k in range(4)], role))
            lses.append(lse_nat)
        c_1 = interleave(got)
        lse_1 = send(jnp.stack(lses), lambda z, y, x, c: (2 * c + z // 2, y, x, z % 2))
        s_1 = x_1.astype(F32) + emb[0]
        h_1, m_1, up_1, act_1 = mlp_forward(s_1, c_1)
        x_2 = (h_1.astype(F32) + dot_nt(act_1, w2_t)).astype(BF16)

        side = send(x_2, other_core)
        over = send(x_2, in_group(2))
        x_2_seq = jnp.concatenate(unscramble([x_2, side, over, send(over, other_core)], role), axis=0)
        u_2_seq = rms_norm(x_2_seq.astype(F32) + emb[1]).astype(BF16)
        qkv_2 = dot_nn(u_2_seq, w_qkv_role).astype(BF16)
        got, lse_2 = [], []
        for j in range(2):
            c_heads, lse = attn_fwd(qkv_2, j)
            got.append(exchange([c_heads[i * blk:(i + 1) * blk] for i in range(4)]))
            lse_2.append(lse)
        c_2 = interleave(got)
        s_2 = x_2.astype(F32) + emb[1]
        h_2, m_2, up_2, act_2 = mlp_forward(s_2, c_2)

        def mlp_backward(d_next, h, up):
            d_act = dot_nn(d_next, w2_t).astype(BF16)
            d_up = jax.vjp(jax.nn.gelu, up.astype(F32))[1](d_act.astype(F32))[0].astype(BF16)
            d_m = dot_nt(d_up, w1).astype(BF16)
            d_h = jax.vjp(rms_norm, h.astype(F32))[1](d_m.astype(F32))[0]
            return d_up, (d_next.astype(F32) + d_h).astype(BF16)

        def attn_backward(d_mid, qkv, lse, s_f, u_seq, ahead):
            d_c = dot_nn(d_mid, wo_t).astype(BF16)
            pairs, grads = [], []
            for j in range(2):
                heads = exchange([d_c[:, i * head_cols + j * PAIR:i * head_cols + (j + 1) * PAIR] for i in range(4)])
                heads = jnp.concatenate(heads, axis=0)
                if ahead is not None and j == 0:
                    heads, ahead = lax.optimization_barrier((heads, ahead))
                d_heads = attn_bwd(qkv, heads, lse[j], j)
                grads.append(dot_tn(u_seq, d_heads))
                pairs.append(exchange([d_heads[i * blk:(i + 1) * blk] for i in range(4)]))
            d_qkv = interleave(pairs)
            d_u = dot_nt(d_qkv, w_qkv).astype(BF16)
            d_s = jax.vjp(rms_norm, s_f)[1](d_u.astype(F32))[0]
            return grads, (d_mid.astype(F32) + d_s).astype(BF16), ahead

        d_up_2, d_mid_2 = mlp_backward(cot, h_2, up_2)
        grads_2, d_2, _ = attn_backward(d_mid_2, qkv_2, lse_2, s_2, u_2_seq, None)

        u_1_seq = rms_norm(x_seq.astype(F32) + emb[0]).astype(BF16)
        qkv_1 = dot_nn(u_1_seq, w_qkv_role).astype(BF16)
        d_up_1, d_mid_1 = mlp_backward(d_2, h_1, up_1)

        first, second = jnp.where(core == 0, x, y), jnp.where(core == 0, y, x)

        def at(i, j):
            return jnp.where(core == 0, j * 2 + i, i * 2 + j)

        order = [at(1 - first, second), at(1 - first, 1 - second), at(first, 1 - second), at(first, second)]

        column = jnp.stack(order) * 2 + core

        def products(sides):
            lefts, rights = [], []
            for left, right in sides:
                lefts += [left, send(left, other_core)]
                rights += [right, send(right, other_core)]
            return grad_products(column, lefts, rights)

        def reduce_grad(prods):
            away, mid, keep = prods
            away = send(away, swap_first)
            mid = send(mid + away[piece:], swap_second)
            total = (keep + away[:piece] + mid).reshape(piece, 2, 2, -1)
            near = send(pick(total, 1 - z % 2, 2), lambda z, y, x, c: (z ^ 1, y, x, c))
            total = pick(total, z % 2, 2) + near
            far = send(pick(total, 1 - z // 2, 1), lambda z, y, x, c: (z ^ 2, y, x, c))
            total = pick(total, z // 2, 1) + far
            return lax.all_gather(total, 'data', axis=0, tiled=True)

        ahead = (products([(cot, act_2), (d_2, act_1)]), products([(m_2, d_up_2), (m_1, d_up_1)]),
                 products([(d_mid_2, c_2), (d_mid_1, c_1)]))
        grads_1, d_1, ahead = attn_backward(d_mid_1, qkv_1, lse_1, s_1, u_1_seq, ahead)
        g_w2 = reduce_grad(ahead[0]).T
        g_w1 = reduce_grad(ahead[1])
        g_wo = reduce_grad(ahead[2]).T

        def reduce_heads(j):
            total = (grads_1[j] + grads_2[j]).reshape(4, 2 * piece, -1)
            parts = [pick(total, i, 0) for i in order]
            away = send(jnp.stack(parts[:2]), swap_first)
            mid = send(parts[2] + away[1], swap_second)
            total = parts[3] + away[0] + mid
            total = send(total, lambda z, y, x, c: (2 * (z % 2) + c, y, x, z // 2))
            total = total.reshape(2, piece, -1)
            return pick(total, core, 0) + send(pick(total, 1 - core, 0), other_core)

        g_qkv = lax.all_gather(jnp.concatenate([reduce_heads(0), reduce_heads(1)], axis=1), 'data', axis=0, tiled=True)
        g_q, g_k, g_v = (jnp.concatenate([g_qkv[:, (3 * j + i) * PAIR:(3 * j + i + 1) * PAIR] for j in range(2)], axis=1)
                         for i in range(3))

        beside = send(d_1, lambda z, y, x, c: (z, y, x, 1 - c) if 1 - c == z // 2 else None)
        cross = [send(d_1, lambda z, y, x, c: (z ^ 2, y, x, c ^ k) if c ^ k == z // 2 else None) for k in (0, 1)]
        across = [send(d_1, lambda z, y, x, c: (z ^ 1, y, x, c ^ k) if c ^ k == z // 2 else None) for k in (0, 1)]
        passed = [send(v, lambda z, y, x, c: (z ^ 1, y, x, c) if c != z // 2 else None) for v in cross]
        near = [jnp.where(owner, a, b) for a, b in zip((d_1, beside), cross)]
        far = [jnp.where(owner, a, b) for a, b in zip(across, passed)]
        d_x = jnp.concatenate(unscramble(near + far, role), axis=0)[None]
        return g_q, g_k, g_v, g_wo, g_w1, g_w2, d_x

    return jax.shard_map(device_step, mesh=mesh,
                         in_specs=(spec_act, spec_act, spec_rep, spec_col, spec_col, spec_col, spec_row, spec_col, spec_row),
                         out_specs=(spec_col, spec_col, spec_col, spec_row, spec_col, spec_row, spec_act),
                         check_vma=False)
```

```python
import functools
import math

import jax
import jax.numpy as jnp
from jax import lax
from jax.experimental import pallas as pl
from jax.experimental.pallas import tpu as pltpu
from jax.sharding import PartitionSpec as P


HEAD_DIM = 64
EPS_NORM = 1e-6
SCALE = HEAD_DIM ** -0.5
EXP2_SCALE = SCALE * math.log2(math.e)
PAIR = 2 * HEAD_DIM
FWD_ROWS = 512
BWD_ROWS = 256
KEYS = 256
INTERPRET = False
AXES = ('model', 'data')
BF16 = jnp.bfloat16
F32 = jnp.float32
MESH = pl.DeviceIdType.MESH


def rms_norm(values):
    return values * lax.rsqrt(jnp.mean(values * values, axis=-1, keepdims=True) + EPS_NORM)


def dot_nt(a, b):
    return lax.dot_general(a, b, (((1,), (1,)), ((), ())), preferred_element_type=F32)


def dot_nn(a, b):
    return lax.dot_general(a, b, (((1,), (0,)), ((), ())), preferred_element_type=F32)


def dot_tn(a, b):
    return lax.dot_general(a, b, (((0,), (0,)), ((), ())), preferred_element_type=F32)


def attn_fwd_kernel(q_ref, k_ref, v_ref, o_ref, lse_ref, vt_ref, *e_refs):
    @pl.when(pl.program_id(0) == 0)
    def _():
        vt_ref[...] = v_ref[...].T

    outs, sums = attend_rows(q_ref[...], k_ref, vt_ref, e_refs)
    o_ref[...] = jnp.concatenate(outs, axis=0).T.astype(BF16)
    for head in range(2):
        lse_ref[head:head + 1, :] = sums[head]


def attn_fwd(qkv, pair):
    seq = qkv.shape[0]
    rows = min(FWD_ROWS, seq)
    return pl.pallas_call(
        attn_fwd_kernel,
        grid=(seq // rows,),
        in_specs=[
            pl.BlockSpec((rows, PAIR), lambda i: (i, pair)),
            pl.BlockSpec((seq, PAIR), lambda i: (0, 2 + pair)),
            pl.BlockSpec((seq, PAIR), lambda i: (0, 4 + pair)),
        ],
        out_specs=[
            pl.BlockSpec((rows, PAIR), lambda i: (i, 0)),
            pl.BlockSpec((2, rows), lambda i: (0, i)),
        ],
        out_shape=[jax.ShapeDtypeStruct((seq, PAIR), BF16), jax.ShapeDtypeStruct((2, seq), F32)],
        scratch_shapes=[pltpu.VMEM((PAIR, seq), BF16)] + [pltpu.VMEM((seq, rows), F32)] * 2,
        compiler_params=pltpu.CompilerParams(vmem_limit_bytes=60 << 20),
        cost_estimate=pl.CostEstimate(
            flops=16 * seq * seq * PAIR, bytes_accessed=8 * seq * PAIR, transcendentals=seq * seq * 2),
        interpret=INTERPRET,
        name="attn_fwd",
    )(qkv, qkv, qkv)


def attn_bwd_kernel(q_ref, k_ref, v_ref, do_ref, lse_ref, out_ref, kt_ref, dk_acc, dv_acc, p_cat, ds_cat):
    step = pl.program_id(0)

    @pl.when(step == 0)
    def _():
        kt_ref[...] = k_ref[...].T
        dk_acc[...] = jnp.zeros_like(dk_acc)
        dv_acc[...] = jnp.zeros_like(dv_acc)

    block = q_ref.shape[0]
    out_ref[pl.ds(pl.multiple_of(step * block, block), block), :PAIR] = backward_rows(
        q_ref[...], do_ref[...], lse_ref[...], k_ref, v_ref, kt_ref, p_cat, ds_cat, dk_acc, dv_acc)

    @pl.when(step == pl.num_programs(0) - 1)
    def _():
        out_ref[:, PAIR:2 * PAIR] = (dk_acc[...] * SCALE).astype(BF16)
        out_ref[:, 2 * PAIR:] = dv_acc[...].astype(BF16)


def attn_bwd(qkv, d_context, lse, pair):
    seq = qkv.shape[0]
    full = lambda column: pl.BlockSpec((seq, PAIR), lambda i: (0, column))
    rows = lambda column: pl.BlockSpec((BWD_ROWS, PAIR), lambda i: (i, column))
    return pl.pallas_call(
        attn_bwd_kernel,
        grid=(seq // BWD_ROWS,),
        in_specs=[rows(pair), full(2 + pair), full(4 + pair), rows(0), pl.BlockSpec((2, BWD_ROWS), lambda i: (0, i))],
        out_specs=pl.BlockSpec((seq, 3 * PAIR), lambda i: (0, 0)),
        out_shape=jax.ShapeDtypeStruct((seq, 3 * PAIR), BF16),
        scratch_shapes=[
            pltpu.VMEM((PAIR, seq), BF16),
            pltpu.VMEM((seq, PAIR), F32),
            pltpu.VMEM((seq, PAIR), F32),
            pltpu.VMEM((seq, 2 * BWD_ROWS), BF16),
            pltpu.VMEM((seq, 2 * BWD_ROWS), BF16),
        ],
        compiler_params=pltpu.CompilerParams(vmem_limit_bytes=60 << 20),
        cost_estimate=pl.CostEstimate(
            flops=40 * seq * seq * PAIR, bytes_accessed=14 * seq * PAIR, transcendentals=seq * seq * 2),
        interpret=INTERPRET,
        name="attn_bwd",
    )(qkv, qkv, qkv, d_context, lse)


def attend_rows(q, k_ref, v_t, e_refs):
    count = k_ref.shape[0] // KEYS
    lane = lax.broadcasted_iota(jnp.int32, q.shape, 1)
    q_heads = [jnp.where(lane // HEAD_DIM == head, q, jnp.zeros_like(q)) for head in range(2)]
    tops, run, total, outs, sums = [[], []], [None, None], [None, None], [], []
    for j in range(count):
        keys = slice(j * KEYS, (j + 1) * KEYS)
        for head in range(2):
            scores = dot_nt(k_ref[keys, :], q_heads[head])
            top = jnp.max(scores, axis=0, keepdims=True) * EXP2_SCALE
            if j:
                top = jnp.maximum(top, run[head])
            weights = jnp.exp2(scores * EXP2_SCALE - top)
            part = jnp.sum(weights, axis=0, keepdims=True)
            total[head] = total[head] * jnp.exp2(run[head] - top) + part if j else part
            run[head] = top
            tops[head].append(top)
            e_refs[head][keys, :] = weights
    for head in range(2):
        inverse = 1.0 / total[head]
        out = None
        for j in range(count):
            keys = slice(j * KEYS, (j + 1) * KEYS)
            factor = inverse * jnp.exp2(tops[head][j] - run[head])
            probs = (e_refs[head][keys, :] * factor).astype(BF16)
            part = dot_nn(v_t[head * HEAD_DIM:(head + 1) * HEAD_DIM, keys], probs)
            out = out + part if j else part
        sums.append(run[head] + jnp.log2(total[head]))
        outs.append(out)
    return outs, sums


class Place:
    def __init__(self):
        self.z = lax.axis_index('model')
        d = lax.axis_index('data')
        self.y, self.x, self.c = d // 4, d // 2 % 2, d % 2
        z = self.z
        self.z_by = {1: z + 1 - 2 * (z % 2), 2: (z + 2) % 4, 3: 3 - z}
        x, y, c = self.x, self.y, self.c
        self.xa, self.ya = x + (1 - c) * (1 - 2 * x), y + c * (1 - 2 * y)
        self.xb, self.yb = x + c * (1 - 2 * x), y + (1 - c) * (1 - 2 * y)
        self.role = z % 2 * 2 + c
        self.owner = c == z // 2

    def piece(self, y, x, c=None):
        return y * 4 + x * 2 + (self.c if c is None else c)

    def device(self, z=None, y=None, x=None, c=None):
        z, y, x, c = (own if given is None else given for given, own in zip((z, y, x, c), (self.z, self.y, self.x, self.c)))
        return {'model': z, 'data': y * 4 + x * 2 + c}

    def peers(self):
        column = [self.device(z=z, c=c) for z in (self.z, *self.z_by.values()) for c in (self.c, 1 - self.c)][1:]
        return column + [self.device(x=1 - self.x), self.device(y=1 - self.y)]

    def meet(self):
        barrier = pltpu.get_barrier_semaphore()
        peers = self.peers()
        for peer in peers:
            pl.semaphore_signal(barrier, inc=1, device_id=peer, device_id_type=MESH)
        pl.semaphore_wait(barrier, len(peers))


class Copies:
    def __init__(self, send_sem, recv_sem):
        self.send_sem, self.recv_sem, self.used, self.sent = send_sem, recv_sem, 0, []

    def make(self, src, dst, device):
        n, self.used = self.used, self.used + 1
        copy = pltpu.make_async_remote_copy(
            src_ref=src, dst_ref=dst, send_sem=self.send_sem.at[n], recv_sem=self.recv_sem.at[n],
            device_id=device, device_id_type=MESH)
        self.sent.append(copy)
        return copy

    def start(self, src, dst, device):
        copy = self.make(src, dst, device)
        copy.start()
        return copy


def first_kernel(x_ref, cot_ref, emb_ref, wq_ref, wk_ref, wv_ref, wo_ref, w1_ref, w2_ref,
                 c1_ref, lse_ref, xs_ref, cot_loc_ref, full_o, full_1, full_2, full_qkv,
                 qkv_s, vt_s, e_a, e_b, c_buf, lse_s, cot_s, local_sem, send_sem, recv_sem, c_send, c_recv, one_send, one_recv):
    seq, d_model = x_ref.shape
    blk = seq // 4
    head_cols = wq_ref.shape[1]
    here = Place()
    z, core, role, owner = here.z, here.c, here.role, here.owner
    here.meet()
    copies = Copies(send_sem, recv_sem)

    def span(index, count):
        return pl.ds(pl.multiple_of(index * count, count), count)

    ff_cols, out_rows, piece = w1_ref.shape[1], wo_ref.shape[0] // 8, d_model // 8
    hidden = w2_ref.shape[0] // 8

    def block_qkv(zz, e):
        return full_qkv.at[span(e, piece), span(zz, 3 * head_cols)]

    units = {
        'o': lambda zz, e: full_o.at[zz, span(e, out_rows), :],
        '1': lambda zz, e: full_1.at[span(e, piece), span(zz, ff_cols)],
        '2': lambda zz, e: full_2.at[zz, span(e, hidden), :],
        'qkv': block_qkv,
    }

    def own_parts(name, e):
        if name == 'o':
            return [(wo_ref.at[span(e, out_rows), :], units[name](z, e))]
        if name == '1':
            return [(w1_ref.at[span(e, piece), :], units[name](z, e))]
        if name == '2':
            return [(w2_ref.at[span(e, hidden), :], units[name](z, e))]
        return [(ref.at[span(e, piece), :],
                 full_qkv.at[span(e, piece), pl.ds(pl.multiple_of((z * 3 + t) * head_cols, head_cols), head_cols)])
                for t, ref in enumerate((wq_ref, wk_ref, wv_ref))]

    mine = here.piece(here.y, here.x)
    by_a = here.piece(here.ya, here.xa)
    by_b = here.piece(here.yb, here.xb)
    by_ab = here.piece(1 - here.y, 1 - here.x)
    to_a, to_b = here.device(y=here.ya, x=here.xa), here.device(y=here.yb, x=here.xb)
    partner = here.device(c=1 - core)
    stage_z, stage_a, stage_b1, stage_b2, stage_c = {}, {}, {}, {}, {}
    names = ('o', '1', '2', 'qkv')

    for name in names:
        stage_z[name] = {k: [copies.start(src, dst, here.device(z=here.z_by[k])) for src, dst in own_parts(name, mine)]
                         for k in (1, 2, 3)}

    def forward_z(name):
        stage_a[name], stage_b1[name] = [], []
        for k in (1, 2, 3):
            for copy in stage_z[name][k]:
                copy.wait_recv()
            block = units[name](here.z_by[k], mine)
            stage_a[name].append(copies.start(block, block, to_a))
            stage_b1[name].append(copies.start(block, block, to_b))

    def forward_a(name):
        stage_b2[name] = []
        for k in (1, 2, 3):
            stage_a[name][k - 1].wait_recv()
            block = units[name](here.z_by[k], by_a)
            stage_b2[name].append(copies.start(block, block, to_b))

    def forward_b(name):
        stage_c[name] = []
        for k in (1, 2, 3):
            stage_b1[name][k - 1].wait_recv()
            stage_b2[name][k - 1].wait_recv()
            for e in (mine, by_a, by_b, by_ab):
                block = units[name](here.z_by[k], e)
                stage_c[name].append(copies.start(block, block, partner))

    locals_ = []

    def copy_local(src, dst):
        copy = pltpu.make_async_copy(src, dst, local_sem.at[len(locals_)])
        locals_.append(copy)
        copy.start()

    copy_local(w1_ref, full_1.at[:, span(z, ff_cols)])
    copy_local(w2_ref, full_2.at[z])
    copy_local(wo_ref, full_o.at[z])
    for t, ref in enumerate((wq_ref, wk_ref, wv_ref)):
        copy_local(ref, full_qkv.at[:, pl.ds(pl.multiple_of((z * 3 + t) * head_cols, head_cols), head_cols)])
    other_role = z % 2 * 2 + 1 - core
    give_x = pltpu.make_async_remote_copy(
        src_ref=x_ref, dst_ref=xs_ref, send_sem=one_send.at[0], recv_sem=one_recv.at[0], device_id=partner, device_id_type=MESH)
    give_cot = pltpu.make_async_remote_copy(
        src_ref=cot_ref.at[span(other_role, blk), :], dst_ref=cot_loc_ref, send_sem=one_send.at[1], recv_sem=one_recv.at[1],
        device_id=partner, device_id_type=MESH)
    keep_x = pltpu.make_async_copy(x_ref, xs_ref, local_sem.at[6])
    take_cot = pltpu.make_async_copy(cot_ref.at[span(role, blk), :], cot_s, local_sem.at[7])
    keep_cot = pltpu.make_async_copy(cot_s, cot_loc_ref, local_sem.at[8])

    @pl.when(owner)
    def _():
        give_x.start()
        give_cot.start()
        keep_x.start()
        take_cot.start()

    def project(i, _):
        rows = span(i, blk)
        values = x_ref[rows, :].astype(F32) + emb_ref[...]
        unit = (values * lax.rsqrt(jnp.mean(values * values, axis=-1, keepdims=True) + EPS_NORM)).astype(BF16)
        for t, ref in enumerate((wq_ref, wk_ref, wv_ref)):
            qkv_s[rows, t * head_cols:(t + 1) * head_cols] = dot_nn(unit, ref[...]).astype(BF16)
        return 0

    lax.fori_loop(0, 4, project, 0)

    def context_copy(j, i):
        src = c_buf.at[j, span(i, blk), :]
        dst = c1_ref.at[:, pl.ds(pl.multiple_of((z * 2 + j) * PAIR, PAIR), PAIR)]
        target_z, target_c = 2 * core + i // 2, i % 2
        remote = pltpu.make_async_remote_copy(
            src_ref=src, dst_ref=dst, send_sem=c_send.at[j * 4 + i], recv_sem=c_recv.at[j * 4 + z],
            device_id=here.device(z=target_z, c=target_c), device_id_type=MESH)
        local = pltpu.make_async_copy(src, dst, c_recv.at[j * 4 + z])
        return remote, local, jnp.logical_and(target_z == z, target_c == core)

    def send_context(j, i):
        remote, local, to_self = context_copy(j, i)
        pl.when(to_self)(local.start)
        pl.when(jnp.logical_not(to_self))(remote.start)

    moves = {(0, 1): [(forward_z, 'o')], (0, 2): [(forward_a, 'o')], (0, 3): [(forward_b, 'o')],
             (1, 2): [(forward_z, '1')], (1, 3): [(forward_a, '1')]}
    for j in range(2):
        vt_s[...] = qkv_s[:, (4 + j) * PAIR:(5 + j) * PAIR].T
        k_view = qkv_s.at[:, (2 + j) * PAIR:(3 + j) * PAIR]
        for i in range(4):
            if i or j:
                send_context(j if i else 0, i - 1 if i else 3)
            for step, name in moves.get((j, i), ()):
                step(name)
            rows = slice(i * blk, (i + 1) * blk)
            outs, sums = attend_rows(qkv_s[rows, j * PAIR:(j + 1) * PAIR], k_view, vt_s, (e_a, e_b))
            c_buf[j, rows, :] = jnp.concatenate(outs, axis=0).T.astype(BF16)
            for head in range(2):
                lse_s[2 * j + head:2 * j + head + 1, rows] = sums[head]

    @pl.when(owner)
    def _():
        take_cot.wait()
        keep_cot.start()

    forward_z('2')
    send_context(1, 3)
    give_lse = pltpu.make_async_remote_copy(
        src_ref=lse_s, dst_ref=lse_ref, send_sem=one_send.at[2], recv_sem=one_recv.at[2],
        device_id=here.device(z=2 * core + z // 2, c=z % 2), device_id_type=MESH)
    keep_lse = pltpu.make_async_copy(lse_s, lse_ref, local_sem.at[9])
    lse_stays = jnp.logical_and(2 * core + z // 2 == z, z % 2 == core)
    pl.when(lse_stays)(keep_lse.start)
    pl.when(jnp.logical_not(lse_stays))(give_lse.start)
    forward_b('1')
    forward_a('2')
    forward_z('qkv')
    forward_b('2')
    forward_a('qkv')
    forward_b('qkv')

    for j in range(2):
        for zz in range(4):
            pltpu.make_async_copy(c_buf.at[j, :blk, :], c1_ref.at[:, :PAIR], c_recv.at[j * 4 + zz]).wait()
        for i in range(4):
            remote, _, to_self = context_copy(j, i)
            pl.when(jnp.logical_not(to_self))(remote.wait_send)
    pl.when(lse_stays)(keep_lse.wait)

    @pl.when(jnp.logical_not(lse_stays))
    def _():
        give_lse.wait_send()
        give_lse.wait_recv()

    @pl.when(owner)
    def _():
        give_x.wait_send()
        give_cot.wait_send()
        keep_x.wait()
        keep_cot.wait()

    @pl.when(jnp.logical_not(owner))
    def _():
        give_x.wait_recv()
        give_cot.wait_recv()

    for copy in locals_:
        copy.wait()
    for name in names:
        for copy in stage_c[name]:
            copy.wait_recv()
    for copy in copies.sent:
        copy.wait_send()


def first_call(x, cot, emb, w_q, w_k, w_v, w_o, w_1, w_2):
    seq, d_model = x.shape
    head_cols, ff_cols, blk = w_q.shape[1], w_1.shape[1], seq // 4
    anywhere = pl.BlockSpec(memory_space=pl.ANY)
    in_vmem = pl.BlockSpec(memory_space=pltpu.VMEM)
    copies = 18 + 12 + 24 + 48
    return pl.pallas_call(
        first_kernel,
        in_specs=[in_vmem, anywhere] + [in_vmem] * 7,
        out_specs=[anywhere] * 8,
        out_shape=[
            jax.ShapeDtypeStruct((blk, d_model), BF16),
            jax.ShapeDtypeStruct((4, seq), F32),
            jax.ShapeDtypeStruct((seq, d_model), BF16),
            jax.ShapeDtypeStruct((blk, d_model), BF16),
            jax.ShapeDtypeStruct((4, *w_o.shape), BF16),
            jax.ShapeDtypeStruct((d_model, 4 * ff_cols), BF16),
            jax.ShapeDtypeStruct((4, *w_2.shape), BF16),
            jax.ShapeDtypeStruct((d_model, 12 * head_cols), BF16),
        ],
        scratch_shapes=[
            pltpu.VMEM((seq, 3 * head_cols), BF16),
            pltpu.VMEM((PAIR, seq), BF16),
            pltpu.VMEM((seq, blk), F32),
            pltpu.VMEM((seq, blk), F32),
            pltpu.VMEM((2, seq, PAIR), BF16),
            pltpu.VMEM((4, seq), F32),
            pltpu.VMEM((blk, d_model), BF16),
            pltpu.SemaphoreType.DMA((10,)),
            pltpu.SemaphoreType.DMA((copies,)),
            pltpu.SemaphoreType.DMA((copies,)),
            pltpu.SemaphoreType.DMA((8,)),
            pltpu.SemaphoreType.DMA((8,)),
            pltpu.SemaphoreType.DMA((3,)),
            pltpu.SemaphoreType.DMA((3,)),
        ],
        compiler_params=pltpu.CompilerParams(vmem_limit_bytes=60 << 20, collective_id=0, has_side_effects=True),
        cost_estimate=pl.CostEstimate(
            flops=64 * seq * seq * PAIR, bytes_accessed=64 * seq * d_model, transcendentals=seq * seq * 4),
        name="first",
    )(x, cot, emb, w_q, w_k, w_v, w_o, w_1, w_2)


def grad_kernel(by_left, _, *refs):
    lefts, rights, (away_ref, mid_ref, keep_ref, left_t, right_s) = refs[:16], refs[16:20], refs[20:]
    count, piece = lefts[0].shape
    step = pl.program_id(0)

    @pl.when(step == 0 if not by_left else step >= 0)
    def _():
        for i in range(16):
            left_t[i % 4 * piece:(i % 4 + 1) * piece, i // 4 * count:(i // 4 + 1) * count] = lefts[i][...].T

    @pl.when(step == 0 if by_left else step >= 0)
    def _():
        for i in range(4):
            right_s[i * count:(i + 1) * count, :] = rights[i][...]

    total = dot_nn(left_t[...], right_s[...])
    away_ref[0] = total[:2 * piece]
    mid_ref[0] = total[2 * piece:3 * piece]
    keep_ref[0] = total[3 * piece:]


def grad_products(order, lefts, rights, by_left=False):
    count = rights[0].shape[0]
    tile = rights[0].shape[1] // (1 if by_left else 4)
    piece = lefts[0].shape[1] // (32 if by_left else 8)
    if by_left:
        left_spec = lambda n: pl.BlockSpec((count, piece), lambda i, order: (0, i * 8 + order[n]))
        right_spec = pl.BlockSpec((count, tile), lambda i, order: (0, 0))
    else:
        left_spec = lambda n: pl.BlockSpec((count, piece), lambda i, order: (0, order[n]))
        right_spec = pl.BlockSpec((count, tile), lambda i, order: (0, i))
    return pl.pallas_call(
        functools.partial(grad_kernel, by_left),
        grid_spec=pltpu.PrefetchScalarGridSpec(
            num_scalar_prefetch=1,
            grid=(4,),
            in_specs=[left_spec(n) for _ in range(4) for n in range(4)] + [right_spec] * 4,
            out_specs=[pl.BlockSpec((1, n * piece, tile), lambda i, order: (i, 0, 0)) for n in (2, 1, 1)],
            scratch_shapes=[pltpu.VMEM((4 * piece, 4 * count), BF16), pltpu.VMEM((4 * count, tile), BF16)],
        ),
        out_shape=[jax.ShapeDtypeStruct((4, n * piece, tile), F32) for n in (2, 1, 1)],
        compiler_params=pltpu.CompilerParams(vmem_limit_bytes=60 << 20),
        cost_estimate=pl.CostEstimate(
            flops=128 * count * piece * tile, bytes_accessed=8 * count * (4 * piece + 4 * tile) + 64 * piece * tile,
            transcendentals=0),
        interpret=INTERPRET,
        name="grad",
    )(order, *[left for left in lefts for _ in range(4)], *rights)


def backward_rows(q, d_out, lse, k_ref, v_ref, k_t, p_cat, ds_cat, dk_acc, dv_acc):
    block = q.shape[0]
    lane = lax.broadcasted_iota(jnp.int32, q.shape, 1)
    q_heads, do_heads, dqs = [], [], []
    for head in range(2):
        mine = lane // HEAD_DIM == head
        q_head = jnp.where(mine, q, jnp.zeros_like(q))
        do_head = jnp.where(mine, d_out, jnp.zeros_like(d_out))
        scores = dot_nt(k_ref[...], q_head)
        probs = jnp.exp2(scores * EXP2_SCALE - lse[head:head + 1, :])
        d_probs = dot_nt(v_ref[...], do_head).astype(BF16).astype(F32)
        inner = jnp.sum(probs * d_probs, axis=0, keepdims=True)
        cols = slice(head * block, (head + 1) * block)
        p_cat[:, cols] = probs.astype(BF16)
        ds_cat[:, cols] = (probs * (d_probs - inner)).astype(BF16)
        dqs.append(dot_nn(k_t[head * HEAD_DIM:(head + 1) * HEAD_DIM, :], ds_cat[:, cols]))
        q_heads.append(q_head)
        do_heads.append(do_head)
    dv_acc[...] += dot_nn(p_cat[...], jnp.concatenate(do_heads, axis=0))
    dk_acc[...] += dot_nn(ds_cat[...], jnp.concatenate(q_heads, axis=0))
    return (jnp.concatenate(dqs, axis=0).T * SCALE).astype(BF16)


def last_kernel(qkv_ref, dc_ref, lse_ref, dmid_ref, x_ref, emb_ref, wqkv_ref, u_ref, gqkv2_ref,
                r2_ref, mid2_ref, keep2_ref, away1_ref, mid1_ref, keep1_ref, awayo_ref, mido_ref, keepo_ref,
                dx_ref, g1_ref, g2_ref, go_ref, gq_ref, gk_ref, gv_ref,
                dch, k_t, dk_acc, dv_acc, p_cat, ds_cat, d_heads, d_qkv, buf, buf_o, second, second_o, tmp, tmp_o,
                third, third_o, sum_1, sum_2, sum_o, qa, qb, q1, q2, q3, q4, d_1, w_s, u_s, g_s,
                local_sem, load_sem, send_sem, recv_sem, dc_send, dc_recv, dq_send, dq_recv, z_send, z_recv, x_send, x_recv,
                p_send, p_recv):
    seq = qkv_ref.shape[0]
    blk = seq // 4
    head_cols = 2 * PAIR
    here = Place()
    z, core, role, owner = here.z, here.c, here.role, here.owner
    here.meet()
    copies = Copies(send_sem, recv_sem)
    waits = []

    def span(index, count):
        return pl.ds(pl.multiple_of(index * count, count), count)

    def load(src, dst, n):
        copy = pltpu.make_async_copy(src, dst, load_sem.at[n])
        copy.start()
        return copy

    no = jnp.logical_not
    to_a, to_b = here.device(y=here.ya, x=here.xa), here.device(y=here.yb, x=here.xb)
    partner = here.device(c=1 - core)
    member = [here.device(z=z // 2 * 2 + i // 2, c=i % 2) for i in range(4)]
    piece = tmp.shape[1]

    def dc_copy(i):
        return pltpu.make_async_remote_copy(
            src_ref=dc_ref.at[:, i * head_cols:(i + 1) * head_cols], dst_ref=dch.at[span(role, blk), :],
            send_sem=dc_send.at[i], recv_sem=dc_recv.at[role], device_id=member[i], device_id_type=MESH)

    for i in range(4):
        pl.when(role != i)(dc_copy(i).start)

        @pl.when(role == i)
        def _():
            dch[i * blk:(i + 1) * blk, :] = dc_ref[:, i * head_cols:(i + 1) * head_cols]

    firsts = {('1', q): copies.start(away1_ref.at[q], buf.at[4 + q], to_a) for q in range(4)}
    firsts['o'] = copies.start(awayo_ref, buf_o, to_a)
    w2_loads = [load(r2_ref.at[q], buf.at[q], q) for q in range(4)]
    seconds = {(w, q): copies.make(buf.at[u + q, piece:, :], second.at[u + q], to_b) for w, u in (('2', 0), ('1', 4)) for q in range(4)}
    seconds['o'] = copies.make(buf_o.at[:, piece:, :], second_o, to_b)

    def add_mid(unit):
        if unit == 'o':
            mid, keep, t, n = mido_ref, keepo_ref, tmp_o, 4
            bottom, top = buf_o.at[:, piece:, :], buf_o.at[:, :piece, :]
        else:
            w, q = unit
            mid, keep = (mid2_ref.at[q], keep2_ref.at[q]) if w == '2' else (mid1_ref.at[q], keep1_ref.at[q])
            u = q if w == '2' else 4 + q
            t, n, bottom, top = tmp, 6, buf.at[u, piece:, :], buf.at[u, :piece, :]
        loads = [load(mid, t.at[0], n), load(keep, t.at[1], n + 1)]
        if unit == 'o' or unit[0] == '1':
            firsts[unit].wait_recv()
        else:
            w2_loads[unit[1]].wait()
        for copy in loads:
            copy.wait()
        bottom[...] += t[0]
        top[...] += t[1]
        seconds[unit].start()

    def z_copy(unit, q):
        if unit == 'o':
            src, dst, n = buf_o.at[q, :piece, :], third_o.at[z], 8
        else:
            w = 0 if unit == '2' else 1
            src, dst, n = buf.at[4 * w + q, :piece, :], third.at[w, z], 4 * w
        return pltpu.make_async_remote_copy(
            src_ref=src, dst_ref=dst, send_sem=z_send.at[n + q], recv_sem=z_recv.at[n + z],
            device_id=here.device(z=q), device_id_type=MESH)

    def finish(unit):
        seconds[unit].wait_recv()
        if unit == 'o':
            buf_o[:, :piece, :] += second_o[...]
            for q in range(4):
                pl.when(z != q)(z_copy('o', q).start)
        else:
            w, q = unit
            u = q if w == '2' else 4 + q
            buf[u, :piece, :] += second[u]
            pl.when(z != q)(z_copy(w, q).start)

    mine, by_a = here.piece(here.y, here.x), here.piece(here.ya, here.xa)
    by_b, by_ab = here.piece(here.yb, here.xb), here.piece(1 - here.y, 1 - here.x)
    gathers = {}

    def total(unit):
        out, got, n = {'2': (sum_2, third.at[0], 0), '1': (sum_1, third.at[1], 4), 'o': (sum_o, third_o, 8)}[unit]
        if unit == 'o':
            out[...] = buf_o[z, :piece, :]
        else:
            out[...] = buf[n + z, :piece, :]
        for zz in range(4):
            @pl.when(z != zz)
            def _():
                pltpu.make_async_copy(out, got.at[zz], z_recv.at[n + zz]).wait()
                out[...] += got[zz]

    def gather_start(name, src, out, n):
        rows = lambda e: out.at[span(e, piece), :]
        keep = pltpu.make_async_copy(src, rows(mine), local_sem.at[n])
        keep.start()
        waits.append(keep)
        gathers[name] = dict(src=src, rows=rows, a=copies.start(src, rows(mine), to_a), b1=copies.start(src, rows(mine), to_b))

    def gather_second(name):
        g = gathers[name]
        g['a'].wait_recv()
        g['b2'] = copies.start(g['rows'](by_a), g['rows'](by_a), to_b)

    def gather_core(name):
        g = gathers[name]
        g['c'] = [copies.start(g['src'], g['rows'](mine), partner), copies.start(g['rows'](by_a), g['rows'](by_a), partner)]
        g['b1'].wait_recv()
        g['c'].append(copies.start(g['rows'](by_b), g['rows'](by_b), partner))
        g['b2'].wait_recv()
        g['c'].append(copies.start(g['rows'](by_ab), g['rows'](by_ab), partner))

    def dq_copy(j, i, t):
        col = t * head_cols + j * PAIR
        return pltpu.make_async_remote_copy(
            src_ref=d_heads.at[i * blk:(i + 1) * blk, col:col + PAIR],
            dst_ref=d_qkv.at[:, pl.ds(pl.multiple_of(role * 3 * head_cols + col, PAIR), PAIR)],
            send_sem=dq_send.at[(j * 4 + i) * 3 + t], recv_sem=dq_recv.at[(j * 4 + role) * 3 + t],
            device_id=member[i], device_id_type=MESH)

    def send_d_heads(j):
        for i in range(4):
            @pl.when(role != i)
            def _():
                for t in range(3):
                    dq_copy(j, i, t).start()

    for i in range(4):
        @pl.when(role != i)
        def _():
            pltpu.make_async_copy(dc_ref.at[:, :head_cols], dch.at[:blk, :], dc_recv.at[i]).wait()

    moves = {(0, 0): [(add_mid, ('2', 0))], (0, 1): [(add_mid, ('2', 1))], (0, 2): [(add_mid, ('2', 2))],
             (0, 3): [(add_mid, ('2', 3))], (0, 5): [(add_mid, ('1', 0))], (0, 6): [(finish, ('2', 0))],
             (1, 0): [(send_d_heads, 0), (finish, ('2', 1))], (1, 1): [(add_mid, ('1', 1))], (1, 3): [(finish, ('2', 2))],
             (1, 4): [(add_mid, ('1', 2))], (1, 6): [(finish, ('2', 3))]}
    steps = seq // BWD_ROWS
    for j in range(2):
        k_view, v_view = qkv_ref.at[:, (2 + j) * PAIR:(3 + j) * PAIR], qkv_ref.at[:, (4 + j) * PAIR:(5 + j) * PAIR]
        k_t[...] = k_view[...].T
        dk_acc[...] = jnp.zeros_like(dk_acc)
        dv_acc[...] = jnp.zeros_like(dv_acc)

        def block(i, _):
            for n in range(8):
                if (j, n) in moves:
                    @pl.when(i == min(n, steps - 1))
                    def _():
                        for move, what in moves[(j, n)]:
                            move(what)
            rows = span(i, BWD_ROWS)
            cols = slice(j * PAIR, (j + 1) * PAIR)
            d_heads[rows, cols] = backward_rows(
                qkv_ref[rows, cols], dch[rows, cols], lse_ref[2 * j:2 * j + 2, rows], k_view, v_view,
                k_t, p_cat, ds_cat, dk_acc, dv_acc)
            return 0

        lax.fori_loop(0, steps, block, 0)
        d_heads[:, head_cols + j * PAIR:head_cols + (j + 1) * PAIR] = (dk_acc[...] * SCALE).astype(BF16)
        d_heads[:, 2 * head_cols + j * PAIR:2 * head_cols + (j + 1) * PAIR] = dv_acc[...].astype(BF16)

    quarter = 2 * piece
    index = [here.ya * 2 + here.xa, (1 - here.y) * 2 + 1 - here.x, here.yb * 2 + here.xb, here.y * 2 + here.x]

    def quarter_loads(n):
        return [load(u_ref.at[:, span(index[n], quarter)], u_s.at[n % 2], 8 + n % 2),
                load(gqkv2_ref.at[span(index[n], quarter), :], g_s.at[n % 2], 10 + n % 2)]

    pending = quarter_loads(0)
    for i in range(4):
        @pl.when(role == i)
        def _():
            d_qkv[:, i * 3 * head_cols:(i + 1) * 3 * head_cols] = d_heads[i * blk:(i + 1) * blk, :]
    send_d_heads(1)
    targets = [qa.at[0], qa.at[1], qb.at[0], qb.at[1]]
    first_q = None
    for n in range(4):
        ahead = quarter_loads(n + 1) if n < 3 else []
        for copy in pending:
            copy.wait()
        targets[n][...] = dot_tn(u_s[n % 2], d_heads[...]) + g_s[n % 2]
        pending = ahead
        if n == 2:
            first_q = copies.start(qa, q1, to_a)

    add_mid(('1', 3))
    finish(('1', 0))
    w_rows = w_s.shape[1]
    chunks = wqkv_ref.shape[0] // w_rows
    w_load = load(wqkv_ref.at[:w_rows, :], w_s.at[0], 12)
    for j in range(2):
        for i in range(4):
            @pl.when(role != i)
            def _():
                for t in range(3):
                    pltpu.make_async_copy(d_heads.at[:blk, :PAIR], d_qkv.at[:, :PAIR], dq_recv.at[(j * 4 + i) * 3 + t]).wait()
    for n in range(chunks):
        ahead = load(wqkv_ref.at[(n + 1) * w_rows:(n + 2) * w_rows, :], w_s.at[(n + 1) % 2], 12 + (n + 1) % 2) if n + 1 < chunks else None
        w_load.wait()
        d_1[:, n * w_rows:(n + 1) * w_rows] = dot_nt(d_qkv[...], w_s[n % 2]).astype(BF16)
        w_load = ahead

    count = min(128, blk)
    for n in range(blk // count):
        rows = slice(n * count, (n + 1) * count)
        values = x_ref[rows, :].astype(F32) + emb_ref[...]
        up = d_1[rows, :].astype(F32)
        inverse = lax.rsqrt(jnp.mean(values * values, axis=-1, keepdims=True) + EPS_NORM)
        inner = jnp.mean(values * up, axis=-1, keepdims=True)
        d_1[rows, :] = (dmid_ref[rows, :].astype(F32) + inverse * up - values * (inverse * inverse * inverse * inner)).astype(BF16)

    own_seq = z // 2
    rows_dx = span(role, blk)

    def dx_copy(n, device):
        slot = [0, 1 + core, 3 + core][n]
        return pltpu.make_async_remote_copy(
            src_ref=d_1, dst_ref=dx_ref.at[rows_dx, :], send_sem=x_send.at[n], recv_sem=x_recv.at[slot],
            device_id=device, device_id_type=MESH)

    dx_side = dx_copy(0, partner)
    dx_next = dx_copy(1, here.device(z=here.z_by[1], c=own_seq))
    dx_cross = dx_copy(2, here.device(z=here.z_by[2], c=own_seq))
    dx_keep = pltpu.make_async_copy(d_1, dx_ref.at[rows_dx, :], local_sem.at[8])

    def dx_pass(cc):
        rows = span(z % 2 * 2 + cc, blk)
        return pltpu.make_async_remote_copy(
            src_ref=dx_ref.at[rows, :], dst_ref=dx_ref.at[rows, :], send_sem=x_send.at[3 + cc], recv_sem=x_recv.at[5 + cc],
            device_id=here.device(z=here.z_by[1]), device_id_type=MESH)

    add_mid('o')
    dx_cross.start()
    dx_next.start()
    pl.when(owner)(dx_keep.start)
    pl.when(no(owner))(dx_side.start)

    def dx_got(slot):
        pltpu.make_async_copy(d_1, dx_ref.at[:blk, :], x_recv.at[slot]).wait()

    first_q.wait_recv()
    qb[0] += q1[1]
    qb[1] += q1[0]
    second_q = copies.start(qb.at[0], q2, to_b)
    finish(('1', 1))
    total('2')
    finish(('1', 2))
    gather_start('2', sum_2, g2_ref, 0)
    finish(('1', 3))
    finish('o')
    second_q.wait_recv()
    qb[1] += q2[...]
    plane_stays = jnp.logical_and(2 * (z % 2) + core == z, z // 2 == core)
    plane_q = pltpu.make_async_remote_copy(
        src_ref=qb.at[1], dst_ref=q3, send_sem=p_send.at[0], recv_sem=p_recv.at[0],
        device_id=here.device(z=2 * (z % 2) + core, c=z // 2), device_id_type=MESH)

    @pl.when(plane_stays)
    def _():
        q3[...] = qb[1]

    pl.when(no(plane_stays))(plane_q.start)
    gather_second('2')

    @pl.when(no(owner))
    def _():
        for cc in range(2):
            dx_got(3 + cc)
            dx_pass(cc).start()

    total('1')
    total('o')
    gather_start('1', sum_1, g1_ref, 1)
    gather_start('o', sum_o, go_ref, 2)
    gather_core('2')
    pl.when(no(plane_stays))(plane_q.wait_recv)
    give_q = copies.start(q3.at[span(1 - core, piece), :], q4.at[0], partner)
    gather_second('1')
    gather_second('o')
    give_q.wait_recv()
    q4[1] = q4[0] + q3[span(core, piece), :]
    for t, (name, out) in enumerate((('q', gq_ref), ('k', gk_ref), ('v', gv_ref))):
        gather_start(name, q4.at[1, :, t * head_cols:(t + 1) * head_cols], out, 3 + t)
    gather_core('1')
    gather_core('o')
    for name in 'qkv':
        gather_second(name)
    for name in 'qkv':
        gather_core(name)

    @pl.when(owner)
    def _():
        for slot in (0, 1, 2):
            dx_got(slot)
        dx_keep.wait()

    @pl.when(no(owner))
    def _():
        dx_side.wait_send()
        for cc in range(2):
            dx_got(5 + cc)
            dx_pass(cc).wait_send()

    for g in gathers.values():
        for copy in g['c']:
            copy.wait_recv()
    for copy in waits:
        copy.wait()
    for copy in copies.sent:
        copy.wait_send()
    dx_cross.wait_send()
    dx_next.wait_send()
    pl.when(no(plane_stays))(plane_q.wait_send)
    for i in range(4):
        @pl.when(role != i)
        def _():
            dc_copy(i).wait_send()
            for j in range(2):
                for t in range(3):
                    dq_copy(j, i, t).wait_send()

        for unit in '21o':
            pl.when(z != i)(z_copy(unit, i).wait_send)


def last_call(qkv, d_c, lse, d_mid, x, emb, w_qkv, u_seq, g_qkv, w2_parts, w1_parts, wo_parts):
    seq, d_model = u_seq.shape
    blk, piece = seq // 4, d_model // 8
    n1, no = w1_parts[0].shape[2], wo_parts[0].shape[2]
    assert w2_parts[0].shape[1:] == (2 * piece, n1)
    heads3 = qkv.shape[1]
    anywhere = pl.BlockSpec(memory_space=pl.ANY)
    in_vmem = pl.BlockSpec(memory_space=pltpu.VMEM)
    copies = 5 + 9 + 6 * 7 + 3
    dma = pltpu.SemaphoreType.DMA
    w_rows = min(256, d_model)
    return pl.pallas_call(
        last_kernel,
        in_specs=[in_vmem] * 6 + [anywhere] * 12,
        out_specs=[anywhere] * 7,
        out_shape=[
            jax.ShapeDtypeStruct((seq, d_model), BF16),
            jax.ShapeDtypeStruct((d_model, n1), F32),
            jax.ShapeDtypeStruct((8 * piece, n1), F32),
            jax.ShapeDtypeStruct((d_model, no), F32),
        ] + [jax.ShapeDtypeStruct((d_model, heads3 // 3), F32)] * 3,
        scratch_shapes=[
            pltpu.VMEM((seq, heads3 // 3), BF16),
            pltpu.VMEM((PAIR, seq), BF16),
            pltpu.VMEM((seq, PAIR), F32),
            pltpu.VMEM((seq, PAIR), F32),
            pltpu.VMEM((seq, 2 * BWD_ROWS), BF16),
            pltpu.VMEM((seq, 2 * BWD_ROWS), BF16),
            pltpu.VMEM((seq, heads3), BF16),
            pltpu.VMEM((blk, 4 * heads3), BF16),
            pltpu.VMEM((8, 2 * piece, n1), F32),
            pltpu.VMEM((4, 2 * piece, no), F32),
            pltpu.VMEM((8, piece, n1), F32),
            pltpu.VMEM((4, piece, no), F32),
            pltpu.VMEM((2, piece, n1), F32),
            pltpu.VMEM((2, 4, piece, no), F32),
            pltpu.VMEM((2, 4, piece, n1), F32),
            pltpu.VMEM((4, piece, no), F32),
            pltpu.VMEM((piece, n1), F32),
            pltpu.VMEM((piece, n1), F32),
            pltpu.VMEM((piece, no), F32),
            pltpu.VMEM((2, 2 * piece, heads3), F32),
            pltpu.VMEM((2, 2 * piece, heads3), F32),
            pltpu.VMEM((2, 2 * piece, heads3), F32),
            pltpu.VMEM((2 * piece, heads3), F32),
            pltpu.VMEM((2 * piece, heads3), F32),
            pltpu.VMEM((2, piece, heads3), F32),
            pltpu.VMEM((blk, d_model), BF16),
            pltpu.VMEM((2, w_rows, 4 * heads3), BF16),
            pltpu.VMEM((2, seq, 2 * piece), BF16),
            pltpu.VMEM((2, 2 * piece, heads3), F32),
            dma((9,)), dma((14,)), dma((copies,)), dma((copies,)),
            dma((4,)), dma((4,)), dma((24,)), dma((24,)), dma((12,)), dma((12,)), dma((5,)), dma((7,)), dma((1,)), dma((1,)),
        ],
        compiler_params=pltpu.CompilerParams(vmem_limit_bytes=63 << 20, collective_id=1, has_side_effects=True),
        cost_estimate=pl.CostEstimate(
            flops=160 * seq * seq * PAIR, bytes_accessed=128 * seq * d_model, transcendentals=seq * seq * 4),
        name="last",
    )(qkv, d_c, lse, d_mid, x, emb, w_qkv, u_seq, g_qkv, *w2_parts, *w1_parts, *wo_parts)


def lin(z, y, x, c):
    return z * 8 + y * 4 + x * 2 + c


def send(value, to):
    pairs = []
    for z in range(4):
        for y in range(2):
            for x in range(2):
                for c in range(2):
                    dst = to(z, y, x, c)
                    if dst is not None:
                        pairs.append((lin(z, y, x, c), lin(*dst)))
    return lax.ppermute(value, AXES, pairs)


def role_of(z, c):
    return (z % 2) * 2 + c


def in_group(k):
    def to(z, y, x, c):
        role = role_of(z, c) ^ k
        return (z // 2 * 2 + role // 2, y, x, role % 2)

    return to


def other_core(z, y, x, c):
    return (z, y, x, 1 - c)


def swap_first(z, y, x, c):
    return (z, y, 1 - x, c) if c == 0 else (z, 1 - y, x, c)


def unscramble(parts, role):
    odd, high = role % 2 == 1, role // 2 == 1
    a = [jnp.where(odd, parts[i ^ 1], parts[i]) for i in range(4)]
    return [jnp.where(high, a[i ^ 2], a[i]) for i in range(4)]


def rows_of(value, index, count):
    return lax.dynamic_slice_in_dim(value, index * count, count, axis=0)


def solution(mesh):
    spec_col = P(None, 'model')
    spec_row = P('model', None)
    spec_act = P('data', None, None)
    spec_rep = P(None, None)

    def device_step(x_in, cot_out, step_emb, w_q, w_k, w_v, w_o, w_1, w_2):
        seq, d_model = x_in.shape[1:]
        head_cols = w_q.shape[1]
        blk = seq // 4
        z = lax.axis_index('model')
        d = lax.axis_index('data')
        y, x, core = d // 4, d // 2 % 2, d % 2
        role = z % 2 * 2 + core
        owner = core == z // 2
        emb = step_emb.astype(F32)

        c_1, lse_1, x_seq, cot, wo, w1, w2, w_qkv = first_call(
            x_in[0], cot_out[0], emb[:1], w_q, w_k, w_v, w_o, w_1, w_2)
        wo, w2 = wo.reshape(-1, d_model), w2.reshape(-1, d_model)
        w_qkv_role = lax.dynamic_slice_in_dim(w_qkv, role * 3 * head_cols, 3 * head_cols, axis=1)
        x_1 = rows_of(x_seq, role, blk)

        def exchange(parts):
            swapped = unscramble(parts, role)
            got = [swapped[0]] + [send(swapped[k], in_group(k)) for k in (1, 2, 3)]
            return unscramble(got, role)

        def mlp_forward(x_f, context):
            h = (x_f + dot_nn(context, wo)).astype(BF16)
            m = rms_norm(h.astype(F32)).astype(BF16)
            up = dot_nn(m, w1).astype(BF16)
            act = jax.nn.gelu(up.astype(F32)).astype(BF16)
            return h, m, up, act

        def interleave(pairs):
            return jnp.concatenate([pairs[j][i] for i in range(4) for j in range(2)], axis=1)

        s_1 = x_1.astype(F32) + emb[0]
        h_1, m_1, up_1, act_1 = mlp_forward(s_1, c_1)
        x_2 = (h_1.astype(F32) + dot_nn(act_1, w2)).astype(BF16)

        side = send(x_2, other_core)
        over = send(x_2, in_group(2))
        x_2_seq = jnp.concatenate(unscramble([x_2, side, over, send(over, other_core)], role), axis=0)
        u_2_seq = rms_norm(x_2_seq.astype(F32) + emb[1]).astype(BF16)
        qkv_2 = dot_nn(u_2_seq, w_qkv_role).astype(BF16)
        got, lse_2 = [], []
        for j in range(2):
            c_heads, lse = attn_fwd(qkv_2, j)
            got.append(exchange([c_heads[i * blk:(i + 1) * blk] for i in range(4)]))
            lse_2.append(lse)
        c_2 = interleave(got)
        lse_2 = jnp.concatenate(lse_2, axis=0)
        s_2 = x_2.astype(F32) + emb[1]
        h_2, m_2, up_2, act_2 = mlp_forward(s_2, c_2)

        def mlp_backward(d_next, h, up):
            d_act = dot_nt(d_next, w2).astype(BF16)
            d_up = jax.vjp(jax.nn.gelu, up.astype(F32))[1](d_act.astype(F32))[0].astype(BF16)
            d_m = dot_nt(d_up, w1).astype(BF16)
            d_h = jax.vjp(rms_norm, h.astype(F32))[1](d_m.astype(F32))[0]
            return d_up, (d_next.astype(F32) + d_h).astype(BF16)

        d_up_2, d_mid_2 = mlp_backward(cot, h_2, up_2)
        d_c = dot_nt(d_mid_2, wo).astype(BF16)
        pairs, grads = [], []
        for j in range(2):
            heads = exchange([d_c[:, i * head_cols + j * PAIR:i * head_cols + (j + 1) * PAIR] for i in range(4)])
            d_heads = attn_bwd(qkv_2, jnp.concatenate(heads, axis=0), lse_2[2 * j:2 * j + 2], j)
            grads.append(dot_tn(u_2_seq, d_heads))
            pairs.append(exchange([d_heads[i * blk:(i + 1) * blk] for i in range(4)]))
        d_qkv = jnp.concatenate(
            [pairs[j][i][:, t * PAIR:(t + 1) * PAIR] for i in range(4) for t in range(3) for j in range(2)], axis=1)
        g_qkv_2 = jnp.concatenate([grads[j][:, t * PAIR:(t + 1) * PAIR] for t in range(3) for j in range(2)], axis=1)
        d_u = dot_nt(d_qkv, w_qkv).astype(BF16)
        d_s = jax.vjp(rms_norm, s_2)[1](d_u.astype(F32))[0]
        d_2 = (d_mid_2.astype(F32) + d_s).astype(BF16)

        u_1_seq = rms_norm(x_seq.astype(F32) + emb[0]).astype(BF16)
        qkv_1 = dot_nn(u_1_seq, w_qkv_role).astype(BF16)

        first, second = jnp.where(core == 0, x, y), jnp.where(core == 0, y, x)

        def at(i, j):
            return jnp.where(core == 0, j * 2 + i, i * 2 + j)

        order = [at(1 - first, second), at(1 - first, 1 - second), at(first, 1 - second), at(first, second)]
        column = jnp.stack(order) * 2 + core

        def products(sides, by_left=False):
            lefts, rights = [], []
            for left, right in sides:
                lefts += [left, send(left, other_core)]
                rights += [right, send(right, other_core)]
            return grad_products(column, lefts, rights, by_left)

        away, mid, keep = products([(act_2, cot), (act_1, d_2)], True)
        d_2, away = lax.optimization_barrier((d_2, away))
        w2_parts = (send(away, swap_first), mid, keep)
        d_up_1, d_mid_1 = mlp_backward(d_2, h_1, up_1)
        w1_parts = products([(m_2, d_up_2), (m_1, d_up_1)])
        wo_parts = products([(d_mid_2, c_2), (d_mid_1, c_1)])
        d_c = dot_nt(d_mid_1, wo).astype(BF16)
        d_x, g_w1, g_w2, g_wo, g_q, g_k, g_v = last_call(
            qkv_1, d_c, lse_1, d_mid_1, x_1, emb[:1], w_qkv, u_1_seq, g_qkv_2, w2_parts, w1_parts, wo_parts)
        return g_q, g_k, g_v, g_wo.T, g_w1, g_w2, d_x[None]

    return jax.shard_map(device_step, mesh=mesh,
                         in_specs=(spec_act, spec_act, spec_rep, spec_col, spec_col, spec_col, spec_row, spec_col, spec_row),
                         out_specs=(spec_col, spec_col, spec_col, spec_row, spec_col, spec_row, spec_act),
                         check_vma=False)
```

```python
import functools
import math

import jax
import jax.numpy as jnp
from jax import lax
from jax.experimental import pallas as pl
from jax.experimental.pallas import tpu as pltpu
from jax.sharding import PartitionSpec as P


HEAD_DIM = 64
EPS_NORM = 1e-6
SCALE = HEAD_DIM ** -0.5
EXP2_SCALE = SCALE * math.log2(math.e)
PAIR = 2 * HEAD_DIM
FWD_ROWS = 512
BWD_ROWS = 256
KEYS = 256
INTERPRET = False
AXES = ('model', 'data')
BF16 = jnp.bfloat16
F32 = jnp.float32
MESH = pl.DeviceIdType.MESH


def rms_norm(values):
    return values * lax.rsqrt(jnp.mean(values * values, axis=-1, keepdims=True) + EPS_NORM)


def dot_nt(a, b):
    return lax.dot_general(a, b, (((1,), (1,)), ((), ())), preferred_element_type=F32)


def dot_nn(a, b):
    return lax.dot_general(a, b, (((1,), (0,)), ((), ())), preferred_element_type=F32)


def dot_tn(a, b):
    return lax.dot_general(a, b, (((0,), (0,)), ((), ())), preferred_element_type=F32)


def attn_fwd_kernel(q_ref, k_ref, v_ref, o_ref, lse_ref, vt_ref, *e_refs):
    @pl.when(pl.program_id(0) == 0)
    def _():
        vt_ref[...] = v_ref[...].T

    outs, sums = attend_rows(q_ref[...], k_ref, vt_ref, e_refs)
    o_ref[...] = jnp.concatenate(outs, axis=0).T.astype(BF16)
    for head in range(2):
        lse_ref[head:head + 1, :] = sums[head]


def attn_fwd(qkv, pair):
    seq = qkv.shape[0]
    rows = min(FWD_ROWS, seq)
    return pl.pallas_call(
        attn_fwd_kernel,
        grid=(seq // rows,),
        in_specs=[
            pl.BlockSpec((rows, PAIR), lambda i: (i, pair)),
            pl.BlockSpec((seq, PAIR), lambda i: (0, 2 + pair)),
            pl.BlockSpec((seq, PAIR), lambda i: (0, 4 + pair)),
        ],
        out_specs=[
            pl.BlockSpec((rows, PAIR), lambda i: (i, 0)),
            pl.BlockSpec((2, rows), lambda i: (0, i)),
        ],
        out_shape=[jax.ShapeDtypeStruct((seq, PAIR), BF16), jax.ShapeDtypeStruct((2, seq), F32)],
        scratch_shapes=[pltpu.VMEM((PAIR, seq), BF16)] + [pltpu.VMEM((seq, rows), F32)] * 2,
        compiler_params=pltpu.CompilerParams(vmem_limit_bytes=60 << 20),
        cost_estimate=pl.CostEstimate(
            flops=16 * seq * seq * PAIR, bytes_accessed=8 * seq * PAIR, transcendentals=seq * seq * 2),
        interpret=INTERPRET,
        name="attn_fwd",
    )(qkv, qkv, qkv)


def attn_bwd_kernel(q_ref, k_ref, v_ref, do_ref, lse_ref, out_ref, kt_ref, dk_acc, dv_acc, p_cat, ds_cat):
    step = pl.program_id(0)

    @pl.when(step == 0)
    def _():
        kt_ref[...] = k_ref[...].T
        dk_acc[...] = jnp.zeros_like(dk_acc)
        dv_acc[...] = jnp.zeros_like(dv_acc)

    block = q_ref.shape[0]
    out_ref[pl.ds(pl.multiple_of(step * block, block), block), :PAIR] = backward_rows(
        q_ref[...], do_ref[...], lse_ref[...], k_ref, v_ref, kt_ref, p_cat, ds_cat, dk_acc, dv_acc)

    @pl.when(step == pl.num_programs(0) - 1)
    def _():
        out_ref[:, PAIR:2 * PAIR] = (dk_acc[...] * SCALE).astype(BF16)
        out_ref[:, 2 * PAIR:] = dv_acc[...].astype(BF16)


def attn_bwd(qkv, d_context, lse, pair):
    seq = qkv.shape[0]
    full = lambda column: pl.BlockSpec((seq, PAIR), lambda i: (0, column))
    rows = lambda column: pl.BlockSpec((BWD_ROWS, PAIR), lambda i: (i, column))
    return pl.pallas_call(
        attn_bwd_kernel,
        grid=(seq // BWD_ROWS,),
        in_specs=[rows(pair), full(2 + pair), full(4 + pair), rows(0), pl.BlockSpec((2, BWD_ROWS), lambda i: (0, i))],
        out_specs=pl.BlockSpec((seq, 3 * PAIR), lambda i: (0, 0)),
        out_shape=jax.ShapeDtypeStruct((seq, 3 * PAIR), BF16),
        scratch_shapes=[
            pltpu.VMEM((PAIR, seq), BF16),
            pltpu.VMEM((seq, PAIR), F32),
            pltpu.VMEM((seq, PAIR), F32),
            pltpu.VMEM((seq, 2 * BWD_ROWS), BF16),
            pltpu.VMEM((seq, 2 * BWD_ROWS), BF16),
        ],
        compiler_params=pltpu.CompilerParams(vmem_limit_bytes=60 << 20),
        cost_estimate=pl.CostEstimate(
            flops=40 * seq * seq * PAIR, bytes_accessed=14 * seq * PAIR, transcendentals=seq * seq * 2),
        interpret=INTERPRET,
        name="attn_bwd",
    )(qkv, qkv, qkv, d_context, lse)


def attend_rows(q, k_ref, v_t, e_refs):
    count = k_ref.shape[0] // KEYS
    lane = lax.broadcasted_iota(jnp.int32, q.shape, 1)
    q_heads = [jnp.where(lane // HEAD_DIM == head, q, jnp.zeros_like(q)) for head in range(2)]
    tops, run, total, outs, sums = [[], []], [None, None], [None, None], [], []
    for j in range(count):
        keys = slice(j * KEYS, (j + 1) * KEYS)
        for head in range(2):
            scores = dot_nt(k_ref[keys, :], q_heads[head])
            top = jnp.max(scores, axis=0, keepdims=True) * EXP2_SCALE
            if j:
                top = jnp.maximum(top, run[head])
            weights = jnp.exp2(scores * EXP2_SCALE - top)
            part = jnp.sum(weights, axis=0, keepdims=True)
            total[head] = total[head] * jnp.exp2(run[head] - top) + part if j else part
            run[head] = top
            tops[head].append(top)
            e_refs[head][keys, :] = weights
    for head in range(2):
        inverse = 1.0 / total[head]
        out = None
        for j in range(count):
            keys = slice(j * KEYS, (j + 1) * KEYS)
            factor = inverse * jnp.exp2(tops[head][j] - run[head])
            probs = (e_refs[head][keys, :] * factor).astype(BF16)
            part = dot_nn(v_t[head * HEAD_DIM:(head + 1) * HEAD_DIM, keys], probs)
            out = out + part if j else part
        sums.append(run[head] + jnp.log2(total[head]))
        outs.append(out)
    return outs, sums


class Place:
    def __init__(self):
        self.z = lax.axis_index('model')
        d = lax.axis_index('data')
        self.y, self.x, self.c = d // 4, d // 2 % 2, d % 2
        z = self.z
        self.z_by = {1: z + 1 - 2 * (z % 2), 2: (z + 2) % 4, 3: 3 - z}
        x, y, c = self.x, self.y, self.c
        self.xa, self.ya = x + (1 - c) * (1 - 2 * x), y + c * (1 - 2 * y)
        self.xb, self.yb = x + c * (1 - 2 * x), y + (1 - c) * (1 - 2 * y)
        self.role = z % 2 * 2 + c
        self.owner = c == z // 2

    def piece(self, y, x, c=None):
        return y * 4 + x * 2 + (self.c if c is None else c)

    def device(self, z=None, y=None, x=None, c=None):
        z, y, x, c = (own if given is None else given for given, own in zip((z, y, x, c), (self.z, self.y, self.x, self.c)))
        return {'model': z, 'data': y * 4 + x * 2 + c}

    def peers(self):
        column = [self.device(z=z, c=c) for z in (self.z, *self.z_by.values()) for c in (self.c, 1 - self.c)][1:]
        return column + [self.device(x=1 - self.x), self.device(y=1 - self.y)]

    def meet(self):
        barrier = pltpu.get_barrier_semaphore()
        peers = self.peers()
        for peer in peers:
            pl.semaphore_signal(barrier, inc=1, device_id=peer, device_id_type=MESH)
        pl.semaphore_wait(barrier, len(peers))


class Copies:
    def __init__(self, send_sem, recv_sem):
        self.send_sem, self.recv_sem, self.used, self.sent = send_sem, recv_sem, 0, []

    def make(self, src, dst, device):
        n, self.used = self.used, self.used + 1
        copy = pltpu.make_async_remote_copy(
            src_ref=src, dst_ref=dst, send_sem=self.send_sem.at[n], recv_sem=self.recv_sem.at[n],
            device_id=device, device_id_type=MESH)
        self.sent.append(copy)
        return copy

    def start(self, src, dst, device):
        copy = self.make(src, dst, device)
        copy.start()
        return copy


def first_kernel(x_ref, cot_ref, emb_ref, wq_ref, wk_ref, wv_ref, wo_ref, w1_ref, w2_ref,
                 c1_ref, lse_ref, xs_ref, cot_loc_ref, full_o, full_1, full_2, full_qkv,
                 qkv_s, vt_s, e_a, e_b, c_buf, lse_s, cot_s, local_sem, send_sem, recv_sem, c_send, c_recv, one_send, one_recv):
    seq, d_model = x_ref.shape
    blk = seq // 4
    head_cols = wq_ref.shape[1]
    here = Place()
    z, core, role, owner = here.z, here.c, here.role, here.owner
    here.meet()
    copies = Copies(send_sem, recv_sem)

    def span(index, count):
        return pl.ds(pl.multiple_of(index * count, count), count)

    ff_cols, out_rows, piece = w1_ref.shape[1], wo_ref.shape[0] // 8, d_model // 8
    hidden = w2_ref.shape[0] // 8

    def block_qkv(zz, e):
        return full_qkv.at[span(e, piece), span(zz, 3 * head_cols)]

    units = {
        'o': lambda zz, e: full_o.at[zz, span(e, out_rows), :],
        '1': lambda zz, e: full_1.at[span(e, piece), span(zz, ff_cols)],
        '2': lambda zz, e: full_2.at[zz, span(e, hidden), :],
        'qkv': block_qkv,
    }

    def own_parts(name, e):
        if name == 'o':
            return [(wo_ref.at[span(e, out_rows), :], units[name](z, e))]
        if name == '1':
            return [(w1_ref.at[span(e, piece), :], units[name](z, e))]
        if name == '2':
            return [(w2_ref.at[span(e, hidden), :], units[name](z, e))]
        return [(ref.at[span(e, piece), :],
                 full_qkv.at[span(e, piece), pl.ds(pl.multiple_of((z * 3 + t) * head_cols, head_cols), head_cols)])
                for t, ref in enumerate((wq_ref, wk_ref, wv_ref))]

    mine = here.piece(here.y, here.x)
    by_a = here.piece(here.ya, here.xa)
    by_b = here.piece(here.yb, here.xb)
    by_ab = here.piece(1 - here.y, 1 - here.x)
    to_a, to_b = here.device(y=here.ya, x=here.xa), here.device(y=here.yb, x=here.xb)
    partner = here.device(c=1 - core)
    stage_z, stage_a, stage_b1, stage_b2, stage_c = {}, {}, {}, {}, {}
    names = ('o', '1', '2', 'qkv')

    for name in names:
        stage_z[name] = {k: [copies.start(src, dst, here.device(z=here.z_by[k])) for src, dst in own_parts(name, mine)]
                         for k in (1, 2, 3)}

    def forward_z(name):
        stage_a[name], stage_b1[name] = [], []
        for k in (1, 2, 3):
            for copy in stage_z[name][k]:
                copy.wait_recv()
            block = units[name](here.z_by[k], mine)
            stage_a[name].append(copies.start(block, block, to_a))
            stage_b1[name].append(copies.start(block, block, to_b))

    def forward_a(name):
        stage_b2[name] = []
        for k in (1, 2, 3):
            stage_a[name][k - 1].wait_recv()
            block = units[name](here.z_by[k], by_a)
            stage_b2[name].append(copies.start(block, block, to_b))

    def forward_b(name):
        stage_c[name] = []
        for k in (1, 2, 3):
            stage_b1[name][k - 1].wait_recv()
            stage_b2[name][k - 1].wait_recv()
            for e in (mine, by_a, by_b, by_ab):
                block = units[name](here.z_by[k], e)
                stage_c[name].append(copies.start(block, block, partner))

    locals_ = []

    def copy_local(src, dst):
        copy = pltpu.make_async_copy(src, dst, local_sem.at[len(locals_)])
        locals_.append(copy)
        copy.start()

    copy_local(w1_ref, full_1.at[:, span(z, ff_cols)])
    copy_local(w2_ref, full_2.at[z])
    copy_local(wo_ref, full_o.at[z])
    for t, ref in enumerate((wq_ref, wk_ref, wv_ref)):
        copy_local(ref, full_qkv.at[:, pl.ds(pl.multiple_of((z * 3 + t) * head_cols, head_cols), head_cols)])
    other_role = z % 2 * 2 + 1 - core
    give_x = pltpu.make_async_remote_copy(
        src_ref=x_ref, dst_ref=xs_ref, send_sem=one_send.at[0], recv_sem=one_recv.at[0], device_id=partner, device_id_type=MESH)
    give_cot = pltpu.make_async_remote_copy(
        src_ref=cot_ref.at[span(other_role, blk), :], dst_ref=cot_loc_ref, send_sem=one_send.at[1], recv_sem=one_recv.at[1],
        device_id=partner, device_id_type=MESH)
    keep_x = pltpu.make_async_copy(x_ref, xs_ref, local_sem.at[6])
    take_cot = pltpu.make_async_copy(cot_ref.at[span(role, blk), :], cot_s, local_sem.at[7])
    keep_cot = pltpu.make_async_copy(cot_s, cot_loc_ref, local_sem.at[8])

    @pl.when(owner)
    def _():
        give_x.start()
        give_cot.start()
        keep_x.start()
        take_cot.start()

    def project(i, _):
        rows = span(i, blk)
        values = x_ref[rows, :].astype(F32) + emb_ref[...]
        unit = (values * lax.rsqrt(jnp.mean(values * values, axis=-1, keepdims=True) + EPS_NORM)).astype(BF16)
        for t, ref in enumerate((wq_ref, wk_ref, wv_ref)):
            qkv_s[rows, t * head_cols:(t + 1) * head_cols] = dot_nn(unit, ref[...]).astype(BF16)
        return 0

    lax.fori_loop(0, 4, project, 0)

    def context_copy(j, i):
        src = c_buf.at[j, span(i, blk), :]
        dst = c1_ref.at[:, pl.ds(pl.multiple_of((z * 2 + j) * PAIR, PAIR), PAIR)]
        target_z, target_c = 2 * core + i // 2, i % 2
        remote = pltpu.make_async_remote_copy(
            src_ref=src, dst_ref=dst, send_sem=c_send.at[j * 4 + i], recv_sem=c_recv.at[j * 4 + z],
            device_id=here.device(z=target_z, c=target_c), device_id_type=MESH)
        local = pltpu.make_async_copy(src, dst, c_recv.at[j * 4 + z])
        return remote, local, jnp.logical_and(target_z == z, target_c == core)

    def send_context(j, i):
        remote, local, to_self = context_copy(j, i)
        pl.when(to_self)(local.start)
        pl.when(jnp.logical_not(to_self))(remote.start)

    moves = {(0, 1): [(forward_z, 'o')], (0, 2): [(forward_a, 'o')], (0, 3): [(forward_b, 'o')],
             (1, 2): [(forward_z, '1')], (1, 3): [(forward_a, '1')]}
    for j in range(2):
        vt_s[...] = qkv_s[:, (4 + j) * PAIR:(5 + j) * PAIR].T
        k_view = qkv_s.at[:, (2 + j) * PAIR:(3 + j) * PAIR]
        for i in range(4):
            if i or j:
                send_context(j if i else 0, i - 1 if i else 3)
            for step, name in moves.get((j, i), ()):
                step(name)
            rows = slice(i * blk, (i + 1) * blk)
            outs, sums = attend_rows(qkv_s[rows, j * PAIR:(j + 1) * PAIR], k_view, vt_s, (e_a, e_b))
            c_buf[j, rows, :] = jnp.concatenate(outs, axis=0).T.astype(BF16)
            for head in range(2):
                lse_s[2 * j + head:2 * j + head + 1, rows] = sums[head]

    @pl.when(owner)
    def _():
        take_cot.wait()
        keep_cot.start()

    forward_z('2')
    send_context(1, 3)
    give_lse = pltpu.make_async_remote_copy(
        src_ref=lse_s, dst_ref=lse_ref, send_sem=one_send.at[2], recv_sem=one_recv.at[2],
        device_id=here.device(z=2 * core + z // 2, c=z % 2), device_id_type=MESH)
    keep_lse = pltpu.make_async_copy(lse_s, lse_ref, local_sem.at[9])
    lse_stays = jnp.logical_and(2 * core + z // 2 == z, z % 2 == core)
    pl.when(lse_stays)(keep_lse.start)
    pl.when(jnp.logical_not(lse_stays))(give_lse.start)
    forward_b('1')
    forward_a('2')
    forward_z('qkv')
    forward_b('2')
    forward_a('qkv')
    forward_b('qkv')

    for j in range(2):
        for zz in range(4):
            pltpu.make_async_copy(c_buf.at[j, :blk, :], c1_ref.at[:, :PAIR], c_recv.at[j * 4 + zz]).wait()
        for i in range(4):
            remote, _, to_self = context_copy(j, i)
            pl.when(jnp.logical_not(to_self))(remote.wait_send)
    pl.when(lse_stays)(keep_lse.wait)

    @pl.when(jnp.logical_not(lse_stays))
    def _():
        give_lse.wait_send()
        give_lse.wait_recv()

    @pl.when(owner)
    def _():
        give_x.wait_send()
        give_cot.wait_send()
        keep_x.wait()
        keep_cot.wait()

    @pl.when(jnp.logical_not(owner))
    def _():
        give_x.wait_recv()
        give_cot.wait_recv()

    for copy in locals_:
        copy.wait()
    for name in names:
        for copy in stage_c[name]:
            copy.wait_recv()
    for copy in copies.sent:
        copy.wait_send()


def first_call(x, cot, emb, w_q, w_k, w_v, w_o, w_1, w_2):
    seq, d_model = x.shape
    head_cols, ff_cols, blk = w_q.shape[1], w_1.shape[1], seq // 4
    anywhere = pl.BlockSpec(memory_space=pl.ANY)
    in_vmem = pl.BlockSpec(memory_space=pltpu.VMEM)
    copies = 18 + 12 + 24 + 48
    return pl.pallas_call(
        first_kernel,
        in_specs=[in_vmem, anywhere] + [in_vmem] * 7,
        out_specs=[anywhere] * 8,
        out_shape=[
            jax.ShapeDtypeStruct((blk, d_model), BF16),
            jax.ShapeDtypeStruct((4, seq), F32),
            jax.ShapeDtypeStruct((seq, d_model), BF16),
            jax.ShapeDtypeStruct((blk, d_model), BF16),
            jax.ShapeDtypeStruct((4, *w_o.shape), BF16),
            jax.ShapeDtypeStruct((d_model, 4 * ff_cols), BF16),
            jax.ShapeDtypeStruct((4, *w_2.shape), BF16),
            jax.ShapeDtypeStruct((d_model, 12 * head_cols), BF16),
        ],
        scratch_shapes=[
            pltpu.VMEM((seq, 3 * head_cols), BF16),
            pltpu.VMEM((PAIR, seq), BF16),
            pltpu.VMEM((seq, blk), F32),
            pltpu.VMEM((seq, blk), F32),
            pltpu.VMEM((2, seq, PAIR), BF16),
            pltpu.VMEM((4, seq), F32),
            pltpu.VMEM((blk, d_model), BF16),
            pltpu.SemaphoreType.DMA((10,)),
            pltpu.SemaphoreType.DMA((copies,)),
            pltpu.SemaphoreType.DMA((copies,)),
            pltpu.SemaphoreType.DMA((8,)),
            pltpu.SemaphoreType.DMA((8,)),
            pltpu.SemaphoreType.DMA((3,)),
            pltpu.SemaphoreType.DMA((3,)),
        ],
        compiler_params=pltpu.CompilerParams(vmem_limit_bytes=60 << 20, collective_id=0, has_side_effects=True),
        cost_estimate=pl.CostEstimate(
            flops=64 * seq * seq * PAIR, bytes_accessed=64 * seq * d_model, transcendentals=seq * seq * 4),
        name="first",
    )(x, cot, emb, w_q, w_k, w_v, w_o, w_1, w_2)


def grad_kernel(by_left, _, *refs):
    lefts, rights, (away_ref, mid_ref, keep_ref, left_t, right_s) = refs[:16], refs[16:20], refs[20:]
    count, piece = lefts[0].shape
    step = pl.program_id(0)

    @pl.when(step == 0 if not by_left else step >= 0)
    def _():
        for i in range(16):
            left_t[i % 4 * piece:(i % 4 + 1) * piece, i // 4 * count:(i // 4 + 1) * count] = lefts[i][...].T

    @pl.when(step == 0 if by_left else step >= 0)
    def _():
        for i in range(4):
            right_s[i * count:(i + 1) * count, :] = rights[i][...]

    total = dot_nn(left_t[...], right_s[...])
    away_ref[0] = total[:2 * piece]
    mid_ref[0] = total[2 * piece:3 * piece]
    keep_ref[0] = total[3 * piece:]


def grad_products(order, lefts, rights, by_left=False):
    count = rights[0].shape[0]
    tile = rights[0].shape[1] // (1 if by_left else 4)
    piece = lefts[0].shape[1] // (32 if by_left else 8)
    if by_left:
        left_spec = lambda n: pl.BlockSpec((count, piece), lambda i, order: (0, i * 8 + order[n]))
        right_spec = pl.BlockSpec((count, tile), lambda i, order: (0, 0))
    else:
        left_spec = lambda n: pl.BlockSpec((count, piece), lambda i, order: (0, order[n]))
        right_spec = pl.BlockSpec((count, tile), lambda i, order: (0, i))
    return pl.pallas_call(
        functools.partial(grad_kernel, by_left),
        grid_spec=pltpu.PrefetchScalarGridSpec(
            num_scalar_prefetch=1,
            grid=(4,),
            in_specs=[left_spec(n) for _ in range(4) for n in range(4)] + [right_spec] * 4,
            out_specs=[pl.BlockSpec((1, n * piece, tile), lambda i, order: (i, 0, 0)) for n in (2, 1, 1)],
            scratch_shapes=[pltpu.VMEM((4 * piece, 4 * count), BF16), pltpu.VMEM((4 * count, tile), BF16)],
        ),
        out_shape=[jax.ShapeDtypeStruct((4, n * piece, tile), F32) for n in (2, 1, 1)],
        compiler_params=pltpu.CompilerParams(vmem_limit_bytes=60 << 20),
        cost_estimate=pl.CostEstimate(
            flops=128 * count * piece * tile, bytes_accessed=8 * count * (4 * piece + 4 * tile) + 64 * piece * tile,
            transcendentals=0),
        interpret=INTERPRET,
        name="grad",
    )(order, *[left for left in lefts for _ in range(4)], *rights)


def backward_rows(q, d_out, lse, k_ref, v_ref, k_t, p_cat, ds_cat, dk_acc, dv_acc):
    block = q.shape[0]
    lane = lax.broadcasted_iota(jnp.int32, q.shape, 1)
    q_heads, do_heads, dqs = [], [], []
    for head in range(2):
        mine = lane // HEAD_DIM == head
        q_head = jnp.where(mine, q, jnp.zeros_like(q))
        do_head = jnp.where(mine, d_out, jnp.zeros_like(d_out))
        scores = dot_nt(k_ref[...], q_head)
        probs = jnp.exp2(scores * EXP2_SCALE - lse[head:head + 1, :])
        d_probs = dot_nt(v_ref[...], do_head).astype(BF16).astype(F32)
        inner = jnp.sum(probs * d_probs, axis=0, keepdims=True)
        cols = slice(head * block, (head + 1) * block)
        p_cat[:, cols] = probs.astype(BF16)
        ds_cat[:, cols] = (probs * (d_probs - inner)).astype(BF16)
        dqs.append(dot_nn(k_t[head * HEAD_DIM:(head + 1) * HEAD_DIM, :], ds_cat[:, cols]))
        q_heads.append(q_head)
        do_heads.append(do_head)
    dv_acc[...] += dot_nn(p_cat[...], jnp.concatenate(do_heads, axis=0))
    dk_acc[...] += dot_nn(ds_cat[...], jnp.concatenate(q_heads, axis=0))
    return (jnp.concatenate(dqs, axis=0).T * SCALE).astype(BF16)


def last_kernel(qkv_ref, dc_ref, lse_ref, dmid_ref, x_ref, emb_ref, wqkv_ref, u_ref, gqkv2_ref,
                r2_ref, mid2_ref, keep2_ref, *refs):
    lefts = {'1': refs[:4], 'o': refs[8:12]}
    rights = {'1': refs[4:8], 'o': refs[12:16]}
    (dx_ref, g1_ref, g2_ref, go_ref, gq_ref, gk_ref, gv_ref, away1_ref, mid1_ref, keep1_ref, awayo_ref, mido_ref, keepo_ref,
     dch, k_t, dk_acc, dv_acc, p_cat, ds_cat, d_heads, d_qkv, buf, buf_o, second, second_o, tmp, tmp_o,
     third, third_o, sum_1, sum_2, sum_o, qa, qb, q1, q2, q3, q4, d_1, w_s, u_s, g_s,
     left_t, stage,
     local_sem, load_sem, send_sem, recv_sem, dc_send, dc_recv, dq_send, dq_recv, z_send, z_recv, x_send, x_recv,
     p_send, p_recv) = refs[16:]
    seq = qkv_ref.shape[0]
    blk = seq // 4
    head_cols = 2 * PAIR
    here = Place()
    z, core, role, owner = here.z, here.c, here.role, here.owner
    here.meet()
    copies = Copies(send_sem, recv_sem)
    waits = []

    def span(index, count):
        return pl.ds(pl.multiple_of(index * count, count), count)

    def load(src, dst, n):
        copy = pltpu.make_async_copy(src, dst, load_sem.at[n])
        copy.start()
        return copy

    no = jnp.logical_not
    to_a, to_b = here.device(y=here.ya, x=here.xa), here.device(y=here.yb, x=here.xb)
    partner = here.device(c=1 - core)
    member = [here.device(z=z // 2 * 2 + i // 2, c=i % 2) for i in range(4)]
    piece = tmp.shape[1]

    def dc_copy(i):
        return pltpu.make_async_remote_copy(
            src_ref=dc_ref.at[:, i * head_cols:(i + 1) * head_cols], dst_ref=dch.at[span(role, blk), :],
            send_sem=dc_send.at[i], recv_sem=dc_recv.at[role], device_id=member[i], device_id_type=MESH)

    for i in range(4):
        pl.when(role != i)(dc_copy(i).start)

        @pl.when(role == i)
        def _():
            dch[i * blk:(i + 1) * blk, :] = dc_ref[:, i * head_cols:(i + 1) * head_cols]

    half = rights['1'][0].shape[1] // 8
    firsts = {('1', q): [copies.make(away1_ref.at[q, :, h * half:(h + 1) * half], buf.at[4 + q, :, h * half:(h + 1) * half], to_a)
                         for h in range(2)] for q in range(4)}
    firsts['o'] = [copies.make(awayo_ref.at[2 * h:2 * h + 2], buf_o.at[2 * h:2 * h + 2], to_a) for h in range(2)]
    w2_loads = [load(r2_ref.at[q], buf.at[q], q) for q in range(4)]
    seconds = {(w, q): copies.make(buf.at[u + q, piece:, :], second.at[u + q], to_b) for w, u in (('2', 0), ('1', 4)) for q in range(4)}
    seconds['o'] = copies.make(buf_o.at[:, piece:, :], second_o, to_b)

    def add_mid(unit):
        if unit == 'o':
            mid, keep, t, n = mido_ref, keepo_ref, tmp_o, 4
            bottom, top = buf_o.at[:, piece:, :], buf_o.at[:, :piece, :]
        else:
            w, q = unit
            mid, keep = (mid2_ref.at[q], keep2_ref.at[q]) if w == '2' else (mid1_ref.at[q], keep1_ref.at[q])
            u = q if w == '2' else 4 + q
            t, n, bottom, top = tmp, 6, buf.at[u, piece:, :], buf.at[u, :piece, :]
        loads = [load(mid, t.at[0], n), load(keep, t.at[1], n + 1)]
        if unit == 'o' or unit[0] == '1':
            for copy in firsts[unit]:
                copy.wait_recv()
        else:
            w2_loads[unit[1]].wait()
        for copy in loads:
            copy.wait()
        bottom[...] += t[0]
        top[...] += t[1]
        seconds[unit].start()

    def z_copy(unit, q):
        if unit == 'o':
            src, dst, n = buf_o.at[q, :piece, :], third_o.at[z], 8
        else:
            w = 0 if unit == '2' else 1
            src, dst, n = buf.at[4 * w + q, :piece, :], third.at[w, z], 4 * w
        return pltpu.make_async_remote_copy(
            src_ref=src, dst_ref=dst, send_sem=z_send.at[n + q], recv_sem=z_recv.at[n + z],
            device_id=here.device(z=q), device_id_type=MESH)

    def finish(unit):
        seconds[unit].wait_recv()
        if unit == 'o':
            buf_o[:, :piece, :] += second_o[...]
            for q in range(4):
                pl.when(z != q)(z_copy('o', q).start)
        else:
            w, q = unit
            u = q if w == '2' else 4 + q
            buf[u, :piece, :] += second[u]
            pl.when(z != q)(z_copy(w, q).start)

    mine, by_a = here.piece(here.y, here.x), here.piece(here.ya, here.xa)
    by_b, by_ab = here.piece(here.yb, here.xb), here.piece(1 - here.y, 1 - here.x)
    gathers = {}

    def total(unit):
        out, got, n = {'2': (sum_2, third.at[0], 0), '1': (sum_1, third.at[1], 4), 'o': (sum_o, third_o, 8)}[unit]
        if unit == 'o':
            out[...] = buf_o[z, :piece, :]
        else:
            out[...] = buf[n + z, :piece, :]
        for zz in range(4):
            @pl.when(z != zz)
            def _():
                pltpu.make_async_copy(out, got.at[zz], z_recv.at[n + zz]).wait()
                out[...] += got[zz]

    def gather_start(name, src, out, n):
        rows = lambda e: out.at[span(e, piece), :]
        keep = pltpu.make_async_copy(src, rows(mine), local_sem.at[n])
        keep.start()
        waits.append(keep)
        gathers[name] = dict(src=src, rows=rows, a=copies.start(src, rows(mine), to_a), b1=copies.start(src, rows(mine), to_b))

    def gather_second(name):
        g = gathers[name]
        g['a'].wait_recv()
        g['b2'] = copies.start(g['rows'](by_a), g['rows'](by_a), to_b)

    def gather_core(name):
        g = gathers[name]
        g['c'] = [copies.start(g['src'], g['rows'](mine), partner), copies.start(g['rows'](by_a), g['rows'](by_a), partner)]
        g['b1'].wait_recv()
        g['c'].append(copies.start(g['rows'](by_b), g['rows'](by_b), partner))
        g['b2'].wait_recv()
        g['c'].append(copies.start(g['rows'](by_ab), g['rows'](by_ab), partner))

    def dq_copy(j, i, t):
        col = t * head_cols + j * PAIR
        return pltpu.make_async_remote_copy(
            src_ref=d_heads.at[i * blk:(i + 1) * blk, col:col + PAIR],
            dst_ref=d_qkv.at[:, pl.ds(pl.multiple_of(role * 3 * head_cols + col, PAIR), PAIR)],
            send_sem=dq_send.at[(j * 4 + i) * 3 + t], recv_sem=dq_recv.at[(j * 4 + role) * 3 + t],
            device_id=member[i], device_id_type=MESH)

    def send_d_heads(j):
        for i in range(4):
            @pl.when(role != i)
            def _():
                for t in range(3):
                    dq_copy(j, i, t).start()

    index = [here.ya * 2 + here.xa, (1 - here.y) * 2 + 1 - here.x, here.yb * 2 + here.xb, here.y * 2 + here.x]
    spaces = (p_cat, ds_cat)
    parts = [('1', n) for n in range(8)] + [('o', n) for n in range(2)]

    def load_lefts(name):
        for n in range(16):
            pltpu.make_async_copy(
                lefts[name][n // 4].at[:, span(index[n % 4] * 2 + core, piece)],
                d_heads.at[n // 4 * blk:(n // 4 + 1) * blk, n % 4 * piece:(n % 4 + 1) * piece], load_sem.at[14]).start()

    def load_rights(s):
        name, n = parts[s]
        for i in range(4):
            pltpu.make_async_copy(
                rights[name][i].at[:, n * half:(n + 1) * half], spaces[s % 2].at[i * blk:(i + 1) * blk, :],
                load_sem.at[15 + s % 2]).start()

    def stored(s):
        pltpu.make_async_copy(stage.at[s % 2], stage.at[s % 2], load_sem.at[17 + s % 2]).wait()

    def send_part(s):
        name, n = parts[s]
        if name == '1':
            firsts[('1', n // 2)][n % 2].start()
        else:
            firsts['o'][n].start()

    load_lefts('1')
    load_rights(0)
    for s in range(len(parts)):
        name, n = parts[s]
        if n == 0:
            every = d_heads.at[:, :4 * piece]
            pltpu.make_async_copy(every, every, load_sem.at[14]).wait()
            left_t[...] = every[...].T
            if name == '1':
                load_lefts('o')
        if s + 1 < len(parts):
            load_rights(s + 1)
        space = spaces[s % 2]
        pltpu.make_async_copy(space, space, load_sem.at[15 + s % 2]).wait()
        if s >= 1:
            stored(s - 1)
            send_part(s - 1)
        stage[s % 2] = dot_nn(left_t[...], space[...])
        if s < 8 and s % 2 == 1:
            add_mid(('2', s // 2))
        for row, ref in ((0, (away1_ref, awayo_ref)), (2 * piece, (mid1_ref, mido_ref)), (3 * piece, (keep1_ref, keepo_ref))):
            count = 2 * piece if row == 0 else piece
            rows = slice(row, row + count)
            if name == '1':
                pltpu.make_async_copy(stage.at[s % 2, rows, :], ref[0].at[n // 2, :, n % 2 * half:(n % 2 + 1) * half],
                                      load_sem.at[17 + s % 2]).start()
            else:
                for k in range(2):
                    pltpu.make_async_copy(stage.at[s % 2, rows, k * (half // 2):(k + 1) * (half // 2)], ref[1].at[2 * n + k],
                                          load_sem.at[17 + s % 2]).start()
    stored(len(parts) - 1)
    send_part(len(parts) - 1)

    for i in range(4):
        @pl.when(role != i)
        def _():
            pltpu.make_async_copy(dc_ref.at[:, :head_cols], dch.at[:blk, :], dc_recv.at[i]).wait()

    moves = {(0, 1): [(finish, ('2', 0))], (0, 4): [(finish, ('2', 1)), (add_mid, ('1', 0))], (0, 7): [(finish, ('2', 2))],
             (1, 0): [(send_d_heads, 0)], (1, 2): [(finish, ('2', 3)), (add_mid, ('1', 1))], (1, 4): [(finish, ('1', 0))],
             (1, 6): [(add_mid, ('1', 2))]}
    steps = seq // BWD_ROWS
    for j in range(2):
        k_view, v_view = qkv_ref.at[:, (2 + j) * PAIR:(3 + j) * PAIR], qkv_ref.at[:, (4 + j) * PAIR:(5 + j) * PAIR]
        k_t[...] = k_view[...].T
        dk_acc[...] = jnp.zeros_like(dk_acc)
        dv_acc[...] = jnp.zeros_like(dv_acc)

        def block(i, _):
            for n in range(8):
                if (j, n) in moves:
                    @pl.when(i == min(n, steps - 1))
                    def _():
                        for move, what in moves[(j, n)]:
                            move(what)
            rows = span(i, BWD_ROWS)
            cols = slice(j * PAIR, (j + 1) * PAIR)
            d_heads[rows, cols] = backward_rows(
                qkv_ref[rows, cols], dch[rows, cols], lse_ref[2 * j:2 * j + 2, rows], k_view, v_view,
                k_t, p_cat, ds_cat, dk_acc, dv_acc)
            return 0

        lax.fori_loop(0, steps, block, 0)
        d_heads[:, head_cols + j * PAIR:head_cols + (j + 1) * PAIR] = (dk_acc[...] * SCALE).astype(BF16)
        d_heads[:, 2 * head_cols + j * PAIR:2 * head_cols + (j + 1) * PAIR] = dv_acc[...].astype(BF16)

    quarter = 2 * piece

    def quarter_loads(n):
        return [load(u_ref.at[:, span(index[n], quarter)], u_s.at[n % 2], 8 + n % 2),
                load(gqkv2_ref.at[span(index[n], quarter), :], g_s.at[n % 2], 10 + n % 2)]

    pending = quarter_loads(0)
    for i in range(4):
        @pl.when(role == i)
        def _():
            d_qkv[:, i * 3 * head_cols:(i + 1) * 3 * head_cols] = d_heads[i * blk:(i + 1) * blk, :]
    send_d_heads(1)
    targets = [qa.at[0], qa.at[1], qb.at[0], qb.at[1]]
    first_q = None
    for n in range(4):
        ahead = quarter_loads(n + 1) if n < 3 else []
        for copy in pending:
            copy.wait()
        targets[n][...] = dot_tn(u_s[n % 2], d_heads[...]) + g_s[n % 2]
        pending = ahead
        if n == 2:
            first_q = copies.start(qa, q1, to_a)

    add_mid(('1', 3))
    w_rows = w_s.shape[1]
    chunks = wqkv_ref.shape[0] // w_rows
    w_load = load(wqkv_ref.at[:w_rows, :], w_s.at[0], 12)
    for j in range(2):
        for i in range(4):
            @pl.when(role != i)
            def _():
                for t in range(3):
                    pltpu.make_async_copy(d_heads.at[:blk, :PAIR], d_qkv.at[:, :PAIR], dq_recv.at[(j * 4 + i) * 3 + t]).wait()
    for n in range(chunks):
        ahead = load(wqkv_ref.at[(n + 1) * w_rows:(n + 2) * w_rows, :], w_s.at[(n + 1) % 2], 12 + (n + 1) % 2) if n + 1 < chunks else None
        w_load.wait()
        d_1[:, n * w_rows:(n + 1) * w_rows] = dot_nt(d_qkv[...], w_s[n % 2]).astype(BF16)
        w_load = ahead

    count = min(128, blk)
    for n in range(blk // count):
        rows = slice(n * count, (n + 1) * count)
        values = x_ref[rows, :].astype(F32) + emb_ref[...]
        up = d_1[rows, :].astype(F32)
        inverse = lax.rsqrt(jnp.mean(values * values, axis=-1, keepdims=True) + EPS_NORM)
        inner = jnp.mean(values * up, axis=-1, keepdims=True)
        d_1[rows, :] = (dmid_ref[rows, :].astype(F32) + inverse * up - values * (inverse * inverse * inverse * inner)).astype(BF16)

    own_seq = z // 2
    rows_dx = span(role, blk)

    def dx_copy(n, device):
        slot = [0, 1 + core, 3 + core][n]
        return pltpu.make_async_remote_copy(
            src_ref=d_1, dst_ref=dx_ref.at[rows_dx, :], send_sem=x_send.at[n], recv_sem=x_recv.at[slot],
            device_id=device, device_id_type=MESH)

    dx_side = dx_copy(0, partner)
    dx_next = dx_copy(1, here.device(z=here.z_by[1], c=own_seq))
    dx_cross = dx_copy(2, here.device(z=here.z_by[2], c=own_seq))
    dx_keep = pltpu.make_async_copy(d_1, dx_ref.at[rows_dx, :], local_sem.at[8])

    def dx_pass(cc):
        rows = span(z % 2 * 2 + cc, blk)
        return pltpu.make_async_remote_copy(
            src_ref=dx_ref.at[rows, :], dst_ref=dx_ref.at[rows, :], send_sem=x_send.at[3 + cc], recv_sem=x_recv.at[5 + cc],
            device_id=here.device(z=here.z_by[1]), device_id_type=MESH)

    add_mid('o')
    dx_cross.start()
    dx_next.start()
    pl.when(owner)(dx_keep.start)
    pl.when(no(owner))(dx_side.start)

    def dx_got(slot):
        pltpu.make_async_copy(d_1, dx_ref.at[:blk, :], x_recv.at[slot]).wait()

    first_q.wait_recv()
    qb[0] += q1[1]
    qb[1] += q1[0]
    second_q = copies.start(qb.at[0], q2, to_b)
    finish(('1', 1))
    total('2')
    finish(('1', 2))
    gather_start('2', sum_2, g2_ref, 0)
    finish(('1', 3))
    finish('o')
    second_q.wait_recv()
    qb[1] += q2[...]
    plane_stays = jnp.logical_and(2 * (z % 2) + core == z, z // 2 == core)
    plane_q = pltpu.make_async_remote_copy(
        src_ref=qb.at[1], dst_ref=q3, send_sem=p_send.at[0], recv_sem=p_recv.at[0],
        device_id=here.device(z=2 * (z % 2) + core, c=z // 2), device_id_type=MESH)

    @pl.when(plane_stays)
    def _():
        q3[...] = qb[1]

    pl.when(no(plane_stays))(plane_q.start)
    gather_second('2')

    @pl.when(no(owner))
    def _():
        for cc in range(2):
            dx_got(3 + cc)
            dx_pass(cc).start()

    total('1')
    total('o')
    gather_start('1', sum_1, g1_ref, 1)
    gather_start('o', sum_o, go_ref, 2)
    gather_core('2')
    pl.when(no(plane_stays))(plane_q.wait_recv)
    give_q = copies.start(q3.at[span(1 - core, piece), :], q4.at[0], partner)
    gather_second('1')
    gather_second('o')
    give_q.wait_recv()
    q4[1] = q4[0] + q3[span(core, piece), :]
    for t, (name, out) in enumerate((('q', gq_ref), ('k', gk_ref), ('v', gv_ref))):
        gather_start(name, q4.at[1, :, t * head_cols:(t + 1) * head_cols], out, 3 + t)
    gather_core('1')
    gather_core('o')
    for name in 'qkv':
        gather_second(name)
    for name in 'qkv':
        gather_core(name)

    @pl.when(owner)
    def _():
        for slot in (0, 1, 2):
            dx_got(slot)
        dx_keep.wait()

    @pl.when(no(owner))
    def _():
        dx_side.wait_send()
        for cc in range(2):
            dx_got(5 + cc)
            dx_pass(cc).wait_send()

    for g in gathers.values():
        for copy in g['c']:
            copy.wait_recv()
    for copy in waits:
        copy.wait()
    for copy in copies.sent:
        copy.wait_send()
    dx_cross.wait_send()
    dx_next.wait_send()
    pl.when(no(plane_stays))(plane_q.wait_send)
    for i in range(4):
        @pl.when(role != i)
        def _():
            dc_copy(i).wait_send()
            for j in range(2):
                for t in range(3):
                    dq_copy(j, i, t).wait_send()

        for unit in '21o':
            pl.when(z != i)(z_copy(unit, i).wait_send)


def last_call(qkv, d_c, lse, d_mid, x, emb, w_qkv, u_seq, g_qkv, w2_parts, w1_sides, wo_sides):
    seq, d_model = u_seq.shape
    blk, piece = seq // 4, d_model // 8
    n1, no = w1_sides[4].shape[1] // 4, wo_sides[4].shape[1] // 4
    assert n1 == 2 * 2 * BWD_ROWS and no * 2 == 2 * BWD_ROWS
    assert w2_parts[0].shape[1:] == (2 * piece, n1)
    heads3 = qkv.shape[1]
    anywhere = pl.BlockSpec(memory_space=pl.ANY)
    in_vmem = pl.BlockSpec(memory_space=pltpu.VMEM)
    copies = 10 + 9 + 6 * 7 + 3
    dma = pltpu.SemaphoreType.DMA
    w_rows = min(128, d_model)
    return pl.pallas_call(
        last_kernel,
        in_specs=[in_vmem] * 6 + [anywhere] * 22,
        out_specs=[anywhere] * 13,
        out_shape=[
            jax.ShapeDtypeStruct((seq, d_model), BF16),
            jax.ShapeDtypeStruct((d_model, n1), F32),
            jax.ShapeDtypeStruct((8 * piece, n1), F32),
            jax.ShapeDtypeStruct((d_model, no), F32),
        ] + [jax.ShapeDtypeStruct((d_model, heads3 // 3), F32)] * 3
        + [jax.ShapeDtypeStruct((4, k * piece, n), F32) for n in (n1, no) for k in (2, 1, 1)],
        scratch_shapes=[
            pltpu.VMEM((seq, heads3 // 3), BF16),
            pltpu.VMEM((PAIR, seq), BF16),
            pltpu.VMEM((seq, PAIR), F32),
            pltpu.VMEM((seq, PAIR), F32),
            pltpu.VMEM((seq, 2 * BWD_ROWS), BF16),
            pltpu.VMEM((seq, 2 * BWD_ROWS), BF16),
            pltpu.VMEM((seq, heads3), BF16),
            pltpu.VMEM((blk, 4 * heads3), BF16),
            pltpu.VMEM((8, 2 * piece, n1), F32),
            pltpu.VMEM((4, 2 * piece, no), F32),
            pltpu.VMEM((8, piece, n1), F32),
            pltpu.VMEM((4, piece, no), F32),
            pltpu.VMEM((2, piece, n1), F32),
            pltpu.VMEM((2, 4, piece, no), F32),
            pltpu.VMEM((2, 4, piece, n1), F32),
            pltpu.VMEM((4, piece, no), F32),
            pltpu.VMEM((piece, n1), F32),
            pltpu.VMEM((piece, n1), F32),
            pltpu.VMEM((piece, no), F32),
            pltpu.VMEM((2, 2 * piece, heads3), F32),
            pltpu.VMEM((2, 2 * piece, heads3), F32),
            pltpu.VMEM((2, 2 * piece, heads3), F32),
            pltpu.VMEM((2 * piece, heads3), F32),
            pltpu.VMEM((2 * piece, heads3), F32),
            pltpu.VMEM((2, piece, heads3), F32),
            pltpu.VMEM((blk, d_model), BF16),
            pltpu.VMEM((2, w_rows, 4 * heads3), BF16),
            pltpu.VMEM((2, seq, 2 * piece), BF16),
            pltpu.VMEM((2, 2 * piece, heads3), F32),
            pltpu.VMEM((4 * piece, seq), BF16),
            pltpu.VMEM((2, 4 * piece, 2 * BWD_ROWS), F32),
            dma((9,)), dma((19,)), dma((copies,)), dma((copies,)),
            dma((4,)), dma((4,)), dma((24,)), dma((24,)), dma((12,)), dma((12,)), dma((5,)), dma((7,)), dma((1,)), dma((1,)),
        ],
        compiler_params=pltpu.CompilerParams(vmem_limit_bytes=63 << 20, collective_id=1, has_side_effects=True),
        cost_estimate=pl.CostEstimate(
            flops=160 * seq * seq * PAIR, bytes_accessed=128 * seq * d_model, transcendentals=seq * seq * 4),
        name="last",
    )(qkv, d_c, lse, d_mid, x, emb, w_qkv, u_seq, g_qkv, *w2_parts, *w1_sides, *wo_sides)[:7]


def lin(z, y, x, c):
    return z * 8 + y * 4 + x * 2 + c


def send(value, to):
    pairs = []
    for z in range(4):
        for y in range(2):
            for x in range(2):
                for c in range(2):
                    dst = to(z, y, x, c)
                    if dst is not None:
                        pairs.append((lin(z, y, x, c), lin(*dst)))
    return lax.ppermute(value, AXES, pairs)


def role_of(z, c):
    return (z % 2) * 2 + c


def in_group(k):
    def to(z, y, x, c):
        role = role_of(z, c) ^ k
        return (z // 2 * 2 + role // 2, y, x, role % 2)

    return to


def other_core(z, y, x, c):
    return (z, y, x, 1 - c)


def swap_first(z, y, x, c):
    return (z, y, 1 - x, c) if c == 0 else (z, 1 - y, x, c)


def unscramble(parts, role):
    odd, high = role % 2 == 1, role // 2 == 1
    a = [jnp.where(odd, parts[i ^ 1], parts[i]) for i in range(4)]
    return [jnp.where(high, a[i ^ 2], a[i]) for i in range(4)]


def rows_of(value, index, count):
    return lax.dynamic_slice_in_dim(value, index * count, count, axis=0)


def solution(mesh):
    spec_col = P(None, 'model')
    spec_row = P('model', None)
    spec_act = P('data', None, None)
    spec_rep = P(None, None)

    def device_step(x_in, cot_out, step_emb, w_q, w_k, w_v, w_o, w_1, w_2):
        seq, d_model = x_in.shape[1:]
        head_cols = w_q.shape[1]
        blk = seq // 4
        z = lax.axis_index('model')
        d = lax.axis_index('data')
        y, x, core = d // 4, d // 2 % 2, d % 2
        role = z % 2 * 2 + core
        owner = core == z // 2
        emb = step_emb.astype(F32)

        c_1, lse_1, x_seq, cot, wo, w1, w2, w_qkv = first_call(
            x_in[0], cot_out[0], emb[:1], w_q, w_k, w_v, w_o, w_1, w_2)
        wo, w2 = wo.reshape(-1, d_model), w2.reshape(-1, d_model)
        w_qkv_role = lax.dynamic_slice_in_dim(w_qkv, role * 3 * head_cols, 3 * head_cols, axis=1)
        x_1 = rows_of(x_seq, role, blk)

        def exchange(parts):
            swapped = unscramble(parts, role)
            got = [swapped[0]] + [send(swapped[k], in_group(k)) for k in (1, 2, 3)]
            return unscramble(got, role)

        def mlp_forward(x_f, context):
            h = (x_f + dot_nn(context, wo)).astype(BF16)
            m = rms_norm(h.astype(F32)).astype(BF16)
            up = dot_nn(m, w1).astype(BF16)
            act = jax.nn.gelu(up.astype(F32)).astype(BF16)
            return h, m, up, act

        def interleave(pairs):
            return jnp.concatenate([pairs[j][i] for i in range(4) for j in range(2)], axis=1)

        s_1 = x_1.astype(F32) + emb[0]
        h_1, m_1, up_1, act_1 = mlp_forward(s_1, c_1)
        x_2 = (h_1.astype(F32) + dot_nn(act_1, w2)).astype(BF16)

        side = send(x_2, other_core)
        over = send(x_2, in_group(2))
        x_2_seq = jnp.concatenate(unscramble([x_2, side, over, send(over, other_core)], role), axis=0)
        u_2_seq = rms_norm(x_2_seq.astype(F32) + emb[1]).astype(BF16)
        qkv_2 = dot_nn(u_2_seq, w_qkv_role).astype(BF16)
        got, lse_2 = [], []
        for j in range(2):
            c_heads, lse = attn_fwd(qkv_2, j)
            got.append(exchange([c_heads[i * blk:(i + 1) * blk] for i in range(4)]))
            lse_2.append(lse)
        c_2 = interleave(got)
        lse_2 = jnp.concatenate(lse_2, axis=0)
        s_2 = x_2.astype(F32) + emb[1]
        h_2, m_2, up_2, act_2 = mlp_forward(s_2, c_2)

        def mlp_backward(d_next, h, up):
            d_act = dot_nt(d_next, w2).astype(BF16)
            d_up = jax.vjp(jax.nn.gelu, up.astype(F32))[1](d_act.astype(F32))[0].astype(BF16)
            d_m = dot_nt(d_up, w1).astype(BF16)
            d_h = jax.vjp(rms_norm, h.astype(F32))[1](d_m.astype(F32))[0]
            return d_up, (d_next.astype(F32) + d_h).astype(BF16)

        d_up_2, d_mid_2 = mlp_backward(cot, h_2, up_2)
        d_c = dot_nt(d_mid_2, wo).astype(BF16)
        pairs, grads = [], []
        for j in range(2):
            heads = exchange([d_c[:, i * head_cols + j * PAIR:i * head_cols + (j + 1) * PAIR] for i in range(4)])
            d_heads = attn_bwd(qkv_2, jnp.concatenate(heads, axis=0), lse_2[2 * j:2 * j + 2], j)
            grads.append(dot_tn(u_2_seq, d_heads))
            pairs.append(exchange([d_heads[i * blk:(i + 1) * blk] for i in range(4)]))
        d_qkv = jnp.concatenate(
            [pairs[j][i][:, t * PAIR:(t + 1) * PAIR] for i in range(4) for t in range(3) for j in range(2)], axis=1)
        g_qkv_2 = jnp.concatenate([grads[j][:, t * PAIR:(t + 1) * PAIR] for t in range(3) for j in range(2)], axis=1)
        d_u = dot_nt(d_qkv, w_qkv).astype(BF16)
        d_s = jax.vjp(rms_norm, s_2)[1](d_u.astype(F32))[0]
        d_2 = (d_mid_2.astype(F32) + d_s).astype(BF16)

        u_1_seq = rms_norm(x_seq.astype(F32) + emb[0]).astype(BF16)
        qkv_1 = dot_nn(u_1_seq, w_qkv_role).astype(BF16)

        first, second = jnp.where(core == 0, x, y), jnp.where(core == 0, y, x)

        def at(i, j):
            return jnp.where(core == 0, j * 2 + i, i * 2 + j)

        order = [at(1 - first, second), at(1 - first, 1 - second), at(first, 1 - second), at(first, second)]
        column = jnp.stack(order) * 2 + core

        def both_cores(sides):
            lefts, rights = [], []
            for left, right in sides:
                lefts += [left, send(left, other_core)]
                rights += [right, send(right, other_core)]
            return lefts, rights

        lefts, rights = both_cores([(act_2, cot), (act_1, d_2)])
        away, mid, keep = grad_products(column, lefts, rights, True)
        d_2, away = lax.optimization_barrier((d_2, away))
        w2_parts = (send(away, swap_first), mid, keep)
        d_up_1, d_mid_1 = mlp_backward(d_2, h_1, up_1)
        w1_sides = sum(both_cores([(m_2, d_up_2), (m_1, d_up_1)]), [])
        wo_sides = sum(both_cores([(d_mid_2, c_2), (d_mid_1, c_1)]), [])
        d_c = dot_nt(d_mid_1, wo).astype(BF16)
        d_x, g_w1, g_w2, g_wo, g_q, g_k, g_v = last_call(
            qkv_1, d_c, lse_1, d_mid_1, x_1, emb[:1], w_qkv, u_1_seq, g_qkv_2, w2_parts, w1_sides, wo_sides)
        return g_q, g_k, g_v, g_wo.T, g_w1, g_w2, d_x[None]

    return jax.shard_map(device_step, mesh=mesh,
                         in_specs=(spec_act, spec_act, spec_rep, spec_col, spec_col, spec_col, spec_row, spec_col, spec_row),
                         out_specs=(spec_col, spec_col, spec_col, spec_row, spec_col, spec_row, spec_act),
                         check_vma=False)
```

```python
import functools
import math

import jax
import jax.numpy as jnp
from jax import lax
from jax.experimental import pallas as pl
from jax.experimental.pallas import tpu as pltpu
from jax.sharding import PartitionSpec as P


HEAD_DIM = 64
EPS_NORM = 1e-6
SCALE = HEAD_DIM ** -0.5
EXP2_SCALE = SCALE * math.log2(math.e)
PAIR = 2 * HEAD_DIM
BWD_ROWS = 256
KEYS = 256
INTERPRET = False
AXES = ('model', 'data')
BF16 = jnp.bfloat16
F32 = jnp.float32
MESH = pl.DeviceIdType.MESH


def rms_norm(values):
    return values * lax.rsqrt(jnp.mean(values * values, axis=-1, keepdims=True) + EPS_NORM)


def dot_nt(a, b):
    return lax.dot_general(a, b, (((1,), (1,)), ((), ())), preferred_element_type=F32)


def dot_nn(a, b):
    return lax.dot_general(a, b, (((1,), (0,)), ((), ())), preferred_element_type=F32)


def dot_tn(a, b):
    return lax.dot_general(a, b, (((0,), (0,)), ((), ())), preferred_element_type=F32)


def attend_rows(q, k_ref, v_t, e_refs):
    count = k_ref.shape[0] // KEYS
    lane = lax.broadcasted_iota(jnp.int32, q.shape, 1)
    q_heads = [jnp.where(lane // HEAD_DIM == head, q, jnp.zeros_like(q)) for head in range(2)]
    tops, run, total, outs, sums = [[], []], [None, None], [None, None], [], []
    for j in range(count):
        keys = slice(j * KEYS, (j + 1) * KEYS)
        for head in range(2):
            scores = dot_nt(k_ref[keys, :], q_heads[head])
            top = jnp.max(scores, axis=0, keepdims=True) * EXP2_SCALE
            if j:
                top = jnp.maximum(top, run[head])
            weights = jnp.exp2(scores * EXP2_SCALE - top)
            part = jnp.sum(weights, axis=0, keepdims=True)
            total[head] = total[head] * jnp.exp2(run[head] - top) + part if j else part
            run[head] = top
            tops[head].append(top)
            e_refs[head][keys, :] = weights
    for head in range(2):
        inverse = 1.0 / total[head]
        out = None
        for j in range(count):
            keys = slice(j * KEYS, (j + 1) * KEYS)
            factor = inverse * jnp.exp2(tops[head][j] - run[head])
            probs = (e_refs[head][keys, :] * factor).astype(BF16)
            part = dot_nn(v_t[head * HEAD_DIM:(head + 1) * HEAD_DIM, keys], probs)
            out = out + part if j else part
        sums.append(run[head] + jnp.log2(total[head]))
        outs.append(out)
    return outs, sums


class Place:
    def __init__(self):
        self.z = lax.axis_index('model')
        d = lax.axis_index('data')
        self.y, self.x, self.c = d // 4, d // 2 % 2, d % 2
        z = self.z
        self.z_by = {1: z + 1 - 2 * (z % 2), 2: (z + 2) % 4, 3: 3 - z}
        x, y, c = self.x, self.y, self.c
        self.xa, self.ya = x + (1 - c) * (1 - 2 * x), y + c * (1 - 2 * y)
        self.xb, self.yb = x + c * (1 - 2 * x), y + (1 - c) * (1 - 2 * y)
        self.role = z % 2 * 2 + c
        self.owner = c == z // 2

    def piece(self, y, x, c=None):
        return y * 4 + x * 2 + (self.c if c is None else c)

    def device(self, z=None, y=None, x=None, c=None):
        z, y, x, c = (own if given is None else given for given, own in zip((z, y, x, c), (self.z, self.y, self.x, self.c)))
        return {'model': z, 'data': y * 4 + x * 2 + c}

    def peers(self):
        column = [self.device(z=z, c=c) for z in (self.z, *self.z_by.values()) for c in (self.c, 1 - self.c)][1:]
        return column + [self.device(x=1 - self.x), self.device(y=1 - self.y)]

    def meet(self):
        barrier = pltpu.get_barrier_semaphore()
        peers = self.peers()
        for peer in peers:
            pl.semaphore_signal(barrier, inc=1, device_id=peer, device_id_type=MESH)
        pl.semaphore_wait(barrier, len(peers))


class Copies:
    def __init__(self, send_sem, recv_sem):
        self.send_sem, self.recv_sem, self.used, self.sent = send_sem, recv_sem, 0, []

    def make(self, src, dst, device):
        n, self.used = self.used, self.used + 1
        copy = pltpu.make_async_remote_copy(
            src_ref=src, dst_ref=dst, send_sem=self.send_sem.at[n], recv_sem=self.recv_sem.at[n],
            device_id=device, device_id_type=MESH)
        self.sent.append(copy)
        return copy

    def start(self, src, dst, device):
        copy = self.make(src, dst, device)
        copy.start()
        return copy


def first_kernel(x_ref, cot_ref, emb_ref, wq_ref, wk_ref, wv_ref, wo_ref, w1_ref, w2_ref,
                 c1_ref, lse_ref, xs_ref, cot_loc_ref, full_o, full_1, full_2, full_qkv,
                 qkv_s, vt_s, e_a, e_b, c_buf, lse_s, cot_s, local_sem, send_sem, recv_sem, c_send, c_recv, one_send, one_recv):
    seq, d_model = x_ref.shape
    blk = seq // 4
    head_cols = wq_ref.shape[1]
    here = Place()
    z, core, role, owner = here.z, here.c, here.role, here.owner
    here.meet()
    copies = Copies(send_sem, recv_sem)

    def span(index, count):
        return pl.ds(pl.multiple_of(index * count, count), count)

    ff_cols, out_rows, piece = w1_ref.shape[1], wo_ref.shape[0] // 8, d_model // 8
    hidden = w2_ref.shape[0] // 8

    def block_qkv(zz, e):
        return full_qkv.at[span(e, piece), span(zz, 3 * head_cols)]

    units = {
        'o': lambda zz, e: full_o.at[zz, span(e, out_rows), :],
        '1': lambda zz, e: full_1.at[span(e, piece), span(zz, ff_cols)],
        '2': lambda zz, e: full_2.at[zz, span(e, hidden), :],
        'qkv': block_qkv,
    }

    def own_parts(name, e):
        if name == 'o':
            return [(wo_ref.at[span(e, out_rows), :], units[name](z, e))]
        if name == '1':
            return [(w1_ref.at[span(e, piece), :], units[name](z, e))]
        if name == '2':
            return [(w2_ref.at[span(e, hidden), :], units[name](z, e))]
        return [(ref.at[span(e, piece), :],
                 full_qkv.at[span(e, piece), pl.ds(pl.multiple_of((z * 3 + t) * head_cols, head_cols), head_cols)])
                for t, ref in enumerate((wq_ref, wk_ref, wv_ref))]

    mine = here.piece(here.y, here.x)
    by_a = here.piece(here.ya, here.xa)
    by_b = here.piece(here.yb, here.xb)
    by_ab = here.piece(1 - here.y, 1 - here.x)
    to_a, to_b = here.device(y=here.ya, x=here.xa), here.device(y=here.yb, x=here.xb)
    partner = here.device(c=1 - core)
    stage_z, stage_a, stage_b1, stage_b2, stage_c = {}, {}, {}, {}, {}
    names = ('o', '1', '2', 'qkv')

    for name in names:
        stage_z[name] = {k: [copies.start(src, dst, here.device(z=here.z_by[k])) for src, dst in own_parts(name, mine)]
                         for k in (1, 2, 3)}

    def forward_z(name):
        stage_a[name], stage_b1[name] = [], []
        for k in (1, 2, 3):
            for copy in stage_z[name][k]:
                copy.wait_recv()
            block = units[name](here.z_by[k], mine)
            stage_a[name].append(copies.start(block, block, to_a))
            stage_b1[name].append(copies.start(block, block, to_b))

    def forward_a(name):
        stage_b2[name] = []
        for k in (1, 2, 3):
            stage_a[name][k - 1].wait_recv()
            block = units[name](here.z_by[k], by_a)
            stage_b2[name].append(copies.start(block, block, to_b))

    def forward_b(name):
        stage_c[name] = []
        for k in (1, 2, 3):
            stage_b1[name][k - 1].wait_recv()
            stage_b2[name][k - 1].wait_recv()
            for e in (mine, by_a, by_b, by_ab):
                block = units[name](here.z_by[k], e)
                stage_c[name].append(copies.start(block, block, partner))

    locals_ = []

    def copy_local(src, dst):
        copy = pltpu.make_async_copy(src, dst, local_sem.at[len(locals_)])
        locals_.append(copy)
        copy.start()

    copy_local(w1_ref, full_1.at[:, span(z, ff_cols)])
    copy_local(w2_ref, full_2.at[z])
    copy_local(wo_ref, full_o.at[z])
    for t, ref in enumerate((wq_ref, wk_ref, wv_ref)):
        copy_local(ref, full_qkv.at[:, pl.ds(pl.multiple_of((z * 3 + t) * head_cols, head_cols), head_cols)])
    other_role = z % 2 * 2 + 1 - core
    give_x = pltpu.make_async_remote_copy(
        src_ref=x_ref, dst_ref=xs_ref, send_sem=one_send.at[0], recv_sem=one_recv.at[0], device_id=partner, device_id_type=MESH)
    give_cot = pltpu.make_async_remote_copy(
        src_ref=cot_ref.at[span(other_role, blk), :], dst_ref=cot_loc_ref, send_sem=one_send.at[1], recv_sem=one_recv.at[1],
        device_id=partner, device_id_type=MESH)
    keep_x = pltpu.make_async_copy(x_ref, xs_ref, local_sem.at[6])
    take_cot = pltpu.make_async_copy(cot_ref.at[span(role, blk), :], cot_s, local_sem.at[7])
    keep_cot = pltpu.make_async_copy(cot_s, cot_loc_ref, local_sem.at[8])

    @pl.when(owner)
    def _():
        give_x.start()
        give_cot.start()
        keep_x.start()
        take_cot.start()

    def project(i, _):
        rows = span(i, blk)
        values = x_ref[rows, :].astype(F32) + emb_ref[...]
        unit = (values * lax.rsqrt(jnp.mean(values * values, axis=-1, keepdims=True) + EPS_NORM)).astype(BF16)
        for t, ref in enumerate((wq_ref, wk_ref, wv_ref)):
            qkv_s[rows, t * head_cols:(t + 1) * head_cols] = dot_nn(unit, ref[...]).astype(BF16)
        return 0

    lax.fori_loop(0, 4, project, 0)

    def context_copy(j, i):
        src = c_buf.at[j, span(i, blk), :]
        dst = c1_ref.at[:, pl.ds(pl.multiple_of((z * 2 + j) * PAIR, PAIR), PAIR)]
        target_z, target_c = 2 * core + i // 2, i % 2
        remote = pltpu.make_async_remote_copy(
            src_ref=src, dst_ref=dst, send_sem=c_send.at[j * 4 + i], recv_sem=c_recv.at[j * 4 + z],
            device_id=here.device(z=target_z, c=target_c), device_id_type=MESH)
        local = pltpu.make_async_copy(src, dst, c_recv.at[j * 4 + z])
        return remote, local, jnp.logical_and(target_z == z, target_c == core)

    def send_context(j, i):
        remote, local, to_self = context_copy(j, i)
        pl.when(to_self)(local.start)
        pl.when(jnp.logical_not(to_self))(remote.start)

    moves = {(0, 1): [(forward_z, 'o')], (0, 2): [(forward_a, 'o')], (0, 3): [(forward_b, 'o')],
             (1, 2): [(forward_z, '1')], (1, 3): [(forward_a, '1')]}
    for j in range(2):
        vt_s[...] = qkv_s[:, (4 + j) * PAIR:(5 + j) * PAIR].T
        k_view = qkv_s.at[:, (2 + j) * PAIR:(3 + j) * PAIR]
        for i in range(4):
            if i or j:
                send_context(j if i else 0, i - 1 if i else 3)
            for step, name in moves.get((j, i), ()):
                step(name)
            rows = slice(i * blk, (i + 1) * blk)
            outs, sums = attend_rows(qkv_s[rows, j * PAIR:(j + 1) * PAIR], k_view, vt_s, (e_a, e_b))
            c_buf[j, rows, :] = jnp.concatenate(outs, axis=0).T.astype(BF16)
            for head in range(2):
                lse_s[2 * j + head:2 * j + head + 1, rows] = sums[head]

    @pl.when(owner)
    def _():
        take_cot.wait()
        keep_cot.start()

    forward_z('2')
    send_context(1, 3)
    give_lse = pltpu.make_async_remote_copy(
        src_ref=lse_s, dst_ref=lse_ref, send_sem=one_send.at[2], recv_sem=one_recv.at[2],
        device_id=here.device(z=2 * core + z // 2, c=z % 2), device_id_type=MESH)
    keep_lse = pltpu.make_async_copy(lse_s, lse_ref, local_sem.at[9])
    lse_stays = jnp.logical_and(2 * core + z // 2 == z, z % 2 == core)
    pl.when(lse_stays)(keep_lse.start)
    pl.when(jnp.logical_not(lse_stays))(give_lse.start)
    forward_b('1')
    forward_a('2')
    forward_z('qkv')
    forward_b('2')
    forward_a('qkv')
    forward_b('qkv')

    for j in range(2):
        for zz in range(4):
            pltpu.make_async_copy(c_buf.at[j, :blk, :], c1_ref.at[:, :PAIR], c_recv.at[j * 4 + zz]).wait()
        for i in range(4):
            remote, _, to_self = context_copy(j, i)
            pl.when(jnp.logical_not(to_self))(remote.wait_send)
    pl.when(lse_stays)(keep_lse.wait)

    @pl.when(jnp.logical_not(lse_stays))
    def _():
        give_lse.wait_send()
        give_lse.wait_recv()

    @pl.when(owner)
    def _():
        give_x.wait_send()
        give_cot.wait_send()
        keep_x.wait()
        keep_cot.wait()

    @pl.when(jnp.logical_not(owner))
    def _():
        give_x.wait_recv()
        give_cot.wait_recv()

    for copy in locals_:
        copy.wait()
    for name in names:
        for copy in stage_c[name]:
            copy.wait_recv()
    for copy in copies.sent:
        copy.wait_send()


def first_call(x, cot, emb, w_q, w_k, w_v, w_o, w_1, w_2):
    seq, d_model = x.shape
    head_cols, ff_cols, blk = w_q.shape[1], w_1.shape[1], seq // 4
    anywhere = pl.BlockSpec(memory_space=pl.ANY)
    in_vmem = pl.BlockSpec(memory_space=pltpu.VMEM)
    copies = 18 + 12 + 24 + 48
    return pl.pallas_call(
        first_kernel,
        in_specs=[in_vmem, anywhere] + [in_vmem] * 7,
        out_specs=[anywhere] * 8,
        out_shape=[
            jax.ShapeDtypeStruct((blk, d_model), BF16),
            jax.ShapeDtypeStruct((4, seq), F32),
            jax.ShapeDtypeStruct((seq, d_model), BF16),
            jax.ShapeDtypeStruct((blk, d_model), BF16),
            jax.ShapeDtypeStruct((4, *w_o.shape), BF16),
            jax.ShapeDtypeStruct((d_model, 4 * ff_cols), BF16),
            jax.ShapeDtypeStruct((4, *w_2.shape), BF16),
            jax.ShapeDtypeStruct((d_model, 12 * head_cols), BF16),
        ],
        scratch_shapes=[
            pltpu.VMEM((seq, 3 * head_cols), BF16),
            pltpu.VMEM((PAIR, seq), BF16),
            pltpu.VMEM((seq, blk), F32),
            pltpu.VMEM((seq, blk), F32),
            pltpu.VMEM((2, seq, PAIR), BF16),
            pltpu.VMEM((4, seq), F32),
            pltpu.VMEM((blk, d_model), BF16),
            pltpu.SemaphoreType.DMA((10,)),
            pltpu.SemaphoreType.DMA((copies,)),
            pltpu.SemaphoreType.DMA((copies,)),
            pltpu.SemaphoreType.DMA((8,)),
            pltpu.SemaphoreType.DMA((8,)),
            pltpu.SemaphoreType.DMA((3,)),
            pltpu.SemaphoreType.DMA((3,)),
        ],
        compiler_params=pltpu.CompilerParams(vmem_limit_bytes=60 << 20, collective_id=0, has_side_effects=True),
        cost_estimate=pl.CostEstimate(
            flops=64 * seq * seq * PAIR, bytes_accessed=64 * seq * d_model, transcendentals=seq * seq * 4),
        name="first",
    )(x, cot, emb, w_q, w_k, w_v, w_o, w_1, w_2)


def unit_rows(values, emb):
    values = values.astype(F32) + emb
    return (values * lax.rsqrt(jnp.mean(values * values, axis=-1, keepdims=True) + EPS_NORM)).astype(BF16)


def forward_kernel(x_ref, emb_ref, xs1_ref, wqkv_ref,
                   c_ref, lse_ref, u2_ref, qkv2_ref, u1_ref, qkv1_ref,
                   w_s, blocks, u_s, qkv_s, x1_s, u1_s, qkv1_s, v_t, e_a, e_b, c_buf, lse_s,
                   local_sem, first_sem, out_sem, x_send, x_recv, c_send, c_recv):
    seq = xs1_ref.shape[0]
    blk = seq // 4
    head_cols = 2 * PAIR
    here = Place()
    z, core, role = here.z, here.c, here.role

    def span(index, count):
        return pl.ds(pl.multiple_of(index * count, count), count)

    w_load = pltpu.make_async_copy(wqkv_ref.at[:, span(role, 3 * head_cols)], w_s, local_sem.at[0])
    w_load.start()
    x1_load = [pltpu.make_async_copy(xs1_ref.at[i * blk:(i + 1) * blk, :], x1_s.at[i % 2], first_sem.at[i % 2]) for i in range(4)]
    x1_load[0].start()
    here.meet()
    partner, across = here.device(c=1 - core), here.device(z=here.z_by[1])
    role_side, role_over = z % 2 * 2 + 1 - core, (1 - z % 2) * 2 + core
    role_last = (1 - z % 2) * 2 + 1 - core

    def x_copy(n, src, slot, device):
        return pltpu.make_async_remote_copy(
            src_ref=src, dst_ref=blocks.at[slot], send_sem=x_send.at[n], recv_sem=x_recv.at[n],
            device_id=device, device_id_type=MESH)

    over, side = x_copy(0, x_ref, 0, across), x_copy(1, x_ref, 1, partner)
    last = x_copy(2, blocks.at[0], 2, partner)
    over.start()
    side.start()

    def project(src, at_role):
        rows = span(at_role, blk)
        unit = unit_rows(src, emb_ref[1:2, :])
        u_s[rows, :] = unit
        qkv_s[rows, :] = dot_nn(unit, w_s[...]).astype(BF16)

    w_load.wait()
    project(x_ref[...], role)
    side.wait_recv()
    project(blocks[1], role_side)

    stores = []
    for i in range(4):
        if i < 3:
            x1_load[i + 1].start()
        x1_load[i].wait()
        if i >= 2:
            for copy in stores[i - 2]:
                copy.wait()
        unit = unit_rows(x1_s[i % 2], emb_ref[0:1, :])
        u1_s[i % 2] = unit
        qkv1_s[i % 2] = dot_nn(unit, w_s[...]).astype(BF16)
        stores.append([pltpu.make_async_copy(u1_s.at[i % 2], u1_ref.at[i * blk:(i + 1) * blk, :], out_sem.at[i % 2]),
                       pltpu.make_async_copy(qkv1_s.at[i % 2], qkv1_ref.at[i * blk:(i + 1) * blk, :], out_sem.at[2 + i % 2])])
        for copy in stores[i]:
            copy.start()

    over.wait_recv()
    last.start()
    project(blocks[0], role_over)
    last.wait_recv()
    project(blocks[2], role_last)
    keep_u = pltpu.make_async_copy(u_s, u2_ref, local_sem.at[1])
    keep_qkv = pltpu.make_async_copy(qkv_s, qkv2_ref, local_sem.at[2])
    keep_u.start()
    keep_qkv.start()

    member = [here.device(z=z // 2 * 2 + i // 2, c=i % 2) for i in range(4)]

    def c_copy(j, i):
        src = c_buf.at[j, i * blk:(i + 1) * blk, :]
        dst = c_ref.at[:, pl.ds(pl.multiple_of((role * 2 + j) * PAIR, PAIR), PAIR)]
        remote = pltpu.make_async_remote_copy(
            src_ref=src, dst_ref=dst, send_sem=c_send.at[j * 4 + i], recv_sem=c_recv.at[j * 4 + role],
            device_id=member[i], device_id_type=MESH)
        return remote, pltpu.make_async_copy(src, dst, c_recv.at[j * 4 + role])

    def send_context(j, i):
        remote, local = c_copy(j, i)
        pl.when(role == i)(local.start)
        pl.when(role != i)(remote.start)

    for j in range(2):
        v_t[...] = qkv_s[:, (4 + j) * PAIR:(5 + j) * PAIR].T
        k_view = qkv_s.at[:, (2 + j) * PAIR:(3 + j) * PAIR]
        for i in range(4):
            if i or j:
                send_context(j if i else 0, i - 1 if i else 3)
            rows = slice(i * blk, (i + 1) * blk)
            outs, sums = attend_rows(qkv_s[rows, j * PAIR:(j + 1) * PAIR], k_view, v_t, (e_a, e_b))
            c_buf[j, rows, :] = jnp.concatenate(outs, axis=0).T.astype(BF16)
            for head in range(2):
                lse_s[2 * j + head:2 * j + head + 1, rows] = sums[head]
    lse_ref[...] = lse_s[...]
    send_context(1, 3)
    for j in range(2):
        for i in range(4):
            pltpu.make_async_copy(c_buf.at[j, :blk, :], c_ref.at[:, :PAIR], c_recv.at[j * 4 + i]).wait()
            pl.when(role != i)(c_copy(j, i)[0].wait_send)
    for copy in (over, side, last):
        copy.wait_send()
    for group in stores[2:]:
        for copy in group:
            copy.wait()
    keep_u.wait()
    keep_qkv.wait()


def forward_call(x, emb, xs_1, w_qkv):
    blk, d_model = x.shape
    seq, head_cols = 4 * blk, 2 * PAIR
    anywhere = pl.BlockSpec(memory_space=pl.ANY)
    in_vmem = pl.BlockSpec(memory_space=pltpu.VMEM)
    dma = pltpu.SemaphoreType.DMA
    return pl.pallas_call(
        forward_kernel,
        in_specs=[in_vmem, in_vmem, anywhere, anywhere],
        out_specs=[anywhere, in_vmem] + [anywhere] * 4,
        out_shape=[
            jax.ShapeDtypeStruct((blk, d_model), BF16),
            jax.ShapeDtypeStruct((4, seq), F32),
        ] + [jax.ShapeDtypeStruct((seq, n), BF16) for n in (d_model, 3 * head_cols)] * 2,
        scratch_shapes=[
            pltpu.VMEM((d_model, 3 * head_cols), BF16),
            pltpu.VMEM((3, blk, d_model), BF16),
            pltpu.VMEM((seq, d_model), BF16),
            pltpu.VMEM((seq, 3 * head_cols), BF16),
            pltpu.VMEM((2, blk, d_model), BF16),
            pltpu.VMEM((2, blk, d_model), BF16),
            pltpu.VMEM((2, blk, 3 * head_cols), BF16),
            pltpu.VMEM((PAIR, seq), BF16),
            pltpu.VMEM((seq, blk), F32),
            pltpu.VMEM((seq, blk), F32),
            pltpu.VMEM((2, seq, PAIR), BF16),
            pltpu.VMEM((4, seq), F32),
            dma((3,)), dma((2,)), dma((4,)), dma((3,)), dma((3,)), dma((8,)), dma((8,)),
        ],
        compiler_params=pltpu.CompilerParams(vmem_limit_bytes=60 << 20, collective_id=2, has_side_effects=True),
        cost_estimate=pl.CostEstimate(
            flops=64 * seq * seq * PAIR, bytes_accessed=32 * seq * d_model, transcendentals=seq * seq * 4),
        name="forward",
    )(x, emb, xs_1, w_qkv)


def through_norm(values, up, d_mid):
    inverse = lax.rsqrt(jnp.mean(values * values, axis=-1, keepdims=True) + EPS_NORM)
    inner = jnp.mean(values * up, axis=-1, keepdims=True)
    return (d_mid.astype(F32) + inverse * up - values * (inverse * inverse * inverse * inner)).astype(BF16)


def backward_kernel(qkv_ref, dc_ref, lse_ref, dmid_ref, x_ref, emb_ref, wqkv_ref, u_ref,
                    d_ref, other_ref, g_ref,
                    dch, k_t, dk_acc, dv_acc, p_cat, ds_cat, d_heads, d_qkv, d_u, w_s, u_s, g_s,
                    load_sem, out_sem, dc_send, dc_recv, dq_send, dq_recv, d_send, d_recv):
    seq = qkv_ref.shape[0]
    blk = seq // 4
    head_cols = 2 * PAIR
    here = Place()
    z, core, role = here.z, here.c, here.role
    here.meet()
    member = [here.device(z=z // 2 * 2 + i // 2, c=i % 2) for i in range(4)]

    def span(index, count):
        return pl.ds(pl.multiple_of(index * count, count), count)

    def load(src, dst, n):
        copy = pltpu.make_async_copy(src, dst, load_sem.at[n])
        copy.start()
        return copy

    def dc_copy(j, i):
        col = i * head_cols + j * PAIR
        return pltpu.make_async_remote_copy(
            src_ref=dc_ref.at[:, col:col + PAIR], dst_ref=dch.at[span(role, blk), j * PAIR:(j + 1) * PAIR],
            send_sem=dc_send.at[j * 4 + i], recv_sem=dc_recv.at[j * 4 + role], device_id=member[i], device_id_type=MESH)

    for j in range(2):
        for i in range(4):
            pl.when(role != i)(dc_copy(j, i).start)
    for i in range(4):
        @pl.when(role == i)
        def _():
            dch[i * blk:(i + 1) * blk, :] = dc_ref[:, i * head_cols:(i + 1) * head_cols]

    def dq_copy(j, i, t):
        col = t * head_cols + j * PAIR
        return pltpu.make_async_remote_copy(
            src_ref=d_heads.at[i * blk:(i + 1) * blk, col:col + PAIR],
            dst_ref=d_qkv.at[:, pl.ds(pl.multiple_of(role * 3 * head_cols + col, PAIR), PAIR)],
            send_sem=dq_send.at[(j * 4 + i) * 3 + t], recv_sem=dq_recv.at[(j * 4 + role) * 3 + t],
            device_id=member[i], device_id_type=MESH)

    def send_d_heads(j):
        for i in range(4):
            @pl.when(role != i)
            def _():
                for t in range(3):
                    dq_copy(j, i, t).start()

    steps = seq // BWD_ROWS
    for j in range(2):
        for i in range(4):
            @pl.when(role != i)
            def _():
                pltpu.make_async_copy(dc_ref.at[:, :PAIR], dch.at[:blk, :PAIR], dc_recv.at[j * 4 + i]).wait()
        k_view, v_view = qkv_ref.at[:, (2 + j) * PAIR:(3 + j) * PAIR], qkv_ref.at[:, (4 + j) * PAIR:(5 + j) * PAIR]
        k_t[...] = k_view[...].T
        dk_acc[...] = jnp.zeros_like(dk_acc)
        dv_acc[...] = jnp.zeros_like(dv_acc)

        def block(i, _):
            if j == 1:
                @pl.when(i == 1)
                def _():
                    send_d_heads(0)
            rows = span(i, BWD_ROWS)
            cols = slice(j * PAIR, (j + 1) * PAIR)
            d_heads[rows, cols] = backward_rows(
                qkv_ref[rows, cols], dch[rows, cols], lse_ref[2 * j:2 * j + 2, rows], k_view, v_view,
                k_t, p_cat, ds_cat, dk_acc, dv_acc)
            return 0

        lax.fori_loop(0, steps, block, 0)
        d_heads[:, head_cols + j * PAIR:head_cols + (j + 1) * PAIR] = (dk_acc[...] * SCALE).astype(BF16)
        d_heads[:, 2 * head_cols + j * PAIR:2 * head_cols + (j + 1) * PAIR] = dv_acc[...].astype(BF16)

    quarter = u_s.shape[2]
    pending = load(u_ref.at[:, :quarter], u_s.at[0], 0)
    for i in range(4):
        @pl.when(role == i)
        def _():
            d_qkv[:, i * 3 * head_cols:(i + 1) * 3 * head_cols] = d_heads[i * blk:(i + 1) * blk, :]
    send_d_heads(1)
    stores = []
    count = u_ref.shape[1] // quarter
    for n in range(count):
        ahead = load(u_ref.at[:, (n + 1) * quarter:(n + 2) * quarter], u_s.at[(n + 1) % 2], (n + 1) % 2) if n + 1 < count else None
        pending.wait()
        if n >= 2:
            stores[n - 2].wait()
        g_s[n % 2] = dot_tn(u_s[n % 2], d_heads[...])
        stores.append(pltpu.make_async_copy(g_s.at[n % 2], g_ref.at[n * quarter:(n + 1) * quarter, :], out_sem.at[n % 2]))
        stores[n].start()
        pending = ahead
    w_rows = w_s.shape[1]
    chunks = wqkv_ref.shape[0] // w_rows
    w_load = load(wqkv_ref.at[:w_rows, :], w_s.at[0], 2)
    for j in range(2):
        for i in range(4):
            @pl.when(role != i)
            def _():
                for t in range(3):
                    pltpu.make_async_copy(d_heads.at[:blk, :PAIR], d_qkv.at[:, :PAIR], dq_recv.at[(j * 4 + i) * 3 + t]).wait()
    for n in range(chunks):
        ahead = load(wqkv_ref.at[(n + 1) * w_rows:(n + 2) * w_rows, :], w_s.at[(n + 1) % 2], 2 + (n + 1) % 2) if n + 1 < chunks else None
        w_load.wait()
        d_u[:, n * w_rows:(n + 1) * w_rows] = dot_nt(d_qkv[...], w_s[n % 2]).astype(BF16)
        w_load = ahead
    rows_each = min(128, blk)
    for n in range(blk // rows_each):
        rows = slice(n * rows_each, (n + 1) * rows_each)
        d_u[rows, :] = through_norm(x_ref[rows, :].astype(F32) + emb_ref[...], d_u[rows, :].astype(F32), dmid_ref[rows, :])
    keep = pltpu.make_async_copy(d_u, d_ref, out_sem.at[2])
    keep.start()
    stores[count - 2].wait()
    stores[count - 1].wait()
    give = pltpu.make_async_remote_copy(
        src_ref=d_u, dst_ref=other_ref, send_sem=d_send.at[0], recv_sem=d_recv.at[0],
        device_id=here.device(c=1 - core), device_id_type=MESH)
    give.start()
    for i in range(4):
        @pl.when(role != i)
        def _():
            for j in range(2):
                dc_copy(j, i).wait_send()
                for t in range(3):
                    dq_copy(j, i, t).wait_send()
    keep.wait()
    give.wait()


def backward_call(qkv, d_c, lse, d_mid, x, emb, w_qkv, u_seq):
    seq, d_model = u_seq.shape
    blk, heads3 = seq // 4, qkv.shape[1]
    anywhere = pl.BlockSpec(memory_space=pl.ANY)
    in_vmem = pl.BlockSpec(memory_space=pltpu.VMEM)
    dma = pltpu.SemaphoreType.DMA
    quarter = d_model // 4
    return pl.pallas_call(
        backward_kernel,
        in_specs=[in_vmem] * 6 + [anywhere] * 2,
        out_specs=[anywhere] * 3,
        out_shape=[
            jax.ShapeDtypeStruct((blk, d_model), BF16),
            jax.ShapeDtypeStruct((blk, d_model), BF16),
            jax.ShapeDtypeStruct((d_model, heads3), F32),
        ],
        scratch_shapes=[
            pltpu.VMEM((seq, heads3 // 3), BF16),
            pltpu.VMEM((PAIR, seq), BF16),
            pltpu.VMEM((seq, PAIR), F32),
            pltpu.VMEM((seq, PAIR), F32),
            pltpu.VMEM((seq, 2 * BWD_ROWS), BF16),
            pltpu.VMEM((seq, 2 * BWD_ROWS), BF16),
            pltpu.VMEM((seq, heads3), BF16),
            pltpu.VMEM((blk, 4 * heads3), BF16),
            pltpu.VMEM((blk, d_model), BF16),
            pltpu.VMEM((2, quarter, 4 * heads3), BF16),
            pltpu.VMEM((2, seq, quarter), BF16),
            pltpu.VMEM((2, quarter, heads3), F32),
            dma((4,)), dma((3,)), dma((8,)), dma((8,)), dma((24,)), dma((24,)), dma((1,)), dma((1,)),
        ],
        compiler_params=pltpu.CompilerParams(vmem_limit_bytes=60 << 20, collective_id=3, has_side_effects=True),
        cost_estimate=pl.CostEstimate(
            flops=160 * seq * seq * PAIR, bytes_accessed=64 * seq * d_model, transcendentals=seq * seq * 4),
        name="backward",
    )(qkv, d_c, lse, d_mid, x, emb, w_qkv, u_seq)


def grad_kernel(by_left, _, *refs):
    lefts, rights, (away_ref, mid_ref, keep_ref, left_t, right_s) = refs[:16], refs[16:20], refs[20:]
    count, piece = lefts[0].shape
    step = pl.program_id(0)

    @pl.when(step == 0 if not by_left else step >= 0)
    def _():
        for i in range(16):
            left_t[i % 4 * piece:(i % 4 + 1) * piece, i // 4 * count:(i // 4 + 1) * count] = lefts[i][...].T

    @pl.when(step == 0 if by_left else step >= 0)
    def _():
        for i in range(4):
            right_s[i * count:(i + 1) * count, :] = rights[i][...]

    total = dot_nn(left_t[...], right_s[...])
    away_ref[0] = total[:2 * piece]
    mid_ref[0] = total[2 * piece:3 * piece]
    keep_ref[0] = total[3 * piece:]


def grad_products(order, lefts, rights, by_left=False):
    count = rights[0].shape[0]
    tile = rights[0].shape[1] // (1 if by_left else 4)
    piece = lefts[0].shape[1] // (32 if by_left else 8)
    if by_left:
        left_spec = lambda n: pl.BlockSpec((count, piece), lambda i, order: (0, i * 8 + order[n]))
        right_spec = pl.BlockSpec((count, tile), lambda i, order: (0, 0))
    else:
        left_spec = lambda n: pl.BlockSpec((count, piece), lambda i, order: (0, order[n]))
        right_spec = pl.BlockSpec((count, tile), lambda i, order: (0, i))
    return pl.pallas_call(
        functools.partial(grad_kernel, by_left),
        grid_spec=pltpu.PrefetchScalarGridSpec(
            num_scalar_prefetch=1,
            grid=(4,),
            in_specs=[left_spec(n) for _ in range(4) for n in range(4)] + [right_spec] * 4,
            out_specs=[pl.BlockSpec((1, n * piece, tile), lambda i, order: (i, 0, 0)) for n in (2, 1, 1)],
            scratch_shapes=[pltpu.VMEM((4 * piece, 4 * count), BF16), pltpu.VMEM((4 * count, tile), BF16)],
        ),
        out_shape=[jax.ShapeDtypeStruct((4, n * piece, tile), F32) for n in (2, 1, 1)],
        compiler_params=pltpu.CompilerParams(vmem_limit_bytes=60 << 20),
        cost_estimate=pl.CostEstimate(
            flops=128 * count * piece * tile, bytes_accessed=8 * count * (4 * piece + 4 * tile) + 64 * piece * tile,
            transcendentals=0),
        interpret=INTERPRET,
        name="grad",
    )(order, *[left for left in lefts for _ in range(4)], *rights)


def backward_rows(q, d_out, lse, k_ref, v_ref, k_t, p_cat, ds_cat, dk_acc, dv_acc):
    block = q.shape[0]
    lane = lax.broadcasted_iota(jnp.int32, q.shape, 1)
    q_heads, do_heads, dqs = [], [], []
    for head in range(2):
        mine = lane // HEAD_DIM == head
        q_head = jnp.where(mine, q, jnp.zeros_like(q))
        do_head = jnp.where(mine, d_out, jnp.zeros_like(d_out))
        scores = dot_nt(k_ref[...], q_head)
        probs = jnp.exp2(scores * EXP2_SCALE - lse[head:head + 1, :])
        d_probs = dot_nt(v_ref[...], do_head).astype(BF16).astype(F32)
        inner = jnp.sum(probs * d_probs, axis=0, keepdims=True)
        cols = slice(head * block, (head + 1) * block)
        p_cat[:, cols] = probs.astype(BF16)
        ds_cat[:, cols] = (probs * (d_probs - inner)).astype(BF16)
        dqs.append(dot_nn(k_t[head * HEAD_DIM:(head + 1) * HEAD_DIM, :], ds_cat[:, cols]))
        q_heads.append(q_head)
        do_heads.append(do_head)
    dv_acc[...] += dot_nn(p_cat[...], jnp.concatenate(do_heads, axis=0))
    dk_acc[...] += dot_nn(ds_cat[...], jnp.concatenate(q_heads, axis=0))
    return (jnp.concatenate(dqs, axis=0).T * SCALE).astype(BF16)


def last_kernel(qkv_ref, dc_ref, lse_ref, dmid_ref, x_ref, emb_ref, wqkv_ref, u_ref, gqkv2_ref,
                r2_ref, mid2_ref, keep2_ref, *refs):
    lefts = {'1': refs[:4], 'o': refs[8:12]}
    rights = {'1': refs[4:8], 'o': refs[12:16]}
    (dx_ref, g1_ref, g2_ref, go_ref, gq_ref, gk_ref, gv_ref, away1_ref, mid1_ref, keep1_ref, awayo_ref, mido_ref, keepo_ref,
     dch, k_t, dk_acc, dv_acc, p_cat, ds_cat, d_heads, d_qkv, buf, buf_o, second, second_o, tmp, tmp_o,
     third, third_o, sum_1, sum_2, sum_o, qa, qb, q1, q2, q3, q4, d_1, w_s, u_s, g_s,
     left_t, stage,
     local_sem, load_sem, send_sem, recv_sem, dc_send, dc_recv, dq_send, dq_recv, z_send, z_recv, x_send, x_recv,
     p_send, p_recv) = refs[16:]
    seq = qkv_ref.shape[0]
    blk = seq // 4
    head_cols = 2 * PAIR
    here = Place()
    z, core, role, owner = here.z, here.c, here.role, here.owner
    here.meet()
    copies = Copies(send_sem, recv_sem)
    waits = []

    def span(index, count):
        return pl.ds(pl.multiple_of(index * count, count), count)

    def load(src, dst, n):
        copy = pltpu.make_async_copy(src, dst, load_sem.at[n])
        copy.start()
        return copy

    no = jnp.logical_not
    to_a, to_b = here.device(y=here.ya, x=here.xa), here.device(y=here.yb, x=here.xb)
    partner = here.device(c=1 - core)
    member = [here.device(z=z // 2 * 2 + i // 2, c=i % 2) for i in range(4)]
    piece = tmp.shape[1]

    def dc_copy(i):
        return pltpu.make_async_remote_copy(
            src_ref=dc_ref.at[:, i * head_cols:(i + 1) * head_cols], dst_ref=dch.at[span(role, blk), :],
            send_sem=dc_send.at[i], recv_sem=dc_recv.at[role], device_id=member[i], device_id_type=MESH)

    for i in range(4):
        pl.when(role != i)(dc_copy(i).start)

        @pl.when(role == i)
        def _():
            dch[i * blk:(i + 1) * blk, :] = dc_ref[:, i * head_cols:(i + 1) * head_cols]

    half = rights['1'][0].shape[1] // 8
    firsts = {('1', q): [copies.make(away1_ref.at[q, :, h * half:(h + 1) * half], buf.at[4 + q, :, h * half:(h + 1) * half], to_a)
                         for h in range(2)] for q in range(4)}
    firsts['o'] = [copies.make(awayo_ref.at[2 * h:2 * h + 2], buf_o.at[2 * h:2 * h + 2], to_a) for h in range(2)]
    w2_loads = [load(r2_ref.at[q], buf.at[q], q) for q in range(4)]
    seconds = {(w, q): copies.make(buf.at[u + q, piece:, :], second.at[u + q], to_b) for w, u in (('2', 0), ('1', 4)) for q in range(4)}
    seconds['o'] = copies.make(buf_o.at[:, piece:, :], second_o, to_b)

    def add_mid(unit):
        if unit == 'o':
            mid, keep, t, n = mido_ref, keepo_ref, tmp_o, 4
            bottom, top = buf_o.at[:, piece:, :], buf_o.at[:, :piece, :]
        else:
            w, q = unit
            mid, keep = (mid2_ref.at[q], keep2_ref.at[q]) if w == '2' else (mid1_ref.at[q], keep1_ref.at[q])
            u = q if w == '2' else 4 + q
            t, n, bottom, top = tmp, 6, buf.at[u, piece:, :], buf.at[u, :piece, :]
        loads = [load(mid, t.at[0], n), load(keep, t.at[1], n + 1)]
        if unit == 'o' or unit[0] == '1':
            for copy in firsts[unit]:
                copy.wait_recv()
        else:
            w2_loads[unit[1]].wait()
        for copy in loads:
            copy.wait()
        bottom[...] += t[0]
        top[...] += t[1]
        seconds[unit].start()

    def z_copy(unit, q):
        if unit == 'o':
            src, dst, n = buf_o.at[q, :piece, :], third_o.at[z], 8
        else:
            w = 0 if unit == '2' else 1
            src, dst, n = buf.at[4 * w + q, :piece, :], third.at[w, z], 4 * w
        return pltpu.make_async_remote_copy(
            src_ref=src, dst_ref=dst, send_sem=z_send.at[n + q], recv_sem=z_recv.at[n + z],
            device_id=here.device(z=q), device_id_type=MESH)

    def finish(unit):
        seconds[unit].wait_recv()
        if unit == 'o':
            buf_o[:, :piece, :] += second_o[...]
            for q in range(4):
                pl.when(z != q)(z_copy('o', q).start)
        else:
            w, q = unit
            u = q if w == '2' else 4 + q
            buf[u, :piece, :] += second[u]
            pl.when(z != q)(z_copy(w, q).start)

    mine, by_a = here.piece(here.y, here.x), here.piece(here.ya, here.xa)
    by_b, by_ab = here.piece(here.yb, here.xb), here.piece(1 - here.y, 1 - here.x)
    gathers = {}

    def total(unit):
        out, got, n = {'2': (sum_2, third.at[0], 0), '1': (sum_1, third.at[1], 4), 'o': (sum_o, third_o, 8)}[unit]
        if unit == 'o':
            out[...] = buf_o[z, :piece, :]
        else:
            out[...] = buf[n + z, :piece, :]
        for zz in range(4):
            @pl.when(z != zz)
            def _():
                pltpu.make_async_copy(out, got.at[zz], z_recv.at[n + zz]).wait()
                out[...] += got[zz]

    def gather_start(name, src, out, n):
        rows = lambda e: out.at[span(e, piece), :]
        keep = pltpu.make_async_copy(src, rows(mine), local_sem.at[n])
        keep.start()
        waits.append(keep)
        gathers[name] = dict(src=src, rows=rows, a=copies.start(src, rows(mine), to_a), b1=copies.start(src, rows(mine), to_b))

    def gather_second(name):
        g = gathers[name]
        g['a'].wait_recv()
        g['b2'] = copies.start(g['rows'](by_a), g['rows'](by_a), to_b)

    def gather_core(name):
        g = gathers[name]
        g['c'] = [copies.start(g['src'], g['rows'](mine), partner), copies.start(g['rows'](by_a), g['rows'](by_a), partner)]
        g['b1'].wait_recv()
        g['c'].append(copies.start(g['rows'](by_b), g['rows'](by_b), partner))
        g['b2'].wait_recv()
        g['c'].append(copies.start(g['rows'](by_ab), g['rows'](by_ab), partner))

    def dq_copy(j, i, t):
        col = t * head_cols + j * PAIR
        return pltpu.make_async_remote_copy(
            src_ref=d_heads.at[i * blk:(i + 1) * blk, col:col + PAIR],
            dst_ref=d_qkv.at[:, pl.ds(pl.multiple_of(role * 3 * head_cols + col, PAIR), PAIR)],
            send_sem=dq_send.at[(j * 4 + i) * 3 + t], recv_sem=dq_recv.at[(j * 4 + role) * 3 + t],
            device_id=member[i], device_id_type=MESH)

    def send_d_heads(j):
        for i in range(4):
            @pl.when(role != i)
            def _():
                for t in range(3):
                    dq_copy(j, i, t).start()

    index = [here.ya * 2 + here.xa, (1 - here.y) * 2 + 1 - here.x, here.yb * 2 + here.xb, here.y * 2 + here.x]
    spaces = (p_cat, ds_cat)
    parts = [('1', n) for n in range(8)] + [('o', n) for n in range(2)]

    def load_lefts(name):
        for n in range(16):
            pltpu.make_async_copy(
                lefts[name][n // 4].at[:, span(index[n % 4] * 2 + core, piece)],
                d_heads.at[n // 4 * blk:(n // 4 + 1) * blk, n % 4 * piece:(n % 4 + 1) * piece], load_sem.at[14]).start()

    def load_rights(s):
        name, n = parts[s]
        for i in range(4):
            pltpu.make_async_copy(
                rights[name][i].at[:, n * half:(n + 1) * half], spaces[s % 2].at[i * blk:(i + 1) * blk, :],
                load_sem.at[15 + s % 2]).start()

    def stored(s):
        pltpu.make_async_copy(stage.at[s % 2], stage.at[s % 2], load_sem.at[17 + s % 2]).wait()

    def send_part(s):
        name, n = parts[s]
        if name == '1':
            firsts[('1', n // 2)][n % 2].start()
        else:
            firsts['o'][n].start()

    load_lefts('1')
    load_rights(0)
    for s in range(len(parts)):
        name, n = parts[s]
        if n == 0:
            every = d_heads.at[:, :4 * piece]
            pltpu.make_async_copy(every, every, load_sem.at[14]).wait()
            left_t[...] = every[...].T
            if name == '1':
                load_lefts('o')
        if s + 1 < len(parts):
            load_rights(s + 1)
        space = spaces[s % 2]
        pltpu.make_async_copy(space, space, load_sem.at[15 + s % 2]).wait()
        if s >= 1:
            stored(s - 1)
            send_part(s - 1)
        stage[s % 2] = dot_nn(left_t[...], space[...])
        if s < 8 and s % 2 == 1:
            add_mid(('2', s // 2))
        for row, ref in ((0, (away1_ref, awayo_ref)), (2 * piece, (mid1_ref, mido_ref)), (3 * piece, (keep1_ref, keepo_ref))):
            count = 2 * piece if row == 0 else piece
            rows = slice(row, row + count)
            if name == '1':
                pltpu.make_async_copy(stage.at[s % 2, rows, :], ref[0].at[n // 2, :, n % 2 * half:(n % 2 + 1) * half],
                                      load_sem.at[17 + s % 2]).start()
            else:
                for k in range(2):
                    pltpu.make_async_copy(stage.at[s % 2, rows, k * (half // 2):(k + 1) * (half // 2)], ref[1].at[2 * n + k],
                                          load_sem.at[17 + s % 2]).start()
    stored(len(parts) - 1)
    send_part(len(parts) - 1)

    for i in range(4):
        @pl.when(role != i)
        def _():
            pltpu.make_async_copy(dc_ref.at[:, :head_cols], dch.at[:blk, :], dc_recv.at[i]).wait()

    moves = {(0, 1): [(finish, ('2', 0))], (0, 4): [(finish, ('2', 1)), (add_mid, ('1', 0))], (0, 7): [(finish, ('2', 2))],
             (1, 0): [(send_d_heads, 0)], (1, 2): [(finish, ('2', 3)), (add_mid, ('1', 1))], (1, 4): [(finish, ('1', 0))],
             (1, 6): [(add_mid, ('1', 2))]}
    steps = seq // BWD_ROWS
    for j in range(2):
        k_view, v_view = qkv_ref.at[:, (2 + j) * PAIR:(3 + j) * PAIR], qkv_ref.at[:, (4 + j) * PAIR:(5 + j) * PAIR]
        k_t[...] = k_view[...].T
        dk_acc[...] = jnp.zeros_like(dk_acc)
        dv_acc[...] = jnp.zeros_like(dv_acc)

        def block(i, _):
            for n in range(8):
                if (j, n) in moves:
                    @pl.when(i == min(n, steps - 1))
                    def _():
                        for move, what in moves[(j, n)]:
                            move(what)
            rows = span(i, BWD_ROWS)
            cols = slice(j * PAIR, (j + 1) * PAIR)
            d_heads[rows, cols] = backward_rows(
                qkv_ref[rows, cols], dch[rows, cols], lse_ref[2 * j:2 * j + 2, rows], k_view, v_view,
                k_t, p_cat, ds_cat, dk_acc, dv_acc)
            return 0

        lax.fori_loop(0, steps, block, 0)
        d_heads[:, head_cols + j * PAIR:head_cols + (j + 1) * PAIR] = (dk_acc[...] * SCALE).astype(BF16)
        d_heads[:, 2 * head_cols + j * PAIR:2 * head_cols + (j + 1) * PAIR] = dv_acc[...].astype(BF16)

    quarter = 2 * piece

    def quarter_loads(n):
        return [load(u_ref.at[:, span(index[n], quarter)], u_s.at[n % 2], 8 + n % 2),
                load(gqkv2_ref.at[span(index[n], quarter), :], g_s.at[n % 2], 10 + n % 2)]

    pending = quarter_loads(0)
    for i in range(4):
        @pl.when(role == i)
        def _():
            d_qkv[:, i * 3 * head_cols:(i + 1) * 3 * head_cols] = d_heads[i * blk:(i + 1) * blk, :]
    send_d_heads(1)
    targets = [qa.at[0], qa.at[1], qb.at[0], qb.at[1]]
    first_q = None
    for n in range(4):
        ahead = quarter_loads(n + 1) if n < 3 else []
        for copy in pending:
            copy.wait()
        targets[n][...] = dot_tn(u_s[n % 2], d_heads[...]) + g_s[n % 2]
        pending = ahead
        if n == 2:
            first_q = copies.start(qa, q1, to_a)

    add_mid(('1', 3))
    w_rows = w_s.shape[1]
    chunks = wqkv_ref.shape[0] // w_rows
    w_load = load(wqkv_ref.at[:w_rows, :], w_s.at[0], 12)
    for j in range(2):
        for i in range(4):
            @pl.when(role != i)
            def _():
                for t in range(3):
                    pltpu.make_async_copy(d_heads.at[:blk, :PAIR], d_qkv.at[:, :PAIR], dq_recv.at[(j * 4 + i) * 3 + t]).wait()
    for n in range(chunks):
        ahead = load(wqkv_ref.at[(n + 1) * w_rows:(n + 2) * w_rows, :], w_s.at[(n + 1) % 2], 12 + (n + 1) % 2) if n + 1 < chunks else None
        w_load.wait()
        d_1[:, n * w_rows:(n + 1) * w_rows] = dot_nt(d_qkv[...], w_s[n % 2]).astype(BF16)
        w_load = ahead

    count = min(128, blk)
    for n in range(blk // count):
        rows = slice(n * count, (n + 1) * count)
        d_1[rows, :] = through_norm(x_ref[rows, :].astype(F32) + emb_ref[...], d_1[rows, :].astype(F32), dmid_ref[rows, :])

    own_seq = z // 2
    rows_dx = span(role, blk)

    def dx_copy(n, device):
        slot = [0, 1 + core, 3 + core][n]
        return pltpu.make_async_remote_copy(
            src_ref=d_1, dst_ref=dx_ref.at[rows_dx, :], send_sem=x_send.at[n], recv_sem=x_recv.at[slot],
            device_id=device, device_id_type=MESH)

    dx_side = dx_copy(0, partner)
    dx_next = dx_copy(1, here.device(z=here.z_by[1], c=own_seq))
    dx_cross = dx_copy(2, here.device(z=here.z_by[2], c=own_seq))
    dx_keep = pltpu.make_async_copy(d_1, dx_ref.at[rows_dx, :], local_sem.at[8])

    def dx_pass(cc):
        rows = span(z % 2 * 2 + cc, blk)
        return pltpu.make_async_remote_copy(
            src_ref=dx_ref.at[rows, :], dst_ref=dx_ref.at[rows, :], send_sem=x_send.at[3 + cc], recv_sem=x_recv.at[5 + cc],
            device_id=here.device(z=here.z_by[1]), device_id_type=MESH)

    add_mid('o')
    dx_cross.start()
    dx_next.start()
    pl.when(owner)(dx_keep.start)
    pl.when(no(owner))(dx_side.start)

    def dx_got(slot):
        pltpu.make_async_copy(d_1, dx_ref.at[:blk, :], x_recv.at[slot]).wait()

    first_q.wait_recv()
    qb[0] += q1[1]
    qb[1] += q1[0]
    second_q = copies.start(qb.at[0], q2, to_b)
    finish(('1', 1))
    total('2')
    finish(('1', 2))
    gather_start('2', sum_2, g2_ref, 0)
    finish(('1', 3))
    finish('o')
    second_q.wait_recv()
    qb[1] += q2[...]
    plane_stays = jnp.logical_and(2 * (z % 2) + core == z, z // 2 == core)
    plane_q = pltpu.make_async_remote_copy(
        src_ref=qb.at[1], dst_ref=q3, send_sem=p_send.at[0], recv_sem=p_recv.at[0],
        device_id=here.device(z=2 * (z % 2) + core, c=z // 2), device_id_type=MESH)

    @pl.when(plane_stays)
    def _():
        q3[...] = qb[1]

    pl.when(no(plane_stays))(plane_q.start)
    gather_second('2')

    @pl.when(no(owner))
    def _():
        for cc in range(2):
            dx_got(3 + cc)
            dx_pass(cc).start()

    total('1')
    total('o')
    gather_start('1', sum_1, g1_ref, 1)
    gather_start('o', sum_o, go_ref, 2)
    gather_core('2')
    pl.when(no(plane_stays))(plane_q.wait_recv)
    give_q = copies.start(q3.at[span(1 - core, piece), :], q4.at[0], partner)
    gather_second('1')
    gather_second('o')
    give_q.wait_recv()
    q4[1] = q4[0] + q3[span(core, piece), :]
    for t, (name, out) in enumerate((('q', gq_ref), ('k', gk_ref), ('v', gv_ref))):
        gather_start(name, q4.at[1, :, t * head_cols:(t + 1) * head_cols], out, 3 + t)
    gather_core('1')
    gather_core('o')
    for name in 'qkv':
        gather_second(name)
    for name in 'qkv':
        gather_core(name)

    @pl.when(owner)
    def _():
        for slot in (0, 1, 2):
            dx_got(slot)
        dx_keep.wait()

    @pl.when(no(owner))
    def _():
        dx_side.wait_send()
        for cc in range(2):
            dx_got(5 + cc)
            dx_pass(cc).wait_send()

    for g in gathers.values():
        for copy in g['c']:
            copy.wait_recv()
    for copy in waits:
        copy.wait()
    for copy in copies.sent:
        copy.wait_send()
    dx_cross.wait_send()
    dx_next.wait_send()
    pl.when(no(plane_stays))(plane_q.wait_send)
    for i in range(4):
        @pl.when(role != i)
        def _():
            dc_copy(i).wait_send()
            for j in range(2):
                for t in range(3):
                    dq_copy(j, i, t).wait_send()

        for unit in '21o':
            pl.when(z != i)(z_copy(unit, i).wait_send)


def last_call(qkv, d_c, lse, d_mid, x, emb, w_qkv, u_seq, g_qkv, w2_parts, w1_sides, wo_sides):
    seq, d_model = u_seq.shape
    blk, piece = seq // 4, d_model // 8
    n1, no = w1_sides[4].shape[1] // 4, wo_sides[4].shape[1] // 4
    assert n1 == 2 * 2 * BWD_ROWS and no * 2 == 2 * BWD_ROWS
    assert w2_parts[0].shape[1:] == (2 * piece, n1)
    heads3 = qkv.shape[1]
    anywhere = pl.BlockSpec(memory_space=pl.ANY)
    in_vmem = pl.BlockSpec(memory_space=pltpu.VMEM)
    copies = 10 + 9 + 6 * 7 + 3
    dma = pltpu.SemaphoreType.DMA
    w_rows = min(128, d_model)
    return pl.pallas_call(
        last_kernel,
        in_specs=[in_vmem] * 6 + [anywhere] * 22,
        out_specs=[anywhere] * 13,
        out_shape=[
            jax.ShapeDtypeStruct((seq, d_model), BF16),
            jax.ShapeDtypeStruct((d_model, n1), F32),
            jax.ShapeDtypeStruct((8 * piece, n1), F32),
            jax.ShapeDtypeStruct((d_model, no), F32),
        ] + [jax.ShapeDtypeStruct((d_model, heads3 // 3), F32)] * 3
        + [jax.ShapeDtypeStruct((4, k * piece, n), F32) for n in (n1, no) for k in (2, 1, 1)],
        scratch_shapes=[
            pltpu.VMEM((seq, heads3 // 3), BF16),
            pltpu.VMEM((PAIR, seq), BF16),
            pltpu.VMEM((seq, PAIR), F32),
            pltpu.VMEM((seq, PAIR), F32),
            pltpu.VMEM((seq, 2 * BWD_ROWS), BF16),
            pltpu.VMEM((seq, 2 * BWD_ROWS), BF16),
            pltpu.VMEM((seq, heads3), BF16),
            pltpu.VMEM((blk, 4 * heads3), BF16),
            pltpu.VMEM((8, 2 * piece, n1), F32),
            pltpu.VMEM((4, 2 * piece, no), F32),
            pltpu.VMEM((8, piece, n1), F32),
            pltpu.VMEM((4, piece, no), F32),
            pltpu.VMEM((2, piece, n1), F32),
            pltpu.VMEM((2, 4, piece, no), F32),
            pltpu.VMEM((2, 4, piece, n1), F32),
            pltpu.VMEM((4, piece, no), F32),
            pltpu.VMEM((piece, n1), F32),
            pltpu.VMEM((piece, n1), F32),
            pltpu.VMEM((piece, no), F32),
            pltpu.VMEM((2, 2 * piece, heads3), F32),
            pltpu.VMEM((2, 2 * piece, heads3), F32),
            pltpu.VMEM((2, 2 * piece, heads3), F32),
            pltpu.VMEM((2 * piece, heads3), F32),
            pltpu.VMEM((2 * piece, heads3), F32),
            pltpu.VMEM((2, piece, heads3), F32),
            pltpu.VMEM((blk, d_model), BF16),
            pltpu.VMEM((2, w_rows, 4 * heads3), BF16),
            pltpu.VMEM((2, seq, 2 * piece), BF16),
            pltpu.VMEM((2, 2 * piece, heads3), F32),
            pltpu.VMEM((4 * piece, seq), BF16),
            pltpu.VMEM((2, 4 * piece, 2 * BWD_ROWS), F32),
            dma((9,)), dma((19,)), dma((copies,)), dma((copies,)),
            dma((4,)), dma((4,)), dma((24,)), dma((24,)), dma((12,)), dma((12,)), dma((5,)), dma((7,)), dma((1,)), dma((1,)),
        ],
        compiler_params=pltpu.CompilerParams(vmem_limit_bytes=63 << 20, collective_id=1, has_side_effects=True),
        cost_estimate=pl.CostEstimate(
            flops=160 * seq * seq * PAIR, bytes_accessed=128 * seq * d_model, transcendentals=seq * seq * 4),
        name="last",
    )(qkv, d_c, lse, d_mid, x, emb, w_qkv, u_seq, g_qkv, *w2_parts, *w1_sides, *wo_sides)[:7]


def lin(z, y, x, c):
    return z * 8 + y * 4 + x * 2 + c


def send(value, to):
    pairs = []
    for z in range(4):
        for y in range(2):
            for x in range(2):
                for c in range(2):
                    dst = to(z, y, x, c)
                    if dst is not None:
                        pairs.append((lin(z, y, x, c), lin(*dst)))
    return lax.ppermute(value, AXES, pairs)


def other_core(z, y, x, c):
    return (z, y, x, 1 - c)


def swap_first(z, y, x, c):
    return (z, y, 1 - x, c) if c == 0 else (z, 1 - y, x, c)


def rows_of(value, index, count):
    return lax.dynamic_slice_in_dim(value, index * count, count, axis=0)


def solution(mesh):
    spec_col = P(None, 'model')
    spec_row = P('model', None)
    spec_act = P('data', None, None)
    spec_rep = P(None, None)

    def device_step(x_in, cot_out, step_emb, w_q, w_k, w_v, w_o, w_1, w_2):
        seq, d_model = x_in.shape[1:]
        blk = seq // 4
        z = lax.axis_index('model')
        d = lax.axis_index('data')
        y, x, core = d // 4, d // 2 % 2, d % 2
        role = z % 2 * 2 + core
        owner = core == z // 2
        emb = step_emb.astype(F32)

        c_1, lse_1, x_seq, cot, wo, w1, w2, w_qkv = first_call(
            x_in[0], cot_out[0], emb[:1], w_q, w_k, w_v, w_o, w_1, w_2)
        wo, w2 = wo.reshape(-1, d_model), w2.reshape(-1, d_model)
        x_1 = rows_of(x_seq, role, blk)

        def mlp_forward(x_f, context):
            h = (x_f + dot_nn(context, wo)).astype(BF16)
            m = rms_norm(h.astype(F32)).astype(BF16)
            up = dot_nn(m, w1).astype(BF16)
            act = jax.nn.gelu(up.astype(F32)).astype(BF16)
            return h, m, up, act

        s_1 = x_1.astype(F32) + emb[0]
        h_1, m_1, up_1, act_1 = mlp_forward(s_1, c_1)
        x_2 = (h_1.astype(F32) + dot_nn(act_1, w2)).astype(BF16)

        c_2, lse_2, u_2_seq, qkv_2, u_1_seq, qkv_1 = forward_call(x_2, emb, x_seq, w_qkv)
        s_2 = x_2.astype(F32) + emb[1]
        h_2, m_2, up_2, act_2 = mlp_forward(s_2, c_2)

        def mlp_backward(d_next, h, up):
            d_act = dot_nt(d_next, w2).astype(BF16)
            d_up = jax.vjp(jax.nn.gelu, up.astype(F32))[1](d_act.astype(F32))[0].astype(BF16)
            d_m = dot_nt(d_up, w1).astype(BF16)
            d_h = jax.vjp(rms_norm, h.astype(F32))[1](d_m.astype(F32))[0]
            return d_up, (d_next.astype(F32) + d_h).astype(BF16)

        d_up_2, d_mid_2 = mlp_backward(cot, h_2, up_2)
        d_2, d_2_other, g_qkv_2 = backward_call(
            qkv_2, dot_nt(d_mid_2, wo).astype(BF16), lse_2, d_mid_2, x_2, emb[1:], w_qkv, u_2_seq)

        first, second = jnp.where(core == 0, x, y), jnp.where(core == 0, y, x)

        def at(i, j):
            return jnp.where(core == 0, j * 2 + i, i * 2 + j)

        order = [at(1 - first, second), at(1 - first, 1 - second), at(first, 1 - second), at(first, second)]
        column = jnp.stack(order) * 2 + core

        def both_cores(sides):
            lefts, rights = [], []
            for left, right in sides:
                lefts += [left, send(left, other_core)]
                rights += [right, send(right, other_core)]
            return lefts, rights

        lefts, rights = both_cores([(act_2, cot)])
        lefts += [act_1, send(act_1, other_core)]
        rights += [d_2, d_2_other]
        away, mid, keep = grad_products(column, lefts, rights, True)
        d_2, away = lax.optimization_barrier((d_2, away))
        w2_parts = (send(away, swap_first), mid, keep)
        d_up_1, d_mid_1 = mlp_backward(d_2, h_1, up_1)
        w1_sides = sum(both_cores([(m_2, d_up_2), (m_1, d_up_1)]), [])
        wo_sides = sum(both_cores([(d_mid_2, c_2), (d_mid_1, c_1)]), [])
        d_c = dot_nt(d_mid_1, wo).astype(BF16)
        d_x, g_w1, g_w2, g_wo, g_q, g_k, g_v = last_call(
            qkv_1, d_c, lse_1, d_mid_1, x_1, emb[:1], w_qkv, u_1_seq, g_qkv_2, w2_parts, w1_sides, wo_sides)
        return g_q, g_k, g_v, g_wo.T, g_w1, g_w2, d_x[None]

    return jax.shard_map(device_step, mesh=mesh,
                         in_specs=(spec_act, spec_act, spec_rep, spec_col, spec_col, spec_col, spec_row, spec_col, spec_row),
                         out_specs=(spec_col, spec_col, spec_col, spec_row, spec_col, spec_row, spec_act),
                         check_vma=False)
```

```python
import functools
import math

import jax
import jax.numpy as jnp
from jax import lax
from jax.experimental import pallas as pl
from jax.experimental.pallas import tpu as pltpu
from jax.sharding import PartitionSpec as P


HEAD_DIM = 64
EPS_NORM = 1e-6
SCALE = HEAD_DIM ** -0.5
EXP2_SCALE = SCALE * math.log2(math.e)
PAIR = 2 * HEAD_DIM
BWD_ROWS = 256
KEYS = 256
HIDDEN = 512
INTERPRET = False
AXES = ('model', 'data')
BF16 = jnp.bfloat16
F32 = jnp.float32
MESH = pl.DeviceIdType.MESH


def dot_nt(a, b):
    return lax.dot_general(a, b, (((1,), (1,)), ((), ())), preferred_element_type=F32)


def dot_nn(a, b):
    return lax.dot_general(a, b, (((1,), (0,)), ((), ())), preferred_element_type=F32)


def dot_tn(a, b):
    return lax.dot_general(a, b, (((0,), (0,)), ((), ())), preferred_element_type=F32)


def attend_rows(q, k_ref, v_t, e_refs):
    count = k_ref.shape[0] // KEYS
    lane = lax.broadcasted_iota(jnp.int32, q.shape, 1)
    q_heads = [jnp.where(lane // HEAD_DIM == head, q, jnp.zeros_like(q)) for head in range(2)]
    tops, run, total, outs, sums = [[], []], [None, None], [None, None], [], []
    for j in range(count):
        keys = slice(j * KEYS, (j + 1) * KEYS)
        for head in range(2):
            scores = dot_nt(k_ref[keys, :], q_heads[head])
            top = jnp.max(scores, axis=0, keepdims=True) * EXP2_SCALE
            if j:
                top = jnp.maximum(top, run[head])
            weights = jnp.exp2(scores * EXP2_SCALE - top)
            part = jnp.sum(weights, axis=0, keepdims=True)
            total[head] = total[head] * jnp.exp2(run[head] - top) + part if j else part
            run[head] = top
            tops[head].append(top)
            e_refs[head][keys, :] = weights
    for head in range(2):
        inverse = 1.0 / total[head]
        out = None
        for j in range(count):
            keys = slice(j * KEYS, (j + 1) * KEYS)
            factor = inverse * jnp.exp2(tops[head][j] - run[head])
            probs = (e_refs[head][keys, :] * factor).astype(BF16)
            part = dot_nn(v_t[head * HEAD_DIM:(head + 1) * HEAD_DIM, keys], probs)
            out = out + part if j else part
        sums.append(run[head] + jnp.log2(total[head]))
        outs.append(out)
    return outs, sums


class Place:
    def __init__(self):
        self.z = lax.axis_index('model')
        d = lax.axis_index('data')
        self.y, self.x, self.c = d // 4, d // 2 % 2, d % 2
        z = self.z
        self.z_by = {1: z + 1 - 2 * (z % 2), 2: (z + 2) % 4, 3: 3 - z}
        x, y, c = self.x, self.y, self.c
        self.xa, self.ya = x + (1 - c) * (1 - 2 * x), y + c * (1 - 2 * y)
        self.xb, self.yb = x + c * (1 - 2 * x), y + (1 - c) * (1 - 2 * y)
        self.role = z % 2 * 2 + c
        self.owner = c == z // 2

    def piece(self, y, x, c=None):
        return y * 4 + x * 2 + (self.c if c is None else c)

    def device(self, z=None, y=None, x=None, c=None):
        z, y, x, c = (own if given is None else given for given, own in zip((z, y, x, c), (self.z, self.y, self.x, self.c)))
        return {'model': z, 'data': y * 4 + x * 2 + c}

    def peers(self):
        column = [self.device(z=z, c=c) for z in (self.z, *self.z_by.values()) for c in (self.c, 1 - self.c)][1:]
        return column + [self.device(x=1 - self.x), self.device(y=1 - self.y)]

    def meet(self):
        barrier = pltpu.get_barrier_semaphore()
        peers = self.peers()
        for peer in peers:
            pl.semaphore_signal(barrier, inc=1, device_id=peer, device_id_type=MESH)
        pl.semaphore_wait(barrier, len(peers))


class Copies:
    def __init__(self, send_sem, recv_sem):
        self.send_sem, self.recv_sem, self.used, self.sent = send_sem, recv_sem, 0, []

    def make(self, src, dst, device):
        n, self.used = self.used, self.used + 1
        copy = pltpu.make_async_remote_copy(
            src_ref=src, dst_ref=dst, send_sem=self.send_sem.at[n], recv_sem=self.recv_sem.at[n],
            device_id=device, device_id_type=MESH)
        self.sent.append(copy)
        return copy

    def start(self, src, dst, device):
        copy = self.make(src, dst, device)
        copy.start()
        return copy


def first_kernel(x_ref, cot_ref, emb_ref, wq_ref, wk_ref, wv_ref, wo_ref, w1_ref, w2_ref,
                 c1_ref, lse_ref, xs_ref, cot_loc_ref, full_o, full_1, full_2, full_qkv,
                 qkv_s, vt_s, e_a, e_b, c_buf, lse_s, cot_s, local_sem, send_sem, recv_sem, c_send, c_recv, one_send, one_recv):
    seq, d_model = x_ref.shape
    blk = seq // 4
    head_cols = wq_ref.shape[1]
    here = Place()
    z, core, role, owner = here.z, here.c, here.role, here.owner
    here.meet()
    copies = Copies(send_sem, recv_sem)

    def span(index, count):
        return pl.ds(pl.multiple_of(index * count, count), count)

    ff_cols, out_rows, piece = w1_ref.shape[1], wo_ref.shape[0] // 8, d_model // 8
    hidden = w2_ref.shape[0] // 8

    def block_qkv(zz, e):
        return full_qkv.at[span(e, piece), span(zz, 3 * head_cols)]

    units = {
        'o': lambda zz, e: full_o.at[zz, span(e, out_rows), :],
        '1': lambda zz, e: full_1.at[span(e, piece), span(zz, ff_cols)],
        '2': lambda zz, e: full_2.at[zz, span(e, hidden), :],
        'qkv': block_qkv,
    }

    def own_parts(name, e):
        if name == 'o':
            return [(wo_ref.at[span(e, out_rows), :], units[name](z, e))]
        if name == '1':
            return [(w1_ref.at[span(e, piece), :], units[name](z, e))]
        if name == '2':
            return [(w2_ref.at[span(e, hidden), :], units[name](z, e))]
        return [(ref.at[span(e, piece), :],
                 full_qkv.at[span(e, piece), pl.ds(pl.multiple_of((z * 3 + t) * head_cols, head_cols), head_cols)])
                for t, ref in enumerate((wq_ref, wk_ref, wv_ref))]

    mine = here.piece(here.y, here.x)
    by_a = here.piece(here.ya, here.xa)
    by_b = here.piece(here.yb, here.xb)
    by_ab = here.piece(1 - here.y, 1 - here.x)
    to_a, to_b = here.device(y=here.ya, x=here.xa), here.device(y=here.yb, x=here.xb)
    partner = here.device(c=1 - core)
    stage_z, stage_a, stage_b1, stage_b2, stage_c = {}, {}, {}, {}, {}
    names = ('o', '1', '2', 'qkv')

    for name in names:
        stage_z[name] = {k: [copies.start(src, dst, here.device(z=here.z_by[k])) for src, dst in own_parts(name, mine)]
                         for k in (1, 2, 3)}

    def forward_z(name):
        stage_a[name], stage_b1[name] = [], []
        for k in (1, 2, 3):
            for copy in stage_z[name][k]:
                copy.wait_recv()
            block = units[name](here.z_by[k], mine)
            stage_a[name].append(copies.start(block, block, to_a))
            stage_b1[name].append(copies.start(block, block, to_b))

    def forward_a(name):
        stage_b2[name] = []
        for k in (1, 2, 3):
            stage_a[name][k - 1].wait_recv()
            block = units[name](here.z_by[k], by_a)
            stage_b2[name].append(copies.start(block, block, to_b))

    def forward_b(name):
        stage_c[name] = []
        for k in (1, 2, 3):
            stage_b1[name][k - 1].wait_recv()
            stage_b2[name][k - 1].wait_recv()
            for e in (mine, by_a, by_b, by_ab):
                block = units[name](here.z_by[k], e)
                stage_c[name].append(copies.start(block, block, partner))

    locals_ = []

    def copy_local(src, dst):
        copy = pltpu.make_async_copy(src, dst, local_sem.at[len(locals_)])
        locals_.append(copy)
        copy.start()

    copy_local(w1_ref, full_1.at[:, span(z, ff_cols)])
    copy_local(w2_ref, full_2.at[z])
    copy_local(wo_ref, full_o.at[z])
    for t, ref in enumerate((wq_ref, wk_ref, wv_ref)):
        copy_local(ref, full_qkv.at[:, pl.ds(pl.multiple_of((z * 3 + t) * head_cols, head_cols), head_cols)])
    other_role = z % 2 * 2 + 1 - core
    give_x = pltpu.make_async_remote_copy(
        src_ref=x_ref, dst_ref=xs_ref, send_sem=one_send.at[0], recv_sem=one_recv.at[0], device_id=partner, device_id_type=MESH)
    give_cot = pltpu.make_async_remote_copy(
        src_ref=cot_ref.at[span(other_role, blk), :], dst_ref=cot_loc_ref, send_sem=one_send.at[1], recv_sem=one_recv.at[1],
        device_id=partner, device_id_type=MESH)
    keep_x = pltpu.make_async_copy(x_ref, xs_ref, local_sem.at[6])
    take_cot = pltpu.make_async_copy(cot_ref.at[span(role, blk), :], cot_s, local_sem.at[7])
    keep_cot = pltpu.make_async_copy(cot_s, cot_loc_ref, local_sem.at[8])

    @pl.when(owner)
    def _():
        give_x.start()
        give_cot.start()
        keep_x.start()
        take_cot.start()

    def project(i, _):
        rows = span(i, blk)
        values = x_ref[rows, :].astype(F32) + emb_ref[...]
        unit = (values * lax.rsqrt(jnp.mean(values * values, axis=-1, keepdims=True) + EPS_NORM)).astype(BF16)
        for t, ref in enumerate((wq_ref, wk_ref, wv_ref)):
            qkv_s[rows, t * head_cols:(t + 1) * head_cols] = dot_nn(unit, ref[...]).astype(BF16)
        return 0

    lax.fori_loop(0, 4, project, 0)

    def context_copy(j, i):
        src = c_buf.at[j, span(i, blk), :]
        dst = c1_ref.at[:, pl.ds(pl.multiple_of((z * 2 + j) * PAIR, PAIR), PAIR)]
        target_z, target_c = 2 * core + i // 2, i % 2
        remote = pltpu.make_async_remote_copy(
            src_ref=src, dst_ref=dst, send_sem=c_send.at[j * 4 + i], recv_sem=c_recv.at[j * 4 + z],
            device_id=here.device(z=target_z, c=target_c), device_id_type=MESH)
        local = pltpu.make_async_copy(src, dst, c_recv.at[j * 4 + z])
        return remote, local, jnp.logical_and(target_z == z, target_c == core)

    def send_context(j, i):
        remote, local, to_self = context_copy(j, i)
        pl.when(to_self)(local.start)
        pl.when(jnp.logical_not(to_self))(remote.start)

    moves = {(0, 1): [(forward_z, 'o')], (0, 2): [(forward_a, 'o')], (0, 3): [(forward_b, 'o')],
             (1, 2): [(forward_z, '1')], (1, 3): [(forward_a, '1')]}
    for j in range(2):
        vt_s[...] = qkv_s[:, (4 + j) * PAIR:(5 + j) * PAIR].T
        k_view = qkv_s.at[:, (2 + j) * PAIR:(3 + j) * PAIR]
        for i in range(4):
            if i or j:
                send_context(j if i else 0, i - 1 if i else 3)
            for step, name in moves.get((j, i), ()):
                step(name)
            rows = slice(i * blk, (i + 1) * blk)
            outs, sums = attend_rows(qkv_s[rows, j * PAIR:(j + 1) * PAIR], k_view, vt_s, (e_a, e_b))
            c_buf[j, rows, :] = jnp.concatenate(outs, axis=0).T.astype(BF16)
            for head in range(2):
                lse_s[2 * j + head:2 * j + head + 1, rows] = sums[head]

    @pl.when(owner)
    def _():
        take_cot.wait()
        keep_cot.start()

    forward_z('2')
    send_context(1, 3)
    give_lse = pltpu.make_async_remote_copy(
        src_ref=lse_s, dst_ref=lse_ref, send_sem=one_send.at[2], recv_sem=one_recv.at[2],
        device_id=here.device(z=2 * core + z // 2, c=z % 2), device_id_type=MESH)
    keep_lse = pltpu.make_async_copy(lse_s, lse_ref, local_sem.at[9])
    lse_stays = jnp.logical_and(2 * core + z // 2 == z, z % 2 == core)
    pl.when(lse_stays)(keep_lse.start)
    pl.when(jnp.logical_not(lse_stays))(give_lse.start)
    forward_b('1')
    forward_a('2')
    forward_z('qkv')
    forward_b('2')
    forward_a('qkv')
    forward_b('qkv')

    for j in range(2):
        for zz in range(4):
            pltpu.make_async_copy(c_buf.at[j, :blk, :], c1_ref.at[:, :PAIR], c_recv.at[j * 4 + zz]).wait()
        for i in range(4):
            remote, _, to_self = context_copy(j, i)
            pl.when(jnp.logical_not(to_self))(remote.wait_send)
    pl.when(lse_stays)(keep_lse.wait)

    @pl.when(jnp.logical_not(lse_stays))
    def _():
        give_lse.wait_send()
        give_lse.wait_recv()

    @pl.when(owner)
    def _():
        give_x.wait_send()
        give_cot.wait_send()
        keep_x.wait()
        keep_cot.wait()

    @pl.when(jnp.logical_not(owner))
    def _():
        give_x.wait_recv()
        give_cot.wait_recv()

    for copy in locals_:
        copy.wait()
    for name in names:
        for copy in stage_c[name]:
            copy.wait_recv()
    for copy in copies.sent:
        copy.wait_send()


def first_call(x, cot, emb, w_q, w_k, w_v, w_o, w_1, w_2):
    seq, d_model = x.shape
    head_cols, ff_cols, blk = w_q.shape[1], w_1.shape[1], seq // 4
    anywhere = pl.BlockSpec(memory_space=pl.ANY)
    in_vmem = pl.BlockSpec(memory_space=pltpu.VMEM)
    copies = 18 + 12 + 24 + 48
    return pl.pallas_call(
        first_kernel,
        in_specs=[in_vmem, anywhere] + [in_vmem] * 7,
        out_specs=[anywhere] * 8,
        out_shape=[
            jax.ShapeDtypeStruct((blk, d_model), BF16),
            jax.ShapeDtypeStruct((4, seq), F32),
            jax.ShapeDtypeStruct((seq, d_model), BF16),
            jax.ShapeDtypeStruct((blk, d_model), BF16),
            jax.ShapeDtypeStruct((4, *w_o.shape), BF16),
            jax.ShapeDtypeStruct((d_model, 4 * ff_cols), BF16),
            jax.ShapeDtypeStruct((4, *w_2.shape), BF16),
            jax.ShapeDtypeStruct((d_model, 12 * head_cols), BF16),
        ],
        scratch_shapes=[
            pltpu.VMEM((seq, 3 * head_cols), BF16),
            pltpu.VMEM((PAIR, seq), BF16),
            pltpu.VMEM((seq, blk), F32),
            pltpu.VMEM((seq, blk), F32),
            pltpu.VMEM((2, seq, PAIR), BF16),
            pltpu.VMEM((4, seq), F32),
            pltpu.VMEM((blk, d_model), BF16),
            pltpu.SemaphoreType.DMA((10,)),
            pltpu.SemaphoreType.DMA((copies,)),
            pltpu.SemaphoreType.DMA((copies,)),
            pltpu.SemaphoreType.DMA((8,)),
            pltpu.SemaphoreType.DMA((8,)),
            pltpu.SemaphoreType.DMA((3,)),
            pltpu.SemaphoreType.DMA((3,)),
        ],
        compiler_params=pltpu.CompilerParams(vmem_limit_bytes=60 << 20, collective_id=0, has_side_effects=True),
        cost_estimate=pl.CostEstimate(
            flops=64 * seq * seq * PAIR, bytes_accessed=64 * seq * d_model, transcendentals=seq * seq * 4),
        name="first",
    )(x, cot, emb, w_q, w_k, w_v, w_o, w_1, w_2)


def unit_rows(values, emb):
    values = values.astype(F32) + emb
    return (values * lax.rsqrt(jnp.mean(values * values, axis=-1, keepdims=True) + EPS_NORM)).astype(BF16)


def forward_kernel(x_ref, emb_ref, xs1_ref, wqkv_ref,
                   c_ref, lse_ref, u2_ref, qkv2_ref, u1_ref, qkv1_ref,
                   w_s, blocks, u_s, qkv_s, x1_s, u1_s, qkv1_s, v_t, e_a, e_b, c_buf, lse_s,
                   local_sem, first_sem, out_sem, x_send, x_recv, c_send, c_recv):
    seq = xs1_ref.shape[0]
    blk = seq // 4
    head_cols = 2 * PAIR
    here = Place()
    z, core, role = here.z, here.c, here.role

    def span(index, count):
        return pl.ds(pl.multiple_of(index * count, count), count)

    w_load = pltpu.make_async_copy(wqkv_ref.at[:, span(role, 3 * head_cols)], w_s, local_sem.at[0])
    w_load.start()
    x1_load = [pltpu.make_async_copy(xs1_ref.at[i * blk:(i + 1) * blk, :], x1_s.at[i % 2], first_sem.at[i % 2]) for i in range(4)]
    x1_load[0].start()
    here.meet()
    partner, across = here.device(c=1 - core), here.device(z=here.z_by[1])
    role_side, role_over = z % 2 * 2 + 1 - core, (1 - z % 2) * 2 + core
    role_last = (1 - z % 2) * 2 + 1 - core

    def x_copy(n, src, slot, device):
        return pltpu.make_async_remote_copy(
            src_ref=src, dst_ref=blocks.at[slot], send_sem=x_send.at[n], recv_sem=x_recv.at[n],
            device_id=device, device_id_type=MESH)

    over, side = x_copy(0, x_ref, 0, across), x_copy(1, x_ref, 1, partner)
    last = x_copy(2, blocks.at[0], 2, partner)
    over.start()
    side.start()

    def project(src, at_role):
        rows = span(at_role, blk)
        unit = unit_rows(src, emb_ref[1:2, :])
        u_s[rows, :] = unit
        qkv_s[rows, :] = dot_nn(unit, w_s[...]).astype(BF16)

    w_load.wait()
    project(x_ref[...], role)
    side.wait_recv()
    project(blocks[1], role_side)

    stores = []
    for i in range(4):
        if i < 3:
            x1_load[i + 1].start()
        x1_load[i].wait()
        if i >= 2:
            for copy in stores[i - 2]:
                copy.wait()
        unit = unit_rows(x1_s[i % 2], emb_ref[0:1, :])
        u1_s[i % 2] = unit
        qkv1_s[i % 2] = dot_nn(unit, w_s[...]).astype(BF16)
        stores.append([pltpu.make_async_copy(u1_s.at[i % 2], u1_ref.at[i * blk:(i + 1) * blk, :], out_sem.at[i % 2]),
                       pltpu.make_async_copy(qkv1_s.at[i % 2], qkv1_ref.at[i * blk:(i + 1) * blk, :], out_sem.at[2 + i % 2])])
        for copy in stores[i]:
            copy.start()

    over.wait_recv()
    last.start()
    project(blocks[0], role_over)
    last.wait_recv()
    project(blocks[2], role_last)
    keep_u = pltpu.make_async_copy(u_s, u2_ref, local_sem.at[1])
    keep_qkv = pltpu.make_async_copy(qkv_s, qkv2_ref, local_sem.at[2])
    keep_u.start()
    keep_qkv.start()

    member = [here.device(z=z // 2 * 2 + i // 2, c=i % 2) for i in range(4)]

    def c_copy(j, i):
        src = c_buf.at[j, i * blk:(i + 1) * blk, :]
        dst = c_ref.at[:, pl.ds(pl.multiple_of((role * 2 + j) * PAIR, PAIR), PAIR)]
        remote = pltpu.make_async_remote_copy(
            src_ref=src, dst_ref=dst, send_sem=c_send.at[j * 4 + i], recv_sem=c_recv.at[j * 4 + role],
            device_id=member[i], device_id_type=MESH)
        return remote, pltpu.make_async_copy(src, dst, c_recv.at[j * 4 + role])

    def send_context(j, i):
        remote, local = c_copy(j, i)
        pl.when(role == i)(local.start)
        pl.when(role != i)(remote.start)

    for j in range(2):
        v_t[...] = qkv_s[:, (4 + j) * PAIR:(5 + j) * PAIR].T
        k_view = qkv_s.at[:, (2 + j) * PAIR:(3 + j) * PAIR]
        for i in range(4):
            if i or j:
                send_context(j if i else 0, i - 1 if i else 3)
            rows = slice(i * blk, (i + 1) * blk)
            outs, sums = attend_rows(qkv_s[rows, j * PAIR:(j + 1) * PAIR], k_view, v_t, (e_a, e_b))
            c_buf[j, rows, :] = jnp.concatenate(outs, axis=0).T.astype(BF16)
            for head in range(2):
                lse_s[2 * j + head:2 * j + head + 1, rows] = sums[head]
    lse_ref[...] = lse_s[...]
    send_context(1, 3)
    for j in range(2):
        for i in range(4):
            pltpu.make_async_copy(c_buf.at[j, :blk, :], c_ref.at[:, :PAIR], c_recv.at[j * 4 + i]).wait()
            pl.when(role != i)(c_copy(j, i)[0].wait_send)
    for copy in (over, side, last):
        copy.wait_send()
    for group in stores[2:]:
        for copy in group:
            copy.wait()
    keep_u.wait()
    keep_qkv.wait()


def forward_call(x, emb, xs_1, w_qkv):
    blk, d_model = x.shape
    seq, head_cols = 4 * blk, 2 * PAIR
    anywhere = pl.BlockSpec(memory_space=pl.ANY)
    in_vmem = pl.BlockSpec(memory_space=pltpu.VMEM)
    dma = pltpu.SemaphoreType.DMA
    return pl.pallas_call(
        forward_kernel,
        in_specs=[in_vmem, in_vmem, anywhere, anywhere],
        out_specs=[anywhere, in_vmem] + [anywhere] * 4,
        out_shape=[
            jax.ShapeDtypeStruct((blk, d_model), BF16),
            jax.ShapeDtypeStruct((4, seq), F32),
        ] + [jax.ShapeDtypeStruct((seq, n), BF16) for n in (d_model, 3 * head_cols)] * 2,
        scratch_shapes=[
            pltpu.VMEM((d_model, 3 * head_cols), BF16),
            pltpu.VMEM((3, blk, d_model), BF16),
            pltpu.VMEM((seq, d_model), BF16),
            pltpu.VMEM((seq, 3 * head_cols), BF16),
            pltpu.VMEM((2, blk, d_model), BF16),
            pltpu.VMEM((2, blk, d_model), BF16),
            pltpu.VMEM((2, blk, 3 * head_cols), BF16),
            pltpu.VMEM((PAIR, seq), BF16),
            pltpu.VMEM((seq, blk), F32),
            pltpu.VMEM((seq, blk), F32),
            pltpu.VMEM((2, seq, PAIR), BF16),
            pltpu.VMEM((4, seq), F32),
            dma((3,)), dma((2,)), dma((4,)), dma((3,)), dma((3,)), dma((8,)), dma((8,)),
        ],
        compiler_params=pltpu.CompilerParams(vmem_limit_bytes=60 << 20, collective_id=2, has_side_effects=True),
        cost_estimate=pl.CostEstimate(
            flops=64 * seq * seq * PAIR, bytes_accessed=32 * seq * d_model, transcendentals=seq * seq * 4),
        name="forward",
    )(x, emb, xs_1, w_qkv)


def through_norm(values, up, d_mid):
    inverse = lax.rsqrt(jnp.mean(values * values, axis=-1, keepdims=True) + EPS_NORM)
    inner = jnp.mean(values * up, axis=-1, keepdims=True)
    return (d_mid.astype(F32) + inverse * up - values * (inverse * inverse * inverse * inner)).astype(BF16)


def backward_kernel(qkv_ref, dc_ref, lse_ref, dmid_ref, x_ref, emb_ref, wqkv_ref, u_ref,
                    d_ref, other_ref, g_ref,
                    dch, k_t, dk_acc, dv_acc, p_cat, ds_cat, d_heads, d_qkv, d_u, w_s, u_s, g_s,
                    load_sem, out_sem, dc_send, dc_recv, dq_send, dq_recv, d_send, d_recv):
    seq = qkv_ref.shape[0]
    blk = seq // 4
    head_cols = 2 * PAIR
    here = Place()
    z, core, role = here.z, here.c, here.role
    here.meet()
    member = [here.device(z=z // 2 * 2 + i // 2, c=i % 2) for i in range(4)]

    def span(index, count):
        return pl.ds(pl.multiple_of(index * count, count), count)

    def load(src, dst, n):
        copy = pltpu.make_async_copy(src, dst, load_sem.at[n])
        copy.start()
        return copy

    def dc_copy(j, i):
        col = i * head_cols + j * PAIR
        return pltpu.make_async_remote_copy(
            src_ref=dc_ref.at[:, col:col + PAIR], dst_ref=dch.at[span(role, blk), j * PAIR:(j + 1) * PAIR],
            send_sem=dc_send.at[j * 4 + i], recv_sem=dc_recv.at[j * 4 + role], device_id=member[i], device_id_type=MESH)

    for j in range(2):
        for i in range(4):
            pl.when(role != i)(dc_copy(j, i).start)
    for i in range(4):
        @pl.when(role == i)
        def _():
            dch[i * blk:(i + 1) * blk, :] = dc_ref[:, i * head_cols:(i + 1) * head_cols]

    def dq_copy(j, i, t):
        col = t * head_cols + j * PAIR
        return pltpu.make_async_remote_copy(
            src_ref=d_heads.at[i * blk:(i + 1) * blk, col:col + PAIR],
            dst_ref=d_qkv.at[:, pl.ds(pl.multiple_of(role * 3 * head_cols + col, PAIR), PAIR)],
            send_sem=dq_send.at[(j * 4 + i) * 3 + t], recv_sem=dq_recv.at[(j * 4 + role) * 3 + t],
            device_id=member[i], device_id_type=MESH)

    def send_d_heads(j):
        for i in range(4):
            @pl.when(role != i)
            def _():
                for t in range(3):
                    dq_copy(j, i, t).start()

    steps = seq // BWD_ROWS
    for j in range(2):
        for i in range(4):
            @pl.when(role != i)
            def _():
                pltpu.make_async_copy(dc_ref.at[:, :PAIR], dch.at[:blk, :PAIR], dc_recv.at[j * 4 + i]).wait()
        k_view, v_view = qkv_ref.at[:, (2 + j) * PAIR:(3 + j) * PAIR], qkv_ref.at[:, (4 + j) * PAIR:(5 + j) * PAIR]
        k_t[...] = k_view[...].T
        dk_acc[...] = jnp.zeros_like(dk_acc)
        dv_acc[...] = jnp.zeros_like(dv_acc)

        def block(i, _):
            if j == 1:
                @pl.when(i == 1)
                def _():
                    send_d_heads(0)
            rows = span(i, BWD_ROWS)
            cols = slice(j * PAIR, (j + 1) * PAIR)
            d_heads[rows, cols] = backward_rows(
                qkv_ref[rows, cols], dch[rows, cols], lse_ref[2 * j:2 * j + 2, rows], k_view, v_view,
                k_t, p_cat, ds_cat, dk_acc, dv_acc)
            return 0

        lax.fori_loop(0, steps, block, 0)
        d_heads[:, head_cols + j * PAIR:head_cols + (j + 1) * PAIR] = (dk_acc[...] * SCALE).astype(BF16)
        d_heads[:, 2 * head_cols + j * PAIR:2 * head_cols + (j + 1) * PAIR] = dv_acc[...].astype(BF16)

    quarter = u_s.shape[2]
    pending = load(u_ref.at[:, :quarter], u_s.at[0], 0)
    for i in range(4):
        @pl.when(role == i)
        def _():
            d_qkv[:, i * 3 * head_cols:(i + 1) * 3 * head_cols] = d_heads[i * blk:(i + 1) * blk, :]
    send_d_heads(1)
    stores = []
    count = u_ref.shape[1] // quarter
    for n in range(count):
        ahead = load(u_ref.at[:, (n + 1) * quarter:(n + 2) * quarter], u_s.at[(n + 1) % 2], (n + 1) % 2) if n + 1 < count else None
        pending.wait()
        if n >= 2:
            stores[n - 2].wait()
        g_s[n % 2] = dot_tn(u_s[n % 2], d_heads[...])
        stores.append(pltpu.make_async_copy(g_s.at[n % 2], g_ref.at[n * quarter:(n + 1) * quarter, :], out_sem.at[n % 2]))
        stores[n].start()
        pending = ahead
    w_rows = w_s.shape[1]
    chunks = wqkv_ref.shape[0] // w_rows
    w_load = load(wqkv_ref.at[:w_rows, :], w_s.at[0], 2)
    for j in range(2):
        for i in range(4):
            @pl.when(role != i)
            def _():
                for t in range(3):
                    pltpu.make_async_copy(d_heads.at[:blk, :PAIR], d_qkv.at[:, :PAIR], dq_recv.at[(j * 4 + i) * 3 + t]).wait()
    for n in range(chunks):
        ahead = load(wqkv_ref.at[(n + 1) * w_rows:(n + 2) * w_rows, :], w_s.at[(n + 1) % 2], 2 + (n + 1) % 2) if n + 1 < chunks else None
        w_load.wait()
        d_u[:, n * w_rows:(n + 1) * w_rows] = dot_nt(d_qkv[...], w_s[n % 2]).astype(BF16)
        w_load = ahead
    rows_each = min(128, blk)
    for n in range(blk // rows_each):
        rows = slice(n * rows_each, (n + 1) * rows_each)
        d_u[rows, :] = through_norm(x_ref[rows, :].astype(F32) + emb_ref[...], d_u[rows, :].astype(F32), dmid_ref[rows, :])
    keep = pltpu.make_async_copy(d_u, d_ref, out_sem.at[2])
    keep.start()
    stores[count - 2].wait()
    stores[count - 1].wait()
    give = pltpu.make_async_remote_copy(
        src_ref=d_u, dst_ref=other_ref, send_sem=d_send.at[0], recv_sem=d_recv.at[0],
        device_id=here.device(c=1 - core), device_id_type=MESH)
    give.start()
    for i in range(4):
        @pl.when(role != i)
        def _():
            for j in range(2):
                dc_copy(j, i).wait_send()
                for t in range(3):
                    dq_copy(j, i, t).wait_send()
    keep.wait()
    give.wait()


def backward_call(qkv, d_c, lse, d_mid, x, emb, w_qkv, u_seq):
    seq, d_model = u_seq.shape
    blk, heads3 = seq // 4, qkv.shape[1]
    anywhere = pl.BlockSpec(memory_space=pl.ANY)
    in_vmem = pl.BlockSpec(memory_space=pltpu.VMEM)
    dma = pltpu.SemaphoreType.DMA
    quarter = d_model // 4
    return pl.pallas_call(
        backward_kernel,
        in_specs=[in_vmem] * 6 + [anywhere] * 2,
        out_specs=[anywhere] * 3,
        out_shape=[
            jax.ShapeDtypeStruct((blk, d_model), BF16),
            jax.ShapeDtypeStruct((blk, d_model), BF16),
            jax.ShapeDtypeStruct((d_model, heads3), F32),
        ],
        scratch_shapes=[
            pltpu.VMEM((seq, heads3 // 3), BF16),
            pltpu.VMEM((PAIR, seq), BF16),
            pltpu.VMEM((seq, PAIR), F32),
            pltpu.VMEM((seq, PAIR), F32),
            pltpu.VMEM((seq, 2 * BWD_ROWS), BF16),
            pltpu.VMEM((seq, 2 * BWD_ROWS), BF16),
            pltpu.VMEM((seq, heads3), BF16),
            pltpu.VMEM((blk, 4 * heads3), BF16),
            pltpu.VMEM((blk, d_model), BF16),
            pltpu.VMEM((2, quarter, 4 * heads3), BF16),
            pltpu.VMEM((2, seq, quarter), BF16),
            pltpu.VMEM((2, quarter, heads3), F32),
            dma((4,)), dma((3,)), dma((8,)), dma((8,)), dma((24,)), dma((24,)), dma((1,)), dma((1,)),
        ],
        compiler_params=pltpu.CompilerParams(vmem_limit_bytes=60 << 20, collective_id=3, has_side_effects=True),
        cost_estimate=pl.CostEstimate(
            flops=160 * seq * seq * PAIR, bytes_accessed=64 * seq * d_model, transcendentals=seq * seq * 4),
        name="backward",
    )(qkv, d_c, lse, d_mid, x, emb, w_qkv, u_seq)


def rms_rows(values):
    return values * lax.rsqrt(jnp.mean(values * values, axis=-1, keepdims=True) + EPS_NORM)


GELU_IN, GELU_CUBE = math.sqrt(2 / math.pi), 0.044715


def gelu_parts(z):
    square = z * z
    t = jnp.tanh(z * (GELU_IN + (GELU_IN * GELU_CUBE) * square))
    return 0.5 + 0.5 * t, t, square


def hidden_kernel(backward, forward, *refs):
    refs = list(refs)
    take = lambda: refs.pop(0)
    if forward:
        c_ref, x_ref, emb_ref, wo_ref = take(), take(), take(), take()
        w1_ref = take()
    else:
        h_ref, wo_ref, up_ref = take(), take(), take()
    w2_ref = take()
    if backward:
        d_ref, w1b_ref = take(), take()
    if forward:
        h_out, m_out = take(), take()
        up_out, act_out = take(), take()
    if backward:
        dup_out, dmid_out, dc_out = take(), take(), take()
    else:
        x_out = take()
    if forward:
        h_s, m_s = take(), take()
    prev_s, acc = take(), take()
    step, last = pl.program_id(0), pl.num_programs(0) - 1

    if forward:
        @pl.when(step == 0)
        def _():
            h = (x_ref[...].astype(F32) + emb_ref[...] + dot_nn(c_ref[...], wo_ref[...])).astype(BF16)
            m = rms_rows(h.astype(F32)).astype(BF16)
            h_s[...], m_s[...] = h, m
            h_out[...], m_out[...] = h, m

    def first_part():
        slot = step % 2
        if backward:
            d_act = dot_nt(d_ref[...], w2_ref[...]).astype(BF16).astype(F32)
        if forward:
            up = dot_nn(m_s[...], w1_ref[...]).astype(BF16)
            up_out[...] = up
        else:
            up = up_ref[...]
        z = up.astype(F32)
        factor, t, square = gelu_parts(z)
        if forward:
            act = (z * factor).astype(BF16)
            act_out[...] = act
        if backward:
            slope = factor + z * ((1.0 - t * t) * (0.5 * GELU_IN + (1.5 * GELU_IN * GELU_CUBE) * square))
            d_up = (slope * d_act).astype(BF16)
            dup_out[...] = d_up
            prev_s[slot] = d_up
        else:
            prev_s[slot] = act

    def second_part():
        prev = prev_s[1 - step % 2]
        if backward:
            return dot_nt(prev, w1b_ref[...])
        return dot_nn(prev, w2_ref[...])

    pl.when(step == 0)(first_part)

    @pl.when(step == 1)
    def _():
        acc[...] = second_part()
        first_part()

    @pl.when(jnp.logical_and(step > 1, step < last))
    def _():
        acc[...] += second_part()
        first_part()

    @pl.when(step == last)
    def _():
        total = acc[...] + second_part()
        if backward:
            h = (h_s if forward else h_ref)[...].astype(F32)
            d_mid = through_norm(h, total.astype(BF16).astype(F32), d_ref[...])
            dmid_out[...] = d_mid
            dc_out[...] = dot_nt(d_mid, wo_ref[...]).astype(BF16)
        else:
            x_out[...] = (h_s[...].astype(F32) + total).astype(BF16)


def hidden_call(forward, backward, w_o, w_1, w_2, context=None, x=None, emb=None, h=None, up=None, d_next=None):
    blk, d_model = (context if forward else h).shape
    hidden = w_1.shape[1]
    tile = HIDDEN
    steps = hidden // tile
    now, before = (lambda i: jnp.minimum(i, steps - 1)), (lambda i: jnp.maximum(i - 1, 0))
    whole = lambda rows, cols: pl.BlockSpec((rows, cols), lambda i: (0, 0))
    wide = pl.BlockSpec((blk, tile), lambda i: (0, now(i)))
    args, specs = [], []

    def add(value, spec):
        args.append(value)
        specs.append(spec)

    if forward:
        add(context, whole(blk, d_model))
        add(x, whole(blk, d_model))
        add(emb, whole(1, d_model))
        add(w_o, whole(d_model, d_model))
        add(w_1, pl.BlockSpec((d_model, tile), lambda i: (0, now(i))))
    else:
        add(h, whole(blk, d_model))
        add(w_o, whole(d_model, d_model))
        add(up, wide)
    add(w_2, pl.BlockSpec((tile, d_model), (lambda i: (now(i), 0)) if backward else (lambda i: (before(i), 0))))
    if backward:
        add(d_next, whole(blk, d_model))
        add(w_1, pl.BlockSpec((d_model, tile), lambda i: (0, before(i))))
    row = (whole(blk, d_model), jax.ShapeDtypeStruct((blk, d_model), BF16))
    big = (wide, jax.ShapeDtypeStruct((blk, hidden), BF16))
    outs = ([row, row, big, big] if forward else []) + ([big, row, row] if backward else [row])
    return pl.pallas_call(
        functools.partial(hidden_kernel, backward, forward),
        grid=(steps + 1,),
        in_specs=specs,
        out_specs=[spec for spec, _ in outs],
        out_shape=[shape for _, shape in outs],
        scratch_shapes=([pltpu.VMEM((blk, d_model), BF16)] * 2 if forward else [])
        + [pltpu.VMEM((2, blk, tile), BF16), pltpu.VMEM((blk, d_model), F32)],
        compiler_params=pltpu.CompilerParams(vmem_limit_bytes=60 << 20),
        cost_estimate=pl.CostEstimate(
            flops=2 * blk * d_model * (hidden * (3 if forward and backward else 2) + 2 * d_model),
            bytes_accessed=4 * hidden * d_model + 8 * blk * hidden, transcendentals=blk * hidden),
        interpret=INTERPRET,
        name="hidden",
    )(*args)


def grad_kernel(by_left, _, *refs):
    lefts, rights, (away_ref, mid_ref, keep_ref, left_t, right_s) = refs[:16], refs[16:20], refs[20:]
    count, piece = lefts[0].shape
    step = pl.program_id(0)

    @pl.when(step == 0 if not by_left else step >= 0)
    def _():
        for i in range(16):
            left_t[i % 4 * piece:(i % 4 + 1) * piece, i // 4 * count:(i // 4 + 1) * count] = lefts[i][...].T

    @pl.when(step == 0 if by_left else step >= 0)
    def _():
        for i in range(4):
            right_s[i * count:(i + 1) * count, :] = rights[i][...]

    total = dot_nn(left_t[...], right_s[...])
    away_ref[0] = total[:2 * piece]
    mid_ref[0] = total[2 * piece:3 * piece]
    keep_ref[0] = total[3 * piece:]


def grad_products(order, lefts, rights, by_left=False):
    count = rights[0].shape[0]
    tile = rights[0].shape[1] // (1 if by_left else 4)
    piece = lefts[0].shape[1] // (32 if by_left else 8)
    if by_left:
        left_spec = lambda n: pl.BlockSpec((count, piece), lambda i, order: (0, i * 8 + order[n]))
        right_spec = pl.BlockSpec((count, tile), lambda i, order: (0, 0))
    else:
        left_spec = lambda n: pl.BlockSpec((count, piece), lambda i, order: (0, order[n]))
        right_spec = pl.BlockSpec((count, tile), lambda i, order: (0, i))
    return pl.pallas_call(
        functools.partial(grad_kernel, by_left),
        grid_spec=pltpu.PrefetchScalarGridSpec(
            num_scalar_prefetch=1,
            grid=(4,),
            in_specs=[left_spec(n) for _ in range(4) for n in range(4)] + [right_spec] * 4,
            out_specs=[pl.BlockSpec((1, n * piece, tile), lambda i, order: (i, 0, 0)) for n in (2, 1, 1)],
            scratch_shapes=[pltpu.VMEM((4 * piece, 4 * count), BF16), pltpu.VMEM((4 * count, tile), BF16)],
        ),
        out_shape=[jax.ShapeDtypeStruct((4, n * piece, tile), F32) for n in (2, 1, 1)],
        compiler_params=pltpu.CompilerParams(vmem_limit_bytes=60 << 20),
        cost_estimate=pl.CostEstimate(
            flops=128 * count * piece * tile, bytes_accessed=8 * count * (4 * piece + 4 * tile) + 64 * piece * tile,
            transcendentals=0),
        interpret=INTERPRET,
        name="grad",
    )(order, *[left for left in lefts for _ in range(4)], *rights)


def backward_rows(q, d_out, lse, k_ref, v_ref, k_t, p_cat, ds_cat, dk_acc, dv_acc):
    block = q.shape[0]
    lane = lax.broadcasted_iota(jnp.int32, q.shape, 1)
    q_heads, do_heads, dqs = [], [], []
    for head in range(2):
        mine = lane // HEAD_DIM == head
        q_head = jnp.where(mine, q, jnp.zeros_like(q))
        do_head = jnp.where(mine, d_out, jnp.zeros_like(d_out))
        scores = dot_nt(k_ref[...], q_head)
        probs = jnp.exp2(scores * EXP2_SCALE - lse[head:head + 1, :])
        d_probs = dot_nt(v_ref[...], do_head).astype(BF16).astype(F32)
        inner = jnp.sum(probs * d_probs, axis=0, keepdims=True)
        cols = slice(head * block, (head + 1) * block)
        p_cat[:, cols] = probs.astype(BF16)
        ds_cat[:, cols] = (probs * (d_probs - inner)).astype(BF16)
        dqs.append(dot_nn(k_t[head * HEAD_DIM:(head + 1) * HEAD_DIM, :], ds_cat[:, cols]))
        q_heads.append(q_head)
        do_heads.append(do_head)
    dv_acc[...] += dot_nn(p_cat[...], jnp.concatenate(do_heads, axis=0))
    dk_acc[...] += dot_nn(ds_cat[...], jnp.concatenate(q_heads, axis=0))
    return (jnp.concatenate(dqs, axis=0).T * SCALE).astype(BF16)


def last_kernel(qkv_ref, dc_ref, lse_ref, dmid_ref, x_ref, emb_ref, wqkv_ref, u_ref, gqkv2_ref,
                r2_ref, mid2_ref, keep2_ref, *refs):
    lefts = {'1': refs[:4], 'o': refs[8:12]}
    rights = {'1': refs[4:8], 'o': refs[12:16]}
    (dx_ref, g1_ref, g2_ref, go_ref, gq_ref, gk_ref, gv_ref, away1_ref, mid1_ref, keep1_ref, awayo_ref, mido_ref, keepo_ref,
     dch, k_t, dk_acc, dv_acc, p_cat, ds_cat, d_heads, d_qkv, buf, buf_o, second, second_o, tmp, tmp_o,
     third, third_o, sum_1, sum_2, sum_o, qa, qb, q1, q2, q3, q4, d_1, w_s, u_s, g_s,
     left_t, stage,
     local_sem, load_sem, send_sem, recv_sem, dc_send, dc_recv, dq_send, dq_recv, z_send, z_recv, x_send, x_recv,
     p_send, p_recv) = refs[16:]
    seq = qkv_ref.shape[0]
    blk = seq // 4
    head_cols = 2 * PAIR
    here = Place()
    z, core, role, owner = here.z, here.c, here.role, here.owner
    here.meet()
    copies = Copies(send_sem, recv_sem)
    waits = []

    def span(index, count):
        return pl.ds(pl.multiple_of(index * count, count), count)

    def load(src, dst, n):
        copy = pltpu.make_async_copy(src, dst, load_sem.at[n])
        copy.start()
        return copy

    no = jnp.logical_not
    to_a, to_b = here.device(y=here.ya, x=here.xa), here.device(y=here.yb, x=here.xb)
    partner = here.device(c=1 - core)
    member = [here.device(z=z // 2 * 2 + i // 2, c=i % 2) for i in range(4)]
    piece = tmp.shape[1]

    def dc_copy(i):
        return pltpu.make_async_remote_copy(
            src_ref=dc_ref.at[:, i * head_cols:(i + 1) * head_cols], dst_ref=dch.at[span(role, blk), :],
            send_sem=dc_send.at[i], recv_sem=dc_recv.at[role], device_id=member[i], device_id_type=MESH)

    for i in range(4):
        pl.when(role != i)(dc_copy(i).start)

        @pl.when(role == i)
        def _():
            dch[i * blk:(i + 1) * blk, :] = dc_ref[:, i * head_cols:(i + 1) * head_cols]

    half = rights['1'][0].shape[1] // 8
    firsts = {('1', q): [copies.make(away1_ref.at[q, :, h * half:(h + 1) * half], buf.at[4 + q, :, h * half:(h + 1) * half], to_a)
                         for h in range(2)] for q in range(4)}
    firsts['o'] = [copies.make(awayo_ref.at[2 * h:2 * h + 2], buf_o.at[2 * h:2 * h + 2], to_a) for h in range(2)]
    w2_loads = [load(r2_ref.at[q], buf.at[q], q) for q in range(4)]
    seconds = {(w, q): copies.make(buf.at[u + q, piece:, :], second.at[u + q], to_b) for w, u in (('2', 0), ('1', 4)) for q in range(4)}
    seconds['o'] = copies.make(buf_o.at[:, piece:, :], second_o, to_b)

    def add_mid(unit):
        if unit == 'o':
            mid, keep, t, n = mido_ref, keepo_ref, tmp_o, 4
            bottom, top = buf_o.at[:, piece:, :], buf_o.at[:, :piece, :]
        else:
            w, q = unit
            mid, keep = (mid2_ref.at[q], keep2_ref.at[q]) if w == '2' else (mid1_ref.at[q], keep1_ref.at[q])
            u = q if w == '2' else 4 + q
            t, n, bottom, top = tmp, 6, buf.at[u, piece:, :], buf.at[u, :piece, :]
        loads = [load(mid, t.at[0], n), load(keep, t.at[1], n + 1)]
        if unit == 'o' or unit[0] == '1':
            for copy in firsts[unit]:
                copy.wait_recv()
        else:
            w2_loads[unit[1]].wait()
        for copy in loads:
            copy.wait()
        bottom[...] += t[0]
        top[...] += t[1]
        seconds[unit].start()

    def z_copy(unit, q):
        if unit == 'o':
            src, dst, n = buf_o.at[q, :piece, :], third_o.at[z], 8
        else:
            w = 0 if unit == '2' else 1
            src, dst, n = buf.at[4 * w + q, :piece, :], third.at[w, z], 4 * w
        return pltpu.make_async_remote_copy(
            src_ref=src, dst_ref=dst, send_sem=z_send.at[n + q], recv_sem=z_recv.at[n + z],
            device_id=here.device(z=q), device_id_type=MESH)

    def finish(unit):
        seconds[unit].wait_recv()
        if unit == 'o':
            buf_o[:, :piece, :] += second_o[...]
            for q in range(4):
                pl.when(z != q)(z_copy('o', q).start)
        else:
            w, q = unit
            u = q if w == '2' else 4 + q
            buf[u, :piece, :] += second[u]
            pl.when(z != q)(z_copy(w, q).start)

    mine, by_a = here.piece(here.y, here.x), here.piece(here.ya, here.xa)
    by_b, by_ab = here.piece(here.yb, here.xb), here.piece(1 - here.y, 1 - here.x)
    gathers = {}

    def total(unit):
        out, got, n = {'2': (sum_2, third.at[0], 0), '1': (sum_1, third.at[1], 4), 'o': (sum_o, third_o, 8)}[unit]
        if unit == 'o':
            out[...] = buf_o[z, :piece, :]
        else:
            out[...] = buf[n + z, :piece, :]
        for zz in range(4):
            @pl.when(z != zz)
            def _():
                pltpu.make_async_copy(out, got.at[zz], z_recv.at[n + zz]).wait()
                out[...] += got[zz]

    def gather_start(name, src, out, n):
        rows = lambda e: out.at[span(e, piece), :]
        keep = pltpu.make_async_copy(src, rows(mine), local_sem.at[n])
        keep.start()
        waits.append(keep)
        gathers[name] = dict(src=src, rows=rows, a=copies.start(src, rows(mine), to_a), b1=copies.start(src, rows(mine), to_b))

    def gather_second(name):
        g = gathers[name]
        g['a'].wait_recv()
        g['b2'] = copies.start(g['rows'](by_a), g['rows'](by_a), to_b)

    def gather_core(name):
        g = gathers[name]
        g['c'] = [copies.start(g['src'], g['rows'](mine), partner), copies.start(g['rows'](by_a), g['rows'](by_a), partner)]
        g['b1'].wait_recv()
        g['c'].append(copies.start(g['rows'](by_b), g['rows'](by_b), partner))
        g['b2'].wait_recv()
        g['c'].append(copies.start(g['rows'](by_ab), g['rows'](by_ab), partner))

    def dq_copy(j, i, t):
        col = t * head_cols + j * PAIR
        return pltpu.make_async_remote_copy(
            src_ref=d_heads.at[i * blk:(i + 1) * blk, col:col + PAIR],
            dst_ref=d_qkv.at[:, pl.ds(pl.multiple_of(role * 3 * head_cols + col, PAIR), PAIR)],
            send_sem=dq_send.at[(j * 4 + i) * 3 + t], recv_sem=dq_recv.at[(j * 4 + role) * 3 + t],
            device_id=member[i], device_id_type=MESH)

    def send_d_heads(j):
        for i in range(4):
            @pl.when(role != i)
            def _():
                for t in range(3):
                    dq_copy(j, i, t).start()

    index = [here.ya * 2 + here.xa, (1 - here.y) * 2 + 1 - here.x, here.yb * 2 + here.xb, here.y * 2 + here.x]
    spaces = (p_cat, ds_cat)
    parts = [('1', n) for n in range(8)] + [('o', n) for n in range(2)]

    def load_lefts(name):
        for n in range(16):
            pltpu.make_async_copy(
                lefts[name][n // 4].at[:, span(index[n % 4] * 2 + core, piece)],
                d_heads.at[n // 4 * blk:(n // 4 + 1) * blk, n % 4 * piece:(n % 4 + 1) * piece], load_sem.at[14]).start()

    def load_rights(s):
        name, n = parts[s]
        for i in range(4):
            pltpu.make_async_copy(
                rights[name][i].at[:, n * half:(n + 1) * half], spaces[s % 2].at[i * blk:(i + 1) * blk, :],
                load_sem.at[15 + s % 2]).start()

    def stored(s):
        pltpu.make_async_copy(stage.at[s % 2], stage.at[s % 2], load_sem.at[17 + s % 2]).wait()

    def send_part(s):
        name, n = parts[s]
        if name == '1':
            firsts[('1', n // 2)][n % 2].start()
        else:
            firsts['o'][n].start()

    load_lefts('1')
    load_rights(0)
    for s in range(len(parts)):
        name, n = parts[s]
        if n == 0:
            every = d_heads.at[:, :4 * piece]
            pltpu.make_async_copy(every, every, load_sem.at[14]).wait()
            left_t[...] = every[...].T
            if name == '1':
                load_lefts('o')
        if s + 1 < len(parts):
            load_rights(s + 1)
        space = spaces[s % 2]
        pltpu.make_async_copy(space, space, load_sem.at[15 + s % 2]).wait()
        if s >= 1:
            stored(s - 1)
            send_part(s - 1)
        stage[s % 2] = dot_nn(left_t[...], space[...])
        if s < 8 and s % 2 == 1:
            add_mid(('2', s // 2))
        for row, ref in ((0, (away1_ref, awayo_ref)), (2 * piece, (mid1_ref, mido_ref)), (3 * piece, (keep1_ref, keepo_ref))):
            count = 2 * piece if row == 0 else piece
            rows = slice(row, row + count)
            if name == '1':
                pltpu.make_async_copy(stage.at[s % 2, rows, :], ref[0].at[n // 2, :, n % 2 * half:(n % 2 + 1) * half],
                                      load_sem.at[17 + s % 2]).start()
            else:
                for k in range(2):
                    pltpu.make_async_copy(stage.at[s % 2, rows, k * (half // 2):(k + 1) * (half // 2)], ref[1].at[2 * n + k],
                                          load_sem.at[17 + s % 2]).start()
    stored(len(parts) - 1)
    send_part(len(parts) - 1)

    for i in range(4):
        @pl.when(role != i)
        def _():
            pltpu.make_async_copy(dc_ref.at[:, :head_cols], dch.at[:blk, :], dc_recv.at[i]).wait()

    moves = {(0, 1): [(finish, ('2', 0))], (0, 4): [(finish, ('2', 1)), (add_mid, ('1', 0))], (0, 7): [(finish, ('2', 2))],
             (1, 0): [(send_d_heads, 0)], (1, 2): [(finish, ('2', 3)), (add_mid, ('1', 1))], (1, 4): [(finish, ('1', 0))],
             (1, 6): [(add_mid, ('1', 2))]}
    steps = seq // BWD_ROWS
    for j in range(2):
        k_view, v_view = qkv_ref.at[:, (2 + j) * PAIR:(3 + j) * PAIR], qkv_ref.at[:, (4 + j) * PAIR:(5 + j) * PAIR]
        k_t[...] = k_view[...].T
        dk_acc[...] = jnp.zeros_like(dk_acc)
        dv_acc[...] = jnp.zeros_like(dv_acc)

        def block(i, _):
            for n in range(8):
                if (j, n) in moves:
                    @pl.when(i == min(n, steps - 1))
                    def _():
                        for move, what in moves[(j, n)]:
                            move(what)
            rows = span(i, BWD_ROWS)
            cols = slice(j * PAIR, (j + 1) * PAIR)
            d_heads[rows, cols] = backward_rows(
                qkv_ref[rows, cols], dch[rows, cols], lse_ref[2 * j:2 * j + 2, rows], k_view, v_view,
                k_t, p_cat, ds_cat, dk_acc, dv_acc)
            return 0

        lax.fori_loop(0, steps, block, 0)
        d_heads[:, head_cols + j * PAIR:head_cols + (j + 1) * PAIR] = (dk_acc[...] * SCALE).astype(BF16)
        d_heads[:, 2 * head_cols + j * PAIR:2 * head_cols + (j + 1) * PAIR] = dv_acc[...].astype(BF16)

    quarter = 2 * piece

    def quarter_loads(n):
        return [load(u_ref.at[:, span(index[n], quarter)], u_s.at[n % 2], 8 + n % 2),
                load(gqkv2_ref.at[span(index[n], quarter), :], g_s.at[n % 2], 10 + n % 2)]

    pending = quarter_loads(0)
    for i in range(4):
        @pl.when(role == i)
        def _():
            d_qkv[:, i * 3 * head_cols:(i + 1) * 3 * head_cols] = d_heads[i * blk:(i + 1) * blk, :]
    send_d_heads(1)
    targets = [qa.at[0], qa.at[1], qb.at[0], qb.at[1]]
    first_q = None
    for n in range(4):
        ahead = quarter_loads(n + 1) if n < 3 else []
        for copy in pending:
            copy.wait()
        targets[n][...] = dot_tn(u_s[n % 2], d_heads[...]) + g_s[n % 2]
        pending = ahead
        if n == 2:
            first_q = copies.start(qa, q1, to_a)

    add_mid(('1', 3))
    w_rows = w_s.shape[1]
    chunks = wqkv_ref.shape[0] // w_rows
    w_load = load(wqkv_ref.at[:w_rows, :], w_s.at[0], 12)
    for j in range(2):
        for i in range(4):
            @pl.when(role != i)
            def _():
                for t in range(3):
                    pltpu.make_async_copy(d_heads.at[:blk, :PAIR], d_qkv.at[:, :PAIR], dq_recv.at[(j * 4 + i) * 3 + t]).wait()
    for n in range(chunks):
        ahead = load(wqkv_ref.at[(n + 1) * w_rows:(n + 2) * w_rows, :], w_s.at[(n + 1) % 2], 12 + (n + 1) % 2) if n + 1 < chunks else None
        w_load.wait()
        d_1[:, n * w_rows:(n + 1) * w_rows] = dot_nt(d_qkv[...], w_s[n % 2]).astype(BF16)
        w_load = ahead

    count = min(128, blk)
    for n in range(blk // count):
        rows = slice(n * count, (n + 1) * count)
        d_1[rows, :] = through_norm(x_ref[rows, :].astype(F32) + emb_ref[...], d_1[rows, :].astype(F32), dmid_ref[rows, :])

    own_seq = z // 2
    rows_dx = span(role, blk)

    def dx_copy(n, device):
        slot = [0, 1 + core, 3 + core][n]
        return pltpu.make_async_remote_copy(
            src_ref=d_1, dst_ref=dx_ref.at[rows_dx, :], send_sem=x_send.at[n], recv_sem=x_recv.at[slot],
            device_id=device, device_id_type=MESH)

    dx_side = dx_copy(0, partner)
    dx_next = dx_copy(1, here.device(z=here.z_by[1], c=own_seq))
    dx_cross = dx_copy(2, here.device(z=here.z_by[2], c=own_seq))
    dx_keep = pltpu.make_async_copy(d_1, dx_ref.at[rows_dx, :], local_sem.at[8])

    def dx_pass(cc):
        rows = span(z % 2 * 2 + cc, blk)
        return pltpu.make_async_remote_copy(
            src_ref=dx_ref.at[rows, :], dst_ref=dx_ref.at[rows, :], send_sem=x_send.at[3 + cc], recv_sem=x_recv.at[5 + cc],
            device_id=here.device(z=here.z_by[1]), device_id_type=MESH)

    add_mid('o')
    dx_cross.start()
    dx_next.start()
    pl.when(owner)(dx_keep.start)
    pl.when(no(owner))(dx_side.start)

    def dx_got(slot):
        pltpu.make_async_copy(d_1, dx_ref.at[:blk, :], x_recv.at[slot]).wait()

    first_q.wait_recv()
    qb[0] += q1[1]
    qb[1] += q1[0]
    second_q = copies.start(qb.at[0], q2, to_b)
    finish(('1', 1))
    total('2')
    finish(('1', 2))
    gather_start('2', sum_2, g2_ref, 0)
    finish(('1', 3))
    finish('o')
    second_q.wait_recv()
    qb[1] += q2[...]
    plane_stays = jnp.logical_and(2 * (z % 2) + core == z, z // 2 == core)
    plane_q = pltpu.make_async_remote_copy(
        src_ref=qb.at[1], dst_ref=q3, send_sem=p_send.at[0], recv_sem=p_recv.at[0],
        device_id=here.device(z=2 * (z % 2) + core, c=z // 2), device_id_type=MESH)

    @pl.when(plane_stays)
    def _():
        q3[...] = qb[1]

    pl.when(no(plane_stays))(plane_q.start)
    gather_second('2')

    @pl.when(no(owner))
    def _():
        for cc in range(2):
            dx_got(3 + cc)
            dx_pass(cc).start()

    total('1')
    total('o')
    gather_start('1', sum_1, g1_ref, 1)
    gather_start('o', sum_o, go_ref, 2)
    gather_core('2')
    pl.when(no(plane_stays))(plane_q.wait_recv)
    give_q = copies.start(q3.at[span(1 - core, piece), :], q4.at[0], partner)
    gather_second('1')
    gather_second('o')
    give_q.wait_recv()
    q4[1] = q4[0] + q3[span(core, piece), :]
    for t, (name, out) in enumerate((('q', gq_ref), ('k', gk_ref), ('v', gv_ref))):
        gather_start(name, q4.at[1, :, t * head_cols:(t + 1) * head_cols], out, 3 + t)
    gather_core('1')
    gather_core('o')
    for name in 'qkv':
        gather_second(name)
    for name in 'qkv':
        gather_core(name)

    @pl.when(owner)
    def _():
        for slot in (0, 1, 2):
            dx_got(slot)
        dx_keep.wait()

    @pl.when(no(owner))
    def _():
        dx_side.wait_send()
        for cc in range(2):
            dx_got(5 + cc)
            dx_pass(cc).wait_send()

    for g in gathers.values():
        for copy in g['c']:
            copy.wait_recv()
    for copy in waits:
        copy.wait()
    for copy in copies.sent:
        copy.wait_send()
    dx_cross.wait_send()
    dx_next.wait_send()
    pl.when(no(plane_stays))(plane_q.wait_send)
    for i in range(4):
        @pl.when(role != i)
        def _():
            dc_copy(i).wait_send()
            for j in range(2):
                for t in range(3):
                    dq_copy(j, i, t).wait_send()

        for unit in '21o':
            pl.when(z != i)(z_copy(unit, i).wait_send)


def last_call(qkv, d_c, lse, d_mid, x, emb, w_qkv, u_seq, g_qkv, w2_parts, w1_sides, wo_sides):
    seq, d_model = u_seq.shape
    blk, piece = seq // 4, d_model // 8
    n1, no = w1_sides[4].shape[1] // 4, wo_sides[4].shape[1] // 4
    assert n1 == 2 * 2 * BWD_ROWS and no * 2 == 2 * BWD_ROWS
    assert w2_parts[0].shape[1:] == (2 * piece, n1)
    heads3 = qkv.shape[1]
    anywhere = pl.BlockSpec(memory_space=pl.ANY)
    in_vmem = pl.BlockSpec(memory_space=pltpu.VMEM)
    copies = 10 + 9 + 6 * 7 + 3
    dma = pltpu.SemaphoreType.DMA
    w_rows = min(128, d_model)
    return pl.pallas_call(
        last_kernel,
        in_specs=[in_vmem] * 6 + [anywhere] * 22,
        out_specs=[anywhere] * 13,
        out_shape=[
            jax.ShapeDtypeStruct((seq, d_model), BF16),
            jax.ShapeDtypeStruct((d_model, n1), F32),
            jax.ShapeDtypeStruct((8 * piece, n1), F32),
            jax.ShapeDtypeStruct((d_model, no), F32),
        ] + [jax.ShapeDtypeStruct((d_model, heads3 // 3), F32)] * 3
        + [jax.ShapeDtypeStruct((4, k * piece, n), F32) for n in (n1, no) for k in (2, 1, 1)],
        scratch_shapes=[
            pltpu.VMEM((seq, heads3 // 3), BF16),
            pltpu.VMEM((PAIR, seq), BF16),
            pltpu.VMEM((seq, PAIR), F32),
            pltpu.VMEM((seq, PAIR), F32),
            pltpu.VMEM((seq, 2 * BWD_ROWS), BF16),
            pltpu.VMEM((seq, 2 * BWD_ROWS), BF16),
            pltpu.VMEM((seq, heads3), BF16),
            pltpu.VMEM((blk, 4 * heads3), BF16),
            pltpu.VMEM((8, 2 * piece, n1), F32),
            pltpu.VMEM((4, 2 * piece, no), F32),
            pltpu.VMEM((8, piece, n1), F32),
            pltpu.VMEM((4, piece, no), F32),
            pltpu.VMEM((2, piece, n1), F32),
            pltpu.VMEM((2, 4, piece, no), F32),
            pltpu.VMEM((2, 4, piece, n1), F32),
            pltpu.VMEM((4, piece, no), F32),
            pltpu.VMEM((piece, n1), F32),
            pltpu.VMEM((piece, n1), F32),
            pltpu.VMEM((piece, no), F32),
            pltpu.VMEM((2, 2 * piece, heads3), F32),
            pltpu.VMEM((2, 2 * piece, heads3), F32),
            pltpu.VMEM((2, 2 * piece, heads3), F32),
            pltpu.VMEM((2 * piece, heads3), F32),
            pltpu.VMEM((2 * piece, heads3), F32),
            pltpu.VMEM((2, piece, heads3), F32),
            pltpu.VMEM((blk, d_model), BF16),
            pltpu.VMEM((2, w_rows, 4 * heads3), BF16),
            pltpu.VMEM((2, seq, 2 * piece), BF16),
            pltpu.VMEM((2, 2 * piece, heads3), F32),
            pltpu.VMEM((4 * piece, seq), BF16),
            pltpu.VMEM((2, 4 * piece, 2 * BWD_ROWS), F32),
            dma((9,)), dma((19,)), dma((copies,)), dma((copies,)),
            dma((4,)), dma((4,)), dma((24,)), dma((24,)), dma((12,)), dma((12,)), dma((5,)), dma((7,)), dma((1,)), dma((1,)),
        ],
        compiler_params=pltpu.CompilerParams(vmem_limit_bytes=63 << 20, collective_id=1, has_side_effects=True),
        cost_estimate=pl.CostEstimate(
            flops=160 * seq * seq * PAIR, bytes_accessed=128 * seq * d_model, transcendentals=seq * seq * 4),
        name="last",
    )(qkv, d_c, lse, d_mid, x, emb, w_qkv, u_seq, g_qkv, *w2_parts, *w1_sides, *wo_sides)[:7]


def lin(z, y, x, c):
    return z * 8 + y * 4 + x * 2 + c


def send(value, to):
    pairs = []
    for z in range(4):
        for y in range(2):
            for x in range(2):
                for c in range(2):
                    dst = to(z, y, x, c)
                    if dst is not None:
                        pairs.append((lin(z, y, x, c), lin(*dst)))
    return lax.ppermute(value, AXES, pairs)


def other_core(z, y, x, c):
    return (z, y, x, 1 - c)


def swap_first(z, y, x, c):
    return (z, y, 1 - x, c) if c == 0 else (z, 1 - y, x, c)


def rows_of(value, index, count):
    return lax.dynamic_slice_in_dim(value, index * count, count, axis=0)


def solution(mesh):
    spec_col = P(None, 'model')
    spec_row = P('model', None)
    spec_act = P('data', None, None)
    spec_rep = P(None, None)

    def device_step(x_in, cot_out, step_emb, w_q, w_k, w_v, w_o, w_1, w_2):
        seq, d_model = x_in.shape[1:]
        blk = seq // 4
        z = lax.axis_index('model')
        d = lax.axis_index('data')
        y, x, core = d // 4, d // 2 % 2, d % 2
        role = z % 2 * 2 + core
        owner = core == z // 2
        emb = step_emb.astype(F32)

        c_1, lse_1, x_seq, cot, wo, w1, w2, w_qkv = first_call(
            x_in[0], cot_out[0], emb[:1], w_q, w_k, w_v, w_o, w_1, w_2)
        wo, w2 = wo.reshape(-1, d_model), w2.reshape(-1, d_model)
        x_1 = rows_of(x_seq, role, blk)

        h_1, m_1, up_1, act_1, x_2 = hidden_call(True, False, wo, w1, w2, context=c_1, x=x_1, emb=emb[:1])

        c_2, lse_2, u_2_seq, qkv_2, u_1_seq, qkv_1 = forward_call(x_2, emb, x_seq, w_qkv)
        _, m_2, _, act_2, d_up_2, d_mid_2, d_c = hidden_call(True, True, wo, w1, w2, context=c_2, x=x_2, emb=emb[1:], d_next=cot)
        d_2, d_2_other, g_qkv_2 = backward_call(
            qkv_2, d_c, lse_2, d_mid_2, x_2, emb[1:], w_qkv, u_2_seq)

        first, second = jnp.where(core == 0, x, y), jnp.where(core == 0, y, x)

        def at(i, j):
            return jnp.where(core == 0, j * 2 + i, i * 2 + j)

        order = [at(1 - first, second), at(1 - first, 1 - second), at(first, 1 - second), at(first, second)]
        column = jnp.stack(order) * 2 + core

        def both_cores(sides):
            lefts, rights = [], []
            for left, right in sides:
                lefts += [left, send(left, other_core)]
                rights += [right, send(right, other_core)]
            return lefts, rights

        lefts, rights = both_cores([(act_2, cot)])
        lefts += [act_1, send(act_1, other_core)]
        rights += [d_2, d_2_other]
        away, mid, keep = grad_products(column, lefts, rights, True)
        d_2, away = lax.optimization_barrier((d_2, away))
        w2_parts = (send(away, swap_first), mid, keep)
        d_up_1, d_mid_1, d_c = hidden_call(False, True, wo, w1, w2, h=h_1, up=up_1, d_next=d_2)
        w1_sides = sum(both_cores([(m_2, d_up_2), (m_1, d_up_1)]), [])
        wo_sides = sum(both_cores([(d_mid_2, c_2), (d_mid_1, c_1)]), [])
        d_x, g_w1, g_w2, g_wo, g_q, g_k, g_v = last_call(
            qkv_1, d_c, lse_1, d_mid_1, x_1, emb[:1], w_qkv, u_1_seq, g_qkv_2, w2_parts, w1_sides, wo_sides)
        return g_q, g_k, g_v, g_wo.T, g_w1, g_w2, d_x[None]

    return jax.shard_map(device_step, mesh=mesh,
                         in_specs=(spec_act, spec_act, spec_rep, spec_col, spec_col, spec_col, spec_row, spec_col, spec_row),
                         out_specs=(spec_col, spec_col, spec_col, spec_row, spec_col, spec_row, spec_act),
                         check_vma=False)
```

```python
import functools
import math

import jax
import jax.numpy as jnp
from jax import lax
from jax.experimental import pallas as pl
from jax.experimental.pallas import tpu as pltpu
from jax.sharding import PartitionSpec as P


HEAD_DIM = 64
EPS_NORM = 1e-6
SCALE = HEAD_DIM ** -0.5
EXP2_SCALE = SCALE * math.log2(math.e)
PAIR = 2 * HEAD_DIM
FWD_ROWS = 512
BWD_ROWS = 256
KEYS = 256
HIDDEN = 512
INTERPRET = False
AXES = ('model', 'data')
BF16 = jnp.bfloat16
F32 = jnp.float32
MESH = pl.DeviceIdType.MESH

def rms_norm(values):
    return values * lax.rsqrt(jnp.mean(values * values, axis=-1, keepdims=True) + EPS_NORM)


def dot_nt(a, b):
    return lax.dot_general(a, b, (((1,), (1,)), ((), ())), preferred_element_type=F32)


def dot_nn(a, b):
    return lax.dot_general(a, b, (((1,), (0,)), ((), ())), preferred_element_type=F32)


def dot_tn(a, b):
    return lax.dot_general(a, b, (((0,), (0,)), ((), ())), preferred_element_type=F32)


def attend_rows(q, k_ref, v_t, e_refs):
    count = k_ref.shape[0] // KEYS
    lane = lax.broadcasted_iota(jnp.int32, q.shape, 1)
    q_heads = [jnp.where(lane // HEAD_DIM == head, q, jnp.zeros_like(q)) for head in range(2)]
    tops, run, total, outs, sums = [[], []], [None, None], [None, None], [], []
    for j in range(count):
        keys = slice(j * KEYS, (j + 1) * KEYS)
        for head in range(2):
            scores = dot_nt(k_ref[keys, :], q_heads[head])
            top = jnp.max(scores, axis=0, keepdims=True) * EXP2_SCALE
            if j:
                top = jnp.maximum(top, run[head])
            weights = jnp.exp2(scores * EXP2_SCALE - top)
            part = jnp.sum(weights, axis=0, keepdims=True)
            total[head] = total[head] * jnp.exp2(run[head] - top) + part if j else part
            run[head] = top
            tops[head].append(top)
            e_refs[head][keys, :] = weights
    for head in range(2):
        inverse = 1.0 / total[head]
        out = None
        for j in range(count):
            keys = slice(j * KEYS, (j + 1) * KEYS)
            factor = inverse * jnp.exp2(tops[head][j] - run[head])
            probs = (e_refs[head][keys, :] * factor).astype(BF16)
            part = dot_nn(v_t[head * HEAD_DIM:(head + 1) * HEAD_DIM, keys], probs)
            out = out + part if j else part
        sums.append(run[head] + jnp.log2(total[head]))
        outs.append(out)
    return outs, sums


class Place:
    def __init__(self):
        self.z = lax.axis_index('model')
        d = lax.axis_index('data')
        self.y, self.x, self.c = d // 4, d // 2 % 2, d % 2
        z = self.z
        self.z_by = {1: z + 1 - 2 * (z % 2), 2: (z + 2) % 4, 3: 3 - z}
        x, y, c = self.x, self.y, self.c
        self.xa, self.ya = x + (1 - c) * (1 - 2 * x), y + c * (1 - 2 * y)
        self.xb, self.yb = x + c * (1 - 2 * x), y + (1 - c) * (1 - 2 * y)
        self.role = z % 2 * 2 + c
        self.owner = c == z // 2

    def piece(self, y, x, c=None):
        return y * 4 + x * 2 + (self.c if c is None else c)

    def device(self, z=None, y=None, x=None, c=None):
        z, y, x, c = (own if given is None else given for given, own in zip((z, y, x, c), (self.z, self.y, self.x, self.c)))
        return {'model': z, 'data': y * 4 + x * 2 + c}

    def peers(self):
        column = [self.device(z=z, c=c) for z in (self.z, *self.z_by.values()) for c in (self.c, 1 - self.c)][1:]
        return column + [self.device(x=1 - self.x), self.device(y=1 - self.y)]

    def meet(self):
        barrier = pltpu.get_barrier_semaphore()
        peers = self.peers()
        for peer in peers:
            pl.semaphore_signal(barrier, inc=1, device_id=peer, device_id_type=MESH)
        pl.semaphore_wait(barrier, len(peers))


class Copies:
    def __init__(self, send_sem, recv_sem):
        self.send_sem, self.recv_sem, self.used, self.sent = send_sem, recv_sem, 0, []

    def make(self, src, dst, device):
        n, self.used = self.used, self.used + 1
        copy = pltpu.make_async_remote_copy(
            src_ref=src, dst_ref=dst, send_sem=self.send_sem.at[n], recv_sem=self.recv_sem.at[n],
            device_id=device, device_id_type=MESH)
        self.sent.append(copy)
        return copy

    def start(self, src, dst, device):
        copy = self.make(src, dst, device)
        copy.start()
        return copy


def first_kernel(x_ref, cot_ref, emb_ref, wq_ref, wk_ref, wv_ref, wo_ref, w1_ref, w2_ref,
                 c1_ref, lse_ref, xs_ref, cot_loc_ref, full_o, full_1, full_2, full_qkv,
                 qkv_s, vt_s, e_a, e_b, c_buf, lse_s, cot_s, local_sem, send_sem, recv_sem, c_send, c_recv, one_send, one_recv):
    seq, d_model = x_ref.shape
    blk = seq // 4
    head_cols = wq_ref.shape[1]
    here = Place()
    z, core, role, owner = here.z, here.c, here.role, here.owner
    here.meet()
    copies = Copies(send_sem, recv_sem)

    def span(index, count):
        return pl.ds(pl.multiple_of(index * count, count), count)

    ff_cols, out_rows, piece = w1_ref.shape[1], wo_ref.shape[0] // 8, d_model // 8
    hidden = w2_ref.shape[0] // 8

    def block_qkv(zz, e):
        return full_qkv.at[span(e, piece), span(zz, 3 * head_cols)]

    units = {
        'o': lambda zz, e: full_o.at[zz, span(e, out_rows), :],
        '1': lambda zz, e: full_1.at[span(e, piece), span(zz, ff_cols)],
        '2': lambda zz, e: full_2.at[zz, span(e, hidden), :],
        'qkv': block_qkv,
    }

    def own_parts(name, e):
        if name == 'o':
            return [(wo_ref.at[span(e, out_rows), :], units[name](z, e))]
        if name == '1':
            return [(w1_ref.at[span(e, piece), :], units[name](z, e))]
        if name == '2':
            return [(w2_ref.at[span(e, hidden), :], units[name](z, e))]
        return [(ref.at[span(e, piece), :],
                 full_qkv.at[span(e, piece), pl.ds(pl.multiple_of((z * 3 + t) * head_cols, head_cols), head_cols)])
                for t, ref in enumerate((wq_ref, wk_ref, wv_ref))]

    mine = here.piece(here.y, here.x)
    by_a = here.piece(here.ya, here.xa)
    by_b = here.piece(here.yb, here.xb)
    by_ab = here.piece(1 - here.y, 1 - here.x)
    to_a, to_b = here.device(y=here.ya, x=here.xa), here.device(y=here.yb, x=here.xb)
    partner = here.device(c=1 - core)
    stage_z, stage_a, stage_b1, stage_b2, stage_c = {}, {}, {}, {}, {}
    names = ('o', '1', '2', 'qkv')

    for name in names:
        stage_z[name] = {k: [copies.start(src, dst, here.device(z=here.z_by[k])) for src, dst in own_parts(name, mine)]
                         for k in (1, 2, 3)}

    def forward_z(name):
        stage_a[name], stage_b1[name] = [], []
        for k in (1, 2, 3):
            for copy in stage_z[name][k]:
                copy.wait_recv()
            block = units[name](here.z_by[k], mine)
            stage_a[name].append(copies.start(block, block, to_a))
            stage_b1[name].append(copies.start(block, block, to_b))

    def forward_a(name):
        stage_b2[name] = []
        for k in (1, 2, 3):
            stage_a[name][k - 1].wait_recv()
            block = units[name](here.z_by[k], by_a)
            stage_b2[name].append(copies.start(block, block, to_b))

    def forward_b(name):
        stage_c[name] = []
        for k in (1, 2, 3):
            stage_b1[name][k - 1].wait_recv()
            stage_b2[name][k - 1].wait_recv()
            for e in (mine, by_a, by_b, by_ab):
                block = units[name](here.z_by[k], e)
                stage_c[name].append(copies.start(block, block, partner))

    locals_ = []

    def copy_local(src, dst):
        copy = pltpu.make_async_copy(src, dst, local_sem.at[len(locals_)])
        locals_.append(copy)
        copy.start()

    copy_local(w1_ref, full_1.at[:, span(z, ff_cols)])
    copy_local(w2_ref, full_2.at[z])
    copy_local(wo_ref, full_o.at[z])
    for t, ref in enumerate((wq_ref, wk_ref, wv_ref)):
        copy_local(ref, full_qkv.at[:, pl.ds(pl.multiple_of((z * 3 + t) * head_cols, head_cols), head_cols)])
    other_role = z % 2 * 2 + 1 - core
    give_x = pltpu.make_async_remote_copy(
        src_ref=x_ref, dst_ref=xs_ref, send_sem=one_send.at[0], recv_sem=one_recv.at[0], device_id=partner, device_id_type=MESH)
    give_cot = pltpu.make_async_remote_copy(
        src_ref=cot_ref.at[span(other_role, blk), :], dst_ref=cot_loc_ref, send_sem=one_send.at[1], recv_sem=one_recv.at[1],
        device_id=partner, device_id_type=MESH)
    keep_x = pltpu.make_async_copy(x_ref, xs_ref, local_sem.at[6])
    take_cot = pltpu.make_async_copy(cot_ref.at[span(role, blk), :], cot_s, local_sem.at[7])
    keep_cot = pltpu.make_async_copy(cot_s, cot_loc_ref, local_sem.at[8])

    @pl.when(owner)
    def _():
        give_x.start()
        give_cot.start()
        keep_x.start()
        take_cot.start()

    def project(i, _):
        rows = span(i, blk)
        values = x_ref[rows, :].astype(F32) + emb_ref[...]
        unit = (values * lax.rsqrt(jnp.mean(values * values, axis=-1, keepdims=True) + EPS_NORM)).astype(BF16)
        for t, ref in enumerate((wq_ref, wk_ref, wv_ref)):
            qkv_s[rows, t * head_cols:(t + 1) * head_cols] = dot_nn(unit, ref[...]).astype(BF16)
        return 0

    lax.fori_loop(0, 4, project, 0)

    def context_copy(j, i):
        src = c_buf.at[j, span(i, blk), :]
        dst = c1_ref.at[:, pl.ds(pl.multiple_of((z * 2 + j) * PAIR, PAIR), PAIR)]
        target_z, target_c = 2 * core + i // 2, i % 2
        remote = pltpu.make_async_remote_copy(
            src_ref=src, dst_ref=dst, send_sem=c_send.at[j * 4 + i], recv_sem=c_recv.at[j * 4 + z],
            device_id=here.device(z=target_z, c=target_c), device_id_type=MESH)
        local = pltpu.make_async_copy(src, dst, c_recv.at[j * 4 + z])
        return remote, local, jnp.logical_and(target_z == z, target_c == core)

    def send_context(j, i):
        remote, local, to_self = context_copy(j, i)
        pl.when(to_self)(local.start)
        pl.when(jnp.logical_not(to_self))(remote.start)

    moves = {(0, 1): [(forward_z, 'o')], (0, 2): [(forward_a, 'o')], (0, 3): [(forward_b, 'o')],
             (1, 2): [(forward_z, '1')], (1, 3): [(forward_a, '1')]}
    for j in range(2):
        vt_s[...] = qkv_s[:, (4 + j) * PAIR:(5 + j) * PAIR].T
        k_view = qkv_s.at[:, (2 + j) * PAIR:(3 + j) * PAIR]
        for i in range(4):
            if i or j:
                send_context(j if i else 0, i - 1 if i else 3)
            for step, name in moves.get((j, i), ()):
                step(name)
            rows = slice(i * blk, (i + 1) * blk)
            outs, sums = attend_rows(qkv_s[rows, j * PAIR:(j + 1) * PAIR], k_view, vt_s, (e_a, e_b))
            c_buf[j, rows, :] = jnp.concatenate(outs, axis=0).T.astype(BF16)
            for head in range(2):
                lse_s[2 * j + head:2 * j + head + 1, rows] = sums[head]

    @pl.when(owner)
    def _():
        take_cot.wait()
        keep_cot.start()

    forward_z('2')
    send_context(1, 3)
    give_lse = pltpu.make_async_remote_copy(
        src_ref=lse_s, dst_ref=lse_ref, send_sem=one_send.at[2], recv_sem=one_recv.at[2],
        device_id=here.device(z=2 * core + z // 2, c=z % 2), device_id_type=MESH)
    keep_lse = pltpu.make_async_copy(lse_s, lse_ref, local_sem.at[9])
    lse_stays = jnp.logical_and(2 * core + z // 2 == z, z % 2 == core)
    pl.when(lse_stays)(keep_lse.start)
    pl.when(jnp.logical_not(lse_stays))(give_lse.start)
    forward_b('1')
    forward_a('2')
    forward_z('qkv')
    forward_b('2')
    forward_a('qkv')
    forward_b('qkv')

    for j in range(2):
        for zz in range(4):
            pltpu.make_async_copy(c_buf.at[j, :blk, :], c1_ref.at[:, :PAIR], c_recv.at[j * 4 + zz]).wait()
        for i in range(4):
            remote, _, to_self = context_copy(j, i)
            pl.when(jnp.logical_not(to_self))(remote.wait_send)
    pl.when(lse_stays)(keep_lse.wait)

    @pl.when(jnp.logical_not(lse_stays))
    def _():
        give_lse.wait_send()
        give_lse.wait_recv()

    @pl.when(owner)
    def _():
        give_x.wait_send()
        give_cot.wait_send()
        keep_x.wait()
        keep_cot.wait()

    @pl.when(jnp.logical_not(owner))
    def _():
        give_x.wait_recv()
        give_cot.wait_recv()

    for copy in locals_:
        copy.wait()
    for name in names:
        for copy in stage_c[name]:
            copy.wait_recv()
    for copy in copies.sent:
        copy.wait_send()


def first_call(x, cot, emb, w_q, w_k, w_v, w_o, w_1, w_2):
    seq, d_model = x.shape
    head_cols, ff_cols, blk = w_q.shape[1], w_1.shape[1], seq // 4
    anywhere = pl.BlockSpec(memory_space=pl.ANY)
    in_vmem = pl.BlockSpec(memory_space=pltpu.VMEM)
    copies = 18 + 12 + 24 + 48
    return pl.pallas_call(
        first_kernel,
        in_specs=[in_vmem, anywhere] + [in_vmem] * 7,
        out_specs=[anywhere] * 8,
        out_shape=[
            jax.ShapeDtypeStruct((blk, d_model), BF16),
            jax.ShapeDtypeStruct((4, seq), F32),
            jax.ShapeDtypeStruct((seq, d_model), BF16),
            jax.ShapeDtypeStruct((blk, d_model), BF16),
            jax.ShapeDtypeStruct((4, *w_o.shape), BF16),
            jax.ShapeDtypeStruct((d_model, 4 * ff_cols), BF16),
            jax.ShapeDtypeStruct((4, *w_2.shape), BF16),
            jax.ShapeDtypeStruct((d_model, 12 * head_cols), BF16),
        ],
        scratch_shapes=[
            pltpu.VMEM((seq, 3 * head_cols), BF16),
            pltpu.VMEM((PAIR, seq), BF16),
            pltpu.VMEM((seq, blk), F32),
            pltpu.VMEM((seq, blk), F32),
            pltpu.VMEM((2, seq, PAIR), BF16),
            pltpu.VMEM((4, seq), F32),
            pltpu.VMEM((blk, d_model), BF16),
            pltpu.SemaphoreType.DMA((10,)),
            pltpu.SemaphoreType.DMA((copies,)),
            pltpu.SemaphoreType.DMA((copies,)),
            pltpu.SemaphoreType.DMA((8,)),
            pltpu.SemaphoreType.DMA((8,)),
            pltpu.SemaphoreType.DMA((3,)),
            pltpu.SemaphoreType.DMA((3,)),
        ],
        compiler_params=pltpu.CompilerParams(vmem_limit_bytes=60 << 20, collective_id=0, has_side_effects=True),
        cost_estimate=pl.CostEstimate(
            flops=64 * seq * seq * PAIR, bytes_accessed=64 * seq * d_model, transcendentals=seq * seq * 4),
        name="first",
    )(x, cot, emb, w_q, w_k, w_v, w_o, w_1, w_2)


def unit_rows(values, emb):
    values = values.astype(F32) + emb
    return (values * lax.rsqrt(jnp.mean(values * values, axis=-1, keepdims=True) + EPS_NORM)).astype(BF16)


def forward_kernel(x_ref, emb_ref, xs1_ref, wqkv_ref,
                   c_ref, lse_ref, u2_ref, qkv2_ref, u1_ref, qkv1_ref,
                   w_s, blocks, u_s, qkv_s, x1_s, u1_s, qkv1_s, v_t, e_a, e_b, c_buf, lse_s,
                   local_sem, first_sem, out_sem, x_send, x_recv, c_send, c_recv):
    seq = xs1_ref.shape[0]
    blk = seq // 4
    head_cols = 2 * PAIR
    here = Place()
    z, core, role = here.z, here.c, here.role

    def span(index, count):
        return pl.ds(pl.multiple_of(index * count, count), count)

    w_load = pltpu.make_async_copy(wqkv_ref.at[:, span(role, 3 * head_cols)], w_s, local_sem.at[0])
    w_load.start()
    x1_load = [pltpu.make_async_copy(xs1_ref.at[i * blk:(i + 1) * blk, :], x1_s.at[i % 2], first_sem.at[i % 2]) for i in range(4)]
    x1_load[0].start()
    here.meet()
    partner, across = here.device(c=1 - core), here.device(z=here.z_by[1])
    role_side, role_over = z % 2 * 2 + 1 - core, (1 - z % 2) * 2 + core
    role_last = (1 - z % 2) * 2 + 1 - core

    def x_copy(n, src, slot, device):
        return pltpu.make_async_remote_copy(
            src_ref=src, dst_ref=blocks.at[slot], send_sem=x_send.at[n], recv_sem=x_recv.at[n],
            device_id=device, device_id_type=MESH)

    over, side = x_copy(0, x_ref, 0, across), x_copy(1, x_ref, 1, partner)
    last = x_copy(2, blocks.at[0], 2, partner)
    over.start()
    side.start()

    def project(src, at_role):
        rows = span(at_role, blk)
        unit = unit_rows(src, emb_ref[1:2, :])
        u_s[rows, :] = unit
        qkv_s[rows, :] = dot_nn(unit, w_s[...]).astype(BF16)

    w_load.wait()
    project(x_ref[...], role)
    side.wait_recv()
    project(blocks[1], role_side)

    stores = []
    for i in range(4):
        if i < 3:
            x1_load[i + 1].start()
        x1_load[i].wait()
        if i >= 2:
            for copy in stores[i - 2]:
                copy.wait()
        unit = unit_rows(x1_s[i % 2], emb_ref[0:1, :])
        u1_s[i % 2] = unit
        qkv1_s[i % 2] = dot_nn(unit, w_s[...]).astype(BF16)
        stores.append([pltpu.make_async_copy(u1_s.at[i % 2], u1_ref.at[i * blk:(i + 1) * blk, :], out_sem.at[i % 2]),
                       pltpu.make_async_copy(qkv1_s.at[i % 2], qkv1_ref.at[i * blk:(i + 1) * blk, :], out_sem.at[2 + i % 2])])
        for copy in stores[i]:
            copy.start()

    over.wait_recv()
    last.start()
    project(blocks[0], role_over)
    last.wait_recv()
    project(blocks[2], role_last)
    keep_u = pltpu.make_async_copy(u_s, u2_ref, local_sem.at[1])
    keep_qkv = pltpu.make_async_copy(qkv_s, qkv2_ref, local_sem.at[2])
    keep_u.start()
    keep_qkv.start()

    member = [here.device(z=z // 2 * 2 + i // 2, c=i % 2) for i in range(4)]

    def c_copy(j, i):
        src = c_buf.at[j, i * blk:(i + 1) * blk, :]
        dst = c_ref.at[:, pl.ds(pl.multiple_of((role * 2 + j) * PAIR, PAIR), PAIR)]
        remote = pltpu.make_async_remote_copy(
            src_ref=src, dst_ref=dst, send_sem=c_send.at[j * 4 + i], recv_sem=c_recv.at[j * 4 + role],
            device_id=member[i], device_id_type=MESH)
        return remote, pltpu.make_async_copy(src, dst, c_recv.at[j * 4 + role])

    def send_context(j, i):
        remote, local = c_copy(j, i)
        pl.when(role == i)(local.start)
        pl.when(role != i)(remote.start)

    for j in range(2):
        v_t[...] = qkv_s[:, (4 + j) * PAIR:(5 + j) * PAIR].T
        k_view = qkv_s.at[:, (2 + j) * PAIR:(3 + j) * PAIR]
        for i in range(4):
            if i or j:
                send_context(j if i else 0, i - 1 if i else 3)
            rows = slice(i * blk, (i + 1) * blk)
            outs, sums = attend_rows(qkv_s[rows, j * PAIR:(j + 1) * PAIR], k_view, v_t, (e_a, e_b))
            c_buf[j, rows, :] = jnp.concatenate(outs, axis=0).T.astype(BF16)
            for head in range(2):
                lse_s[2 * j + head:2 * j + head + 1, rows] = sums[head]
    lse_ref[...] = lse_s[...]
    send_context(1, 3)
    for j in range(2):
        for i in range(4):
            pltpu.make_async_copy(c_buf.at[j, :blk, :], c_ref.at[:, :PAIR], c_recv.at[j * 4 + i]).wait()
            pl.when(role != i)(c_copy(j, i)[0].wait_send)
    for copy in (over, side, last):
        copy.wait_send()
    for group in stores[2:]:
        for copy in group:
            copy.wait()
    keep_u.wait()
    keep_qkv.wait()


def forward_call(x, emb, xs_1, w_qkv):
    blk, d_model = x.shape
    seq, head_cols = 4 * blk, 2 * PAIR
    anywhere = pl.BlockSpec(memory_space=pl.ANY)
    in_vmem = pl.BlockSpec(memory_space=pltpu.VMEM)
    dma = pltpu.SemaphoreType.DMA
    return pl.pallas_call(
        forward_kernel,
        in_specs=[in_vmem, in_vmem, anywhere, anywhere],
        out_specs=[anywhere, in_vmem] + [anywhere] * 4,
        out_shape=[
            jax.ShapeDtypeStruct((blk, d_model), BF16),
            jax.ShapeDtypeStruct((4, seq), F32),
        ] + [jax.ShapeDtypeStruct((seq, n), BF16) for n in (d_model, 3 * head_cols)] * 2,
        scratch_shapes=[
            pltpu.VMEM((d_model, 3 * head_cols), BF16),
            pltpu.VMEM((3, blk, d_model), BF16),
            pltpu.VMEM((seq, d_model), BF16),
            pltpu.VMEM((seq, 3 * head_cols), BF16),
            pltpu.VMEM((2, blk, d_model), BF16),
            pltpu.VMEM((2, blk, d_model), BF16),
            pltpu.VMEM((2, blk, 3 * head_cols), BF16),
            pltpu.VMEM((PAIR, seq), BF16),
            pltpu.VMEM((seq, blk), F32),
            pltpu.VMEM((seq, blk), F32),
            pltpu.VMEM((2, seq, PAIR), BF16),
            pltpu.VMEM((4, seq), F32),
            dma((3,)), dma((2,)), dma((4,)), dma((3,)), dma((3,)), dma((8,)), dma((8,)),
        ],
        compiler_params=pltpu.CompilerParams(vmem_limit_bytes=60 << 20, collective_id=2, has_side_effects=True),
        cost_estimate=pl.CostEstimate(
            flops=64 * seq * seq * PAIR, bytes_accessed=32 * seq * d_model, transcendentals=seq * seq * 4),
        name="forward",
    )(x, emb, xs_1, w_qkv)


def through_norm(values, up, d_mid):
    inverse = lax.rsqrt(jnp.mean(values * values, axis=-1, keepdims=True) + EPS_NORM)
    inner = jnp.mean(values * up, axis=-1, keepdims=True)
    return (d_mid.astype(F32) + inverse * up - values * (inverse * inverse * inverse * inner)).astype(BF16)


def backward_kernel(shared, qkv_ref, dc_ref, lse_ref, dmid_ref, x_ref, emb_ref, wqkv_ref, u_ref, *refs):
    sources, (d_ref, other_ref, g_ref), shares = refs[:shared], refs[shared:shared + 3], refs[shared + 3:2 * shared + 3]
    (dch, k_t, dk_acc, dv_acc, p_cat, ds_cat, d_heads, d_qkv, d_u, w_s, u_s, g_s,
     load_sem, out_sem, dc_send, dc_recv, dq_send, dq_recv, d_send, d_recv, s_send, s_recv) = refs[2 * shared + 3:]
    seq = qkv_ref.shape[0]
    blk = seq // 4
    head_cols = 2 * PAIR
    here = Place()
    z, core, role = here.z, here.c, here.role
    here.meet()
    member = [here.device(z=z // 2 * 2 + i // 2, c=i % 2) for i in range(4)]

    def span(index, count):
        return pl.ds(pl.multiple_of(index * count, count), count)

    def load(src, dst, n):
        copy = pltpu.make_async_copy(src, dst, load_sem.at[n])
        copy.start()
        return copy

    def dc_copy(j, i):
        col = i * head_cols + j * PAIR
        return pltpu.make_async_remote_copy(
            src_ref=dc_ref.at[:, col:col + PAIR], dst_ref=dch.at[span(role, blk), j * PAIR:(j + 1) * PAIR],
            send_sem=dc_send.at[j * 4 + i], recv_sem=dc_recv.at[j * 4 + role], device_id=member[i], device_id_type=MESH)

    for j in range(2):
        for i in range(4):
            pl.when(role != i)(dc_copy(j, i).start)
    for i in range(4):
        @pl.when(role == i)
        def _():
            dch[i * blk:(i + 1) * blk, :] = dc_ref[:, i * head_cols:(i + 1) * head_cols]

    def dq_copy(j, i, t):
        col = t * head_cols + j * PAIR
        return pltpu.make_async_remote_copy(
            src_ref=d_heads.at[i * blk:(i + 1) * blk, col:col + PAIR],
            dst_ref=d_qkv.at[:, pl.ds(pl.multiple_of(role * 3 * head_cols + col, PAIR), PAIR)],
            send_sem=dq_send.at[(j * 4 + i) * 3 + t], recv_sem=dq_recv.at[(j * 4 + role) * 3 + t],
            device_id=member[i], device_id_type=MESH)

    def send_d_heads(j):
        for i in range(4):
            @pl.when(role != i)
            def _():
                for t in range(3):
                    dq_copy(j, i, t).start()

    shared_copies = [pltpu.make_async_remote_copy(
        src_ref=src, dst_ref=dst, send_sem=s_send.at[n], recv_sem=s_recv.at[n],
        device_id=here.device(c=1 - core), device_id_type=MESH) for n, (src, dst) in enumerate(zip(sources, shares))]

    steps = seq // BWD_ROWS
    for j in range(2):
        for i in range(4):
            @pl.when(role != i)
            def _():
                pltpu.make_async_copy(dc_ref.at[:, :PAIR], dch.at[:blk, :PAIR], dc_recv.at[j * 4 + i]).wait()
        if j == 0:
            for copy in shared_copies:
                copy.start()
        k_view, v_view = qkv_ref.at[:, (2 + j) * PAIR:(3 + j) * PAIR], qkv_ref.at[:, (4 + j) * PAIR:(5 + j) * PAIR]
        k_t[...] = k_view[...].T
        dk_acc[...] = jnp.zeros_like(dk_acc)
        dv_acc[...] = jnp.zeros_like(dv_acc)

        def block(i, _):
            if j == 1:
                @pl.when(i == 1)
                def _():
                    send_d_heads(0)
            rows = span(i, BWD_ROWS)
            cols = slice(j * PAIR, (j + 1) * PAIR)
            d_heads[rows, cols] = backward_rows(
                qkv_ref[rows, cols], dch[rows, cols], lse_ref[2 * j:2 * j + 2, rows], k_view, v_view,
                k_t, p_cat, ds_cat, dk_acc, dv_acc)
            return 0

        lax.fori_loop(0, steps, block, 0)
        d_heads[:, head_cols + j * PAIR:head_cols + (j + 1) * PAIR] = (dk_acc[...] * SCALE).astype(BF16)
        d_heads[:, 2 * head_cols + j * PAIR:2 * head_cols + (j + 1) * PAIR] = dv_acc[...].astype(BF16)

    quarter = u_s.shape[2]
    pending = load(u_ref.at[:, :quarter], u_s.at[0], 0)
    for i in range(4):
        @pl.when(role == i)
        def _():
            d_qkv[:, i * 3 * head_cols:(i + 1) * 3 * head_cols] = d_heads[i * blk:(i + 1) * blk, :]
    send_d_heads(1)
    stores = []
    count = u_ref.shape[1] // quarter
    for n in range(count):
        ahead = load(u_ref.at[:, (n + 1) * quarter:(n + 2) * quarter], u_s.at[(n + 1) % 2], (n + 1) % 2) if n + 1 < count else None
        pending.wait()
        if n >= 2:
            stores[n - 2].wait()
        g_s[n % 2] = dot_tn(u_s[n % 2], d_heads[...])
        stores.append(pltpu.make_async_copy(g_s.at[n % 2], g_ref.at[n * quarter:(n + 1) * quarter, :], out_sem.at[n % 2]))
        stores[n].start()
        pending = ahead
    w_rows = w_s.shape[1]
    chunks = wqkv_ref.shape[0] // w_rows
    w_load = load(wqkv_ref.at[:w_rows, :], w_s.at[0], 2)
    for j in range(2):
        for i in range(4):
            @pl.when(role != i)
            def _():
                for t in range(3):
                    pltpu.make_async_copy(d_heads.at[:blk, :PAIR], d_qkv.at[:, :PAIR], dq_recv.at[(j * 4 + i) * 3 + t]).wait()
    for n in range(chunks):
        ahead = load(wqkv_ref.at[(n + 1) * w_rows:(n + 2) * w_rows, :], w_s.at[(n + 1) % 2], 2 + (n + 1) % 2) if n + 1 < chunks else None
        w_load.wait()
        d_u[:, n * w_rows:(n + 1) * w_rows] = dot_nt(d_qkv[...], w_s[n % 2]).astype(BF16)
        w_load = ahead
    rows_each = min(128, blk)
    for n in range(blk // rows_each):
        rows = slice(n * rows_each, (n + 1) * rows_each)
        d_u[rows, :] = through_norm(x_ref[rows, :].astype(F32) + emb_ref[...], d_u[rows, :].astype(F32), dmid_ref[rows, :])
    keep = pltpu.make_async_copy(d_u, d_ref, out_sem.at[2])
    keep.start()
    stores[count - 2].wait()
    stores[count - 1].wait()
    give = pltpu.make_async_remote_copy(
        src_ref=d_u, dst_ref=other_ref, send_sem=d_send.at[0], recv_sem=d_recv.at[0],
        device_id=here.device(c=1 - core), device_id_type=MESH)
    give.start()
    for i in range(4):
        @pl.when(role != i)
        def _():
            for j in range(2):
                dc_copy(j, i).wait_send()
                for t in range(3):
                    dq_copy(j, i, t).wait_send()
    keep.wait()
    give.wait()
    for copy in shared_copies:
        copy.wait()


def backward_call(qkv, d_c, lse, d_mid, x, emb, w_qkv, u_seq, shared):
    seq, d_model = u_seq.shape
    blk, heads3 = seq // 4, qkv.shape[1]
    anywhere = pl.BlockSpec(memory_space=pl.ANY)
    in_vmem = pl.BlockSpec(memory_space=pltpu.VMEM)
    dma = pltpu.SemaphoreType.DMA
    quarter = d_model // 4
    return pl.pallas_call(
        functools.partial(backward_kernel, len(shared)),
        in_specs=[in_vmem] * 6 + [anywhere] * (2 + len(shared)),
        out_specs=[anywhere] * (3 + len(shared)),
        out_shape=[
            jax.ShapeDtypeStruct((blk, d_model), BF16),
            jax.ShapeDtypeStruct((blk, d_model), BF16),
            jax.ShapeDtypeStruct((d_model, heads3), F32),
        ] + [jax.ShapeDtypeStruct(value.shape, value.dtype) for value in shared],
        scratch_shapes=[
            pltpu.VMEM((seq, heads3 // 3), BF16),
            pltpu.VMEM((PAIR, seq), BF16),
            pltpu.VMEM((seq, PAIR), F32),
            pltpu.VMEM((seq, PAIR), F32),
            pltpu.VMEM((seq, 2 * BWD_ROWS), BF16),
            pltpu.VMEM((seq, 2 * BWD_ROWS), BF16),
            pltpu.VMEM((seq, heads3), BF16),
            pltpu.VMEM((blk, 4 * heads3), BF16),
            pltpu.VMEM((blk, d_model), BF16),
            pltpu.VMEM((2, quarter, 4 * heads3), BF16),
            pltpu.VMEM((2, seq, quarter), BF16),
            pltpu.VMEM((2, quarter, heads3), F32),
            dma((4,)), dma((3,)), dma((8,)), dma((8,)), dma((24,)), dma((24,)), dma((1,)), dma((1,)),
            dma((len(shared),)), dma((len(shared),)),
        ],
        compiler_params=pltpu.CompilerParams(vmem_limit_bytes=60 << 20, collective_id=3, has_side_effects=True),
        cost_estimate=pl.CostEstimate(
            flops=160 * seq * seq * PAIR, bytes_accessed=64 * seq * d_model, transcendentals=seq * seq * 4),
        name="backward",
    )(qkv, d_c, lse, d_mid, x, emb, w_qkv, u_seq, *shared)


def rms_rows(values):
    return values * lax.rsqrt(jnp.mean(values * values, axis=-1, keepdims=True) + EPS_NORM)


GELU_IN, GELU_CUBE = math.sqrt(2 / math.pi), 0.044715


def gelu_parts(z):
    square = z * z
    t = jnp.tanh(z * (GELU_IN + (GELU_IN * GELU_CUBE) * square))
    return 0.5 + 0.5 * t, t, square


def hidden_kernel(backward, forward, *refs):
    refs = list(refs)
    take = lambda: refs.pop(0)
    if forward:
        c_ref, x_ref, emb_ref, wo_ref = take(), take(), take(), take()
        w1_ref = take()
    else:
        h_ref, wo_ref, up_ref = take(), take(), take()
    w2_ref = take()
    if backward:
        d_ref, w1b_ref = take(), take()
    if forward:
        h_out, m_out = take(), take()
        up_out, act_out = take(), take()
    if backward:
        dup_out, dmid_out, dc_out = take(), take(), take()
    else:
        x_out = take()
    if forward:
        h_s, m_s = take(), take()
    prev_s, acc = take(), take()
    step, last = pl.program_id(0), pl.num_programs(0) - 1

    if forward:
        @pl.when(step == 0)
        def _():
            h = (x_ref[...].astype(F32) + emb_ref[...] + dot_nn(c_ref[...], wo_ref[...])).astype(BF16)
            m = rms_rows(h.astype(F32)).astype(BF16)
            h_s[...], m_s[...] = h, m
            h_out[...], m_out[...] = h, m

    def first_part():
        slot = step % 2
        if backward:
            d_act = dot_nt(d_ref[...], w2_ref[...]).astype(BF16).astype(F32)
        if forward:
            up = dot_nn(m_s[...], w1_ref[...]).astype(BF16)
            up_out[...] = up
        else:
            up = up_ref[...]
        z = up.astype(F32)
        factor, t, square = gelu_parts(z)
        if forward:
            act = (z * factor).astype(BF16)
            act_out[...] = act
        if backward:
            slope = factor + z * ((1.0 - t * t) * (0.5 * GELU_IN + (1.5 * GELU_IN * GELU_CUBE) * square))
            d_up = (slope * d_act).astype(BF16)
            dup_out[...] = d_up
            prev_s[slot] = d_up
        else:
            prev_s[slot] = act

    def second_part():
        prev = prev_s[1 - step % 2]
        if backward:
            return dot_nt(prev, w1b_ref[...])
        return dot_nn(prev, w2_ref[...])

    pl.when(step == 0)(first_part)

    @pl.when(step == 1)
    def _():
        acc[...] = second_part()
        first_part()

    @pl.when(jnp.logical_and(step > 1, step < last))
    def _():
        acc[...] += second_part()
        first_part()

    @pl.when(step == last)
    def _():
        total = acc[...] + second_part()
        if backward:
            h = (h_s if forward else h_ref)[...].astype(F32)
            d_mid = through_norm(h, total.astype(BF16).astype(F32), d_ref[...])
            dmid_out[...] = d_mid
            dc_out[...] = dot_nt(d_mid, wo_ref[...]).astype(BF16)
        else:
            x_out[...] = (h_s[...].astype(F32) + total).astype(BF16)


def hidden_call(forward, backward, w_o, w_1, w_2, context=None, x=None, emb=None, h=None, up=None, d_next=None):
    blk, d_model = (context if forward else h).shape
    hidden = w_1.shape[1]
    tile = HIDDEN
    steps = hidden // tile
    now, before = (lambda i: jnp.minimum(i, steps - 1)), (lambda i: jnp.maximum(i - 1, 0))
    whole = lambda rows, cols: pl.BlockSpec((rows, cols), lambda i: (0, 0))
    wide = pl.BlockSpec((blk, tile), lambda i: (0, now(i)))
    args, specs = [], []

    def add(value, spec):
        args.append(value)
        specs.append(spec)

    if forward:
        add(context, whole(blk, d_model))
        add(x, whole(blk, d_model))
        add(emb, whole(1, d_model))
        add(w_o, whole(d_model, d_model))
        add(w_1, pl.BlockSpec((d_model, tile), lambda i: (0, now(i))))
    else:
        add(h, whole(blk, d_model))
        add(w_o, whole(d_model, d_model))
        add(up, wide)
    add(w_2, pl.BlockSpec((tile, d_model), (lambda i: (now(i), 0)) if backward else (lambda i: (before(i), 0))))
    if backward:
        add(d_next, whole(blk, d_model))
        add(w_1, pl.BlockSpec((d_model, tile), lambda i: (0, before(i))))
    row = (whole(blk, d_model), jax.ShapeDtypeStruct((blk, d_model), BF16))
    big = (wide, jax.ShapeDtypeStruct((blk, hidden), BF16))
    outs = ([row, row, big, big] if forward else []) + ([big, row, row] if backward else [row])
    return pl.pallas_call(
        functools.partial(hidden_kernel, backward, forward),
        grid=(steps + 1,),
        in_specs=specs,
        out_specs=[spec for spec, _ in outs],
        out_shape=[shape for _, shape in outs],
        scratch_shapes=([pltpu.VMEM((blk, d_model), BF16)] * 2 if forward else [])
        + [pltpu.VMEM((2, blk, tile), BF16), pltpu.VMEM((blk, d_model), F32)],
        compiler_params=pltpu.CompilerParams(vmem_limit_bytes=60 << 20),
        cost_estimate=pl.CostEstimate(
            flops=2 * blk * d_model * (hidden * (3 if forward and backward else 2) + 2 * d_model),
            bytes_accessed=4 * hidden * d_model + 8 * blk * hidden, transcendentals=blk * hidden),
        interpret=INTERPRET,
        name="hidden",
    )(*args)


def backward_rows(q, d_out, lse, k_ref, v_ref, k_t, p_cat, ds_cat, dk_acc, dv_acc):
    block = q.shape[0]
    lane = lax.broadcasted_iota(jnp.int32, q.shape, 1)
    q_heads, do_heads, dqs = [], [], []
    for head in range(2):
        mine = lane // HEAD_DIM == head
        q_head = jnp.where(mine, q, jnp.zeros_like(q))
        do_head = jnp.where(mine, d_out, jnp.zeros_like(d_out))
        scores = dot_nt(k_ref[...], q_head)
        probs = jnp.exp2(scores * EXP2_SCALE - lse[head:head + 1, :])
        d_probs = dot_nt(v_ref[...], do_head).astype(BF16).astype(F32)
        inner = jnp.sum(probs * d_probs, axis=0, keepdims=True)
        cols = slice(head * block, (head + 1) * block)
        p_cat[:, cols] = probs.astype(BF16)
        ds_cat[:, cols] = (probs * (d_probs - inner)).astype(BF16)
        dqs.append(dot_nn(k_t[head * HEAD_DIM:(head + 1) * HEAD_DIM, :], ds_cat[:, cols]))
        q_heads.append(q_head)
        do_heads.append(do_head)
    dv_acc[...] += dot_nn(p_cat[...], jnp.concatenate(do_heads, axis=0))
    dk_acc[...] += dot_nn(ds_cat[...], jnp.concatenate(q_heads, axis=0))
    return (jnp.concatenate(dqs, axis=0).T * SCALE).astype(BF16)


def last_kernel(qkv_ref, dc_ref, lse_ref, dmid_ref, x_ref, emb_ref, wqkv_ref, u_ref, gqkv2_ref,
                *refs):
    lefts = {'2': refs[:4], '1': refs[8:12], 'o': refs[15:18]}
    rights = {'2': refs[4:8], '1': refs[12:15], 'o': refs[18:22]}
    (dx_ref, g1_ref, g2_ref, go_ref, gq_ref, gk_ref, gv_ref, away2_ref, mid2_ref, keep2_ref,
     away1_ref, mid1_ref, keep1_ref, awayo_ref, mido_ref, keepo_ref, dup_other, dmid_other,
     dch, k_t, dk_acc, dv_acc, p_cat, ds_cat, d_heads, d_qkv, buf, buf_o, second, second_o, tmp, tmp_o,
     third, third_o, sum_1, sum_2, sum_o, qa, qb, q1, q2, q3, q4, d_1, w_s, u_s, g_s,
     left_t, stage,
     local_sem, load_sem, send_sem, recv_sem, dc_send, dc_recv, dq_send, dq_recv, z_send, z_recv, x_send, x_recv,
     p_send, p_recv) = refs[22:]
    seq = qkv_ref.shape[0]
    blk = seq // 4
    head_cols = 2 * PAIR
    here = Place()
    z, core, role, owner = here.z, here.c, here.role, here.owner
    here.meet()
    copies = Copies(send_sem, recv_sem)
    waits = []

    def span(index, count):
        return pl.ds(pl.multiple_of(index * count, count), count)

    def load(src, dst, n):
        copy = pltpu.make_async_copy(src, dst, load_sem.at[n])
        copy.start()
        return copy

    no = jnp.logical_not
    to_a, to_b = here.device(y=here.ya, x=here.xa), here.device(y=here.yb, x=here.xb)
    partner = here.device(c=1 - core)
    member = [here.device(z=z // 2 * 2 + i // 2, c=i % 2) for i in range(4)]
    piece = tmp.shape[1]

    def dc_copy(i):
        return pltpu.make_async_remote_copy(
            src_ref=dc_ref.at[:, i * head_cols:(i + 1) * head_cols], dst_ref=dch.at[span(role, blk), :],
            send_sem=dc_send.at[i], recv_sem=dc_recv.at[role], device_id=member[i], device_id_type=MESH)

    for i in range(4):
        pl.when(role != i)(dc_copy(i).start)

        @pl.when(role == i)
        def _():
            dch[i * blk:(i + 1) * blk, :] = dc_ref[:, i * head_cols:(i + 1) * head_cols]

    half = rights['1'][0].shape[1] // 8
    wide = 2 * half
    dmid_give = copies.start(lefts['o'][2], dmid_other, partner)
    dup_give = [copies.start(rights['1'][2].at[:, q * wide:(q + 1) * wide], dup_other.at[:, q * wide:(q + 1) * wide], partner)
                for q in range(4)]
    lefts['o'] = (*lefts['o'], dmid_other)
    rights['1'] = (*rights['1'], dup_other)
    firsts = {(w, q): [copies.make(ref.at[q, :, h * half:(h + 1) * half], buf.at[u + q, :, h * half:(h + 1) * half], to_a)
                       for h in range(2)] for w, ref, u in (('2', away2_ref, 0), ('1', away1_ref, 4)) for q in range(4)}
    firsts['o'] = [copies.make(awayo_ref.at[2 * h:2 * h + 2], buf_o.at[2 * h:2 * h + 2], to_a) for h in range(2)]
    seconds = {(w, q): copies.make(buf.at[u + q, piece:, :], second.at[u + q], to_b) for w, u in (('2', 0), ('1', 4)) for q in range(4)}
    seconds['o'] = copies.make(buf_o.at[:, piece:, :], second_o, to_b)

    def add_mid(unit):
        if unit == 'o':
            mid, keep, t, n = mido_ref, keepo_ref, tmp_o, 4
            bottom, top = buf_o.at[:, piece:, :], buf_o.at[:, :piece, :]
        else:
            w, q = unit
            mid, keep = (mid2_ref.at[q], keep2_ref.at[q]) if w == '2' else (mid1_ref.at[q], keep1_ref.at[q])
            u = q if w == '2' else 4 + q
            t, n, bottom, top = tmp, 6, buf.at[u, piece:, :], buf.at[u, :piece, :]
        loads = [load(mid, t.at[0], n), load(keep, t.at[1], n + 1)]
        for copy in firsts[unit]:
            copy.wait_recv()
        for copy in loads:
            copy.wait()
        bottom[...] += t[0]
        top[...] += t[1]
        seconds[unit].start()

    sums = {'2': (lambda q: buf.at[q, :piece, :], third.at[0], 0), '1': (lambda q: buf.at[4 + q, :piece, :], third.at[1], 1),
            'o': (lambda q: buf_o.at[q, :piece, :], third_o, 2)}
    far_q = here.z_by[2]

    def near_copy(w, q):
        part, got, n = sums[w]
        return pltpu.make_async_remote_copy(
            src_ref=part(q), dst_ref=got.at[q // 2], send_sem=z_send.at[n * 3 + q // 2], recv_sem=z_recv.at[n * 3 + q // 2],
            device_id=here.device(z=here.z_by[1]), device_id_type=MESH)

    def far_copy(w):
        part, got, n = sums[w]
        return pltpu.make_async_remote_copy(
            src_ref=part(far_q), dst_ref=got.at[2], send_sem=z_send.at[n * 3 + 2], recv_sem=z_recv.at[n * 3 + 2],
            device_id=here.device(z=far_q), device_id_type=MESH)

    def finish(unit):
        seconds[unit].wait_recv()
        if unit == 'o':
            buf_o[:, :piece, :] += second_o[...]
            w, qs = 'o', range(4)
        else:
            w, u = unit[0], unit[1] + (4 if unit[0] == '1' else 0)
            buf[u, :piece, :] += second[u]
            qs = (unit[1],)
        for q in qs:
            pl.when((z + q) % 2 == 1)(near_copy(w, q).start)

    def far(w):
        part, got, n = sums[w]
        for k in range(2):
            pltpu.make_async_copy(got.at[2], got.at[k], z_recv.at[n * 3 + k]).wait()
        theirs, ours = part(far_q), part(z)
        theirs[...] += got[far_q // 2]
        ours[...] += got[z // 2]
        far_copy(w).start()

    mine, by_a = here.piece(here.y, here.x), here.piece(here.ya, here.xa)
    by_b, by_ab = here.piece(here.yb, here.xb), here.piece(1 - here.y, 1 - here.x)
    gathers = {}

    def total(w):
        part, got, n = sums[w]
        out = {'2': sum_2, '1': sum_1, 'o': sum_o}[w]
        far_copy(w).wait_recv()
        out[...] = part(z)[...] + got[2]

    def gather_start(name, src, out, n):
        rows = lambda e: out.at[span(e, piece), :]
        keep = pltpu.make_async_copy(src, rows(mine), local_sem.at[n])
        keep.start()
        waits.append(keep)
        gathers[name] = dict(src=src, rows=rows, a=copies.start(src, rows(mine), to_a), b1=copies.start(src, rows(mine), to_b))

    def gather_second(name):
        g = gathers[name]
        g['a'].wait_recv()
        g['b2'] = copies.start(g['rows'](by_a), g['rows'](by_a), to_b)

    def gather_core(name):
        g = gathers[name]
        g['c'] = [copies.start(g['src'], g['rows'](mine), partner), copies.start(g['rows'](by_a), g['rows'](by_a), partner)]
        g['b1'].wait_recv()
        g['c'].append(copies.start(g['rows'](by_b), g['rows'](by_b), partner))
        g['b2'].wait_recv()
        g['c'].append(copies.start(g['rows'](by_ab), g['rows'](by_ab), partner))

    def dq_copy(j, i, t):
        col = t * head_cols + j * PAIR
        return pltpu.make_async_remote_copy(
            src_ref=d_heads.at[i * blk:(i + 1) * blk, col:col + PAIR],
            dst_ref=d_qkv.at[:, pl.ds(pl.multiple_of(role * 3 * head_cols + col, PAIR), PAIR)],
            send_sem=dq_send.at[(j * 4 + i) * 3 + t], recv_sem=dq_recv.at[(j * 4 + role) * 3 + t],
            device_id=member[i], device_id_type=MESH)

    def send_d_heads(j):
        for i in range(4):
            @pl.when(role != i)
            def _():
                for t in range(3):
                    dq_copy(j, i, t).start()

    index = [here.ya * 2 + here.xa, (1 - here.y) * 2 + 1 - here.x, here.yb * 2 + here.xb, here.y * 2 + here.x]
    spaces = (p_cat, ds_cat)
    parts = [('2', n) for n in range(8)] + [('1', n) for n in range(8)] + [('o', n) for n in range(2)]
    left_loads = [('2', q) for q in range(4)] + [('1', 0), ('o', 0)]

    def load_lefts(name, q):
        for n in range(16):
            pltpu.make_async_copy(
                lefts[name][n // 4].at[:, span(q * 8 + index[n % 4] * 2 + core, piece)],
                d_heads.at[n // 4 * blk:(n // 4 + 1) * blk, n % 4 * piece:(n % 4 + 1) * piece], load_sem.at[14]).start()

    def load_rights(s):
        name, n = parts[s]
        for i in range(4):
            pltpu.make_async_copy(
                rights[name][i].at[:, n * half:(n + 1) * half], spaces[s % 2].at[i * blk:(i + 1) * blk, :],
                load_sem.at[15 + s % 2]).start()

    def stored(s):
        pltpu.make_async_copy(stage.at[s % 2], stage.at[s % 2], load_sem.at[17 + s % 2]).wait()

    def send_part(s):
        name, n = parts[s]
        if name == 'o':
            firsts['o'][n].start()
        else:
            firsts[(name, n // 2)][n % 2].start()

    load_lefts(*left_loads[0])
    load_rights(0)
    load_rights(1)
    for s in range(len(parts)):
        name, n = parts[s]
        if n == 0 or name == '2' and n % 2 == 0:
            every = d_heads.at[:, :4 * piece]
            pltpu.make_async_copy(every, every, load_sem.at[14]).wait()
            left_t[...] = every[...].T
            left_loads.pop(0)
            if left_loads:
                if left_loads[0][0] == 'o':
                    dmid_give.wait_recv()
                load_lefts(*left_loads[0])
        if s + 1 < len(parts) and parts[s + 1][0] != '2':
            if parts[s + 1][0] == '1' and parts[s + 1][1] % 2 == 0:
                dup_give[parts[s + 1][1] // 2].wait_recv()
            load_rights(s + 1)
        space = spaces[s % 2]
        if name != '2' or n < 2:
            pltpu.make_async_copy(space, space, load_sem.at[15 + s % 2]).wait()
        if s >= 1:
            stored(s - 1)
            send_part(s - 1)
        stage[s % 2] = dot_nn(left_t[...], space[...])
        targets = {'2': (away2_ref, mid2_ref, keep2_ref), '1': (away1_ref, mid1_ref, keep1_ref),
                   'o': (awayo_ref, mido_ref, keepo_ref)}[name]
        for row, ref in zip((0, 2 * piece, 3 * piece), targets):
            rows = slice(row, row + (2 * piece if row == 0 else piece))
            if name == 'o':
                for k in range(2):
                    pltpu.make_async_copy(stage.at[s % 2, rows, k * (half // 2):(k + 1) * (half // 2)], ref.at[2 * n + k],
                                          load_sem.at[17 + s % 2]).start()
            else:
                pltpu.make_async_copy(stage.at[s % 2, rows, :], ref.at[n // 2, :, n % 2 * half:(n % 2 + 1) * half],
                                      load_sem.at[17 + s % 2]).start()
    stored(len(parts) - 1)
    send_part(len(parts) - 1)

    for i in range(4):
        @pl.when(role != i)
        def _():
            pltpu.make_async_copy(dc_ref.at[:, :head_cols], dch.at[:blk, :], dc_recv.at[i]).wait()

    moves = {(0, 0): [(add_mid, ('2', 0))], (0, 1): [(add_mid, ('2', 1))], (0, 4): [(finish, ('2', 0))],
             (0, 6): [(add_mid, ('2', 2)), (finish, ('2', 1))], (1, 0): [(send_d_heads, 0)],
             (1, 2): [(finish, ('2', 2)), (add_mid, ('2', 3))], (1, 6): [(finish, ('2', 3))], (1, 7): [(add_mid, ('1', 0))]}
    steps = seq // BWD_ROWS
    for j in range(2):
        k_view, v_view = qkv_ref.at[:, (2 + j) * PAIR:(3 + j) * PAIR], qkv_ref.at[:, (4 + j) * PAIR:(5 + j) * PAIR]
        k_t[...] = k_view[...].T
        dk_acc[...] = jnp.zeros_like(dk_acc)
        dv_acc[...] = jnp.zeros_like(dv_acc)

        def block(i, _):
            for n in range(8):
                if (j, n) in moves:
                    @pl.when(i == min(n, steps - 1))
                    def _():
                        for move, what in moves[(j, n)]:
                            move(what)
            rows = span(i, BWD_ROWS)
            cols = slice(j * PAIR, (j + 1) * PAIR)
            d_heads[rows, cols] = backward_rows(
                qkv_ref[rows, cols], dch[rows, cols], lse_ref[2 * j:2 * j + 2, rows], k_view, v_view,
                k_t, p_cat, ds_cat, dk_acc, dv_acc)
            return 0

        lax.fori_loop(0, steps, block, 0)
        d_heads[:, head_cols + j * PAIR:head_cols + (j + 1) * PAIR] = (dk_acc[...] * SCALE).astype(BF16)
        d_heads[:, 2 * head_cols + j * PAIR:2 * head_cols + (j + 1) * PAIR] = dv_acc[...].astype(BF16)

    quarter = 2 * piece

    def quarter_loads(n):
        return [load(u_ref.at[:, span(index[n], quarter)], u_s.at[n % 2], 8 + n % 2),
                load(gqkv2_ref.at[span(index[n], quarter), :], g_s.at[n % 2], 10 + n % 2)]

    pending = quarter_loads(0)
    for i in range(4):
        @pl.when(role == i)
        def _():
            d_qkv[:, i * 3 * head_cols:(i + 1) * 3 * head_cols] = d_heads[i * blk:(i + 1) * blk, :]
    send_d_heads(1)
    targets = [qa.at[0], qa.at[1], qb.at[0], qb.at[1]]
    first_q = copies.make(qa, q1, to_a)
    for n in range(4):
        ahead = quarter_loads(n + 1) if n < 3 else []
        for copy in pending:
            copy.wait()
        targets[n][...] = dot_tn(u_s[n % 2], d_heads[...]) + g_s[n % 2]
        pending = ahead
        if n == 0:
            far('2')
            add_mid(('1', 1))
            finish(('1', 0))
            finish(('1', 1))
        if n == 2:
            first_q.start()

    add_mid(('1', 2))
    w_rows = w_s.shape[1]
    chunks = wqkv_ref.shape[0] // w_rows
    w_load = load(wqkv_ref.at[:w_rows, :], w_s.at[0], 12)
    for j in range(2):
        for i in range(4):
            @pl.when(role != i)
            def _():
                for t in range(3):
                    pltpu.make_async_copy(d_heads.at[:blk, :PAIR], d_qkv.at[:, :PAIR], dq_recv.at[(j * 4 + i) * 3 + t]).wait()
    for n in range(chunks):
        ahead = load(wqkv_ref.at[(n + 1) * w_rows:(n + 2) * w_rows, :], w_s.at[(n + 1) % 2], 12 + (n + 1) % 2) if n + 1 < chunks else None
        w_load.wait()
        d_1[:, n * w_rows:(n + 1) * w_rows] = dot_nt(d_qkv[...], w_s[n % 2]).astype(BF16)
        w_load = ahead

    count = min(128, blk)
    for n in range(blk // count):
        rows = slice(n * count, (n + 1) * count)
        d_1[rows, :] = through_norm(x_ref[rows, :].astype(F32) + emb_ref[...], d_1[rows, :].astype(F32), dmid_ref[rows, :])

    own_seq, part_rows = z // 2, blk // 2

    def dx_rows(role, h):
        return pl.ds(pl.multiple_of(role * blk + h * part_rows, part_rows), part_rows)

    def dx_copy(n, h, device):
        slot = [0, 1 + core, 3 + core][n]
        return pltpu.make_async_remote_copy(
            src_ref=d_1.at[h * part_rows:(h + 1) * part_rows, :], dst_ref=dx_ref.at[dx_rows(role, h), :],
            send_sem=x_send.at[n * 2 + h], recv_sem=x_recv.at[slot * 2 + h], device_id=device, device_id_type=MESH)

    dx_side = [dx_copy(0, h, partner) for h in range(2)]
    dx_next = [dx_copy(1, h, here.device(z=here.z_by[1], c=own_seq)) for h in range(2)]
    dx_cross = [dx_copy(2, h, here.device(z=far_q, c=own_seq)) for h in range(2)]
    dx_keep = pltpu.make_async_copy(d_1, dx_ref.at[span(role, blk), :], local_sem.at[8])

    def dx_pass(cc, h):
        rows = dx_rows(z % 2 * 2 + cc, h)
        return pltpu.make_async_remote_copy(
            src_ref=dx_ref.at[rows, :], dst_ref=dx_ref.at[rows, :], send_sem=x_send.at[6 + cc * 2 + h],
            recv_sem=x_recv.at[(5 + cc) * 2 + h], device_id=here.device(z=here.z_by[1]), device_id_type=MESH)

    def dx_start(h):
        dx_cross[h].start()
        dx_next[h].start()
        pl.when(no(owner))(dx_side[h].start)

    def dx_got(slot, h):
        rows = d_1.at[:part_rows, :]
        pltpu.make_async_copy(rows, dx_ref.at[:part_rows, :], x_recv.at[slot * 2 + h]).wait()

    def dx_forward(h):
        @pl.when(no(owner))
        def _():
            for cc in range(2):
                dx_got(3 + cc, h)
                dx_pass(cc, h).start()

    finish(('1', 2))
    dx_start(0)
    pl.when(owner)(dx_keep.start)
    add_mid(('1', 3))
    finish(('1', 3))
    add_mid('o')
    dx_forward(0)
    far('1')
    first_q.wait_recv()
    qb[0] += q1[1]
    second_q = copies.start(qb.at[0], q2, to_b)
    qb[1] += q1[0]
    total('2')
    gather_start('2', sum_2, g2_ref, 0)
    second_q.wait_recv()
    qb[1] += q2[...]
    plane_stays = jnp.logical_and(2 * (z % 2) + core == z, z // 2 == core)
    plane_q = pltpu.make_async_remote_copy(
        src_ref=qb.at[1], dst_ref=q3, send_sem=p_send.at[0], recv_sem=p_recv.at[0],
        device_id=here.device(z=2 * (z % 2) + core, c=z // 2), device_id_type=MESH)

    @pl.when(plane_stays)
    def _():
        q3[...] = qb[1]

    pl.when(no(plane_stays))(plane_q.start)
    finish('o')
    total('1')
    gather_start('1', sum_1, g1_ref, 1)
    dx_start(1)
    gather_second('2')
    gather_second('1')
    pl.when(no(plane_stays))(plane_q.wait_recv)
    give_q = copies.start(q3.at[span(1 - core, piece), :], q4.at[0], partner)
    gather_core('2')
    give_q.wait_recv()
    q4[1] = q4[0] + q3[span(core, piece), :]
    far('o')
    for t, (name, out) in enumerate((('q', gq_ref), ('k', gk_ref), ('v', gv_ref))):
        gather_start(name, q4.at[1, :, t * head_cols:(t + 1) * head_cols], out, 3 + t)
    gather_core('1')
    for name in 'qkv':
        gather_second(name)
    for name in 'qkv':
        gather_core(name)
    dx_forward(1)
    total('o')
    gather_start('o', sum_o, go_ref, 2)
    gather_second('o')
    gather_core('o')

    @pl.when(owner)
    def _():
        for h in range(2):
            for slot in (0, 1, 2):
                dx_got(slot, h)
        dx_keep.wait()

    @pl.when(no(owner))
    def _():
        for h in range(2):
            dx_side[h].wait_send()
            for cc in range(2):
                dx_got(5 + cc, h)
                dx_pass(cc, h).wait_send()

    for g in gathers.values():
        for copy in g['c']:
            copy.wait_recv()
    for copy in waits:
        copy.wait()
    for copy in copies.sent:
        copy.wait_send()
    for h in range(2):
        dx_cross[h].wait_send()
        dx_next[h].wait_send()
    pl.when(no(plane_stays))(plane_q.wait_send)
    for i in range(4):
        @pl.when(role != i)
        def _():
            dc_copy(i).wait_send()
            for j in range(2):
                for t in range(3):
                    dq_copy(j, i, t).wait_send()
        for w in '21o':
            pl.when((z + i) % 2 == 1)(near_copy(w, i).wait_send)
    for w in '21o':
        far_copy(w).wait_send()


def last_call(qkv, d_c, lse, d_mid, x, emb, w_qkv, u_seq, g_qkv, w2_sides, w1_sides, wo_sides):
    seq, d_model = u_seq.shape
    blk, piece = seq // 4, d_model // 8
    n1, no = w1_sides[4].shape[1] // 4, wo_sides[3].shape[1] // 4
    assert n1 == d_model == 2 * 2 * BWD_ROWS and no * 2 == 2 * BWD_ROWS
    heads3 = qkv.shape[1]
    anywhere = pl.BlockSpec(memory_space=pl.ANY)
    in_vmem = pl.BlockSpec(memory_space=pltpu.VMEM)
    copies = 5 + 18 + 9 + 6 * 7 + 3
    dma = pltpu.SemaphoreType.DMA
    w_rows = min(128, d_model)
    return pl.pallas_call(
        last_kernel,
        in_specs=[in_vmem] * 6 + [anywhere] * 25,
        out_specs=[anywhere] * 18,
        out_shape=[
            jax.ShapeDtypeStruct((seq, d_model), BF16),
            jax.ShapeDtypeStruct((d_model, n1), F32),
            jax.ShapeDtypeStruct((8 * piece, n1), F32),
            jax.ShapeDtypeStruct((d_model, no), F32),
        ] + [jax.ShapeDtypeStruct((d_model, heads3 // 3), F32)] * 3
        + [jax.ShapeDtypeStruct((4, k * piece, n), F32) for n in (n1, n1, no) for k in (2, 1, 1)]
        + [jax.ShapeDtypeStruct((blk, n), BF16) for n in (4 * n1, d_model)],
        scratch_shapes=[
            pltpu.VMEM((seq, heads3 // 3), BF16),
            pltpu.VMEM((PAIR, seq), BF16),
            pltpu.VMEM((seq, PAIR), F32),
            pltpu.VMEM((seq, PAIR), F32),
            pltpu.VMEM((seq, 2 * BWD_ROWS), BF16),
            pltpu.VMEM((seq, 2 * BWD_ROWS), BF16),
            pltpu.VMEM((seq, heads3), BF16),
            pltpu.VMEM((blk, 4 * heads3), BF16),
            pltpu.VMEM((8, 2 * piece, n1), F32),
            pltpu.VMEM((4, 2 * piece, no), F32),
            pltpu.VMEM((8, piece, n1), F32),
            pltpu.VMEM((4, piece, no), F32),
            pltpu.VMEM((2, piece, n1), F32),
            pltpu.VMEM((2, 4, piece, no), F32),
            pltpu.VMEM((2, 3, piece, n1), F32),
            pltpu.VMEM((3, piece, no), F32),
            pltpu.VMEM((piece, n1), F32),
            pltpu.VMEM((piece, n1), F32),
            pltpu.VMEM((piece, no), F32),
            pltpu.VMEM((2, 2 * piece, heads3), F32),
            pltpu.VMEM((2, 2 * piece, heads3), F32),
            pltpu.VMEM((2, 2 * piece, heads3), F32),
            pltpu.VMEM((2 * piece, heads3), F32),
            pltpu.VMEM((2 * piece, heads3), F32),
            pltpu.VMEM((2, piece, heads3), F32),
            pltpu.VMEM((blk, d_model), BF16),
            pltpu.VMEM((2, w_rows, 4 * heads3), BF16),
            pltpu.VMEM((2, seq, 2 * piece), BF16),
            pltpu.VMEM((2, 2 * piece, heads3), F32),
            pltpu.VMEM((4 * piece, seq), BF16),
            pltpu.VMEM((2, 4 * piece, 2 * BWD_ROWS), F32),
            dma((9,)), dma((19,)), dma((copies,)), dma((copies,)),
            dma((4,)), dma((4,)), dma((24,)), dma((24,)), dma((9,)), dma((9,)), dma((10,)), dma((14,)), dma((1,)), dma((1,)),
        ],
        compiler_params=pltpu.CompilerParams(vmem_limit_bytes=63 << 20, collective_id=1, has_side_effects=True),
        cost_estimate=pl.CostEstimate(
            flops=160 * seq * seq * PAIR, bytes_accessed=128 * seq * d_model, transcendentals=seq * seq * 4),
        name="last",
    )(qkv, d_c, lse, d_mid, x, emb, w_qkv, u_seq, g_qkv, *w2_sides, *w1_sides, *wo_sides)[:7]


def solution(mesh):
    spec_col = P(None, 'model')
    spec_row = P('model', None)
    spec_act = P('data', None, None)
    spec_rep = P(None, None)

    def device_step(x_in, cot_out, step_emb, w_q, w_k, w_v, w_o, w_1, w_2):
        seq, d_model = x_in.shape[1:]
        head_cols = w_q.shape[1]
        blk = seq // 4
        piece = d_model // 8
        z = lax.axis_index('model')
        d = lax.axis_index('data')
        role = z % 2 * 2 + d % 2
        emb = step_emb.astype(F32)

        c_1, lse_1, x_seq, cot, wo, w1, w2, w_qkv = first_call(
            x_in[0], cot_out[0], emb[:1], w_q, w_k, w_v, w_o, w_1, w_2)
        wo, w2 = wo.reshape(-1, d_model), w2.reshape(-1, d_model)
        x_1 = lax.dynamic_slice_in_dim(x_seq, role * blk, blk, axis=0)

        h_1, m_1, up_1, act_1, x_2 = hidden_call(True, False, wo, w1, w2, context=c_1, x=x_1, emb=emb[:1])

        c_2, lse_2, u_2_seq, qkv_2, u_1_seq, qkv_1 = forward_call(x_2, emb, x_seq, w_qkv)
        _, m_2, _, act_2, d_up_2, d_mid_2, d_c = hidden_call(True, True, wo, w1, w2, context=c_2, x=x_2, emb=emb[1:], d_next=cot)
        shared = (act_2, act_1, cot, m_2, m_1, d_up_2, d_mid_2, c_2, c_1)
        d_2, d_2_other, g_qkv_2, *others = backward_call(
            qkv_2, d_c, lse_2, d_mid_2, x_2, emb[1:], w_qkv, u_2_seq, shared)
        act_2o, act_1o, cot_o, m_2o, m_1o, d_up_2o, d_mid_2o, c_2o, c_1o = others
        d_up_1, d_mid_1, d_c = hidden_call(False, True, wo, w1, w2, h=h_1, up=up_1, d_next=d_2)
        w2_parts = (act_2, act_2o, act_1, act_1o, cot, cot_o, d_2, d_2_other)
        w1_sides = (m_2, m_2o, m_1, m_1o, d_up_2, d_up_2o, d_up_1)
        wo_sides = (d_mid_2, d_mid_2o, d_mid_1, c_2, c_2o, c_1, c_1o)
        d_x, g_w1, g_w2, g_wo, g_q, g_k, g_v = last_call(
            qkv_1, d_c, lse_1, d_mid_1, x_1, emb[:1], w_qkv, u_1_seq, g_qkv_2, w2_parts, w1_sides, wo_sides)
        return g_q, g_k, g_v, g_wo.T, g_w1, g_w2, d_x[None]

    return jax.shard_map(device_step, mesh=mesh,
                         in_specs=(spec_act, spec_act, spec_rep, spec_col, spec_col, spec_col, spec_row, spec_col, spec_row),
                         out_specs=(spec_col, spec_col, spec_col, spec_row, spec_col, spec_row, spec_act),
                         check_vma=False)
```

```python
import functools
import math

import jax
import jax.numpy as jnp
from jax import lax
from jax.experimental import pallas as pl
from jax.experimental.pallas import tpu as pltpu
from jax.sharding import PartitionSpec as P


HEAD_DIM = 64
EPS_NORM = 1e-6
SCALE = HEAD_DIM ** -0.5
EXP2_SCALE = SCALE * math.log2(math.e)
PAIR = 2 * HEAD_DIM
FWD_ROWS = 512
BWD_ROWS = 256
KEYS = 256
HIDDEN = 1024
HIDDEN_FIRST = 512
INTERPRET = False
AXES = ('model', 'data')
BF16 = jnp.bfloat16
F32 = jnp.float32
MESH = pl.DeviceIdType.MESH

def rms_norm(values):
    return values * lax.rsqrt(jnp.mean(values * values, axis=-1, keepdims=True) + EPS_NORM)


def dot_nt(a, b):
    return lax.dot_general(a, b, (((1,), (1,)), ((), ())), preferred_element_type=F32)


def dot_nn(a, b):
    return lax.dot_general(a, b, (((1,), (0,)), ((), ())), preferred_element_type=F32)


def dot_tn(a, b):
    return lax.dot_general(a, b, (((0,), (0,)), ((), ())), preferred_element_type=F32)


def attend_rows(q, k_ref, v_t, e_refs):
    count = k_ref.shape[0] // KEYS
    lane = lax.broadcasted_iota(jnp.int32, q.shape, 1)
    q_heads = [jnp.where(lane // HEAD_DIM == head, q, jnp.zeros_like(q)) for head in range(2)]
    tops, run, total, outs, sums = [[], []], [None, None], [None, None], [], []
    for j in range(count):
        keys = slice(j * KEYS, (j + 1) * KEYS)
        for head in range(2):
            scores = dot_nt(k_ref[keys, :], q_heads[head])
            top = jnp.max(scores, axis=0, keepdims=True) * EXP2_SCALE
            if j:
                top = jnp.maximum(top, run[head])
            weights = jnp.exp2(scores * EXP2_SCALE - top)
            part = jnp.sum(weights, axis=0, keepdims=True)
            total[head] = total[head] * jnp.exp2(run[head] - top) + part if j else part
            run[head] = top
            tops[head].append(top)
            e_refs[head][keys, :] = weights
    for head in range(2):
        inverse = 1.0 / total[head]
        out = None
        for j in range(count):
            keys = slice(j * KEYS, (j + 1) * KEYS)
            factor = inverse * jnp.exp2(tops[head][j] - run[head])
            probs = (e_refs[head][keys, :] * factor).astype(BF16)
            part = dot_nn(v_t[head * HEAD_DIM:(head + 1) * HEAD_DIM, keys], probs)
            out = out + part if j else part
        sums.append(run[head] + jnp.log2(total[head]))
        outs.append(out)
    return outs, sums


class Place:
    def __init__(self):
        self.z = lax.axis_index('model')
        d = lax.axis_index('data')
        self.y, self.x, self.c = d // 4, d // 2 % 2, d % 2
        z = self.z
        self.z_by = {1: z + 1 - 2 * (z % 2), 2: (z + 2) % 4, 3: 3 - z}
        x, y, c = self.x, self.y, self.c
        self.xa, self.ya = x + (1 - c) * (1 - 2 * x), y + c * (1 - 2 * y)
        self.xb, self.yb = x + c * (1 - 2 * x), y + (1 - c) * (1 - 2 * y)
        self.role = z % 2 * 2 + c
        self.owner = c == z // 2

    def piece(self, y, x, c=None):
        return y * 4 + x * 2 + (self.c if c is None else c)

    def device(self, z=None, y=None, x=None, c=None):
        z, y, x, c = (own if given is None else given for given, own in zip((z, y, x, c), (self.z, self.y, self.x, self.c)))
        return {'model': z, 'data': y * 4 + x * 2 + c}

    def peers(self):
        column = [self.device(z=z, c=c) for z in (self.z, *self.z_by.values()) for c in (self.c, 1 - self.c)][1:]
        return column + [self.device(x=1 - self.x), self.device(y=1 - self.y)]

    def meet(self):
        barrier = pltpu.get_barrier_semaphore()
        peers = self.peers()
        for peer in peers:
            pl.semaphore_signal(barrier, inc=1, device_id=peer, device_id_type=MESH)
        pl.semaphore_wait(barrier, len(peers))


class Copies:
    def __init__(self, send_sem, recv_sem):
        self.send_sem, self.recv_sem, self.used, self.sent = send_sem, recv_sem, 0, []

    def make(self, src, dst, device):
        n, self.used = self.used, self.used + 1
        copy = pltpu.make_async_remote_copy(
            src_ref=src, dst_ref=dst, send_sem=self.send_sem.at[n], recv_sem=self.recv_sem.at[n],
            device_id=device, device_id_type=MESH)
        self.sent.append(copy)
        return copy

    def start(self, src, dst, device):
        copy = self.make(src, dst, device)
        copy.start()
        return copy


def first_kernel(x_ref, cot_ref, emb_ref, wq_ref, wk_ref, wv_ref, wo_ref, w1_ref, w2_ref,
                 c1_ref, lse_ref, xs_ref, cot_loc_ref, full_o, full_1, full_2, full_qkv,
                 x1_ref, h_ref, m_ref, up_ref, act_ref, x2_ref,
                 qkv_s, vt_s, e_a, e_b, c_buf, lse_s, cot_s, x1_s, c1_s, h_s, m_s, wo_s, w1_s, w2_s, up_s, act_s, acc,
                 local_sem, send_sem, recv_sem, c_send, c_recv, one_send, one_recv, load_sem, out_sem):
    seq, d_model = x_ref.shape
    blk = seq // 4
    head_cols = wq_ref.shape[1]
    here = Place()
    z, core, role, owner = here.z, here.c, here.role, here.owner
    here.meet()
    copies = Copies(send_sem, recv_sem)

    def span(index, count):
        return pl.ds(pl.multiple_of(index * count, count), count)

    ff_cols, out_rows, piece = w1_ref.shape[1], wo_ref.shape[0] // 8, d_model // 8
    hidden = w2_ref.shape[0] // 8

    def block_qkv(zz, e):
        return full_qkv.at[span(e, piece), span(zz, 3 * head_cols)]

    units = {
        'o': lambda zz, e: full_o.at[zz, span(e, out_rows), :],
        '1': lambda zz, e: full_1.at[span(e, piece), span(zz, ff_cols)],
        '2': lambda zz, e: full_2.at[zz, span(e, hidden), :],
        'qkv': block_qkv,
    }

    def own_parts(name, e):
        if name == 'o':
            return [(wo_ref.at[span(e, out_rows), :], units[name](z, e))]
        if name == '1':
            return [(w1_ref.at[span(e, piece), :], units[name](z, e))]
        if name == '2':
            return [(w2_ref.at[span(e, hidden), :], units[name](z, e))]
        return [(ref.at[span(e, piece), :],
                 full_qkv.at[span(e, piece), pl.ds(pl.multiple_of((z * 3 + t) * head_cols, head_cols), head_cols)])
                for t, ref in enumerate((wq_ref, wk_ref, wv_ref))]

    mine = here.piece(here.y, here.x)
    by_a = here.piece(here.ya, here.xa)
    by_b = here.piece(here.yb, here.xb)
    by_ab = here.piece(1 - here.y, 1 - here.x)
    to_a, to_b = here.device(y=here.ya, x=here.xa), here.device(y=here.yb, x=here.xb)
    partner = here.device(c=1 - core)
    stage_z, stage_a, stage_b1, stage_b2, stage_c = {}, {}, {}, {}, {}
    names = ('o', '1', '2', 'qkv')

    def make_b2(name):
        stage_b2[name] = [copies.make(units[name](here.z_by[k], by_a), units[name](here.z_by[k], by_a), to_b) for k in (1, 2, 3)]

    def make_c(name):
        stage_c[name] = [copies.make(units[name](here.z_by[k], e), units[name](here.z_by[k], e), partner)
                         for k in (1, 2, 3) for e in (mine, by_a, by_b, by_ab)]

    for name in names:
        make_b2(name)
        make_c(name)
        stage_z[name] = {k: [copies.start(src, dst, here.device(z=here.z_by[k])) for src, dst in own_parts(name, mine)]
                         for k in (1, 2, 3)}

    def forward_z(name):
        stage_a[name], stage_b1[name] = [], []
        for k in (1, 2, 3):
            for copy in stage_z[name][k]:
                copy.wait_recv()
            block = units[name](here.z_by[k], mine)
            stage_a[name].append(copies.start(block, block, to_a))
            stage_b1[name].append(copies.start(block, block, to_b))

    def forward_a(name):
        for k in range(3):
            stage_a[name][k].wait_recv()
            stage_b2[name][k].start()

    def forward_b(name):
        for k in range(3):
            stage_b1[name][k].wait_recv()
            stage_b2[name][k].wait_recv()
            for copy in stage_c[name][4 * k:4 * k + 4]:
                copy.start()

    locals_ = []

    def copy_local(src, dst):
        copy = pltpu.make_async_copy(src, dst, local_sem.at[len(locals_)])
        locals_.append(copy)
        copy.start()

    copy_local(w1_ref, full_1.at[:, span(z, ff_cols)])
    copy_local(w2_ref, full_2.at[z])
    copy_local(wo_ref, full_o.at[z])
    for t, ref in enumerate((wq_ref, wk_ref, wv_ref)):
        copy_local(ref, full_qkv.at[:, pl.ds(pl.multiple_of((z * 3 + t) * head_cols, head_cols), head_cols)])
    other_role = z % 2 * 2 + 1 - core
    give_x = pltpu.make_async_remote_copy(
        src_ref=x_ref, dst_ref=xs_ref, send_sem=one_send.at[0], recv_sem=one_recv.at[0], device_id=partner, device_id_type=MESH)
    give_cot = pltpu.make_async_remote_copy(
        src_ref=cot_ref.at[span(other_role, blk), :], dst_ref=cot_loc_ref, send_sem=one_send.at[1], recv_sem=one_recv.at[1],
        device_id=partner, device_id_type=MESH)
    keep_x = pltpu.make_async_copy(x_ref, xs_ref, local_sem.at[6])
    take_cot = pltpu.make_async_copy(cot_ref.at[span(role, blk), :], cot_s, local_sem.at[7])
    keep_cot = pltpu.make_async_copy(cot_s, cot_loc_ref, local_sem.at[8])

    @pl.when(owner)
    def _():
        give_x.start()
        give_cot.start()
        keep_x.start()
        take_cot.start()

    def project(i, _):
        rows = span(i, blk)
        unit = unit_rows(x_ref[rows, :], emb_row(emb_ref, 0))
        for t, ref in enumerate((wq_ref, wk_ref, wv_ref)):
            qkv_s[rows, t * head_cols:(t + 1) * head_cols] = dot_nn(unit, ref[...]).astype(BF16)
        return 0

    lax.fori_loop(0, 4, project, 0)

    def context_copy(j, i):
        src = c_buf.at[j, span(i, blk), :]
        dst = c1_ref.at[:, pl.ds(pl.multiple_of((z * 2 + j) * PAIR, PAIR), PAIR)]
        target_z, target_c = 2 * core + i // 2, i % 2
        remote = pltpu.make_async_remote_copy(
            src_ref=src, dst_ref=dst, send_sem=c_send.at[j * 4 + i], recv_sem=c_recv.at[j * 4 + z],
            device_id=here.device(z=target_z, c=target_c), device_id_type=MESH)
        local = pltpu.make_async_copy(src, dst, c_recv.at[j * 4 + z])
        return remote, local, jnp.logical_and(target_z == z, target_c == core)

    def send_context(j, i):
        remote, local, to_self = context_copy(j, i)
        pl.when(to_self)(local.start)
        pl.when(jnp.logical_not(to_self))(remote.start)

    moves = {(0, 1): [(forward_z, 'o')], (0, 2): [(forward_a, 'o')], (0, 3): [(forward_b, 'o')],
             (1, 2): [(forward_z, '1')], (1, 3): [(forward_a, '1')]}
    for j in range(2):
        vt_s[...] = qkv_s[:, (4 + j) * PAIR:(5 + j) * PAIR].T
        k_view = qkv_s.at[:, (2 + j) * PAIR:(3 + j) * PAIR]
        for i in range(4):
            if i or j:
                send_context(j if i else 0, i - 1 if i else 3)
            for step, name in moves.get((j, i), ()):
                step(name)
            rows = slice(i * blk, (i + 1) * blk)
            outs, sums = attend_rows(qkv_s[rows, j * PAIR:(j + 1) * PAIR], k_view, vt_s, (e_a, e_b))
            c_buf[j, rows, :] = jnp.concatenate(outs, axis=0).T.astype(BF16)
            for head in range(2):
                lse_s[2 * j + head:2 * j + head + 1, rows] = sums[head]

    @pl.when(owner)
    def _():
        take_cot.wait()
        keep_cot.start()

    forward_z('2')
    send_context(1, 3)
    give_lse = pltpu.make_async_remote_copy(
        src_ref=lse_s, dst_ref=lse_ref, send_sem=one_send.at[2], recv_sem=one_recv.at[2],
        device_id=here.device(z=2 * core + z // 2, c=z % 2), device_id_type=MESH)
    keep_lse = pltpu.make_async_copy(lse_s, lse_ref, local_sem.at[9])
    lse_stays = jnp.logical_and(2 * core + z // 2 == z, z % 2 == core)
    pl.when(lse_stays)(keep_lse.start)
    pl.when(jnp.logical_not(lse_stays))(give_lse.start)
    forward_b('1')
    forward_z('qkv')

    @pl.when(owner)
    def _():
        keep_x.wait()

    @pl.when(jnp.logical_not(owner))
    def _():
        give_x.wait_recv()

    for j in range(2):
        for zz in range(4):
            pltpu.make_async_copy(c_buf.at[j, :blk, :], c1_ref.at[:, :PAIR], c_recv.at[j * 4 + zz]).wait()

    def load(src, dst, n):
        copy = pltpu.make_async_copy(src, dst, load_sem.at[n])
        copy.start()
        return copy

    loads = [load(xs_ref.at[span(role, blk), :], x1_s, 0), load(c1_ref, c1_s, 1)]
    for copy in locals_:
        copy.wait()
    for copy in stage_c['o']:
        copy.wait_recv()
    loads += [load(full_o.at[zz], wo_s.at[zz * wo_ref.shape[0]:(zz + 1) * wo_ref.shape[0], :], 2 + zz) for zz in range(4)]
    for copy in loads:
        copy.wait()
    h = (x1_s[...].astype(F32) + emb_row(emb_ref, 0) + dot_nn(c1_s[...], wo_s[...])).astype(BF16)
    m = rms_rows(h.astype(F32)).astype(BF16)
    h_s[...], m_s[...] = h, m
    for copy in stage_c['1']:
        copy.wait_recv()
    tile = w1_s.shape[2]
    steps = full_1.shape[1] // tile
    per_plane = full_2.shape[1] // tile

    def w1_load(n):
        return pltpu.make_async_copy(full_1.at[:, span(n, tile)], w1_s.at[n % 2], load_sem.at[6 + n % 2])

    def w2_load(n):
        return pltpu.make_async_copy(full_2.at[n // per_plane, span(n % per_plane, tile), :], w2_s.at[n % 2], load_sem.at[8 + n % 2])

    def up_store(n):
        return pltpu.make_async_copy(up_s.at[n % 2], up_ref.at[:, span(n, tile)], out_sem.at[n % 2])

    w1_load(0).start()

    def up_part(n, _):
        @pl.when(n + 1 < steps)
        def _():
            w1_load(n + 1).start()

        @pl.when(n == steps // 2)
        def _():
            forward_a('2')

        @pl.when(n == steps - 1)
        def _():
            forward_a('qkv')

        w1_load(n).wait()

        @pl.when(n >= 2)
        def _():
            up_store(n - 2).wait()

        up = dot_nn(m_s[...], w1_s[n % 2]).astype(BF16)
        up_s[n % 2] = up
        factor = gelu_parts(up.astype(F32))[0]
        act_s[:, span(n, tile)] = (up.astype(F32) * factor).astype(BF16)
        up_store(n).start()
        return 0

    lax.fori_loop(0, steps, up_part, 0)
    forward_b('2')
    outs = [pltpu.make_async_copy(src, dst, out_sem.at[2 + n]) for n, (src, dst) in enumerate(
        ((x1_s, x1_ref), (h_s, h_ref), (m_s, m_ref), (act_s, act_ref)))]
    for copy in outs:
        copy.start()
    for copy in stage_c['2']:
        copy.wait_recv()
    w2_load(0).start()
    acc[...] = jnp.zeros_like(acc)

    def down_part(n, _):
        @pl.when(n + 1 < steps)
        def _():
            w2_load(n + 1).start()

        @pl.when(n == steps // 2)
        def _():
            forward_b('qkv')

        w2_load(n).wait()
        acc[...] += dot_nn(act_s[:, span(n, tile)], w2_s[n % 2])
        return 0

    lax.fori_loop(0, steps, down_part, 0)
    c1_s[...] = (h_s[...].astype(F32) + acc[...]).astype(BF16)
    out_x2 = pltpu.make_async_copy(c1_s, x2_ref, out_sem.at[6])
    for j in range(2):
        for i in range(4):
            remote, _, to_self = context_copy(j, i)
            pl.when(jnp.logical_not(to_self))(remote.wait_send)
    pl.when(lse_stays)(keep_lse.wait)

    @pl.when(jnp.logical_not(lse_stays))
    def _():
        give_lse.wait_send()
        give_lse.wait_recv()

    out_x2.start()

    @pl.when(owner)
    def _():
        give_x.wait_send()
        give_cot.wait_send()
        keep_cot.wait()

    @pl.when(jnp.logical_not(owner))
    def _():
        give_cot.wait_recv()

    for n in range(steps - 2, steps):
        up_store(n).wait()
    for copy in outs:
        copy.wait()
    out_x2.wait()
    for copy in stage_c['qkv']:
        copy.wait_recv()
    for copy in copies.sent:
        copy.wait_send()


def first_call(x, cot, emb, w_q, w_k, w_v, w_o, w_1, w_2):
    seq, d_model = x.shape
    head_cols, ff_cols, blk = w_q.shape[1], w_1.shape[1], seq // 4
    anywhere = pl.BlockSpec(memory_space=pl.ANY)
    in_vmem = pl.BlockSpec(memory_space=pltpu.VMEM)
    copies = 18 + 12 + 24 + 48
    hidden, tile = 4 * ff_cols, min(HIDDEN_FIRST, ff_cols)
    shape = jax.ShapeDtypeStruct
    dma = pltpu.SemaphoreType.DMA
    return pl.pallas_call(
        first_kernel,
        in_specs=[in_vmem, anywhere] + [in_vmem] * 7,
        out_specs=[anywhere] * 14,
        out_shape=[
            shape((blk, d_model), BF16),
            shape((4, seq), F32),
            shape((seq, d_model), BF16),
            shape((blk, d_model), BF16),
            shape((4, *w_o.shape), BF16),
            shape((d_model, hidden), BF16),
            shape((4, *w_2.shape), BF16),
            shape((d_model, 12 * head_cols), BF16),
            shape((blk, d_model), BF16),
            shape((blk, d_model), BF16),
            shape((blk, d_model), BF16),
            shape((blk, hidden), BF16),
            shape((blk, hidden), BF16),
            shape((blk, d_model), BF16),
        ],
        scratch_shapes=[
            pltpu.VMEM((seq, 3 * head_cols), BF16),
            pltpu.VMEM((PAIR, seq), BF16),
            pltpu.VMEM((seq, blk), F32),
            pltpu.VMEM((seq, blk), F32),
            pltpu.VMEM((2, seq, PAIR), BF16),
            pltpu.VMEM((4, seq), F32),
            pltpu.VMEM((blk, d_model), BF16),
            pltpu.VMEM((blk, d_model), BF16),
            pltpu.VMEM((blk, d_model), BF16),
            pltpu.VMEM((blk, d_model), BF16),
            pltpu.VMEM((blk, d_model), BF16),
            pltpu.VMEM((d_model, d_model), BF16),
            pltpu.VMEM((2, d_model, tile), BF16),
            pltpu.VMEM((2, tile, d_model), BF16),
            pltpu.VMEM((2, blk, tile), BF16),
            pltpu.VMEM((blk, hidden), BF16),
            pltpu.VMEM((blk, d_model), F32),
            dma((10,)), dma((copies,)), dma((copies,)), dma((8,)), dma((8,)), dma((3,)), dma((3,)), dma((10,)), dma((7,)),
        ],
        compiler_params=pltpu.CompilerParams(vmem_limit_bytes=60 << 20, collective_id=0, has_side_effects=True),
        cost_estimate=pl.CostEstimate(
            flops=64 * seq * seq * PAIR, bytes_accessed=64 * seq * d_model, transcendentals=seq * seq * 4),
        name="first",
    )(x, cot, emb, w_q, w_k, w_v, w_o, w_1, w_2)


def emb_row(emb_ref, row):
    return emb_ref[...].astype(F32)[row:row + 1, :]


def unit_rows(values, emb):
    values = values.astype(F32) + emb
    return (values * lax.rsqrt(jnp.mean(values * values, axis=-1, keepdims=True) + EPS_NORM)).astype(BF16)


def forward_kernel(x_ref, emb_ref, xs1_ref, wqkv_ref,
                   c_ref, lse_ref, u2_ref, qkv2_ref, u1_ref, qkv1_ref,
                   w_s, blocks, u_s, qkv_s, x1_s, u1_s, qkv1_s, v_t, e_a, e_b, c_buf, lse_s,
                   local_sem, first_sem, out_sem, x_send, x_recv, c_send, c_recv):
    seq = xs1_ref.shape[0]
    blk = seq // 4
    head_cols = 2 * PAIR
    here = Place()
    z, core, role = here.z, here.c, here.role

    def span(index, count):
        return pl.ds(pl.multiple_of(index * count, count), count)

    w_load = pltpu.make_async_copy(wqkv_ref.at[:, span(role, 3 * head_cols)], w_s, local_sem.at[0])
    w_load.start()
    x1_load = [pltpu.make_async_copy(xs1_ref.at[i * blk:(i + 1) * blk, :], x1_s.at[i % 2], first_sem.at[i % 2]) for i in range(4)]
    x1_load[0].start()
    here.meet()
    partner, across = here.device(c=1 - core), here.device(z=here.z_by[1])
    role_side, role_over = z % 2 * 2 + 1 - core, (1 - z % 2) * 2 + core
    role_last = (1 - z % 2) * 2 + 1 - core

    def x_copy(n, src, slot, device):
        return pltpu.make_async_remote_copy(
            src_ref=src, dst_ref=blocks.at[slot], send_sem=x_send.at[n], recv_sem=x_recv.at[n],
            device_id=device, device_id_type=MESH)

    over, side = x_copy(0, x_ref, 0, across), x_copy(1, x_ref, 1, partner)
    last = x_copy(2, blocks.at[0], 2, partner)
    over.start()
    side.start()

    def project(src, at_role):
        rows = span(at_role, blk)
        unit = unit_rows(src, emb_row(emb_ref, 1))
        u_s[rows, :] = unit
        qkv_s[rows, :] = dot_nn(unit, w_s[...]).astype(BF16)

    w_load.wait()
    project(x_ref[...], role)
    side.wait_recv()
    project(blocks[1], role_side)

    stores = []
    for i in range(4):
        if i < 3:
            x1_load[i + 1].start()
        x1_load[i].wait()
        if i >= 2:
            for copy in stores[i - 2]:
                copy.wait()
        unit = unit_rows(x1_s[i % 2], emb_row(emb_ref, 0))
        u1_s[i % 2] = unit
        qkv1_s[i % 2] = dot_nn(unit, w_s[...]).astype(BF16)
        stores.append([pltpu.make_async_copy(u1_s.at[i % 2], u1_ref.at[i * blk:(i + 1) * blk, :], out_sem.at[i % 2]),
                       pltpu.make_async_copy(qkv1_s.at[i % 2], qkv1_ref.at[i * blk:(i + 1) * blk, :], out_sem.at[2 + i % 2])])
        for copy in stores[i]:
            copy.start()

    over.wait_recv()
    last.start()
    project(blocks[0], role_over)
    last.wait_recv()
    project(blocks[2], role_last)
    keep_u = pltpu.make_async_copy(u_s, u2_ref, local_sem.at[1])
    keep_qkv = pltpu.make_async_copy(qkv_s, qkv2_ref, local_sem.at[2])
    keep_u.start()
    keep_qkv.start()

    member = [here.device(z=z // 2 * 2 + i // 2, c=i % 2) for i in range(4)]

    def c_copy(j, i):
        src = c_buf.at[j, i * blk:(i + 1) * blk, :]
        dst = c_ref.at[:, pl.ds(pl.multiple_of((role * 2 + j) * PAIR, PAIR), PAIR)]
        remote = pltpu.make_async_remote_copy(
            src_ref=src, dst_ref=dst, send_sem=c_send.at[j * 4 + i], recv_sem=c_recv.at[j * 4 + role],
            device_id=member[i], device_id_type=MESH)
        return remote, pltpu.make_async_copy(src, dst, c_recv.at[j * 4 + role])

    def send_context(j, i):
        remote, local = c_copy(j, i)
        pl.when(role == i)(local.start)
        pl.when(role != i)(remote.start)

    for j in range(2):
        v_t[...] = qkv_s[:, (4 + j) * PAIR:(5 + j) * PAIR].T
        k_view = qkv_s.at[:, (2 + j) * PAIR:(3 + j) * PAIR]
        for i in range(4):
            if i or j:
                send_context(j if i else 0, i - 1 if i else 3)
            rows = slice(i * blk, (i + 1) * blk)
            outs, sums = attend_rows(qkv_s[rows, j * PAIR:(j + 1) * PAIR], k_view, v_t, (e_a, e_b))
            c_buf[j, rows, :] = jnp.concatenate(outs, axis=0).T.astype(BF16)
            for head in range(2):
                lse_s[2 * j + head:2 * j + head + 1, rows] = sums[head]
    lse_ref[...] = lse_s[...]
    send_context(1, 3)
    for j in range(2):
        for i in range(4):
            pltpu.make_async_copy(c_buf.at[j, :blk, :], c_ref.at[:, :PAIR], c_recv.at[j * 4 + i]).wait()
            pl.when(role != i)(c_copy(j, i)[0].wait_send)
    for copy in (over, side, last):
        copy.wait_send()
    for group in stores[2:]:
        for copy in group:
            copy.wait()
    keep_u.wait()
    keep_qkv.wait()


def forward_call(x, emb, xs_1, w_qkv):
    blk, d_model = x.shape
    seq, head_cols = 4 * blk, 2 * PAIR
    anywhere = pl.BlockSpec(memory_space=pl.ANY)
    in_vmem = pl.BlockSpec(memory_space=pltpu.VMEM)
    dma = pltpu.SemaphoreType.DMA
    return pl.pallas_call(
        forward_kernel,
        in_specs=[in_vmem, in_vmem, anywhere, anywhere],
        out_specs=[anywhere, in_vmem] + [anywhere] * 4,
        out_shape=[
            jax.ShapeDtypeStruct((blk, d_model), BF16),
            jax.ShapeDtypeStruct((4, seq), F32),
        ] + [jax.ShapeDtypeStruct((seq, n), BF16) for n in (d_model, 3 * head_cols)] * 2,
        scratch_shapes=[
            pltpu.VMEM((d_model, 3 * head_cols), BF16),
            pltpu.VMEM((3, blk, d_model), BF16),
            pltpu.VMEM((seq, d_model), BF16),
            pltpu.VMEM((seq, 3 * head_cols), BF16),
            pltpu.VMEM((2, blk, d_model), BF16),
            pltpu.VMEM((2, blk, d_model), BF16),
            pltpu.VMEM((2, blk, 3 * head_cols), BF16),
            pltpu.VMEM((PAIR, seq), BF16),
            pltpu.VMEM((seq, blk), F32),
            pltpu.VMEM((seq, blk), F32),
            pltpu.VMEM((2, seq, PAIR), BF16),
            pltpu.VMEM((4, seq), F32),
            dma((3,)), dma((2,)), dma((4,)), dma((3,)), dma((3,)), dma((8,)), dma((8,)),
        ],
        compiler_params=pltpu.CompilerParams(vmem_limit_bytes=60 << 20, collective_id=2, has_side_effects=True),
        cost_estimate=pl.CostEstimate(
            flops=64 * seq * seq * PAIR, bytes_accessed=32 * seq * d_model, transcendentals=seq * seq * 4),
        name="forward",
    )(x, emb, xs_1, w_qkv)


def through_norm(values, up, d_mid):
    inverse = lax.rsqrt(jnp.mean(values * values, axis=-1, keepdims=True) + EPS_NORM)
    inner = jnp.mean(values * up, axis=-1, keepdims=True)
    return (d_mid.astype(F32) + inverse * up - values * (inverse * inverse * inverse * inner)).astype(BF16)


def backward_kernel(shared, qkv_ref, dc_ref, lse_ref, dmid_ref, x_ref, emb_ref, wqkv_ref, u_ref, *refs):
    sources, (d_ref, other_ref, g_ref), shares = refs[:shared], refs[shared:shared + 3], refs[shared + 3:2 * shared + 3]
    (dch, k_t, dk_acc, dv_acc, p_cat, ds_cat, d_heads, d_qkv, d_u, w_s, u_s, g_s,
     load_sem, out_sem, dc_send, dc_recv, dq_send, dq_recv, d_send, d_recv, s_send, s_recv) = refs[2 * shared + 3:]
    seq = qkv_ref.shape[0]
    blk = seq // 4
    head_cols = 2 * PAIR
    here = Place()
    z, core, role = here.z, here.c, here.role
    here.meet()
    member = [here.device(z=z // 2 * 2 + i // 2, c=i % 2) for i in range(4)]

    def span(index, count):
        return pl.ds(pl.multiple_of(index * count, count), count)

    def load(src, dst, n):
        copy = pltpu.make_async_copy(src, dst, load_sem.at[n])
        copy.start()
        return copy

    def dc_copy(j, i):
        col = i * head_cols + j * PAIR
        return pltpu.make_async_remote_copy(
            src_ref=dc_ref.at[:, col:col + PAIR], dst_ref=dch.at[span(role, blk), j * PAIR:(j + 1) * PAIR],
            send_sem=dc_send.at[j * 4 + i], recv_sem=dc_recv.at[j * 4 + role], device_id=member[i], device_id_type=MESH)

    for j in range(2):
        for i in range(4):
            pl.when(role != i)(dc_copy(j, i).start)
    for i in range(4):
        @pl.when(role == i)
        def _():
            dch[i * blk:(i + 1) * blk, :] = dc_ref[:, i * head_cols:(i + 1) * head_cols]

    def dq_copy(j, i, t):
        col = t * head_cols + j * PAIR
        return pltpu.make_async_remote_copy(
            src_ref=d_heads.at[i * blk:(i + 1) * blk, col:col + PAIR],
            dst_ref=d_qkv.at[:, pl.ds(pl.multiple_of(role * 3 * head_cols + col, PAIR), PAIR)],
            send_sem=dq_send.at[(j * 4 + i) * 3 + t], recv_sem=dq_recv.at[(j * 4 + role) * 3 + t],
            device_id=member[i], device_id_type=MESH)

    def send_d_heads(j, ts):
        for i in range(4):
            @pl.when(role != i)
            def _():
                for t in ts:
                    dq_copy(j, i, t).start()

    shared_copies = [pltpu.make_async_remote_copy(
        src_ref=src, dst_ref=dst, send_sem=s_send.at[n], recv_sem=s_recv.at[n],
        device_id=here.device(c=1 - core), device_id_type=MESH) for n, (src, dst) in enumerate(zip(sources, shares))]

    steps = seq // BWD_ROWS
    for j in range(2):
        for i in range(4):
            @pl.when(role != i)
            def _():
                pltpu.make_async_copy(dc_ref.at[:, :PAIR], dch.at[:blk, :PAIR], dc_recv.at[j * 4 + i]).wait()
        if j == 0:
            for copy in shared_copies:
                copy.start()
        k_view, v_view = qkv_ref.at[:, (2 + j) * PAIR:(3 + j) * PAIR], qkv_ref.at[:, (4 + j) * PAIR:(5 + j) * PAIR]
        k_t[...] = k_view[...].T
        dk_acc[...] = jnp.zeros_like(dk_acc)
        dv_acc[...] = jnp.zeros_like(dv_acc)

        def block(i, _):
            if j == 1:
                @pl.when(i == 1)
                def _():
                    send_d_heads(0, (0, 1, 2))

                for target in range(3):
                    @pl.when(jnp.logical_and(i == (target + 1) * (steps // 4) + steps // 8, role != target))
                    def _():
                        dq_copy(1, target, 0).start()
            rows = span(i, BWD_ROWS)
            cols = slice(j * PAIR, (j + 1) * PAIR)
            d_heads[rows, cols] = backward_rows(
                qkv_ref[rows, cols], dch[rows, cols], lse_ref[2 * j:2 * j + 2, rows], k_view, v_view,
                k_t, p_cat, ds_cat, dk_acc, dv_acc)
            return 0

        lax.fori_loop(0, steps, block, 0)
        d_heads[:, head_cols + j * PAIR:head_cols + (j + 1) * PAIR] = (dk_acc[...] * SCALE).astype(BF16)
        d_heads[:, 2 * head_cols + j * PAIR:2 * head_cols + (j + 1) * PAIR] = dv_acc[...].astype(BF16)

    quarter = u_s.shape[2]
    pending = load(u_ref.at[:, :quarter], u_s.at[0], 0)
    for i in range(4):
        @pl.when(role == i)
        def _():
            d_qkv[:, i * 3 * head_cols:(i + 1) * 3 * head_cols] = d_heads[i * blk:(i + 1) * blk, :]
    pl.when(role != 3)(dq_copy(1, 3, 0).start)
    send_d_heads(1, (1, 2))
    stores = []
    count = u_ref.shape[1] // quarter
    for n in range(count):
        ahead = load(u_ref.at[:, (n + 1) * quarter:(n + 2) * quarter], u_s.at[(n + 1) % 2], (n + 1) % 2) if n + 1 < count else None
        pending.wait()
        if n >= 2:
            stores[n - 2].wait()
        g_s[n % 2] = dot_tn(u_s[n % 2], d_heads[...])
        stores.append(pltpu.make_async_copy(g_s.at[n % 2], g_ref.at[n * quarter:(n + 1) * quarter, :], out_sem.at[n % 2]))
        stores[n].start()
        pending = ahead
    w_rows = w_s.shape[1]
    chunks = wqkv_ref.shape[0] // w_rows
    w_load = load(wqkv_ref.at[:w_rows, :], w_s.at[0], 2)
    for j in range(2):
        for i in range(4):
            @pl.when(role != i)
            def _():
                for t in range(3):
                    pltpu.make_async_copy(d_heads.at[:blk, :PAIR], d_qkv.at[:, :PAIR], dq_recv.at[(j * 4 + i) * 3 + t]).wait()
    for n in range(chunks):
        ahead = load(wqkv_ref.at[(n + 1) * w_rows:(n + 2) * w_rows, :], w_s.at[(n + 1) % 2], 2 + (n + 1) % 2) if n + 1 < chunks else None
        w_load.wait()
        d_u[:, n * w_rows:(n + 1) * w_rows] = dot_nt(d_qkv[...], w_s[n % 2]).astype(BF16)
        w_load = ahead
    rows_each = min(128, blk)
    for n in range(blk // rows_each):
        rows = slice(n * rows_each, (n + 1) * rows_each)
        d_u[rows, :] = through_norm(x_ref[rows, :].astype(F32) + emb_row(emb_ref, 1), d_u[rows, :].astype(F32), dmid_ref[rows, :])
    keep = pltpu.make_async_copy(d_u, d_ref, out_sem.at[2])
    keep.start()
    stores[count - 2].wait()
    stores[count - 1].wait()
    give = pltpu.make_async_remote_copy(
        src_ref=d_u, dst_ref=other_ref, send_sem=d_send.at[0], recv_sem=d_recv.at[0],
        device_id=here.device(c=1 - core), device_id_type=MESH)
    give.start()
    for i in range(4):
        @pl.when(role != i)
        def _():
            for j in range(2):
                dc_copy(j, i).wait_send()
                for t in range(3):
                    dq_copy(j, i, t).wait_send()
    keep.wait()
    give.wait()
    for copy in shared_copies:
        copy.wait()


def backward_call(qkv, d_c, lse, d_mid, x, emb, w_qkv, u_seq, shared):
    seq, d_model = u_seq.shape
    blk, heads3 = seq // 4, qkv.shape[1]
    anywhere = pl.BlockSpec(memory_space=pl.ANY)
    in_vmem = pl.BlockSpec(memory_space=pltpu.VMEM)
    dma = pltpu.SemaphoreType.DMA
    quarter = d_model // 4
    return pl.pallas_call(
        functools.partial(backward_kernel, len(shared)),
        in_specs=[in_vmem] * 6 + [anywhere] * (2 + len(shared)),
        out_specs=[anywhere] * (3 + len(shared)),
        out_shape=[
            jax.ShapeDtypeStruct((blk, d_model), BF16),
            jax.ShapeDtypeStruct((blk, d_model), BF16),
            jax.ShapeDtypeStruct((d_model, heads3), F32),
        ] + [jax.ShapeDtypeStruct(value.shape, value.dtype) for value in shared],
        scratch_shapes=[
            pltpu.VMEM((seq, heads3 // 3), BF16),
            pltpu.VMEM((PAIR, seq), BF16),
            pltpu.VMEM((seq, PAIR), F32),
            pltpu.VMEM((seq, PAIR), F32),
            pltpu.VMEM((seq, 2 * BWD_ROWS), BF16),
            pltpu.VMEM((seq, 2 * BWD_ROWS), BF16),
            pltpu.VMEM((seq, heads3), BF16),
            pltpu.VMEM((blk, 4 * heads3), BF16),
            pltpu.VMEM((blk, d_model), BF16),
            pltpu.VMEM((2, quarter, 4 * heads3), BF16),
            pltpu.VMEM((2, seq, quarter), BF16),
            pltpu.VMEM((2, quarter, heads3), F32),
            dma((4,)), dma((3,)), dma((8,)), dma((8,)), dma((24,)), dma((24,)), dma((1,)), dma((1,)),
            dma((len(shared),)), dma((len(shared),)),
        ],
        compiler_params=pltpu.CompilerParams(vmem_limit_bytes=60 << 20, collective_id=3, has_side_effects=True),
        cost_estimate=pl.CostEstimate(
            flops=160 * seq * seq * PAIR, bytes_accessed=64 * seq * d_model, transcendentals=seq * seq * 4),
        name="backward",
    )(qkv, d_c, lse, d_mid, x, emb, w_qkv, u_seq, *shared)


def rms_rows(values):
    return values * lax.rsqrt(jnp.mean(values * values, axis=-1, keepdims=True) + EPS_NORM)


GELU_IN, GELU_CUBE = math.sqrt(2 / math.pi), 0.044715


def gelu_parts(z):
    square = z * z
    t = jnp.tanh(z * (GELU_IN + (GELU_IN * GELU_CUBE) * square))
    return 0.5 + 0.5 * t, t, square


def hidden_kernel(backward, forward, *refs):
    refs = list(refs)
    take = lambda: refs.pop(0)
    if forward:
        c_ref, x_ref, emb_ref, wo_ref = take(), take(), take(), take()
        w1_ref = take()
    else:
        h_ref, wo_ref, up_ref = take(), take(), take()
    w2_ref = take()
    if backward:
        d_ref, w1b_ref = take(), take()
    if forward:
        h_out, m_out = take(), take()
        up_out, act_out = take(), take()
    if backward:
        dup_out, dmid_out, dc_out = take(), take(), take()
    else:
        x_out = take()
    if forward:
        h_s, m_s = take(), take()
    prev_s, acc = take(), take()
    step, last = pl.program_id(0), pl.num_programs(0) - 1

    if forward:
        @pl.when(step == 0)
        def _():
            h = (x_ref[...].astype(F32) + emb_row(emb_ref, 1) + dot_nn(c_ref[...], wo_ref[...])).astype(BF16)
            m = rms_rows(h.astype(F32)).astype(BF16)
            h_s[...], m_s[...] = h, m
            h_out[...], m_out[...] = h, m

    def first_part():
        slot = step % 2
        if backward:
            d_act = dot_nt(d_ref[...], w2_ref[...]).astype(BF16).astype(F32)
        if forward:
            up = dot_nn(m_s[...], w1_ref[...]).astype(BF16)
            up_out[...] = up
        else:
            up = up_ref[...]
        z = up.astype(F32)
        factor, t, square = gelu_parts(z)
        if forward:
            act = (z * factor).astype(BF16)
            act_out[...] = act
        if backward:
            slope = factor + z * ((1.0 - t * t) * (0.5 * GELU_IN + (1.5 * GELU_IN * GELU_CUBE) * square))
            d_up = (slope * d_act).astype(BF16)
            dup_out[...] = d_up
            prev_s[slot] = d_up
        else:
            prev_s[slot] = act

    def second_part():
        prev = prev_s[1 - step % 2]
        if backward:
            return dot_nt(prev, w1b_ref[...])
        return dot_nn(prev, w2_ref[...])

    pl.when(step == 0)(first_part)

    @pl.when(step == 1)
    def _():
        acc[...] = second_part()
        first_part()

    @pl.when(jnp.logical_and(step > 1, step < last))
    def _():
        acc[...] += second_part()
        first_part()

    @pl.when(step == last)
    def _():
        total = acc[...] + second_part()
        if backward:
            h = (h_s if forward else h_ref)[...].astype(F32)
            d_mid = through_norm(h, total.astype(BF16).astype(F32), d_ref[...])
            dmid_out[...] = d_mid
            dc_out[...] = dot_nt(d_mid, wo_ref[...]).astype(BF16)
        else:
            x_out[...] = (h_s[...].astype(F32) + total).astype(BF16)


def hidden_call(forward, backward, w_o, w_1, w_2, context=None, x=None, emb=None, h=None, up=None, d_next=None):
    blk, d_model = (context if forward else h).shape
    hidden = w_1.shape[1]
    tile = HIDDEN
    steps = hidden // tile
    now, before = (lambda i: jnp.minimum(i, steps - 1)), (lambda i: jnp.maximum(i - 1, 0))
    whole = lambda rows, cols: pl.BlockSpec((rows, cols), lambda i: (0, 0))
    wide = pl.BlockSpec((blk, tile), lambda i: (0, now(i)))
    args, specs = [], []

    def add(value, spec):
        args.append(value)
        specs.append(spec)

    if forward:
        add(context, whole(blk, d_model))
        add(x, whole(blk, d_model))
        add(emb, whole(2, d_model))
        add(w_o, whole(d_model, d_model))
        add(w_1, pl.BlockSpec((d_model, tile), lambda i: (0, now(i))))
    else:
        add(h, whole(blk, d_model))
        add(w_o, whole(d_model, d_model))
        add(up, wide)
    add(w_2, pl.BlockSpec((tile, d_model), (lambda i: (now(i), 0)) if backward else (lambda i: (before(i), 0))))
    if backward:
        add(d_next, whole(blk, d_model))
        add(w_1, pl.BlockSpec((d_model, tile), lambda i: (0, before(i))))
    row = (whole(blk, d_model), jax.ShapeDtypeStruct((blk, d_model), BF16))
    big = (wide, jax.ShapeDtypeStruct((blk, hidden), BF16))
    outs = ([row, row, big, big] if forward else []) + ([big, row, row] if backward else [row])
    return pl.pallas_call(
        functools.partial(hidden_kernel, backward, forward),
        grid=(steps + 1,),
        in_specs=specs,
        out_specs=[spec for spec, _ in outs],
        out_shape=[shape for _, shape in outs],
        scratch_shapes=([pltpu.VMEM((blk, d_model), BF16)] * 2 if forward else [])
        + [pltpu.VMEM((2, blk, tile), BF16), pltpu.VMEM((blk, d_model), F32)],
        compiler_params=pltpu.CompilerParams(vmem_limit_bytes=60 << 20),
        cost_estimate=pl.CostEstimate(
            flops=2 * blk * d_model * (hidden * (3 if forward and backward else 2) + 2 * d_model),
            bytes_accessed=4 * hidden * d_model + 8 * blk * hidden, transcendentals=blk * hidden),
        interpret=INTERPRET,
        name="hidden",
    )(*args)


def backward_rows(q, d_out, lse, k_ref, v_ref, k_t, p_cat, ds_cat, dk_acc, dv_acc):
    block = q.shape[0]
    lane = lax.broadcasted_iota(jnp.int32, q.shape, 1)
    q_heads, do_heads, dqs = [], [], []
    for head in range(2):
        mine = lane // HEAD_DIM == head
        q_head = jnp.where(mine, q, jnp.zeros_like(q))
        do_head = jnp.where(mine, d_out, jnp.zeros_like(d_out))
        scores = dot_nt(k_ref[...], q_head)
        probs = jnp.exp2(scores * EXP2_SCALE - lse[head:head + 1, :])
        d_probs = dot_nt(v_ref[...], do_head).astype(BF16).astype(F32)
        inner = jnp.sum(probs * d_probs, axis=0, keepdims=True)
        cols = slice(head * block, (head + 1) * block)
        p_cat[:, cols] = probs.astype(BF16)
        ds_cat[:, cols] = (probs * (d_probs - inner)).astype(BF16)
        dqs.append(dot_nn(k_t[head * HEAD_DIM:(head + 1) * HEAD_DIM, :], ds_cat[:, cols]))
        q_heads.append(q_head)
        do_heads.append(do_head)
    dv_acc[...] += dot_nn(p_cat[...], jnp.concatenate(do_heads, axis=0))
    dk_acc[...] += dot_nn(ds_cat[...], jnp.concatenate(q_heads, axis=0))
    return (jnp.concatenate(dqs, axis=0).T * SCALE).astype(BF16)


def last_kernel(qkv_ref, dc_ref, lse_ref, dmid_ref, x_ref, emb_ref, wqkv_ref, u_ref, gqkv2_ref,
                *refs):
    lefts = {'2': refs[:4], '1': refs[8:12], 'o': refs[15:18]}
    rights = {'2': refs[4:8], '1': refs[12:15], 'o': refs[18:22]}
    (dx_ref, g1_ref, g2_ref, go_ref, gq_ref, gk_ref, gv_ref, away2_ref, mid2_ref, keep2_ref,
     away1_ref, mid1_ref, keep1_ref, awayo_ref, mido_ref, keepo_ref, dup_other, dmid_other,
     dch, k_t, dk_acc, dv_acc, p_cat, ds_cat, d_heads, d_qkv, buf, buf_o, second, second_o, tmp, tmp_o,
     third, third_o, sum_1, sum_2, sum_o, qa, qb, q1, q2, q3, q4, d_1, w_s, u_s, g_s,
     left_t, stage,
     local_sem, load_sem, send_sem, recv_sem, dc_send, dc_recv, dq_send, dq_recv, z_send, z_recv, x_send, x_recv,
     p_send, p_recv) = refs[22:]
    seq = qkv_ref.shape[0]
    blk = seq // 4
    head_cols = 2 * PAIR
    here = Place()
    z, core, role, owner = here.z, here.c, here.role, here.owner
    here.meet()
    copies = Copies(send_sem, recv_sem)
    waits = []

    def span(index, count):
        return pl.ds(pl.multiple_of(index * count, count), count)

    def load(src, dst, n):
        copy = pltpu.make_async_copy(src, dst, load_sem.at[n])
        copy.start()
        return copy

    no = jnp.logical_not
    to_a, to_b = here.device(y=here.ya, x=here.xa), here.device(y=here.yb, x=here.xb)
    partner = here.device(c=1 - core)
    member = [here.device(z=z // 2 * 2 + i // 2, c=i % 2) for i in range(4)]
    piece = tmp.shape[1]

    def dc_copy(i):
        return pltpu.make_async_remote_copy(
            src_ref=dc_ref.at[:, i * head_cols:(i + 1) * head_cols], dst_ref=dch.at[span(role, blk), :],
            send_sem=dc_send.at[i], recv_sem=dc_recv.at[role], device_id=member[i], device_id_type=MESH)

    for i in range(4):
        pl.when(role != i)(dc_copy(i).start)

        @pl.when(role == i)
        def _():
            dch[i * blk:(i + 1) * blk, :] = dc_ref[:, i * head_cols:(i + 1) * head_cols]

    half = rights['1'][0].shape[1] // 8
    wide = 2 * half
    dmid_give = copies.start(lefts['o'][2], dmid_other, partner)
    dup_give = [copies.start(rights['1'][2].at[:, q * wide:(q + 1) * wide], dup_other.at[:, q * wide:(q + 1) * wide], partner)
                for q in range(4)]
    lefts['o'] = (*lefts['o'], dmid_other)
    rights['1'] = (*rights['1'], dup_other)
    firsts = {(w, q): [copies.make(ref.at[q, :, h * half:(h + 1) * half], buf.at[u + q, :, h * half:(h + 1) * half], to_a)
                       for h in range(2)] for w, ref, u in (('2', away2_ref, 0), ('1', away1_ref, 4)) for q in range(4)}
    firsts['o'] = [copies.make(awayo_ref.at[2 * h:2 * h + 2], buf_o.at[2 * h:2 * h + 2], to_a) for h in range(2)]
    seconds = {(w, q): copies.make(buf.at[u + q, piece:, :], second.at[u + q], to_b) for w, u in (('2', 0), ('1', 4)) for q in range(4)}
    seconds['o'] = copies.make(buf_o.at[:, piece:, :], second_o, to_b)

    def add_mid(unit):
        if unit == 'o':
            mid, keep, t, n = mido_ref, keepo_ref, tmp_o, 4
            bottom, top = buf_o.at[:, piece:, :], buf_o.at[:, :piece, :]
        else:
            w, q = unit
            mid, keep = (mid2_ref.at[q], keep2_ref.at[q]) if w == '2' else (mid1_ref.at[q], keep1_ref.at[q])
            u = q if w == '2' else 4 + q
            t, n, bottom, top = tmp, 6, buf.at[u, piece:, :], buf.at[u, :piece, :]
        loads = [load(mid, t.at[0], n), load(keep, t.at[1], n + 1)]
        for copy in firsts[unit]:
            copy.wait_recv()
        for copy in loads:
            copy.wait()
        bottom[...] += t[0]
        top[...] += t[1]
        seconds[unit].start()

    sums = {'2': (lambda q: buf.at[q, :piece, :], third.at[0], 0), '1': (lambda q: buf.at[4 + q, :piece, :], third.at[1], 1),
            'o': (lambda q: buf_o.at[q, :piece, :], third_o, 2)}
    far_q = here.z_by[2]

    def near_copy(w, q):
        part, got, n = sums[w]
        return pltpu.make_async_remote_copy(
            src_ref=part(q), dst_ref=got.at[q // 2], send_sem=z_send.at[n * 3 + q // 2], recv_sem=z_recv.at[n * 3 + q // 2],
            device_id=here.device(z=here.z_by[1]), device_id_type=MESH)

    def far_copy(w):
        part, got, n = sums[w]
        return pltpu.make_async_remote_copy(
            src_ref=part(far_q), dst_ref=got.at[2], send_sem=z_send.at[n * 3 + 2], recv_sem=z_recv.at[n * 3 + 2],
            device_id=here.device(z=far_q), device_id_type=MESH)

    def finish(unit):
        seconds[unit].wait_recv()
        if unit == 'o':
            buf_o[:, :piece, :] += second_o[...]
            w, qs = 'o', range(4)
        else:
            w, u = unit[0], unit[1] + (4 if unit[0] == '1' else 0)
            buf[u, :piece, :] += second[u]
            qs = (unit[1],)
        for q in qs:
            pl.when((z + q) % 2 == 1)(near_copy(w, q).start)

    def far(w):
        part, got, n = sums[w]
        for k in range(2):
            pltpu.make_async_copy(got.at[2], got.at[k], z_recv.at[n * 3 + k]).wait()
        theirs, ours = part(far_q), part(z)
        theirs[...] += got[far_q // 2]
        ours[...] += got[z // 2]
        far_copy(w).start()

    mine, by_a = here.piece(here.y, here.x), here.piece(here.ya, here.xa)
    by_b, by_ab = here.piece(here.yb, here.xb), here.piece(1 - here.y, 1 - here.x)
    gathers = {}

    def total(w):
        part, got, n = sums[w]
        out = {'2': sum_2, '1': sum_1, 'o': sum_o}[w]
        far_copy(w).wait_recv()
        out[...] = part(z)[...] + got[2]

    def gather_start(name, src, out, n):
        rows = lambda e: out.at[span(e, piece), :]
        keep = pltpu.make_async_copy(src, rows(mine), local_sem.at[n])
        keep.start()
        waits.append(keep)
        gathers[name] = dict(src=src, rows=rows, a=copies.start(src, rows(mine), to_a), b1=copies.start(src, rows(mine), to_b))

    def gather_second(name):
        g = gathers[name]
        g['a'].wait_recv()
        g['b2'] = copies.start(g['rows'](by_a), g['rows'](by_a), to_b)

    def gather_core(name):
        g = gathers[name]
        g['c'] = [copies.start(g['src'], g['rows'](mine), partner), copies.start(g['rows'](by_a), g['rows'](by_a), partner)]
        g['b1'].wait_recv()
        g['c'].append(copies.start(g['rows'](by_b), g['rows'](by_b), partner))
        g['b2'].wait_recv()
        g['c'].append(copies.start(g['rows'](by_ab), g['rows'](by_ab), partner))

    def dq_copy(j, i, t):
        col = t * head_cols + j * PAIR
        return pltpu.make_async_remote_copy(
            src_ref=d_heads.at[i * blk:(i + 1) * blk, col:col + PAIR],
            dst_ref=d_qkv.at[:, pl.ds(pl.multiple_of(role * 3 * head_cols + col, PAIR), PAIR)],
            send_sem=dq_send.at[(j * 4 + i) * 3 + t], recv_sem=dq_recv.at[(j * 4 + role) * 3 + t],
            device_id=member[i], device_id_type=MESH)

    def send_d_heads(j):
        for i in range(4):
            @pl.when(role != i)
            def _():
                for t in range(3):
                    dq_copy(j, i, t).start()

    index = [here.ya * 2 + here.xa, (1 - here.y) * 2 + 1 - here.x, here.yb * 2 + here.xb, here.y * 2 + here.x]
    spaces = (p_cat, ds_cat)
    parts = [('2', n) for n in range(8)] + [('1', n) for n in range(8)] + [('o', n) for n in range(2)]
    left_loads = [('2', q) for q in range(4)] + [('1', 0), ('o', 0)]

    def load_lefts(name, q):
        for n in range(16):
            pltpu.make_async_copy(
                lefts[name][n // 4].at[:, span(q * 8 + index[n % 4] * 2 + core, piece)],
                d_heads.at[n // 4 * blk:(n // 4 + 1) * blk, n % 4 * piece:(n % 4 + 1) * piece], load_sem.at[14]).start()

    def load_rights(s):
        name, n = parts[s]
        for i in range(4):
            pltpu.make_async_copy(
                rights[name][i].at[:, n * half:(n + 1) * half], spaces[s % 2].at[i * blk:(i + 1) * blk, :],
                load_sem.at[15 + s % 2]).start()

    def stored(s):
        pltpu.make_async_copy(stage.at[s % 2], stage.at[s % 2], load_sem.at[17 + s % 2]).wait()

    def send_part(s):
        name, n = parts[s]
        if name == 'o':
            firsts['o'][n].start()
        else:
            firsts[(name, n // 2)][n % 2].start()

    load_lefts(*left_loads[0])
    load_rights(0)
    load_rights(1)
    for s in range(len(parts)):
        name, n = parts[s]
        if n == 0 or name == '2' and n % 2 == 0:
            every = d_heads.at[:, :4 * piece]
            pltpu.make_async_copy(every, every, load_sem.at[14]).wait()
            left_t[...] = every[...].T
            left_loads.pop(0)
            if left_loads:
                if left_loads[0][0] == 'o':
                    dmid_give.wait_recv()
                load_lefts(*left_loads[0])
        if s + 1 < len(parts) and parts[s + 1][0] != '2':
            if parts[s + 1][0] == '1' and parts[s + 1][1] % 2 == 0:
                dup_give[parts[s + 1][1] // 2].wait_recv()
            load_rights(s + 1)
        space = spaces[s % 2]
        if name != '2' or n < 2:
            pltpu.make_async_copy(space, space, load_sem.at[15 + s % 2]).wait()
        if s >= 1:
            stored(s - 1)
            send_part(s - 1)
        stage[s % 2] = dot_nn(left_t[...], space[...])
        targets = {'2': (away2_ref, mid2_ref, keep2_ref), '1': (away1_ref, mid1_ref, keep1_ref),
                   'o': (awayo_ref, mido_ref, keepo_ref)}[name]
        for row, ref in zip((0, 2 * piece, 3 * piece), targets):
            rows = slice(row, row + (2 * piece if row == 0 else piece))
            if name == 'o':
                for k in range(2):
                    pltpu.make_async_copy(stage.at[s % 2, rows, k * (half // 2):(k + 1) * (half // 2)], ref.at[2 * n + k],
                                          load_sem.at[17 + s % 2]).start()
            else:
                pltpu.make_async_copy(stage.at[s % 2, rows, :], ref.at[n // 2, :, n % 2 * half:(n % 2 + 1) * half],
                                      load_sem.at[17 + s % 2]).start()
    stored(len(parts) - 1)
    send_part(len(parts) - 1)

    for i in range(4):
        @pl.when(role != i)
        def _():
            pltpu.make_async_copy(dc_ref.at[:, :head_cols], dch.at[:blk, :], dc_recv.at[i]).wait()

    moves = {(0, 0): [(add_mid, ('2', 0))], (0, 1): [(add_mid, ('2', 1))], (0, 4): [(finish, ('2', 0))],
             (0, 6): [(add_mid, ('2', 2)), (finish, ('2', 1))], (1, 0): [(send_d_heads, 0)],
             (1, 2): [(finish, ('2', 2)), (add_mid, ('2', 3))], (1, 6): [(finish, ('2', 3))], (1, 7): [(add_mid, ('1', 0))]}
    steps = seq // BWD_ROWS
    for j in range(2):
        k_view, v_view = qkv_ref.at[:, (2 + j) * PAIR:(3 + j) * PAIR], qkv_ref.at[:, (4 + j) * PAIR:(5 + j) * PAIR]
        k_t[...] = k_view[...].T
        dk_acc[...] = jnp.zeros_like(dk_acc)
        dv_acc[...] = jnp.zeros_like(dv_acc)

        def block(i, _):
            for n in range(8):
                if (j, n) in moves:
                    @pl.when(i == min(n, steps - 1))
                    def _():
                        for move, what in moves[(j, n)]:
                            move(what)
            rows = span(i, BWD_ROWS)
            cols = slice(j * PAIR, (j + 1) * PAIR)
            d_heads[rows, cols] = backward_rows(
                qkv_ref[rows, cols], dch[rows, cols], lse_ref[2 * j:2 * j + 2, rows], k_view, v_view,
                k_t, p_cat, ds_cat, dk_acc, dv_acc)
            return 0

        lax.fori_loop(0, steps, block, 0)
        d_heads[:, head_cols + j * PAIR:head_cols + (j + 1) * PAIR] = (dk_acc[...] * SCALE).astype(BF16)
        d_heads[:, 2 * head_cols + j * PAIR:2 * head_cols + (j + 1) * PAIR] = dv_acc[...].astype(BF16)

    quarter = 2 * piece

    def quarter_loads(n):
        return [load(u_ref.at[:, span(index[n], quarter)], u_s.at[n % 2], 8 + n % 2),
                load(gqkv2_ref.at[span(index[n], quarter), :], g_s.at[n % 2], 10 + n % 2)]

    pending = quarter_loads(0)
    for i in range(4):
        @pl.when(role == i)
        def _():
            d_qkv[:, i * 3 * head_cols:(i + 1) * 3 * head_cols] = d_heads[i * blk:(i + 1) * blk, :]
    send_d_heads(1)
    targets = [qa.at[0], qa.at[1], qb.at[0], qb.at[1]]
    first_q = copies.make(qa, q1, to_a)
    for n in range(4):
        ahead = quarter_loads(n + 1) if n < 3 else []
        for copy in pending:
            copy.wait()
        targets[n][...] = dot_tn(u_s[n % 2], d_heads[...]) + g_s[n % 2]
        pending = ahead
        if n == 0:
            far('2')
            add_mid(('1', 1))
            finish(('1', 0))
            finish(('1', 1))
        if n == 2:
            first_q.start()

    add_mid(('1', 2))
    w_rows = w_s.shape[1]
    chunks = wqkv_ref.shape[0] // w_rows
    w_load = load(wqkv_ref.at[:w_rows, :], w_s.at[0], 12)
    for j in range(2):
        for i in range(4):
            @pl.when(role != i)
            def _():
                for t in range(3):
                    pltpu.make_async_copy(d_heads.at[:blk, :PAIR], d_qkv.at[:, :PAIR], dq_recv.at[(j * 4 + i) * 3 + t]).wait()
    for n in range(chunks):
        ahead = load(wqkv_ref.at[(n + 1) * w_rows:(n + 2) * w_rows, :], w_s.at[(n + 1) % 2], 12 + (n + 1) % 2) if n + 1 < chunks else None
        w_load.wait()
        d_1[:, n * w_rows:(n + 1) * w_rows] = dot_nt(d_qkv[...], w_s[n % 2]).astype(BF16)
        w_load = ahead

    count = min(128, blk)
    for n in range(blk // count):
        rows = slice(n * count, (n + 1) * count)
        d_1[rows, :] = through_norm(x_ref[rows, :].astype(F32) + emb_row(emb_ref, 0), d_1[rows, :].astype(F32), dmid_ref[rows, :])

    own_seq, part_rows = z // 2, blk // 2

    def dx_rows(role, h):
        return pl.ds(pl.multiple_of(role * blk + h * part_rows, part_rows), part_rows)

    def dx_copy(n, h, device):
        slot = [0, 1 + core, 3 + core][n]
        return pltpu.make_async_remote_copy(
            src_ref=d_1.at[h * part_rows:(h + 1) * part_rows, :], dst_ref=dx_ref.at[dx_rows(role, h), :],
            send_sem=x_send.at[n * 2 + h], recv_sem=x_recv.at[slot * 2 + h], device_id=device, device_id_type=MESH)

    dx_side = [dx_copy(0, h, partner) for h in range(2)]
    dx_next = [dx_copy(1, h, here.device(z=here.z_by[1], c=own_seq)) for h in range(2)]
    dx_cross = [dx_copy(2, h, here.device(z=far_q, c=own_seq)) for h in range(2)]
    dx_keep = pltpu.make_async_copy(d_1, dx_ref.at[span(role, blk), :], local_sem.at[8])

    def dx_pass(cc, h):
        rows = dx_rows(z % 2 * 2 + cc, h)
        return pltpu.make_async_remote_copy(
            src_ref=dx_ref.at[rows, :], dst_ref=dx_ref.at[rows, :], send_sem=x_send.at[6 + cc * 2 + h],
            recv_sem=x_recv.at[(5 + cc) * 2 + h], device_id=here.device(z=here.z_by[1]), device_id_type=MESH)

    def dx_start(h):
        dx_cross[h].start()
        dx_next[h].start()
        pl.when(no(owner))(dx_side[h].start)

    def dx_got(slot, h):
        rows = d_1.at[:part_rows, :]
        pltpu.make_async_copy(rows, dx_ref.at[:part_rows, :], x_recv.at[slot * 2 + h]).wait()

    def dx_forward(h):
        @pl.when(no(owner))
        def _():
            for cc in range(2):
                dx_got(3 + cc, h)
                dx_pass(cc, h).start()

    finish(('1', 2))
    dx_start(0)
    pl.when(owner)(dx_keep.start)
    add_mid(('1', 3))
    finish(('1', 3))
    add_mid('o')
    dx_forward(0)
    far('1')
    first_q.wait_recv()
    qb[0] += q1[1]
    second_q = copies.start(qb.at[0], q2, to_b)
    qb[1] += q1[0]
    total('2')
    gather_start('2', sum_2, g2_ref, 0)
    second_q.wait_recv()
    qb[1] += q2[...]
    plane_stays = jnp.logical_and(2 * (z % 2) + core == z, z // 2 == core)
    plane_q = pltpu.make_async_remote_copy(
        src_ref=qb.at[1], dst_ref=q3, send_sem=p_send.at[0], recv_sem=p_recv.at[0],
        device_id=here.device(z=2 * (z % 2) + core, c=z // 2), device_id_type=MESH)

    @pl.when(plane_stays)
    def _():
        q3[...] = qb[1]

    pl.when(no(plane_stays))(plane_q.start)
    finish('o')
    total('1')
    gather_start('1', sum_1, g1_ref, 1)
    dx_start(1)
    gather_second('2')
    gather_second('1')
    pl.when(no(plane_stays))(plane_q.wait_recv)
    give_q = copies.start(q3.at[span(1 - core, piece), :], q4.at[0], partner)
    gather_core('2')
    give_q.wait_recv()
    q4[1] = q4[0] + q3[span(core, piece), :]
    far('o')
    for t, (name, out) in enumerate((('q', gq_ref), ('k', gk_ref), ('v', gv_ref))):
        gather_start(name, q4.at[1, :, t * head_cols:(t + 1) * head_cols], out, 3 + t)
    gather_core('1')
    for name in 'qkv':
        gather_second(name)
    for name in 'qkv':
        gather_core(name)
    dx_forward(1)
    total('o')
    gather_start('o', sum_o, go_ref, 2)
    gather_second('o')
    gather_core('o')

    @pl.when(owner)
    def _():
        for h in range(2):
            for slot in (0, 1, 2):
                dx_got(slot, h)
        dx_keep.wait()

    @pl.when(no(owner))
    def _():
        for h in range(2):
            dx_side[h].wait_send()
            for cc in range(2):
                dx_got(5 + cc, h)
                dx_pass(cc, h).wait_send()

    for g in gathers.values():
        for copy in g['c']:
            copy.wait_recv()
    for copy in waits:
        copy.wait()
    for copy in copies.sent:
        copy.wait_send()
    for h in range(2):
        dx_cross[h].wait_send()
        dx_next[h].wait_send()
    pl.when(no(plane_stays))(plane_q.wait_send)
    for i in range(4):
        @pl.when(role != i)
        def _():
            dc_copy(i).wait_send()
            for j in range(2):
                for t in range(3):
                    dq_copy(j, i, t).wait_send()
        for w in '21o':
            pl.when((z + i) % 2 == 1)(near_copy(w, i).wait_send)
    for w in '21o':
        far_copy(w).wait_send()


def last_call(qkv, d_c, lse, d_mid, x, emb, w_qkv, u_seq, g_qkv, w2_sides, w1_sides, wo_sides):
    seq, d_model = u_seq.shape
    blk, piece = seq // 4, d_model // 8
    n1, no = w1_sides[4].shape[1] // 4, wo_sides[3].shape[1] // 4
    assert n1 == d_model == 2 * 2 * BWD_ROWS and no * 2 == 2 * BWD_ROWS
    heads3 = qkv.shape[1]
    anywhere = pl.BlockSpec(memory_space=pl.ANY)
    in_vmem = pl.BlockSpec(memory_space=pltpu.VMEM)
    copies = 5 + 18 + 9 + 6 * 7 + 3
    dma = pltpu.SemaphoreType.DMA
    w_rows = min(128, d_model)
    return pl.pallas_call(
        last_kernel,
        in_specs=[in_vmem] * 6 + [anywhere] * 25,
        out_specs=[anywhere] * 18,
        out_shape=[
            jax.ShapeDtypeStruct((seq, d_model), BF16),
            jax.ShapeDtypeStruct((d_model, n1), F32),
            jax.ShapeDtypeStruct((8 * piece, n1), F32),
            jax.ShapeDtypeStruct((d_model, no), F32),
        ] + [jax.ShapeDtypeStruct((d_model, heads3 // 3), F32)] * 3
        + [jax.ShapeDtypeStruct((4, k * piece, n), F32) for n in (n1, n1, no) for k in (2, 1, 1)]
        + [jax.ShapeDtypeStruct((blk, n), BF16) for n in (4 * n1, d_model)],
        scratch_shapes=[
            pltpu.VMEM((seq, heads3 // 3), BF16),
            pltpu.VMEM((PAIR, seq), BF16),
            pltpu.VMEM((seq, PAIR), F32),
            pltpu.VMEM((seq, PAIR), F32),
            pltpu.VMEM((seq, 2 * BWD_ROWS), BF16),
            pltpu.VMEM((seq, 2 * BWD_ROWS), BF16),
            pltpu.VMEM((seq, heads3), BF16),
            pltpu.VMEM((blk, 4 * heads3), BF16),
            pltpu.VMEM((8, 2 * piece, n1), F32),
            pltpu.VMEM((4, 2 * piece, no), F32),
            pltpu.VMEM((8, piece, n1), F32),
            pltpu.VMEM((4, piece, no), F32),
            pltpu.VMEM((2, piece, n1), F32),
            pltpu.VMEM((2, 4, piece, no), F32),
            pltpu.VMEM((2, 3, piece, n1), F32),
            pltpu.VMEM((3, piece, no), F32),
            pltpu.VMEM((piece, n1), F32),
            pltpu.VMEM((piece, n1), F32),
            pltpu.VMEM((piece, no), F32),
            pltpu.VMEM((2, 2 * piece, heads3), F32),
            pltpu.VMEM((2, 2 * piece, heads3), F32),
            pltpu.VMEM((2, 2 * piece, heads3), F32),
            pltpu.VMEM((2 * piece, heads3), F32),
            pltpu.VMEM((2 * piece, heads3), F32),
            pltpu.VMEM((2, piece, heads3), F32),
            pltpu.VMEM((blk, d_model), BF16),
            pltpu.VMEM((2, w_rows, 4 * heads3), BF16),
            pltpu.VMEM((2, seq, 2 * piece), BF16),
            pltpu.VMEM((2, 2 * piece, heads3), F32),
            pltpu.VMEM((4 * piece, seq), BF16),
            pltpu.VMEM((2, 4 * piece, 2 * BWD_ROWS), F32),
            dma((9,)), dma((19,)), dma((copies,)), dma((copies,)),
            dma((4,)), dma((4,)), dma((24,)), dma((24,)), dma((9,)), dma((9,)), dma((10,)), dma((14,)), dma((1,)), dma((1,)),
        ],
        compiler_params=pltpu.CompilerParams(vmem_limit_bytes=63 << 20, collective_id=1, has_side_effects=True),
        cost_estimate=pl.CostEstimate(
            flops=160 * seq * seq * PAIR, bytes_accessed=128 * seq * d_model, transcendentals=seq * seq * 4),
        name="last",
    )(qkv, d_c, lse, d_mid, x, emb, w_qkv, u_seq, g_qkv, *w2_sides, *w1_sides, *wo_sides)[:7]


def solution(mesh):
    spec_col = P(None, 'model')
    spec_row = P('model', None)
    spec_act = P('data', None, None)
    spec_rep = P(None, None)

    def device_step(x_in, cot_out, step_emb, w_q, w_k, w_v, w_o, w_1, w_2):
        d_model = x_in.shape[2]
        c_1, lse_1, x_seq, cot, wo, w1, w2, w_qkv, x_1, h_1, m_1, up_1, act_1, x_2 = first_call(
            x_in[0], cot_out[0], step_emb, w_q, w_k, w_v, w_o, w_1, w_2)
        wo, w2 = wo.reshape(-1, d_model), w2.reshape(-1, d_model)

        c_2, lse_2, u_2_seq, qkv_2, u_1_seq, qkv_1 = forward_call(x_2, step_emb, x_seq, w_qkv)
        _, m_2, _, act_2, d_up_2, d_mid_2, d_c = hidden_call(True, True, wo, w1, w2, context=c_2, x=x_2, emb=step_emb, d_next=cot)
        shared = (act_2, act_1, cot, m_2, m_1, d_up_2, d_mid_2, c_2, c_1)
        d_2, d_2_other, g_qkv_2, *others = backward_call(
            qkv_2, d_c, lse_2, d_mid_2, x_2, step_emb, w_qkv, u_2_seq, shared)
        act_2o, act_1o, cot_o, m_2o, m_1o, d_up_2o, d_mid_2o, c_2o, c_1o = others
        d_up_1, d_mid_1, d_c = hidden_call(False, True, wo, w1, w2, h=h_1, up=up_1, d_next=d_2)
        w2_parts = (act_2, act_2o, act_1, act_1o, cot, cot_o, d_2, d_2_other)
        w1_sides = (m_2, m_2o, m_1, m_1o, d_up_2, d_up_2o, d_up_1)
        wo_sides = (d_mid_2, d_mid_2o, d_mid_1, c_2, c_2o, c_1, c_1o)
        d_x, g_w1, g_w2, g_wo, g_q, g_k, g_v = last_call(
            qkv_1, d_c, lse_1, d_mid_1, x_1, step_emb, w_qkv, u_1_seq, g_qkv_2, w2_parts, w1_sides, wo_sides)
        return g_q, g_k, g_v, g_wo.T, g_w1, g_w2, d_x[None]

    return jax.shard_map(device_step, mesh=mesh,
                         in_specs=(spec_act, spec_act, spec_rep, spec_col, spec_col, spec_col, spec_row, spec_col, spec_row),
                         out_specs=(spec_col, spec_col, spec_col, spec_row, spec_col, spec_row, spec_act),
                         check_vma=False)
```

```python
import functools
import math

import jax
import jax.numpy as jnp
from jax import lax
from jax.experimental import pallas as pl
from jax.experimental.pallas import tpu as pltpu
from jax.sharding import PartitionSpec as P


HEAD_DIM = 64
EPS_NORM = 1e-6
SCALE = HEAD_DIM ** -0.5
EXP2_SCALE = SCALE * math.log2(math.e)
PAIR = 2 * HEAD_DIM
FWD_ROWS = 512
BWD_ROWS = 256
KEYS = 256
HIDDEN = 1024
HIDDEN_FIRST = 512
INTERPRET = False
AXES = ('model', 'data')
BF16 = jnp.bfloat16
F32 = jnp.float32
MESH = pl.DeviceIdType.MESH

def rms_norm(values):
    return values * lax.rsqrt(jnp.mean(values * values, axis=-1, keepdims=True) + EPS_NORM)


def dot_nt(a, b):
    return lax.dot_general(a, b, (((1,), (1,)), ((), ())), preferred_element_type=F32)


def dot_nn(a, b):
    return lax.dot_general(a, b, (((1,), (0,)), ((), ())), preferred_element_type=F32)


def dot_tn(a, b):
    return lax.dot_general(a, b, (((0,), (0,)), ((), ())), preferred_element_type=F32)


def attend_rows(q, k_ref, v_t, e_refs):
    count = k_ref.shape[0] // KEYS
    lane = lax.broadcasted_iota(jnp.int32, q.shape, 1)
    q_heads = [jnp.where(lane // HEAD_DIM == head, q, jnp.zeros_like(q)) for head in range(2)]
    tops, run, total, outs, sums = [[], []], [None, None], [None, None], [], []
    for j in range(count):
        keys = slice(j * KEYS, (j + 1) * KEYS)
        for head in range(2):
            scores = dot_nt(k_ref[keys, :], q_heads[head])
            top = jnp.max(scores, axis=0, keepdims=True) * EXP2_SCALE
            if j:
                top = jnp.maximum(top, run[head])
            weights = jnp.exp2(scores * EXP2_SCALE - top)
            part = jnp.sum(weights, axis=0, keepdims=True)
            total[head] = total[head] * jnp.exp2(run[head] - top) + part if j else part
            run[head] = top
            tops[head].append(top)
            e_refs[head][keys, :] = weights
    for head in range(2):
        inverse = 1.0 / total[head]
        out = None
        for j in range(count):
            keys = slice(j * KEYS, (j + 1) * KEYS)
            factor = inverse * jnp.exp2(tops[head][j] - run[head])
            probs = (e_refs[head][keys, :] * factor).astype(BF16)
            part = dot_nn(v_t[head * HEAD_DIM:(head + 1) * HEAD_DIM, keys], probs)
            out = out + part if j else part
        sums.append(run[head] + jnp.log2(total[head]))
        outs.append(out)
    return outs, sums


class Place:
    def __init__(self):
        self.z = lax.axis_index('model')
        d = lax.axis_index('data')
        self.y, self.x, self.c = d // 4, d // 2 % 2, d % 2
        z = self.z
        self.z_by = {1: z + 1 - 2 * (z % 2), 2: (z + 2) % 4, 3: 3 - z}
        x, y, c = self.x, self.y, self.c
        self.xa, self.ya = x + (1 - c) * (1 - 2 * x), y + c * (1 - 2 * y)
        self.xb, self.yb = x + c * (1 - 2 * x), y + (1 - c) * (1 - 2 * y)
        self.role = z % 2 * 2 + c
        self.owner = c == z // 2

    def piece(self, y, x, c=None):
        return y * 4 + x * 2 + (self.c if c is None else c)

    def device(self, z=None, y=None, x=None, c=None):
        z, y, x, c = (own if given is None else given for given, own in zip((z, y, x, c), (self.z, self.y, self.x, self.c)))
        return {'model': z, 'data': y * 4 + x * 2 + c}

    def peers(self):
        column = [self.device(z=z, c=c) for z in (self.z, *self.z_by.values()) for c in (self.c, 1 - self.c)][1:]
        return column + [self.device(x=1 - self.x), self.device(y=1 - self.y)]

    def meet(self):
        barrier = pltpu.get_barrier_semaphore()
        peers = self.peers()
        for peer in peers:
            pl.semaphore_signal(barrier, inc=1, device_id=peer, device_id_type=MESH)
        pl.semaphore_wait(barrier, len(peers))


class Copies:
    def __init__(self, send_sem, recv_sem):
        self.send_sem, self.recv_sem, self.used, self.sent = send_sem, recv_sem, 0, []

    def make(self, src, dst, device):
        n, self.used = self.used, self.used + 1
        copy = pltpu.make_async_remote_copy(
            src_ref=src, dst_ref=dst, send_sem=self.send_sem.at[n], recv_sem=self.recv_sem.at[n],
            device_id=device, device_id_type=MESH)
        self.sent.append(copy)
        return copy

    def start(self, src, dst, device):
        copy = self.make(src, dst, device)
        copy.start()
        return copy


def first_kernel(x_ref, cot_ref, emb_ref, wq_ref, wk_ref, wv_ref, wo_ref, w1_ref, w2_ref,
                 c1_ref, lse_ref, xs_ref, cot_loc_ref, full_o, full_1, full_2, full_qkv,
                 x1_ref, h_ref, m_ref, up_ref, act_ref, x2_ref,
                 qkv_s, vt_s, e_a, e_b, c_buf, lse_s, cot_s, x1_s, c1_s, h_s, m_s, wo_s, w1_s, w2_s, up_s, act_s, acc,
                 local_sem, send_sem, recv_sem, c_send, c_recv, one_send, one_recv, load_sem, out_sem):
    seq, d_model = x_ref.shape
    blk = seq // 4
    head_cols = wq_ref.shape[1]
    here = Place()
    z, core, role, owner = here.z, here.c, here.role, here.owner
    here.meet()
    copies = Copies(send_sem, recv_sem)

    def span(index, count):
        return pl.ds(pl.multiple_of(index * count, count), count)

    ff_cols, out_rows, piece = w1_ref.shape[1], wo_ref.shape[0] // 8, d_model // 8
    hidden = w2_ref.shape[0] // 8

    def block_qkv(zz, e):
        return full_qkv.at[span(e, piece), span(zz, 3 * head_cols)]

    units = {
        'o': lambda zz, e: full_o.at[zz, span(e, out_rows), :],
        '1': lambda zz, e: full_1.at[span(e, piece), span(zz, ff_cols)],
        '2': lambda zz, e: full_2.at[zz, span(e, hidden), :],
        'qkv': block_qkv,
    }

    def own_parts(name, e):
        if name == 'o':
            return [(wo_ref.at[span(e, out_rows), :], units[name](z, e))]
        if name == '1':
            return [(w1_ref.at[span(e, piece), :], units[name](z, e))]
        if name == '2':
            return [(w2_ref.at[span(e, hidden), :], units[name](z, e))]
        return [(ref.at[span(e, piece), :],
                 full_qkv.at[span(e, piece), pl.ds(pl.multiple_of((z * 3 + t) * head_cols, head_cols), head_cols)])
                for t, ref in enumerate((wq_ref, wk_ref, wv_ref))]

    mine = here.piece(here.y, here.x)
    by_a = here.piece(here.ya, here.xa)
    by_b = here.piece(here.yb, here.xb)
    by_ab = here.piece(1 - here.y, 1 - here.x)
    to_a, to_b = here.device(y=here.ya, x=here.xa), here.device(y=here.yb, x=here.xb)
    partner = here.device(c=1 - core)
    names, order = ('o', '1', '2', 'qkv'), (2, 1, 3)
    stage_z, stage_a, stage_b1, stage_b2, stage_c = {}, {}, {}, {}, {}
    for name in names:
        block = lambda k, e: units[name](here.z_by[k], e)
        make = lambda k, e, device: copies.make(block(k, e), block(k, e), device)
        stage_z[name] = {k: [copies.make(src, dst, here.device(z=here.z_by[k])) for src, dst in own_parts(name, mine)] for k in (1, 2)}
        stage_z[name][3] = [make(2, mine, here.device(z=here.z_by[1]))]
        stage_a[name] = {k: make(k, mine, to_a) for k in order}
        stage_b1[name] = {k: make(k, mine, to_b) for k in order}
        stage_b2[name] = {k: make(k, by_a, to_b) for k in order}
        stage_c[name] = {k: [make(k, e, partner) for e in (mine, by_a, by_b, by_ab)] for k in order}

    def begin_z(name, k):
        for copy in stage_z[name][k]:
            copy.start()

    def arrived(name, k):
        for copy in stage_z[name][k]:
            copy.wait_recv()
        if k == 2:
            begin_z(name, 3)

    def spread(name, k):
        stage_a[name][k].start()
        stage_b1[name][k].start()

    def far_z(name, following=None):
        arrived(name, 2)
        if following:
            begin_z(following, 1)
        spread(name, 2)

    def near_z(name):
        arrived(name, 1)
        spread(name, 1)

    def last_z(name):
        arrived(name, 3)
        spread(name, 3)

    def forward_a(name):
        for k in order:
            stage_a[name][k].wait_recv()
            stage_b2[name][k].start()

    def forward_b(name):
        for k in order:
            stage_b1[name][k].wait_recv()
            stage_b2[name][k].wait_recv()
            for copy in stage_c[name][k]:
                copy.start()

    def gathered(name):
        for k in order:
            for copy in stage_c[name][k]:
                copy.wait_recv()

    for name in names:
        begin_z(name, 2)
    begin_z('o', 1)
    begin_z('1', 1)

    locals_ = []

    def copy_local(src, dst):
        copy = pltpu.make_async_copy(src, dst, local_sem.at[len(locals_)])
        locals_.append(copy)
        copy.start()

    copy_local(w1_ref, full_1.at[:, span(z, ff_cols)])
    copy_local(w2_ref, full_2.at[z])
    copy_local(wo_ref, full_o.at[z])
    for t, ref in enumerate((wq_ref, wk_ref, wv_ref)):
        copy_local(ref, full_qkv.at[:, pl.ds(pl.multiple_of((z * 3 + t) * head_cols, head_cols), head_cols)])
    other_role = z % 2 * 2 + 1 - core
    give_x = pltpu.make_async_remote_copy(
        src_ref=x_ref, dst_ref=xs_ref, send_sem=one_send.at[0], recv_sem=one_recv.at[0], device_id=partner, device_id_type=MESH)
    give_cot = pltpu.make_async_remote_copy(
        src_ref=cot_ref.at[span(other_role, blk), :], dst_ref=cot_loc_ref, send_sem=one_send.at[1], recv_sem=one_recv.at[1],
        device_id=partner, device_id_type=MESH)
    keep_x = pltpu.make_async_copy(x_ref, xs_ref, local_sem.at[6])
    take_cot = pltpu.make_async_copy(cot_ref.at[span(role, blk), :], cot_s, local_sem.at[7])
    keep_cot = pltpu.make_async_copy(cot_s, cot_loc_ref, local_sem.at[8])

    @pl.when(owner)
    def _():
        give_x.start()
        give_cot.start()
        keep_x.start()
        take_cot.start()

    def project(i):
        rows = span(i, blk)
        unit = unit_rows(x_ref[rows, :], emb_row(emb_ref, 0))
        for t, ref in enumerate((wq_ref, wk_ref, wv_ref)):
            qkv_s[rows, t * head_cols:(t + 1) * head_cols] = dot_nn(unit, ref[...]).astype(BF16)

    for i in range(4):
        if i == 3:
            far_z('o')
            near_z('o')
        project(i)

    def context_copy(j, i):
        src = c_buf.at[j, span(i, blk), :]
        dst = c1_ref.at[:, pl.ds(pl.multiple_of((z * 2 + j) * PAIR, PAIR), PAIR)]
        target_z, target_c = 2 * core + i // 2, i % 2
        remote = pltpu.make_async_remote_copy(
            src_ref=src, dst_ref=dst, send_sem=c_send.at[j * 4 + i], recv_sem=c_recv.at[j * 4 + z],
            device_id=here.device(z=target_z, c=target_c), device_id_type=MESH)
        local = pltpu.make_async_copy(src, dst, c_recv.at[j * 4 + z])
        return remote, local, jnp.logical_and(target_z == z, target_c == core)

    def send_context(j, i):
        remote, local, to_self = context_copy(j, i)
        pl.when(to_self)(local.start)
        pl.when(jnp.logical_not(to_self))(remote.start)

    moves = {(0, 2): [(far_z, '1', '2'), (near_z, '1')], (0, 3): [(last_z, 'o')], (1, 1): [(far_z, '2', 'qkv')],
             (1, 2): [(last_z, '1'), (forward_a, 'o')], (1, 3): [(far_z, 'qkv'), (forward_b, 'o')]}
    for j in range(2):
        vt_s[...] = qkv_s[:, (4 + j) * PAIR:(5 + j) * PAIR].T
        k_view = qkv_s.at[:, (2 + j) * PAIR:(3 + j) * PAIR]
        for i in range(4):
            if i or j:
                send_context(j if i else 0, i - 1 if i else 3)
            for move, *what in moves.get((j, i), ()):
                move(*what)
            rows = slice(i * blk, (i + 1) * blk)
            outs, sums = attend_rows(qkv_s[rows, j * PAIR:(j + 1) * PAIR], k_view, vt_s, (e_a, e_b))
            c_buf[j, rows, :] = jnp.concatenate(outs, axis=0).T.astype(BF16)
            for head in range(2):
                lse_s[2 * j + head:2 * j + head + 1, rows] = sums[head]

    @pl.when(owner)
    def _():
        take_cot.wait()
        keep_cot.start()

    forward_a('1')
    near_z('2')
    send_context(1, 3)
    give_lse = pltpu.make_async_remote_copy(
        src_ref=lse_s, dst_ref=lse_ref, send_sem=one_send.at[2], recv_sem=one_recv.at[2],
        device_id=here.device(z=2 * core + z // 2, c=z % 2), device_id_type=MESH)
    keep_lse = pltpu.make_async_copy(lse_s, lse_ref, local_sem.at[9])
    lse_stays = jnp.logical_and(2 * core + z // 2 == z, z % 2 == core)
    pl.when(lse_stays)(keep_lse.start)
    pl.when(jnp.logical_not(lse_stays))(give_lse.start)
    forward_b('1')
    last_z('2')
    near_z('qkv')
    last_z('qkv')

    @pl.when(owner)
    def _():
        keep_x.wait()

    @pl.when(jnp.logical_not(owner))
    def _():
        give_x.wait_recv()

    for j in range(2):
        for zz in range(4):
            pltpu.make_async_copy(c_buf.at[j, :blk, :], c1_ref.at[:, :PAIR], c_recv.at[j * 4 + zz]).wait()

    def load(src, dst, n):
        copy = pltpu.make_async_copy(src, dst, load_sem.at[n])
        copy.start()
        return copy

    loads = [load(xs_ref.at[span(role, blk), :], x1_s, 0), load(c1_ref, c1_s, 1)]
    for copy in locals_:
        copy.wait()
    gathered('o')
    loads += [load(full_o.at[zz], wo_s.at[zz * wo_ref.shape[0]:(zz + 1) * wo_ref.shape[0], :], 2 + zz) for zz in range(4)]
    for copy in loads:
        copy.wait()
    h = (x1_s[...].astype(F32) + emb_row(emb_ref, 0) + dot_nn(c1_s[...], wo_s[...])).astype(BF16)
    m = rms_rows(h.astype(F32)).astype(BF16)
    h_s[...], m_s[...] = h, m
    gathered('1')
    tile = w1_s.shape[2]
    steps = full_1.shape[1] // tile
    per_plane = full_2.shape[1] // tile

    def w1_load(n):
        return pltpu.make_async_copy(full_1.at[:, span(n, tile)], w1_s.at[n % 2], load_sem.at[6 + n % 2])

    def w2_load(n):
        return pltpu.make_async_copy(full_2.at[n // per_plane, span(n % per_plane, tile), :], w2_s.at[n % 2], load_sem.at[8 + n % 2])

    def up_store(n):
        return pltpu.make_async_copy(up_s.at[n % 2], up_ref.at[:, span(n, tile)], out_sem.at[n % 2])

    w1_load(0).start()

    def up_part(n, _):
        @pl.when(n + 1 < steps)
        def _():
            w1_load(n + 1).start()

        @pl.when(n == steps // 8)
        def _():
            forward_a('2')

        @pl.when(n == steps * 5 // 8)
        def _():
            forward_a('qkv')

        w1_load(n).wait()

        @pl.when(n >= 2)
        def _():
            up_store(n - 2).wait()

        up = dot_nn(m_s[...], w1_s[n % 2]).astype(BF16)
        up_s[n % 2] = up
        factor = gelu_parts(up.astype(F32))[0]
        act_s[:, span(n, tile)] = (up.astype(F32) * factor).astype(BF16)
        up_store(n).start()
        return 0

    lax.fori_loop(0, steps, up_part, 0)
    forward_b('2')
    outs = [pltpu.make_async_copy(src, dst, out_sem.at[2 + n]) for n, (src, dst) in enumerate(
        ((x1_s, x1_ref), (h_s, h_ref), (m_s, m_ref), (act_s, act_ref)))]
    for copy in outs:
        copy.start()
    gathered('2')
    w2_load(0).start()
    acc[...] = jnp.zeros_like(acc)

    def down_part(n, _):
        @pl.when(n + 1 < steps)
        def _():
            w2_load(n + 1).start()

        @pl.when(n == steps // 2)
        def _():
            forward_b('qkv')

        w2_load(n).wait()
        acc[...] += dot_nn(act_s[:, span(n, tile)], w2_s[n % 2])
        return 0

    lax.fori_loop(0, steps, down_part, 0)
    c1_s[...] = (h_s[...].astype(F32) + acc[...]).astype(BF16)
    out_x2 = pltpu.make_async_copy(c1_s, x2_ref, out_sem.at[6])
    for j in range(2):
        for i in range(4):
            remote, _, to_self = context_copy(j, i)
            pl.when(jnp.logical_not(to_self))(remote.wait_send)
    pl.when(lse_stays)(keep_lse.wait)

    @pl.when(jnp.logical_not(lse_stays))
    def _():
        give_lse.wait_send()
        give_lse.wait_recv()

    out_x2.start()

    @pl.when(owner)
    def _():
        give_x.wait_send()
        give_cot.wait_send()
        keep_cot.wait()

    @pl.when(jnp.logical_not(owner))
    def _():
        give_cot.wait_recv()

    for n in range(steps - 2, steps):
        up_store(n).wait()
    for copy in outs:
        copy.wait()
    out_x2.wait()
    gathered('qkv')
    for copy in copies.sent:
        copy.wait_send()


def first_call(x, cot, emb, w_q, w_k, w_v, w_o, w_1, w_2):
    seq, d_model = x.shape
    head_cols, ff_cols, blk = w_q.shape[1], w_1.shape[1], seq // 4
    anywhere = pl.BlockSpec(memory_space=pl.ANY)
    in_vmem = pl.BlockSpec(memory_space=pltpu.VMEM)
    copies = 16 + 3 * 12 + 48
    hidden, tile = 4 * ff_cols, min(HIDDEN_FIRST, ff_cols)
    shape = jax.ShapeDtypeStruct
    dma = pltpu.SemaphoreType.DMA
    return pl.pallas_call(
        first_kernel,
        in_specs=[in_vmem, anywhere] + [in_vmem] * 7,
        out_specs=[anywhere] * 14,
        out_shape=[
            shape((blk, d_model), BF16),
            shape((4, seq), F32),
            shape((seq, d_model), BF16),
            shape((blk, d_model), BF16),
            shape((4, *w_o.shape), BF16),
            shape((d_model, hidden), BF16),
            shape((4, *w_2.shape), BF16),
            shape((d_model, 12 * head_cols), BF16),
            shape((blk, d_model), BF16),
            shape((blk, d_model), BF16),
            shape((blk, d_model), BF16),
            shape((blk, hidden), BF16),
            shape((blk, hidden), BF16),
            shape((blk, d_model), BF16),
        ],
        scratch_shapes=[
            pltpu.VMEM((seq, 3 * head_cols), BF16),
            pltpu.VMEM((PAIR, seq), BF16),
            pltpu.VMEM((seq, blk), F32),
            pltpu.VMEM((seq, blk), F32),
            pltpu.VMEM((2, seq, PAIR), BF16),
            pltpu.VMEM((4, seq), F32),
            pltpu.VMEM((blk, d_model), BF16),
            pltpu.VMEM((blk, d_model), BF16),
            pltpu.VMEM((blk, d_model), BF16),
            pltpu.VMEM((blk, d_model), BF16),
            pltpu.VMEM((blk, d_model), BF16),
            pltpu.VMEM((d_model, d_model), BF16),
            pltpu.VMEM((2, d_model, tile), BF16),
            pltpu.VMEM((2, tile, d_model), BF16),
            pltpu.VMEM((2, blk, tile), BF16),
            pltpu.VMEM((blk, hidden), BF16),
            pltpu.VMEM((blk, d_model), F32),
            dma((10,)), dma((copies,)), dma((copies,)), dma((8,)), dma((8,)), dma((3,)), dma((3,)), dma((10,)), dma((7,)),
        ],
        compiler_params=pltpu.CompilerParams(vmem_limit_bytes=60 << 20, collective_id=0, has_side_effects=True),
        cost_estimate=pl.CostEstimate(
            flops=64 * seq * seq * PAIR, bytes_accessed=64 * seq * d_model, transcendentals=seq * seq * 4),
        name="first",
    )(x, cot, emb, w_q, w_k, w_v, w_o, w_1, w_2)


def emb_row(emb_ref, row):
    return emb_ref[...].astype(F32)[row:row + 1, :]


def unit_rows(values, emb):
    values = values.astype(F32) + emb
    return (values * lax.rsqrt(jnp.mean(values * values, axis=-1, keepdims=True) + EPS_NORM)).astype(BF16)


def forward_kernel(x_ref, emb_ref, xs1_ref, wqkv_ref,
                   c_ref, lse_ref, u2_ref, qkv2_ref, u1_ref, qkv1_ref,
                   w_s, blocks, u_s, qkv_s, x1_s, u1_s, qkv1_s, v_t, e_a, e_b, c_buf, lse_s,
                   local_sem, first_sem, out_sem, x_send, x_recv, c_send, c_recv):
    seq = xs1_ref.shape[0]
    blk = seq // 4
    head_cols = 2 * PAIR
    here = Place()
    z, core, role = here.z, here.c, here.role

    def span(index, count):
        return pl.ds(pl.multiple_of(index * count, count), count)

    w_load = pltpu.make_async_copy(wqkv_ref.at[:, span(role, 3 * head_cols)], w_s, local_sem.at[0])
    w_load.start()
    x1_load = [pltpu.make_async_copy(xs1_ref.at[i * blk:(i + 1) * blk, :], x1_s.at[i % 2], first_sem.at[i % 2]) for i in range(4)]
    x1_load[0].start()
    here.meet()
    partner, across = here.device(c=1 - core), here.device(z=here.z_by[1])
    role_side, role_over = z % 2 * 2 + 1 - core, (1 - z % 2) * 2 + core
    role_last = (1 - z % 2) * 2 + 1 - core

    def x_copy(n, src, slot, device):
        return pltpu.make_async_remote_copy(
            src_ref=src, dst_ref=blocks.at[slot], send_sem=x_send.at[n], recv_sem=x_recv.at[n],
            device_id=device, device_id_type=MESH)

    over, side = x_copy(0, x_ref, 0, across), x_copy(1, x_ref, 1, partner)
    last = x_copy(2, blocks.at[0], 2, partner)
    over.start()
    side.start()

    def project(src, at_role):
        rows = span(at_role, blk)
        unit = unit_rows(src, emb_row(emb_ref, 1))
        u_s[rows, :] = unit
        qkv_s[rows, :] = dot_nn(unit, w_s[...]).astype(BF16)

    w_load.wait()
    project(x_ref[...], role)
    side.wait_recv()
    project(blocks[1], role_side)

    stores = []
    for i in range(4):
        if i < 3:
            x1_load[i + 1].start()
        x1_load[i].wait()
        if i >= 2:
            for copy in stores[i - 2]:
                copy.wait()
        unit = unit_rows(x1_s[i % 2], emb_row(emb_ref, 0))
        u1_s[i % 2] = unit
        qkv1_s[i % 2] = dot_nn(unit, w_s[...]).astype(BF16)
        stores.append([pltpu.make_async_copy(u1_s.at[i % 2], u1_ref.at[i * blk:(i + 1) * blk, :], out_sem.at[i % 2]),
                       pltpu.make_async_copy(qkv1_s.at[i % 2], qkv1_ref.at[i * blk:(i + 1) * blk, :], out_sem.at[2 + i % 2])])
        for copy in stores[i]:
            copy.start()

    over.wait_recv()
    last.start()
    project(blocks[0], role_over)
    last.wait_recv()
    project(blocks[2], role_last)
    keep_u = pltpu.make_async_copy(u_s, u2_ref, local_sem.at[1])
    keep_qkv = pltpu.make_async_copy(qkv_s, qkv2_ref, local_sem.at[2])
    keep_u.start()
    keep_qkv.start()

    member = [here.device(z=z // 2 * 2 + i // 2, c=i % 2) for i in range(4)]

    def c_copy(j, i):
        src = c_buf.at[j, i * blk:(i + 1) * blk, :]
        dst = c_ref.at[:, pl.ds(pl.multiple_of((role * 2 + j) * PAIR, PAIR), PAIR)]
        remote = pltpu.make_async_remote_copy(
            src_ref=src, dst_ref=dst, send_sem=c_send.at[j * 4 + i], recv_sem=c_recv.at[j * 4 + role],
            device_id=member[i], device_id_type=MESH)
        return remote, pltpu.make_async_copy(src, dst, c_recv.at[j * 4 + role])

    def send_context(j, i):
        remote, local = c_copy(j, i)
        pl.when(role == i)(local.start)
        pl.when(role != i)(remote.start)

    for j in range(2):
        v_t[...] = qkv_s[:, (4 + j) * PAIR:(5 + j) * PAIR].T
        k_view = qkv_s.at[:, (2 + j) * PAIR:(3 + j) * PAIR]
        for i in range(4):
            if i or j:
                send_context(j if i else 0, i - 1 if i else 3)
            rows = slice(i * blk, (i + 1) * blk)
            outs, sums = attend_rows(qkv_s[rows, j * PAIR:(j + 1) * PAIR], k_view, v_t, (e_a, e_b))
            c_buf[j, rows, :] = jnp.concatenate(outs, axis=0).T.astype(BF16)
            for head in range(2):
                lse_s[2 * j + head:2 * j + head + 1, rows] = sums[head]
    lse_ref[...] = lse_s[...]
    send_context(1, 3)
    for j in range(2):
        for i in range(4):
            pltpu.make_async_copy(c_buf.at[j, :blk, :], c_ref.at[:, :PAIR], c_recv.at[j * 4 + i]).wait()
            pl.when(role != i)(c_copy(j, i)[0].wait_send)
    for copy in (over, side, last):
        copy.wait_send()
    for group in stores[2:]:
        for copy in group:
            copy.wait()
    keep_u.wait()
    keep_qkv.wait()


def forward_call(x, emb, xs_1, w_qkv):
    blk, d_model = x.shape
    seq, head_cols = 4 * blk, 2 * PAIR
    anywhere = pl.BlockSpec(memory_space=pl.ANY)
    in_vmem = pl.BlockSpec(memory_space=pltpu.VMEM)
    dma = pltpu.SemaphoreType.DMA
    return pl.pallas_call(
        forward_kernel,
        in_specs=[in_vmem, in_vmem, anywhere, anywhere],
        out_specs=[anywhere, in_vmem] + [anywhere] * 4,
        out_shape=[
            jax.ShapeDtypeStruct((blk, d_model), BF16),
            jax.ShapeDtypeStruct((4, seq), F32),
        ] + [jax.ShapeDtypeStruct((seq, n), BF16) for n in (d_model, 3 * head_cols)] * 2,
        scratch_shapes=[
            pltpu.VMEM((d_model, 3 * head_cols), BF16),
            pltpu.VMEM((3, blk, d_model), BF16),
            pltpu.VMEM((seq, d_model), BF16),
            pltpu.VMEM((seq, 3 * head_cols), BF16),
            pltpu.VMEM((2, blk, d_model), BF16),
            pltpu.VMEM((2, blk, d_model), BF16),
            pltpu.VMEM((2, blk, 3 * head_cols), BF16),
            pltpu.VMEM((PAIR, seq), BF16),
            pltpu.VMEM((seq, blk), F32),
            pltpu.VMEM((seq, blk), F32),
            pltpu.VMEM((2, seq, PAIR), BF16),
            pltpu.VMEM((4, seq), F32),
            dma((3,)), dma((2,)), dma((4,)), dma((3,)), dma((3,)), dma((8,)), dma((8,)),
        ],
        compiler_params=pltpu.CompilerParams(vmem_limit_bytes=60 << 20, collective_id=2, has_side_effects=True),
        cost_estimate=pl.CostEstimate(
            flops=64 * seq * seq * PAIR, bytes_accessed=32 * seq * d_model, transcendentals=seq * seq * 4),
        name="forward",
    )(x, emb, xs_1, w_qkv)


def through_norm(values, up, d_mid):
    inverse = lax.rsqrt(jnp.mean(values * values, axis=-1, keepdims=True) + EPS_NORM)
    inner = jnp.mean(values * up, axis=-1, keepdims=True)
    return (d_mid.astype(F32) + inverse * up - values * (inverse * inverse * inverse * inner)).astype(BF16)


def backward_kernel(shared, qkv_ref, dc_ref, lse_ref, dmid_ref, x_ref, emb_ref, wqkv_ref, u_ref, *refs):
    sources, (d_ref, other_ref, g_ref), shares = refs[:shared], refs[shared:shared + 3], refs[shared + 3:2 * shared + 3]
    (dch, k_t, dk_acc, dv_acc, p_cat, ds_cat, d_heads, d_qkv, d_u, w_s, u_s, g_s,
     load_sem, out_sem, dc_send, dc_recv, dq_send, dq_recv, d_send, d_recv, s_send, s_recv) = refs[2 * shared + 3:]
    seq = qkv_ref.shape[0]
    blk = seq // 4
    head_cols = 2 * PAIR
    here = Place()
    z, core, role = here.z, here.c, here.role
    here.meet()
    member = [here.device(z=z // 2 * 2 + i // 2, c=i % 2) for i in range(4)]

    def span(index, count):
        return pl.ds(pl.multiple_of(index * count, count), count)

    def load(src, dst, n):
        copy = pltpu.make_async_copy(src, dst, load_sem.at[n])
        copy.start()
        return copy

    def dc_copy(j, i):
        col = i * head_cols + j * PAIR
        return pltpu.make_async_remote_copy(
            src_ref=dc_ref.at[:, col:col + PAIR], dst_ref=dch.at[span(role, blk), j * PAIR:(j + 1) * PAIR],
            send_sem=dc_send.at[j * 4 + i], recv_sem=dc_recv.at[j * 4 + role], device_id=member[i], device_id_type=MESH)

    for j in range(2):
        for i in range(4):
            pl.when(role != i)(dc_copy(j, i).start)
    for i in range(4):
        @pl.when(role == i)
        def _():
            dch[i * blk:(i + 1) * blk, :] = dc_ref[:, i * head_cols:(i + 1) * head_cols]

    def dq_copy(j, i, t):
        col = t * head_cols + j * PAIR
        return pltpu.make_async_remote_copy(
            src_ref=d_heads.at[i * blk:(i + 1) * blk, col:col + PAIR],
            dst_ref=d_qkv.at[:, pl.ds(pl.multiple_of(role * 3 * head_cols + col, PAIR), PAIR)],
            send_sem=dq_send.at[(j * 4 + i) * 3 + t], recv_sem=dq_recv.at[(j * 4 + role) * 3 + t],
            device_id=member[i], device_id_type=MESH)

    def send_d_heads(j, ts):
        for i in range(4):
            @pl.when(role != i)
            def _():
                for t in ts:
                    dq_copy(j, i, t).start()

    shared_copies = [pltpu.make_async_remote_copy(
        src_ref=src, dst_ref=dst, send_sem=s_send.at[n], recv_sem=s_recv.at[n],
        device_id=here.device(c=1 - core), device_id_type=MESH) for n, (src, dst) in enumerate(zip(sources, shares))]

    steps = seq // BWD_ROWS
    for j in range(2):
        for i in range(4):
            @pl.when(role != i)
            def _():
                pltpu.make_async_copy(dc_ref.at[:, :PAIR], dch.at[:blk, :PAIR], dc_recv.at[j * 4 + i]).wait()
        if j == 0:
            for copy in shared_copies:
                copy.start()
        k_view, v_view = qkv_ref.at[:, (2 + j) * PAIR:(3 + j) * PAIR], qkv_ref.at[:, (4 + j) * PAIR:(5 + j) * PAIR]
        k_t[...] = k_view[...].T
        dk_acc[...] = jnp.zeros_like(dk_acc)
        dv_acc[...] = jnp.zeros_like(dv_acc)

        def block(i, _):
            if j == 1:
                @pl.when(i == 1)
                def _():
                    send_d_heads(0, (0, 1, 2))

                for target in range(3):
                    @pl.when(jnp.logical_and(i == (target + 1) * (steps // 4) + steps // 8, role != target))
                    def _():
                        dq_copy(1, target, 0).start()
            rows = span(i, BWD_ROWS)
            cols = slice(j * PAIR, (j + 1) * PAIR)
            d_heads[rows, cols] = backward_rows(
                qkv_ref[rows, cols], dch[rows, cols], lse_ref[2 * j:2 * j + 2, rows], k_view, v_view,
                k_t, p_cat, ds_cat, dk_acc, dv_acc)
            return 0

        lax.fori_loop(0, steps, block, 0)
        d_heads[:, head_cols + j * PAIR:head_cols + (j + 1) * PAIR] = (dk_acc[...] * SCALE).astype(BF16)
        d_heads[:, 2 * head_cols + j * PAIR:2 * head_cols + (j + 1) * PAIR] = dv_acc[...].astype(BF16)

    quarter = u_s.shape[2]
    pending = load(u_ref.at[:, :quarter], u_s.at[0], 0)
    for i in range(4):
        @pl.when(role == i)
        def _():
            d_qkv[:, i * 3 * head_cols:(i + 1) * 3 * head_cols] = d_heads[i * blk:(i + 1) * blk, :]
    pl.when(role != 3)(dq_copy(1, 3, 0).start)
    send_d_heads(1, (1, 2))
    stores = []
    count = u_ref.shape[1] // quarter
    for n in range(count):
        ahead = load(u_ref.at[:, (n + 1) * quarter:(n + 2) * quarter], u_s.at[(n + 1) % 2], (n + 1) % 2) if n + 1 < count else None
        pending.wait()
        if n >= 2:
            stores[n - 2].wait()
        g_s[n % 2] = dot_tn(u_s[n % 2], d_heads[...])
        stores.append(pltpu.make_async_copy(g_s.at[n % 2], g_ref.at[n * quarter:(n + 1) * quarter, :], out_sem.at[n % 2]))
        stores[n].start()
        pending = ahead
    w_rows = w_s.shape[1]
    chunks = wqkv_ref.shape[0] // w_rows
    w_load = load(wqkv_ref.at[:w_rows, :], w_s.at[0], 2)
    for j in range(2):
        for i in range(4):
            @pl.when(role != i)
            def _():
                for t in range(3):
                    pltpu.make_async_copy(d_heads.at[:blk, :PAIR], d_qkv.at[:, :PAIR], dq_recv.at[(j * 4 + i) * 3 + t]).wait()
    for n in range(chunks):
        ahead = load(wqkv_ref.at[(n + 1) * w_rows:(n + 2) * w_rows, :], w_s.at[(n + 1) % 2], 2 + (n + 1) % 2) if n + 1 < chunks else None
        w_load.wait()
        d_u[:, n * w_rows:(n + 1) * w_rows] = dot_nt(d_qkv[...], w_s[n % 2]).astype(BF16)
        w_load = ahead
    rows_each = min(128, blk)
    for n in range(blk // rows_each):
        rows = slice(n * rows_each, (n + 1) * rows_each)
        d_u[rows, :] = through_norm(x_ref[rows, :].astype(F32) + emb_row(emb_ref, 1), d_u[rows, :].astype(F32), dmid_ref[rows, :])
    keep = pltpu.make_async_copy(d_u, d_ref, out_sem.at[2])
    keep.start()
    stores[count - 2].wait()
    stores[count - 1].wait()
    give = pltpu.make_async_remote_copy(
        src_ref=d_u, dst_ref=other_ref, send_sem=d_send.at[0], recv_sem=d_recv.at[0],
        device_id=here.device(c=1 - core), device_id_type=MESH)
    give.start()
    for i in range(4):
        @pl.when(role != i)
        def _():
            for j in range(2):
                dc_copy(j, i).wait_send()
                for t in range(3):
                    dq_copy(j, i, t).wait_send()
    keep.wait()
    give.wait()
    for copy in shared_copies:
        copy.wait()


def backward_call(qkv, d_c, lse, d_mid, x, emb, w_qkv, u_seq, shared):
    seq, d_model = u_seq.shape
    blk, heads3 = seq // 4, qkv.shape[1]
    anywhere = pl.BlockSpec(memory_space=pl.ANY)
    in_vmem = pl.BlockSpec(memory_space=pltpu.VMEM)
    dma = pltpu.SemaphoreType.DMA
    quarter = d_model // 4
    return pl.pallas_call(
        functools.partial(backward_kernel, len(shared)),
        in_specs=[in_vmem] * 6 + [anywhere] * (2 + len(shared)),
        out_specs=[anywhere] * (3 + len(shared)),
        out_shape=[
            jax.ShapeDtypeStruct((blk, d_model), BF16),
            jax.ShapeDtypeStruct((blk, d_model), BF16),
            jax.ShapeDtypeStruct((d_model, heads3), F32),
        ] + [jax.ShapeDtypeStruct(value.shape, value.dtype) for value in shared],
        scratch_shapes=[
            pltpu.VMEM((seq, heads3 // 3), BF16),
            pltpu.VMEM((PAIR, seq), BF16),
            pltpu.VMEM((seq, PAIR), F32),
            pltpu.VMEM((seq, PAIR), F32),
            pltpu.VMEM((seq, 2 * BWD_ROWS), BF16),
            pltpu.VMEM((seq, 2 * BWD_ROWS), BF16),
            pltpu.VMEM((seq, heads3), BF16),
            pltpu.VMEM((blk, 4 * heads3), BF16),
            pltpu.VMEM((blk, d_model), BF16),
            pltpu.VMEM((2, quarter, 4 * heads3), BF16),
            pltpu.VMEM((2, seq, quarter), BF16),
            pltpu.VMEM((2, quarter, heads3), F32),
            dma((4,)), dma((3,)), dma((8,)), dma((8,)), dma((24,)), dma((24,)), dma((1,)), dma((1,)),
            dma((len(shared),)), dma((len(shared),)),
        ],
        compiler_params=pltpu.CompilerParams(vmem_limit_bytes=60 << 20, collective_id=3, has_side_effects=True),
        cost_estimate=pl.CostEstimate(
            flops=160 * seq * seq * PAIR, bytes_accessed=64 * seq * d_model, transcendentals=seq * seq * 4),
        name="backward",
    )(qkv, d_c, lse, d_mid, x, emb, w_qkv, u_seq, *shared)


def rms_rows(values):
    return values * lax.rsqrt(jnp.mean(values * values, axis=-1, keepdims=True) + EPS_NORM)


GELU_IN, GELU_CUBE = math.sqrt(2 / math.pi), 0.044715


def gelu_parts(z):
    square = z * z
    t = jnp.tanh(z * (GELU_IN + (GELU_IN * GELU_CUBE) * square))
    return 0.5 + 0.5 * t, t, square


def hidden_kernel(backward, forward, *refs):
    refs = list(refs)
    take = lambda: refs.pop(0)
    if forward:
        c_ref, x_ref, emb_ref, wo_ref = take(), take(), take(), take()
        w1_ref = take()
    else:
        h_ref, wo_ref, up_ref = take(), take(), take()
    w2_ref = take()
    if backward:
        d_ref, w1b_ref = take(), take()
    if forward:
        h_out, m_out = take(), take()
        up_out, act_out = take(), take()
    if backward:
        dup_out, dmid_out, dc_out = take(), take(), take()
    else:
        x_out = take()
    if forward:
        h_s, m_s = take(), take()
    prev_s, acc = take(), take()
    step, last = pl.program_id(0), pl.num_programs(0) - 1

    if forward:
        @pl.when(step == 0)
        def _():
            h = (x_ref[...].astype(F32) + emb_row(emb_ref, 1) + dot_nn(c_ref[...], wo_ref[...])).astype(BF16)
            m = rms_rows(h.astype(F32)).astype(BF16)
            h_s[...], m_s[...] = h, m
            h_out[...], m_out[...] = h, m

    def first_part():
        slot = step % 2
        if backward:
            d_act = dot_nt(d_ref[...], w2_ref[...]).astype(BF16).astype(F32)
        if forward:
            up = dot_nn(m_s[...], w1_ref[...]).astype(BF16)
            up_out[...] = up
        else:
            up = up_ref[...]
        z = up.astype(F32)
        factor, t, square = gelu_parts(z)
        if forward:
            act = (z * factor).astype(BF16)
            act_out[...] = act
        if backward:
            slope = factor + z * ((1.0 - t * t) * (0.5 * GELU_IN + (1.5 * GELU_IN * GELU_CUBE) * square))
            d_up = (slope * d_act).astype(BF16)
            dup_out[...] = d_up
            prev_s[slot] = d_up
        else:
            prev_s[slot] = act

    def second_part():
        prev = prev_s[1 - step % 2]
        if backward:
            return dot_nt(prev, w1b_ref[...])
        return dot_nn(prev, w2_ref[...])

    pl.when(step == 0)(first_part)

    @pl.when(step == 1)
    def _():
        acc[...] = second_part()
        first_part()

    @pl.when(jnp.logical_and(step > 1, step < last))
    def _():
        acc[...] += second_part()
        first_part()

    @pl.when(step == last)
    def _():
        total = acc[...] + second_part()
        if backward:
            h = (h_s if forward else h_ref)[...].astype(F32)
            d_mid = through_norm(h, total.astype(BF16).astype(F32), d_ref[...])
            dmid_out[...] = d_mid
            dc_out[...] = dot_nt(d_mid, wo_ref[...]).astype(BF16)
        else:
            x_out[...] = (h_s[...].astype(F32) + total).astype(BF16)


def hidden_call(forward, backward, w_o, w_1, w_2, context=None, x=None, emb=None, h=None, up=None, d_next=None):
    blk, d_model = (context if forward else h).shape
    hidden = w_1.shape[1]
    tile = HIDDEN
    steps = hidden // tile
    now, before = (lambda i: jnp.minimum(i, steps - 1)), (lambda i: jnp.maximum(i - 1, 0))
    whole = lambda rows, cols: pl.BlockSpec((rows, cols), lambda i: (0, 0))
    wide = pl.BlockSpec((blk, tile), lambda i: (0, now(i)))
    args, specs = [], []

    def add(value, spec):
        args.append(value)
        specs.append(spec)

    if forward:
        add(context, whole(blk, d_model))
        add(x, whole(blk, d_model))
        add(emb, whole(2, d_model))
        add(w_o, whole(d_model, d_model))
        add(w_1, pl.BlockSpec((d_model, tile), lambda i: (0, now(i))))
    else:
        add(h, whole(blk, d_model))
        add(w_o, whole(d_model, d_model))
        add(up, wide)
    add(w_2, pl.BlockSpec((tile, d_model), (lambda i: (now(i), 0)) if backward else (lambda i: (before(i), 0))))
    if backward:
        add(d_next, whole(blk, d_model))
        add(w_1, pl.BlockSpec((d_model, tile), lambda i: (0, before(i))))
    row = (whole(blk, d_model), jax.ShapeDtypeStruct((blk, d_model), BF16))
    big = (wide, jax.ShapeDtypeStruct((blk, hidden), BF16))
    outs = ([row, row, big, big] if forward else []) + ([big, row, row] if backward else [row])
    return pl.pallas_call(
        functools.partial(hidden_kernel, backward, forward),
        grid=(steps + 1,),
        in_specs=specs,
        out_specs=[spec for spec, _ in outs],
        out_shape=[shape for _, shape in outs],
        scratch_shapes=([pltpu.VMEM((blk, d_model), BF16)] * 2 if forward else [])
        + [pltpu.VMEM((2, blk, tile), BF16), pltpu.VMEM((blk, d_model), F32)],
        compiler_params=pltpu.CompilerParams(vmem_limit_bytes=60 << 20),
        cost_estimate=pl.CostEstimate(
            flops=2 * blk * d_model * (hidden * (3 if forward and backward else 2) + 2 * d_model),
            bytes_accessed=4 * hidden * d_model + 8 * blk * hidden, transcendentals=blk * hidden),
        interpret=INTERPRET,
        name="hidden",
    )(*args)


def backward_rows(q, d_out, lse, k_ref, v_ref, k_t, p_cat, ds_cat, dk_acc, dv_acc):
    block = q.shape[0]
    lane = lax.broadcasted_iota(jnp.int32, q.shape, 1)
    q_heads, do_heads, dqs = [], [], []
    for head in range(2):
        mine = lane // HEAD_DIM == head
        q_head = jnp.where(mine, q, jnp.zeros_like(q))
        do_head = jnp.where(mine, d_out, jnp.zeros_like(d_out))
        scores = dot_nt(k_ref[...], q_head)
        probs = jnp.exp2(scores * EXP2_SCALE - lse[head:head + 1, :])
        d_probs = dot_nt(v_ref[...], do_head).astype(BF16).astype(F32)
        inner = jnp.sum(probs * d_probs, axis=0, keepdims=True)
        cols = slice(head * block, (head + 1) * block)
        p_cat[:, cols] = probs.astype(BF16)
        ds_cat[:, cols] = (probs * (d_probs - inner)).astype(BF16)
        dqs.append(dot_nn(k_t[head * HEAD_DIM:(head + 1) * HEAD_DIM, :], ds_cat[:, cols]))
        q_heads.append(q_head)
        do_heads.append(do_head)
    dv_acc[...] += dot_nn(p_cat[...], jnp.concatenate(do_heads, axis=0))
    dk_acc[...] += dot_nn(ds_cat[...], jnp.concatenate(q_heads, axis=0))
    return (jnp.concatenate(dqs, axis=0).T * SCALE).astype(BF16)


def last_kernel(qkv_ref, dc_ref, lse_ref, dmid_ref, x_ref, emb_ref, wqkv_ref, u_ref, gqkv2_ref,
                *refs):
    lefts = {'2': refs[:4], '1': refs[8:12], 'o': refs[15:18]}
    rights = {'2': refs[4:8], '1': refs[12:15], 'o': refs[18:22]}
    (dx_ref, g1_ref, g2_ref, go_ref, gq_ref, gk_ref, gv_ref, away2_ref, mid2_ref, keep2_ref,
     away1_ref, mid1_ref, keep1_ref, awayo_ref, mido_ref, keepo_ref, dup_other, dmid_other,
     dch, k_t, dk_acc, dv_acc, p_cat, ds_cat, d_heads, d_qkv, buf, buf_o, second, second_o, tmp, tmp_o,
     third, third_o, sum_1, sum_2, sum_o, qa, qb, q1, q2, q3, q4, d_1, w_s, u_s, g_s,
     left_t, stage,
     local_sem, load_sem, send_sem, recv_sem, dc_send, dc_recv, dq_send, dq_recv, z_send, z_recv, x_send, x_recv,
     p_send, p_recv) = refs[22:]
    seq = qkv_ref.shape[0]
    blk = seq // 4
    head_cols = 2 * PAIR
    here = Place()
    z, core, role, owner = here.z, here.c, here.role, here.owner
    here.meet()
    copies = Copies(send_sem, recv_sem)
    waits = []

    def span(index, count):
        return pl.ds(pl.multiple_of(index * count, count), count)

    def load(src, dst, n):
        copy = pltpu.make_async_copy(src, dst, load_sem.at[n])
        copy.start()
        return copy

    no = jnp.logical_not
    to_a, to_b = here.device(y=here.ya, x=here.xa), here.device(y=here.yb, x=here.xb)
    partner = here.device(c=1 - core)
    member = [here.device(z=z // 2 * 2 + i // 2, c=i % 2) for i in range(4)]
    piece = tmp.shape[1]

    def dc_copy(i):
        return pltpu.make_async_remote_copy(
            src_ref=dc_ref.at[:, i * head_cols:(i + 1) * head_cols], dst_ref=dch.at[span(role, blk), :],
            send_sem=dc_send.at[i], recv_sem=dc_recv.at[role], device_id=member[i], device_id_type=MESH)

    for i in range(4):
        pl.when(role != i)(dc_copy(i).start)

        @pl.when(role == i)
        def _():
            dch[i * blk:(i + 1) * blk, :] = dc_ref[:, i * head_cols:(i + 1) * head_cols]

    half = rights['1'][0].shape[1] // 8
    wide = 2 * half
    dmid_give = copies.start(lefts['o'][2], dmid_other, partner)
    dup_give = [copies.start(rights['1'][2].at[:, q * wide:(q + 1) * wide], dup_other.at[:, q * wide:(q + 1) * wide], partner)
                for q in range(4)]
    lefts['o'] = (*lefts['o'], dmid_other)
    rights['1'] = (*rights['1'], dup_other)
    firsts = {(w, q): [copies.make(ref.at[q, :, h * half:(h + 1) * half], buf.at[u + q, :, h * half:(h + 1) * half], to_a)
                       for h in range(2)] for w, ref, u in (('2', away2_ref, 0), ('1', away1_ref, 4)) for q in range(4)}
    firsts['o'] = [copies.make(awayo_ref.at[2 * h:2 * h + 2], buf_o.at[2 * h:2 * h + 2], to_a) for h in range(2)]
    seconds = {(w, q): copies.make(buf.at[u + q, piece:, :], second.at[u + q], to_b) for w, u in (('2', 0), ('1', 4)) for q in range(4)}
    seconds['o'] = copies.make(buf_o.at[:, piece:, :], second_o, to_b)

    def add_mid(unit):
        if unit == 'o':
            mid, keep, t, n = mido_ref, keepo_ref, tmp_o, 4
            bottom, top = buf_o.at[:, piece:, :], buf_o.at[:, :piece, :]
        else:
            w, q = unit
            mid, keep = (mid2_ref.at[q], keep2_ref.at[q]) if w == '2' else (mid1_ref.at[q], keep1_ref.at[q])
            u = q if w == '2' else 4 + q
            t, n, bottom, top = tmp, 6, buf.at[u, piece:, :], buf.at[u, :piece, :]
        loads = [load(mid, t.at[0], n), load(keep, t.at[1], n + 1)]
        for copy in firsts[unit]:
            copy.wait_recv()
        for copy in loads:
            copy.wait()
        bottom[...] += t[0]
        top[...] += t[1]
        seconds[unit].start()

    sums = {'2': (lambda q: buf.at[q, :piece, :], third.at[0], 0), '1': (lambda q: buf.at[4 + q, :piece, :], third.at[1], 1),
            'o': (lambda q: buf_o.at[q, :piece, :], third_o, 2)}
    far_q = here.z_by[2]

    def near_copy(w, q):
        part, got, n = sums[w]
        return pltpu.make_async_remote_copy(
            src_ref=part(q), dst_ref=got.at[q // 2], send_sem=z_send.at[n * 3 + q // 2], recv_sem=z_recv.at[n * 3 + q // 2],
            device_id=here.device(z=here.z_by[1]), device_id_type=MESH)

    def far_copy(w):
        part, got, n = sums[w]
        return pltpu.make_async_remote_copy(
            src_ref=part(far_q), dst_ref=got.at[2], send_sem=z_send.at[n * 3 + 2], recv_sem=z_recv.at[n * 3 + 2],
            device_id=here.device(z=far_q), device_id_type=MESH)

    def finish(unit):
        seconds[unit].wait_recv()
        if unit == 'o':
            buf_o[:, :piece, :] += second_o[...]
            w, qs = 'o', range(4)
        else:
            w, u = unit[0], unit[1] + (4 if unit[0] == '1' else 0)
            buf[u, :piece, :] += second[u]
            qs = (unit[1],)
        for q in qs:
            pl.when((z + q) % 2 == 1)(near_copy(w, q).start)

    def far(w):
        part, got, n = sums[w]
        for k in range(2):
            pltpu.make_async_copy(got.at[2], got.at[k], z_recv.at[n * 3 + k]).wait()
        theirs, ours = part(far_q), part(z)
        theirs[...] += got[far_q // 2]
        ours[...] += got[z // 2]
        far_copy(w).start()

    mine, by_a = here.piece(here.y, here.x), here.piece(here.ya, here.xa)
    by_b, by_ab = here.piece(here.yb, here.xb), here.piece(1 - here.y, 1 - here.x)
    gathers = {}

    def total(w):
        part, got, n = sums[w]
        out = {'2': sum_2, '1': sum_1, 'o': sum_o}[w]
        far_copy(w).wait_recv()
        out[...] = part(z)[...] + got[2]

    def gather_start(name, src, out, n):
        rows = lambda e: out.at[span(e, piece), :]
        keep = pltpu.make_async_copy(src, rows(mine), local_sem.at[n])
        keep.start()
        waits.append(keep)
        gathers[name] = dict(src=src, rows=rows, a=copies.start(src, rows(mine), to_a), b1=copies.start(src, rows(mine), to_b))

    def gather_second(name):
        g = gathers[name]
        g['a'].wait_recv()
        g['b2'] = copies.start(g['rows'](by_a), g['rows'](by_a), to_b)

    def gather_core(name):
        g = gathers[name]
        g['c'] = [copies.start(g['src'], g['rows'](mine), partner), copies.start(g['rows'](by_a), g['rows'](by_a), partner)]
        g['b1'].wait_recv()
        g['c'].append(copies.start(g['rows'](by_b), g['rows'](by_b), partner))
        g['b2'].wait_recv()
        g['c'].append(copies.start(g['rows'](by_ab), g['rows'](by_ab), partner))

    def dq_copy(j, i, t):
        col = t * head_cols + j * PAIR
        return pltpu.make_async_remote_copy(
            src_ref=d_heads.at[i * blk:(i + 1) * blk, col:col + PAIR],
            dst_ref=d_qkv.at[:, pl.ds(pl.multiple_of(role * 3 * head_cols + col, PAIR), PAIR)],
            send_sem=dq_send.at[(j * 4 + i) * 3 + t], recv_sem=dq_recv.at[(j * 4 + role) * 3 + t],
            device_id=member[i], device_id_type=MESH)

    def send_d_heads(j):
        for i in range(4):
            @pl.when(role != i)
            def _():
                for t in range(3):
                    dq_copy(j, i, t).start()

    index = [here.ya * 2 + here.xa, (1 - here.y) * 2 + 1 - here.x, here.yb * 2 + here.xb, here.y * 2 + here.x]
    spaces = (p_cat, ds_cat)
    parts = [('2', n) for n in range(8)] + [('1', n) for n in range(8)] + [('o', n) for n in range(2)]
    left_loads = [('2', q) for q in range(4)] + [('1', 0), ('o', 0)]

    def load_lefts(name, q):
        for n in range(16):
            pltpu.make_async_copy(
                lefts[name][n // 4].at[:, span(q * 8 + index[n % 4] * 2 + core, piece)],
                d_heads.at[n // 4 * blk:(n // 4 + 1) * blk, n % 4 * piece:(n % 4 + 1) * piece], load_sem.at[14]).start()

    def load_rights(s):
        name, n = parts[s]
        for i in range(4):
            pltpu.make_async_copy(
                rights[name][i].at[:, n * half:(n + 1) * half], spaces[s % 2].at[i * blk:(i + 1) * blk, :],
                load_sem.at[15 + s % 2]).start()

    def stored(s):
        pltpu.make_async_copy(stage.at[s % 2], stage.at[s % 2], load_sem.at[17 + s % 2]).wait()

    def send_part(s):
        name, n = parts[s]
        if name == 'o':
            firsts['o'][n].start()
        else:
            firsts[(name, n // 2)][n % 2].start()

    load_lefts(*left_loads[0])
    load_rights(0)
    load_rights(1)
    for s in range(len(parts)):
        name, n = parts[s]
        if n == 0 or name == '2' and n % 2 == 0:
            every = d_heads.at[:, :4 * piece]
            pltpu.make_async_copy(every, every, load_sem.at[14]).wait()
            left_t[...] = every[...].T
            left_loads.pop(0)
            if left_loads:
                if left_loads[0][0] == 'o':
                    dmid_give.wait_recv()
                load_lefts(*left_loads[0])
        if s + 1 < len(parts) and parts[s + 1][0] != '2':
            if parts[s + 1][0] == '1' and parts[s + 1][1] % 2 == 0:
                dup_give[parts[s + 1][1] // 2].wait_recv()
            load_rights(s + 1)
        space = spaces[s % 2]
        if name != '2' or n < 2:
            pltpu.make_async_copy(space, space, load_sem.at[15 + s % 2]).wait()
        if s >= 1:
            stored(s - 1)
            send_part(s - 1)
        stage[s % 2] = dot_nn(left_t[...], space[...])
        targets = {'2': (away2_ref, mid2_ref, keep2_ref), '1': (away1_ref, mid1_ref, keep1_ref),
                   'o': (awayo_ref, mido_ref, keepo_ref)}[name]
        for row, ref in zip((0, 2 * piece, 3 * piece), targets):
            rows = slice(row, row + (2 * piece if row == 0 else piece))
            if name == 'o':
                for k in range(2):
                    pltpu.make_async_copy(stage.at[s % 2, rows, k * (half // 2):(k + 1) * (half // 2)], ref.at[2 * n + k],
                                          load_sem.at[17 + s % 2]).start()
            else:
                pltpu.make_async_copy(stage.at[s % 2, rows, :], ref.at[n // 2, :, n % 2 * half:(n % 2 + 1) * half],
                                      load_sem.at[17 + s % 2]).start()
    stored(len(parts) - 1)
    send_part(len(parts) - 1)

    for i in range(4):
        @pl.when(role != i)
        def _():
            pltpu.make_async_copy(dc_ref.at[:, :head_cols], dch.at[:blk, :], dc_recv.at[i]).wait()

    moves = {(0, 0): [(add_mid, ('2', 0))], (0, 1): [(add_mid, ('2', 1))], (0, 4): [(finish, ('2', 0))],
             (0, 6): [(add_mid, ('2', 2)), (finish, ('2', 1))], (1, 0): [(send_d_heads, 0)],
             (1, 2): [(finish, ('2', 2)), (add_mid, ('2', 3))], (1, 6): [(finish, ('2', 3))], (1, 7): [(add_mid, ('1', 0))]}
    steps = seq // BWD_ROWS
    for j in range(2):
        k_view, v_view = qkv_ref.at[:, (2 + j) * PAIR:(3 + j) * PAIR], qkv_ref.at[:, (4 + j) * PAIR:(5 + j) * PAIR]
        k_t[...] = k_view[...].T
        dk_acc[...] = jnp.zeros_like(dk_acc)
        dv_acc[...] = jnp.zeros_like(dv_acc)

        def block(i, _):
            for n in range(8):
                if (j, n) in moves:
                    @pl.when(i == min(n, steps - 1))
                    def _():
                        for move, what in moves[(j, n)]:
                            move(what)
            rows = span(i, BWD_ROWS)
            cols = slice(j * PAIR, (j + 1) * PAIR)
            d_heads[rows, cols] = backward_rows(
                qkv_ref[rows, cols], dch[rows, cols], lse_ref[2 * j:2 * j + 2, rows], k_view, v_view,
                k_t, p_cat, ds_cat, dk_acc, dv_acc)
            return 0

        lax.fori_loop(0, steps, block, 0)
        d_heads[:, head_cols + j * PAIR:head_cols + (j + 1) * PAIR] = (dk_acc[...] * SCALE).astype(BF16)
        d_heads[:, 2 * head_cols + j * PAIR:2 * head_cols + (j + 1) * PAIR] = dv_acc[...].astype(BF16)

    quarter = 2 * piece

    def quarter_loads(n):
        return [load(u_ref.at[:, span(index[n], quarter)], u_s.at[n % 2], 8 + n % 2),
                load(gqkv2_ref.at[span(index[n], quarter), :], g_s.at[n % 2], 10 + n % 2)]

    pending = quarter_loads(0)
    for i in range(4):
        @pl.when(role == i)
        def _():
            d_qkv[:, i * 3 * head_cols:(i + 1) * 3 * head_cols] = d_heads[i * blk:(i + 1) * blk, :]
    send_d_heads(1)
    targets = [qa.at[0], qa.at[1], qb.at[0], qb.at[1]]
    first_q = copies.make(qa, q1, to_a)
    for n in range(4):
        ahead = quarter_loads(n + 1) if n < 3 else []
        for copy in pending:
            copy.wait()
        targets[n][...] = dot_tn(u_s[n % 2], d_heads[...]) + g_s[n % 2]
        pending = ahead
        if n == 0:
            far('2')
            add_mid(('1', 1))
            finish(('1', 0))
            finish(('1', 1))
        if n == 2:
            first_q.start()

    add_mid(('1', 2))
    w_rows = w_s.shape[1]
    chunks = wqkv_ref.shape[0] // w_rows
    w_load = load(wqkv_ref.at[:w_rows, :], w_s.at[0], 12)
    for j in range(2):
        for i in range(4):
            @pl.when(role != i)
            def _():
                for t in range(3):
                    pltpu.make_async_copy(d_heads.at[:blk, :PAIR], d_qkv.at[:, :PAIR], dq_recv.at[(j * 4 + i) * 3 + t]).wait()
    for n in range(chunks):
        ahead = load(wqkv_ref.at[(n + 1) * w_rows:(n + 2) * w_rows, :], w_s.at[(n + 1) % 2], 12 + (n + 1) % 2) if n + 1 < chunks else None
        w_load.wait()
        d_1[:, n * w_rows:(n + 1) * w_rows] = dot_nt(d_qkv[...], w_s[n % 2]).astype(BF16)
        w_load = ahead

    count = min(128, blk)
    for n in range(blk // count):
        rows = slice(n * count, (n + 1) * count)
        d_1[rows, :] = through_norm(x_ref[rows, :].astype(F32) + emb_row(emb_ref, 0), d_1[rows, :].astype(F32), dmid_ref[rows, :])

    own_seq, part_rows = z // 2, blk // 2

    def dx_rows(role, h):
        return pl.ds(pl.multiple_of(role * blk + h * part_rows, part_rows), part_rows)

    def dx_copy(n, h, device):
        slot = [0, 1 + core, 3 + core][n]
        return pltpu.make_async_remote_copy(
            src_ref=d_1.at[h * part_rows:(h + 1) * part_rows, :], dst_ref=dx_ref.at[dx_rows(role, h), :],
            send_sem=x_send.at[n * 2 + h], recv_sem=x_recv.at[slot * 2 + h], device_id=device, device_id_type=MESH)

    dx_side = [dx_copy(0, h, partner) for h in range(2)]
    dx_next = [dx_copy(1, h, here.device(z=here.z_by[1], c=own_seq)) for h in range(2)]
    dx_cross = [dx_copy(2, h, here.device(z=far_q, c=own_seq)) for h in range(2)]
    dx_keep = pltpu.make_async_copy(d_1, dx_ref.at[span(role, blk), :], local_sem.at[8])

    def dx_pass(cc, h):
        rows = dx_rows(z % 2 * 2 + cc, h)
        return pltpu.make_async_remote_copy(
            src_ref=dx_ref.at[rows, :], dst_ref=dx_ref.at[rows, :], send_sem=x_send.at[6 + cc * 2 + h],
            recv_sem=x_recv.at[(5 + cc) * 2 + h], device_id=here.device(z=here.z_by[1]), device_id_type=MESH)

    def dx_start(h):
        dx_cross[h].start()
        dx_next[h].start()
        pl.when(no(owner))(dx_side[h].start)

    def dx_got(slot, h):
        rows = d_1.at[:part_rows, :]
        pltpu.make_async_copy(rows, dx_ref.at[:part_rows, :], x_recv.at[slot * 2 + h]).wait()

    def dx_forward(h):
        @pl.when(no(owner))
        def _():
            for cc in range(2):
                dx_got(3 + cc, h)
                dx_pass(cc, h).start()

    finish(('1', 2))
    dx_start(0)
    pl.when(owner)(dx_keep.start)
    add_mid(('1', 3))
    finish(('1', 3))
    add_mid('o')
    dx_forward(0)
    far('1')
    first_q.wait_recv()
    qb[0] += q1[1]
    second_q = copies.start(qb.at[0], q2, to_b)
    qb[1] += q1[0]
    total('2')
    gather_start('2', sum_2, g2_ref, 0)
    second_q.wait_recv()
    qb[1] += q2[...]
    plane_stays = jnp.logical_and(2 * (z % 2) + core == z, z // 2 == core)
    plane_q = pltpu.make_async_remote_copy(
        src_ref=qb.at[1], dst_ref=q3, send_sem=p_send.at[0], recv_sem=p_recv.at[0],
        device_id=here.device(z=2 * (z % 2) + core, c=z // 2), device_id_type=MESH)

    @pl.when(plane_stays)
    def _():
        q3[...] = qb[1]

    pl.when(no(plane_stays))(plane_q.start)
    finish('o')
    total('1')
    gather_start('1', sum_1, g1_ref, 1)
    dx_start(1)
    gather_second('2')
    gather_second('1')
    pl.when(no(plane_stays))(plane_q.wait_recv)
    give_q = copies.start(q3.at[span(1 - core, piece), :], q4.at[0], partner)
    gather_core('2')
    give_q.wait_recv()
    q4[1] = q4[0] + q3[span(core, piece), :]
    far('o')
    for t, (name, out) in enumerate((('q', gq_ref), ('k', gk_ref), ('v', gv_ref))):
        gather_start(name, q4.at[1, :, t * head_cols:(t + 1) * head_cols], out, 3 + t)
    gather_core('1')
    for name in 'qkv':
        gather_second(name)
    for name in 'qkv':
        gather_core(name)
    dx_forward(1)
    total('o')
    gather_start('o', sum_o, go_ref, 2)
    gather_second('o')
    gather_core('o')

    @pl.when(owner)
    def _():
        for h in range(2):
            for slot in (0, 1, 2):
                dx_got(slot, h)
        dx_keep.wait()

    @pl.when(no(owner))
    def _():
        for h in range(2):
            dx_side[h].wait_send()
            for cc in range(2):
                dx_got(5 + cc, h)
                dx_pass(cc, h).wait_send()

    for g in gathers.values():
        for copy in g['c']:
            copy.wait_recv()
    for copy in waits:
        copy.wait()
    for copy in copies.sent:
        copy.wait_send()
    for h in range(2):
        dx_cross[h].wait_send()
        dx_next[h].wait_send()
    pl.when(no(plane_stays))(plane_q.wait_send)
    for i in range(4):
        @pl.when(role != i)
        def _():
            dc_copy(i).wait_send()
            for j in range(2):
                for t in range(3):
                    dq_copy(j, i, t).wait_send()
        for w in '21o':
            pl.when((z + i) % 2 == 1)(near_copy(w, i).wait_send)
    for w in '21o':
        far_copy(w).wait_send()


def last_call(qkv, d_c, lse, d_mid, x, emb, w_qkv, u_seq, g_qkv, w2_sides, w1_sides, wo_sides):
    seq, d_model = u_seq.shape
    blk, piece = seq // 4, d_model // 8
    n1, no = w1_sides[4].shape[1] // 4, wo_sides[3].shape[1] // 4
    assert n1 == d_model == 2 * 2 * BWD_ROWS and no * 2 == 2 * BWD_ROWS
    heads3 = qkv.shape[1]
    anywhere = pl.BlockSpec(memory_space=pl.ANY)
    in_vmem = pl.BlockSpec(memory_space=pltpu.VMEM)
    copies = 5 + 18 + 9 + 6 * 7 + 3
    dma = pltpu.SemaphoreType.DMA
    w_rows = min(128, d_model)
    return pl.pallas_call(
        last_kernel,
        in_specs=[in_vmem] * 6 + [anywhere] * 25,
        out_specs=[anywhere] * 18,
        out_shape=[
            jax.ShapeDtypeStruct((seq, d_model), BF16),
            jax.ShapeDtypeStruct((d_model, n1), F32),
            jax.ShapeDtypeStruct((8 * piece, n1), F32),
            jax.ShapeDtypeStruct((d_model, no), F32),
        ] + [jax.ShapeDtypeStruct((d_model, heads3 // 3), F32)] * 3
        + [jax.ShapeDtypeStruct((4, k * piece, n), F32) for n in (n1, n1, no) for k in (2, 1, 1)]
        + [jax.ShapeDtypeStruct((blk, n), BF16) for n in (4 * n1, d_model)],
        scratch_shapes=[
            pltpu.VMEM((seq, heads3 // 3), BF16),
            pltpu.VMEM((PAIR, seq), BF16),
            pltpu.VMEM((seq, PAIR), F32),
            pltpu.VMEM((seq, PAIR), F32),
            pltpu.VMEM((seq, 2 * BWD_ROWS), BF16),
            pltpu.VMEM((seq, 2 * BWD_ROWS), BF16),
            pltpu.VMEM((seq, heads3), BF16),
            pltpu.VMEM((blk, 4 * heads3), BF16),
            pltpu.VMEM((8, 2 * piece, n1), F32),
            pltpu.VMEM((4, 2 * piece, no), F32),
            pltpu.VMEM((8, piece, n1), F32),
            pltpu.VMEM((4, piece, no), F32),
            pltpu.VMEM((2, piece, n1), F32),
            pltpu.VMEM((2, 4, piece, no), F32),
            pltpu.VMEM((2, 3, piece, n1), F32),
            pltpu.VMEM((3, piece, no), F32),
            pltpu.VMEM((piece, n1), F32),
            pltpu.VMEM((piece, n1), F32),
            pltpu.VMEM((piece, no), F32),
            pltpu.VMEM((2, 2 * piece, heads3), F32),
            pltpu.VMEM((2, 2 * piece, heads3), F32),
            pltpu.VMEM((2, 2 * piece, heads3), F32),
            pltpu.VMEM((2 * piece, heads3), F32),
            pltpu.VMEM((2 * piece, heads3), F32),
            pltpu.VMEM((2, piece, heads3), F32),
            pltpu.VMEM((blk, d_model), BF16),
            pltpu.VMEM((2, w_rows, 4 * heads3), BF16),
            pltpu.VMEM((2, seq, 2 * piece), BF16),
            pltpu.VMEM((2, 2 * piece, heads3), F32),
            pltpu.VMEM((4 * piece, seq), BF16),
            pltpu.VMEM((2, 4 * piece, 2 * BWD_ROWS), F32),
            dma((9,)), dma((19,)), dma((copies,)), dma((copies,)),
            dma((4,)), dma((4,)), dma((24,)), dma((24,)), dma((9,)), dma((9,)), dma((10,)), dma((14,)), dma((1,)), dma((1,)),
        ],
        compiler_params=pltpu.CompilerParams(vmem_limit_bytes=63 << 20, collective_id=1, has_side_effects=True),
        cost_estimate=pl.CostEstimate(
            flops=160 * seq * seq * PAIR, bytes_accessed=128 * seq * d_model, transcendentals=seq * seq * 4),
        name="last",
    )(qkv, d_c, lse, d_mid, x, emb, w_qkv, u_seq, g_qkv, *w2_sides, *w1_sides, *wo_sides)[:7]


def solution(mesh):
    spec_col = P(None, 'model')
    spec_row = P('model', None)
    spec_act = P('data', None, None)
    spec_rep = P(None, None)

    def device_step(x_in, cot_out, step_emb, w_q, w_k, w_v, w_o, w_1, w_2):
        d_model = x_in.shape[2]
        c_1, lse_1, x_seq, cot, wo, w1, w2, w_qkv, x_1, h_1, m_1, up_1, act_1, x_2 = first_call(
            x_in[0], cot_out[0], step_emb, w_q, w_k, w_v, w_o, w_1, w_2)
        wo, w2 = wo.reshape(-1, d_model), w2.reshape(-1, d_model)

        c_2, lse_2, u_2_seq, qkv_2, u_1_seq, qkv_1 = forward_call(x_2, step_emb, x_seq, w_qkv)
        _, m_2, _, act_2, d_up_2, d_mid_2, d_c = hidden_call(True, True, wo, w1, w2, context=c_2, x=x_2, emb=step_emb, d_next=cot)
        shared = (act_2, act_1, cot, m_2, m_1, d_up_2, d_mid_2, c_2, c_1)
        d_2, d_2_other, g_qkv_2, *others = backward_call(
            qkv_2, d_c, lse_2, d_mid_2, x_2, step_emb, w_qkv, u_2_seq, shared)
        act_2o, act_1o, cot_o, m_2o, m_1o, d_up_2o, d_mid_2o, c_2o, c_1o = others
        d_up_1, d_mid_1, d_c = hidden_call(False, True, wo, w1, w2, h=h_1, up=up_1, d_next=d_2)
        w2_parts = (act_2, act_2o, act_1, act_1o, cot, cot_o, d_2, d_2_other)
        w1_sides = (m_2, m_2o, m_1, m_1o, d_up_2, d_up_2o, d_up_1)
        wo_sides = (d_mid_2, d_mid_2o, d_mid_1, c_2, c_2o, c_1, c_1o)
        d_x, g_w1, g_w2, g_wo, g_q, g_k, g_v = last_call(
            qkv_1, d_c, lse_1, d_mid_1, x_1, step_emb, w_qkv, u_1_seq, g_qkv_2, w2_parts, w1_sides, wo_sides)
        return g_q, g_k, g_v, g_wo.T, g_w1, g_w2, d_x[None]

    return jax.shard_map(device_step, mesh=mesh,
                         in_specs=(spec_act, spec_act, spec_rep, spec_col, spec_col, spec_col, spec_row, spec_col, spec_row),
                         out_specs=(spec_col, spec_col, spec_col, spec_row, spec_col, spec_row, spec_act),
                         check_vma=False)
```

```python
import functools
import math

import jax
import jax.numpy as jnp
from jax import lax
from jax.experimental import pallas as pl
from jax.experimental.pallas import tpu as pltpu
from jax.sharding import PartitionSpec as P


HEAD_DIM = 64
EPS_NORM = 1e-6
SCALE = HEAD_DIM ** -0.5
EXP2_SCALE = SCALE * math.log2(math.e)
PAIR = 2 * HEAD_DIM
FWD_ROWS = 512
BWD_ROWS = 256
KEYS = 256
HIDDEN = 1024
HIDDEN_FIRST = 512
INTERPRET = False
AXES = ('model', 'data')
BF16 = jnp.bfloat16
F32 = jnp.float32
MESH = pl.DeviceIdType.MESH

def rms_norm(values):
    return values * lax.rsqrt(jnp.mean(values * values, axis=-1, keepdims=True) + EPS_NORM)


def dot_nt(a, b):
    return lax.dot_general(a, b, (((1,), (1,)), ((), ())), preferred_element_type=F32)


def dot_nn(a, b):
    return lax.dot_general(a, b, (((1,), (0,)), ((), ())), preferred_element_type=F32)


def dot_tn(a, b):
    return lax.dot_general(a, b, (((0,), (0,)), ((), ())), preferred_element_type=F32)


def attend_rows(q, k_ref, v_t, e_refs):
    count = k_ref.shape[0] // KEYS
    lane = lax.broadcasted_iota(jnp.int32, q.shape, 1)
    q_heads = [jnp.where(lane // HEAD_DIM == head, q, jnp.zeros_like(q)) for head in range(2)]
    tops, run, total, outs, sums = [[], []], [None, None], [None, None], [], []
    for j in range(count):
        keys = slice(j * KEYS, (j + 1) * KEYS)
        for head in range(2):
            scores = dot_nt(k_ref[keys, :], q_heads[head])
            top = jnp.max(scores, axis=0, keepdims=True) * EXP2_SCALE
            if j:
                top = jnp.maximum(top, run[head])
            weights = jnp.exp2(scores * EXP2_SCALE - top)
            part = jnp.sum(weights, axis=0, keepdims=True)
            total[head] = total[head] * jnp.exp2(run[head] - top) + part if j else part
            run[head] = top
            tops[head].append(top)
            e_refs[head][keys, :] = weights
    for head in range(2):
        inverse = 1.0 / total[head]
        out = None
        for j in range(count):
            keys = slice(j * KEYS, (j + 1) * KEYS)
            factor = inverse * jnp.exp2(tops[head][j] - run[head])
            probs = (e_refs[head][keys, :] * factor).astype(BF16)
            part = dot_nn(v_t[head * HEAD_DIM:(head + 1) * HEAD_DIM, keys], probs)
            out = out + part if j else part
        sums.append(run[head] + jnp.log2(total[head]))
        outs.append(out)
    return outs, sums


class Place:
    def __init__(self):
        self.z = lax.axis_index('model')
        d = lax.axis_index('data')
        self.y, self.x, self.c = d // 4, d // 2 % 2, d % 2
        z = self.z
        self.z_by = {1: z + 1 - 2 * (z % 2), 2: (z + 2) % 4, 3: 3 - z}
        x, y, c = self.x, self.y, self.c
        self.xa, self.ya = x + (1 - c) * (1 - 2 * x), y + c * (1 - 2 * y)
        self.xb, self.yb = x + c * (1 - 2 * x), y + (1 - c) * (1 - 2 * y)
        self.role = z % 2 * 2 + c
        self.owner = c == z // 2

    def piece(self, y, x, c=None):
        return y * 4 + x * 2 + (self.c if c is None else c)

    def device(self, z=None, y=None, x=None, c=None):
        z, y, x, c = (own if given is None else given for given, own in zip((z, y, x, c), (self.z, self.y, self.x, self.c)))
        return {'model': z, 'data': y * 4 + x * 2 + c}

    def peers(self):
        column = [self.device(z=z, c=c) for z in (self.z, *self.z_by.values()) for c in (self.c, 1 - self.c)][1:]
        return column + [self.device(x=1 - self.x), self.device(y=1 - self.y)]

    def meet(self):
        barrier = pltpu.get_barrier_semaphore()
        peers = self.peers()
        for peer in peers:
            pl.semaphore_signal(barrier, inc=1, device_id=peer, device_id_type=MESH)
        pl.semaphore_wait(barrier, len(peers))


class Copies:
    def __init__(self, send_sem, recv_sem):
        self.send_sem, self.recv_sem, self.used, self.sent = send_sem, recv_sem, 0, []

    def make(self, src, dst, device):
        n, self.used = self.used, self.used + 1
        copy = pltpu.make_async_remote_copy(
            src_ref=src, dst_ref=dst, send_sem=self.send_sem.at[n], recv_sem=self.recv_sem.at[n],
            device_id=device, device_id_type=MESH)
        self.sent.append(copy)
        return copy

    def start(self, src, dst, device):
        copy = self.make(src, dst, device)
        copy.start()
        return copy


def first_kernel(x_ref, cot_ref, emb_ref, wq_ref, wk_ref, wv_ref, wo_ref, w1_ref, w2_ref,
                 c1_ref, lse_ref, xs_ref, cot_loc_ref, full_o, full_1, full_2, full_qkv,
                 x1_ref, h_ref, m_ref, up_ref, act_ref, x2_ref,
                 qkv_s, vt_s, e_a, e_b, c_buf, lse_s, cot_s, x1_s, c1_s, h_s, m_s, wo_s, w1_s, w2_s, up_s, act_s, acc,
                 local_sem, send_sem, recv_sem, c_send, c_recv, one_send, one_recv, load_sem, out_sem):
    seq, d_model = x_ref.shape
    blk = seq // 4
    head_cols = wq_ref.shape[1]
    here = Place()
    z, core, role, owner = here.z, here.c, here.role, here.owner
    here.meet()
    copies = Copies(send_sem, recv_sem)

    def span(index, count):
        return pl.ds(pl.multiple_of(index * count, count), count)

    ff_cols, out_rows, piece = w1_ref.shape[1], wo_ref.shape[0] // 8, d_model // 8
    hidden = w2_ref.shape[0] // 8

    def block_qkv(zz, e):
        return full_qkv.at[span(e, piece), span(zz, 3 * head_cols)]

    units = {
        'o': lambda zz, e: full_o.at[zz, span(e, out_rows), :],
        '1': lambda zz, e: full_1.at[span(e, piece), span(zz, ff_cols)],
        '2': lambda zz, e: full_2.at[zz, span(e, hidden), :],
        'qkv': block_qkv,
    }

    def own_parts(name, e):
        if name == 'o':
            return [(wo_ref.at[span(e, out_rows), :], units[name](z, e))]
        if name == '1':
            return [(w1_ref.at[span(e, piece), :], units[name](z, e))]
        if name == '2':
            return [(w2_ref.at[span(e, hidden), :], units[name](z, e))]
        return [(ref.at[span(e, piece), :],
                 full_qkv.at[span(e, piece), pl.ds(pl.multiple_of((z * 3 + t) * head_cols, head_cols), head_cols)])
                for t, ref in enumerate((wq_ref, wk_ref, wv_ref))]

    mine = here.piece(here.y, here.x)
    by_a = here.piece(here.ya, here.xa)
    by_b = here.piece(here.yb, here.xb)
    by_ab = here.piece(1 - here.y, 1 - here.x)
    to_a, to_b = here.device(y=here.ya, x=here.xa), here.device(y=here.yb, x=here.xb)
    partner = here.device(c=1 - core)
    names, order = ('o', '1', '2', 'qkv'), (2, 1, 3)
    stage_z, stage_a, stage_b1, stage_b2, stage_c = {}, {}, {}, {}, {}
    for name in names:
        block = lambda k, e: units[name](here.z_by[k], e)
        make = lambda k, e, device: copies.make(block(k, e), block(k, e), device)
        stage_z[name] = {k: [copies.make(src, dst, here.device(z=here.z_by[k])) for src, dst in own_parts(name, mine)] for k in (1, 2)}
        stage_z[name][3] = [make(2, mine, here.device(z=here.z_by[1]))]
        stage_a[name] = {k: make(k, mine, to_a) for k in order}
        stage_b1[name] = {k: make(k, mine, to_b) for k in order}
        stage_b2[name] = {k: make(k, by_a, to_b) for k in order}
        stage_c[name] = {k: [make(k, e, partner) for e in (mine, by_a, by_b, by_ab)] for k in order}

    def begin_z(name, k):
        for copy in stage_z[name][k]:
            copy.start()

    def arrived(name, k):
        for copy in stage_z[name][k]:
            copy.wait_recv()
        if k == 2:
            begin_z(name, 3)

    def spread(name, k):
        stage_a[name][k].start()
        stage_b1[name][k].start()

    def far_z(name, following=None):
        arrived(name, 2)
        if following:
            begin_z(following, 1)
        spread(name, 2)

    def near_z(name):
        arrived(name, 1)
        spread(name, 1)

    def last_z(name):
        arrived(name, 3)
        spread(name, 3)

    def forward_a(name):
        for k in order:
            stage_a[name][k].wait_recv()
            stage_b2[name][k].start()

    def forward_b(name):
        for k in order:
            stage_b1[name][k].wait_recv()
            stage_b2[name][k].wait_recv()
            for copy in stage_c[name][k]:
                copy.start()

    def gathered(name):
        for k in order:
            for copy in stage_c[name][k]:
                copy.wait_recv()

    for name in names:
        begin_z(name, 2)
    begin_z('o', 1)
    begin_z('1', 1)

    locals_ = []

    def copy_local(src, dst):
        copy = pltpu.make_async_copy(src, dst, local_sem.at[len(locals_)])
        locals_.append(copy)
        copy.start()

    copy_local(w1_ref, full_1.at[:, span(z, ff_cols)])
    copy_local(w2_ref, full_2.at[z])
    copy_local(wo_ref, full_o.at[z])
    for t, ref in enumerate((wq_ref, wk_ref, wv_ref)):
        copy_local(ref, full_qkv.at[:, pl.ds(pl.multiple_of((z * 3 + t) * head_cols, head_cols), head_cols)])
    other_role = z % 2 * 2 + 1 - core
    give_x = pltpu.make_async_remote_copy(
        src_ref=x_ref, dst_ref=xs_ref, send_sem=one_send.at[0], recv_sem=one_recv.at[0], device_id=partner, device_id_type=MESH)
    give_cot = pltpu.make_async_remote_copy(
        src_ref=cot_ref.at[span(other_role, blk), :], dst_ref=cot_loc_ref, send_sem=one_send.at[1], recv_sem=one_recv.at[1],
        device_id=partner, device_id_type=MESH)
    keep_x = pltpu.make_async_copy(x_ref, xs_ref, local_sem.at[6])
    take_cot = pltpu.make_async_copy(cot_ref.at[span(role, blk), :], cot_s, local_sem.at[7])
    keep_cot = pltpu.make_async_copy(cot_s, cot_loc_ref, local_sem.at[8])

    @pl.when(owner)
    def _():
        give_x.start()
        give_cot.start()
        keep_x.start()
        take_cot.start()

    def project(i):
        rows = span(i, blk)
        unit = unit_rows(x_ref[rows, :], emb_row(emb_ref, 0))
        for t, ref in enumerate((wq_ref, wk_ref, wv_ref)):
            qkv_s[rows, t * head_cols:(t + 1) * head_cols] = dot_nn(unit, ref[...]).astype(BF16)

    for i in range(4):
        if i == 3:
            far_z('o')
            near_z('o')
        project(i)

    def context_copy(j, i):
        src = c_buf.at[j, span(i, blk), :]
        dst = c1_ref.at[:, pl.ds(pl.multiple_of((z * 2 + j) * PAIR, PAIR), PAIR)]
        target_z, target_c = 2 * core + i // 2, i % 2
        remote = pltpu.make_async_remote_copy(
            src_ref=src, dst_ref=dst, send_sem=c_send.at[j * 4 + i], recv_sem=c_recv.at[j * 4 + z],
            device_id=here.device(z=target_z, c=target_c), device_id_type=MESH)
        local = pltpu.make_async_copy(src, dst, c_recv.at[j * 4 + z])
        return remote, local, jnp.logical_and(target_z == z, target_c == core)

    def send_context(j, i):
        remote, local, to_self = context_copy(j, i)
        pl.when(to_self)(local.start)
        pl.when(jnp.logical_not(to_self))(remote.start)

    moves = {(0, 2): [(far_z, '1', '2'), (near_z, '1')], (0, 3): [(last_z, 'o')], (1, 1): [(far_z, '2', 'qkv')],
             (1, 2): [(last_z, '1'), (forward_a, 'o')], (1, 3): [(far_z, 'qkv'), (forward_b, 'o')]}
    for j in range(2):
        vt_s[...] = qkv_s[:, (4 + j) * PAIR:(5 + j) * PAIR].T
        k_view = qkv_s.at[:, (2 + j) * PAIR:(3 + j) * PAIR]
        for i in range(4):
            if i or j:
                send_context(j if i else 0, i - 1 if i else 3)
            for move, *what in moves.get((j, i), ()):
                move(*what)
            rows = slice(i * blk, (i + 1) * blk)
            outs, sums = attend_rows(qkv_s[rows, j * PAIR:(j + 1) * PAIR], k_view, vt_s, (e_a, e_b))
            c_buf[j, rows, :] = jnp.concatenate(outs, axis=0).T.astype(BF16)
            for head in range(2):
                lse_s[2 * j + head:2 * j + head + 1, rows] = sums[head]

    @pl.when(owner)
    def _():
        take_cot.wait()
        keep_cot.start()

    forward_a('1')
    near_z('2')
    send_context(1, 3)
    give_lse = pltpu.make_async_remote_copy(
        src_ref=lse_s, dst_ref=lse_ref, send_sem=one_send.at[2], recv_sem=one_recv.at[2],
        device_id=here.device(z=2 * core + z // 2, c=z % 2), device_id_type=MESH)
    keep_lse = pltpu.make_async_copy(lse_s, lse_ref, local_sem.at[9])
    lse_stays = jnp.logical_and(2 * core + z // 2 == z, z % 2 == core)
    pl.when(lse_stays)(keep_lse.start)
    pl.when(jnp.logical_not(lse_stays))(give_lse.start)
    forward_b('1')
    last_z('2')
    near_z('qkv')
    last_z('qkv')

    @pl.when(owner)
    def _():
        keep_x.wait()

    @pl.when(jnp.logical_not(owner))
    def _():
        give_x.wait_recv()

    for j in range(2):
        for zz in range(4):
            pltpu.make_async_copy(c_buf.at[j, :blk, :], c1_ref.at[:, :PAIR], c_recv.at[j * 4 + zz]).wait()

    def load(src, dst, n):
        copy = pltpu.make_async_copy(src, dst, load_sem.at[n])
        copy.start()
        return copy

    loads = [load(xs_ref.at[span(role, blk), :], x1_s, 0), load(c1_ref, c1_s, 1)]
    for copy in locals_:
        copy.wait()
    gathered('o')
    loads += [load(full_o.at[zz], wo_s.at[zz * wo_ref.shape[0]:(zz + 1) * wo_ref.shape[0], :], 2 + zz) for zz in range(4)]
    for copy in loads:
        copy.wait()
    h = (x1_s[...].astype(F32) + emb_row(emb_ref, 0) + dot_nn(c1_s[...], wo_s[...])).astype(BF16)
    m = rms_rows(h.astype(F32)).astype(BF16)
    h_s[...], m_s[...] = h, m
    gathered('1')
    tile = w1_s.shape[2]
    steps = full_1.shape[1] // tile
    per_plane = full_2.shape[1] // tile

    def w1_load(n):
        return pltpu.make_async_copy(full_1.at[:, span(n, tile)], w1_s.at[n % 2], load_sem.at[6 + n % 2])

    def w2_load(n):
        return pltpu.make_async_copy(full_2.at[n // per_plane, span(n % per_plane, tile), :], w2_s.at[n % 2], load_sem.at[8 + n % 2])

    def up_store(n):
        return pltpu.make_async_copy(up_s.at[n % 2], up_ref.at[:, span(n, tile)], out_sem.at[n % 2])

    w1_load(0).start()

    def up_part(n, _):
        @pl.when(n + 1 < steps)
        def _():
            w1_load(n + 1).start()

        @pl.when(n == steps // 8)
        def _():
            forward_a('2')

        @pl.when(n == steps * 5 // 8)
        def _():
            forward_a('qkv')

        w1_load(n).wait()

        @pl.when(n >= 2)
        def _():
            up_store(n - 2).wait()

        up = dot_nn(m_s[...], w1_s[n % 2]).astype(BF16)
        up_s[n % 2] = up
        factor = gelu_parts(up.astype(F32))[0]
        act_s[:, span(n, tile)] = (up.astype(F32) * factor).astype(BF16)
        up_store(n).start()
        return 0

    lax.fori_loop(0, steps, up_part, 0)
    forward_b('2')
    outs = [pltpu.make_async_copy(src, dst, out_sem.at[2 + n]) for n, (src, dst) in enumerate(
        ((x1_s, x1_ref), (h_s, h_ref), (m_s, m_ref), (act_s, act_ref)))]
    for copy in outs:
        copy.start()
    gathered('2')
    w2_load(0).start()
    acc[...] = jnp.zeros_like(acc)

    def down_part(n, _):
        @pl.when(n + 1 < steps)
        def _():
            w2_load(n + 1).start()

        @pl.when(n == steps // 2)
        def _():
            forward_b('qkv')

        w2_load(n).wait()
        acc[...] += dot_nn(act_s[:, span(n, tile)], w2_s[n % 2])
        return 0

    lax.fori_loop(0, steps, down_part, 0)
    c1_s[...] = (h_s[...].astype(F32) + acc[...]).astype(BF16)
    out_x2 = pltpu.make_async_copy(c1_s, x2_ref, out_sem.at[6])
    for j in range(2):
        for i in range(4):
            remote, _, to_self = context_copy(j, i)
            pl.when(jnp.logical_not(to_self))(remote.wait_send)
    pl.when(lse_stays)(keep_lse.wait)

    @pl.when(jnp.logical_not(lse_stays))
    def _():
        give_lse.wait_send()
        give_lse.wait_recv()

    out_x2.start()

    @pl.when(owner)
    def _():
        give_x.wait_send()
        give_cot.wait_send()
        keep_cot.wait()

    @pl.when(jnp.logical_not(owner))
    def _():
        give_cot.wait_recv()

    for n in range(steps - 2, steps):
        up_store(n).wait()
    for copy in outs:
        copy.wait()
    out_x2.wait()
    gathered('qkv')
    for copy in copies.sent:
        copy.wait_send()


def first_call(x, cot, emb, w_q, w_k, w_v, w_o, w_1, w_2):
    seq, d_model = x.shape
    head_cols, ff_cols, blk = w_q.shape[1], w_1.shape[1], seq // 4
    anywhere = pl.BlockSpec(memory_space=pl.ANY)
    in_vmem = pl.BlockSpec(memory_space=pltpu.VMEM)
    copies = 16 + 3 * 12 + 48
    hidden, tile = 4 * ff_cols, min(HIDDEN_FIRST, ff_cols)
    shape = jax.ShapeDtypeStruct
    dma = pltpu.SemaphoreType.DMA
    return pl.pallas_call(
        first_kernel,
        in_specs=[in_vmem, anywhere] + [in_vmem] * 7,
        out_specs=[anywhere] * 14,
        out_shape=[
            shape((blk, d_model), BF16),
            shape((4, seq), F32),
            shape((seq, d_model), BF16),
            shape((blk, d_model), BF16),
            shape((4, *w_o.shape), BF16),
            shape((d_model, hidden), BF16),
            shape((4, *w_2.shape), BF16),
            shape((d_model, 12 * head_cols), BF16),
            shape((blk, d_model), BF16),
            shape((blk, d_model), BF16),
            shape((blk, d_model), BF16),
            shape((blk, hidden), BF16),
            shape((blk, hidden), BF16),
            shape((blk, d_model), BF16),
        ],
        scratch_shapes=[
            pltpu.VMEM((seq, 3 * head_cols), BF16),
            pltpu.VMEM((PAIR, seq), BF16),
            pltpu.VMEM((seq, blk), F32),
            pltpu.VMEM((seq, blk), F32),
            pltpu.VMEM((2, seq, PAIR), BF16),
            pltpu.VMEM((4, seq), F32),
            pltpu.VMEM((blk, d_model), BF16),
            pltpu.VMEM((blk, d_model), BF16),
            pltpu.VMEM((blk, d_model), BF16),
            pltpu.VMEM((blk, d_model), BF16),
            pltpu.VMEM((blk, d_model), BF16),
            pltpu.VMEM((d_model, d_model), BF16),
            pltpu.VMEM((2, d_model, tile), BF16),
            pltpu.VMEM((2, tile, d_model), BF16),
            pltpu.VMEM((2, blk, tile), BF16),
            pltpu.VMEM((blk, hidden), BF16),
            pltpu.VMEM((blk, d_model), F32),
            dma((10,)), dma((copies,)), dma((copies,)), dma((8,)), dma((8,)), dma((3,)), dma((3,)), dma((10,)), dma((7,)),
        ],
        compiler_params=pltpu.CompilerParams(vmem_limit_bytes=60 << 20, collective_id=0, has_side_effects=True),
        cost_estimate=pl.CostEstimate(
            flops=64 * seq * seq * PAIR, bytes_accessed=64 * seq * d_model, transcendentals=seq * seq * 4),
        name="first",
    )(x, cot, emb, w_q, w_k, w_v, w_o, w_1, w_2)


def emb_row(emb_ref, row):
    return emb_ref[...].astype(F32)[row:row + 1, :]


def unit_rows(values, emb):
    values = values.astype(F32) + emb
    return (values * lax.rsqrt(jnp.mean(values * values, axis=-1, keepdims=True) + EPS_NORM)).astype(BF16)


def forward_kernel(x_ref, emb_ref, xs1_ref, wqkv_ref,
                   c_ref, lse_ref, u2_ref, qkv2_ref, u1_ref, qkv1_ref,
                   w_s, blocks, u_s, qkv_s, x1_s, u1_s, qkv1_s, v_t, e_a, e_b, c_buf, lse_s,
                   local_sem, first_sem, out_sem, x_send, x_recv, c_send, c_recv):
    seq = xs1_ref.shape[0]
    blk = seq // 4
    head_cols = 2 * PAIR
    here = Place()
    z, core, role = here.z, here.c, here.role

    def span(index, count):
        return pl.ds(pl.multiple_of(index * count, count), count)

    w_load = pltpu.make_async_copy(wqkv_ref.at[:, span(role, 3 * head_cols)], w_s, local_sem.at[0])
    w_load.start()
    x1_load = [pltpu.make_async_copy(xs1_ref.at[i * blk:(i + 1) * blk, :], x1_s.at[i % 2], first_sem.at[i % 2]) for i in range(4)]
    x1_load[0].start()
    here.meet()
    partner, across = here.device(c=1 - core), here.device(z=here.z_by[1])
    role_side, role_over = z % 2 * 2 + 1 - core, (1 - z % 2) * 2 + core
    role_last = (1 - z % 2) * 2 + 1 - core

    def x_copy(n, src, slot, device):
        return pltpu.make_async_remote_copy(
            src_ref=src, dst_ref=blocks.at[slot], send_sem=x_send.at[n], recv_sem=x_recv.at[n],
            device_id=device, device_id_type=MESH)

    over, side = x_copy(0, x_ref, 0, across), x_copy(1, x_ref, 1, partner)
    last = x_copy(2, blocks.at[0], 2, partner)
    over.start()
    side.start()

    def project(src, at_role):
        rows = span(at_role, blk)
        unit = unit_rows(src, emb_row(emb_ref, 1))
        u_s[rows, :] = unit
        qkv_s[rows, :] = dot_nn(unit, w_s[...]).astype(BF16)

    w_load.wait()
    project(x_ref[...], role)
    side.wait_recv()
    project(blocks[1], role_side)

    stores = []
    for i in range(4):
        if i < 3:
            x1_load[i + 1].start()
        x1_load[i].wait()
        if i >= 2:
            for copy in stores[i - 2]:
                copy.wait()
        unit = unit_rows(x1_s[i % 2], emb_row(emb_ref, 0))
        u1_s[i % 2] = unit
        qkv1_s[i % 2] = dot_nn(unit, w_s[...]).astype(BF16)
        stores.append([pltpu.make_async_copy(u1_s.at[i % 2], u1_ref.at[i * blk:(i + 1) * blk, :], out_sem.at[i % 2]),
                       pltpu.make_async_copy(qkv1_s.at[i % 2], qkv1_ref.at[i * blk:(i + 1) * blk, :], out_sem.at[2 + i % 2])])
        for copy in stores[i]:
            copy.start()

    over.wait_recv()
    last.start()
    project(blocks[0], role_over)
    last.wait_recv()
    project(blocks[2], role_last)
    keep_u = pltpu.make_async_copy(u_s, u2_ref, local_sem.at[1])
    keep_qkv = pltpu.make_async_copy(qkv_s, qkv2_ref, local_sem.at[2])
    keep_u.start()
    keep_qkv.start()

    member = [here.device(z=z // 2 * 2 + i // 2, c=i % 2) for i in range(4)]

    def c_copy(j, i):
        src = c_buf.at[j, i * blk:(i + 1) * blk, :]
        dst = c_ref.at[:, pl.ds(pl.multiple_of((role * 2 + j) * PAIR, PAIR), PAIR)]
        remote = pltpu.make_async_remote_copy(
            src_ref=src, dst_ref=dst, send_sem=c_send.at[j * 4 + i], recv_sem=c_recv.at[j * 4 + role],
            device_id=member[i], device_id_type=MESH)
        return remote, pltpu.make_async_copy(src, dst, c_recv.at[j * 4 + role])

    def send_context(j, i):
        remote, local = c_copy(j, i)
        pl.when(role == i)(local.start)
        pl.when(role != i)(remote.start)

    for j in range(2):
        v_t[...] = qkv_s[:, (4 + j) * PAIR:(5 + j) * PAIR].T
        k_view = qkv_s.at[:, (2 + j) * PAIR:(3 + j) * PAIR]
        for i in range(4):
            if i or j:
                send_context(j if i else 0, i - 1 if i else 3)
            rows = slice(i * blk, (i + 1) * blk)
            outs, sums = attend_rows(qkv_s[rows, j * PAIR:(j + 1) * PAIR], k_view, v_t, (e_a, e_b))
            c_buf[j, rows, :] = jnp.concatenate(outs, axis=0).T.astype(BF16)
            for head in range(2):
                lse_s[2 * j + head:2 * j + head + 1, rows] = sums[head]
    lse_ref[...] = lse_s[...]
    send_context(1, 3)
    for j in range(2):
        for i in range(4):
            pltpu.make_async_copy(c_buf.at[j, :blk, :], c_ref.at[:, :PAIR], c_recv.at[j * 4 + i]).wait()
            pl.when(role != i)(c_copy(j, i)[0].wait_send)
    for copy in (over, side, last):
        copy.wait_send()
    for group in stores[2:]:
        for copy in group:
            copy.wait()
    keep_u.wait()
    keep_qkv.wait()


def forward_call(x, emb, xs_1, w_qkv):
    blk, d_model = x.shape
    seq, head_cols = 4 * blk, 2 * PAIR
    anywhere = pl.BlockSpec(memory_space=pl.ANY)
    in_vmem = pl.BlockSpec(memory_space=pltpu.VMEM)
    dma = pltpu.SemaphoreType.DMA
    return pl.pallas_call(
        forward_kernel,
        in_specs=[in_vmem, in_vmem, anywhere, anywhere],
        out_specs=[anywhere, in_vmem] + [anywhere] * 4,
        out_shape=[
            jax.ShapeDtypeStruct((blk, d_model), BF16),
            jax.ShapeDtypeStruct((4, seq), F32),
        ] + [jax.ShapeDtypeStruct((seq, n), BF16) for n in (d_model, 3 * head_cols)] * 2,
        scratch_shapes=[
            pltpu.VMEM((d_model, 3 * head_cols), BF16),
            pltpu.VMEM((3, blk, d_model), BF16),
            pltpu.VMEM((seq, d_model), BF16),
            pltpu.VMEM((seq, 3 * head_cols), BF16),
            pltpu.VMEM((2, blk, d_model), BF16),
            pltpu.VMEM((2, blk, d_model), BF16),
            pltpu.VMEM((2, blk, 3 * head_cols), BF16),
            pltpu.VMEM((PAIR, seq), BF16),
            pltpu.VMEM((seq, blk), F32),
            pltpu.VMEM((seq, blk), F32),
            pltpu.VMEM((2, seq, PAIR), BF16),
            pltpu.VMEM((4, seq), F32),
            dma((3,)), dma((2,)), dma((4,)), dma((3,)), dma((3,)), dma((8,)), dma((8,)),
        ],
        compiler_params=pltpu.CompilerParams(vmem_limit_bytes=60 << 20, collective_id=2, has_side_effects=True),
        cost_estimate=pl.CostEstimate(
            flops=64 * seq * seq * PAIR, bytes_accessed=32 * seq * d_model, transcendentals=seq * seq * 4),
        name="forward",
    )(x, emb, xs_1, w_qkv)


def through_norm(values, up, d_mid):
    inverse = lax.rsqrt(jnp.mean(values * values, axis=-1, keepdims=True) + EPS_NORM)
    inner = jnp.mean(values * up, axis=-1, keepdims=True)
    return (d_mid.astype(F32) + inverse * up - values * (inverse * inverse * inverse * inner)).astype(BF16)


def backward_kernel(shared, qkv_ref, dc_ref, lse_ref, dmid_ref, x_ref, emb_ref, wqkv_ref, u_ref, *refs):
    sources, (d_ref, other_ref, g_ref), shares = refs[:shared], refs[shared:shared + 3], refs[shared + 3:2 * shared + 3]
    (dch, k_t, dk_acc, dv_acc, p_cat, ds_cat, p_cat2, ds_cat2, d_heads, d_qkv, d_u, w_s, u_s, g_s,
     load_sem, out_sem, dc_send, dc_recv, dq_send, dq_recv, d_send, d_recv, s_send, s_recv) = refs[2 * shared + 3:]
    seq = qkv_ref.shape[0]
    blk = seq // 4
    head_cols = 2 * PAIR
    here = Place()
    z, core, role = here.z, here.c, here.role
    here.meet()
    member = [here.device(z=z // 2 * 2 + i // 2, c=i % 2) for i in range(4)]

    def span(index, count):
        return pl.ds(pl.multiple_of(index * count, count), count)

    def load(src, dst, n):
        copy = pltpu.make_async_copy(src, dst, load_sem.at[n])
        copy.start()
        return copy

    def dc_copy(j, i):
        col = i * head_cols + j * PAIR
        return pltpu.make_async_remote_copy(
            src_ref=dc_ref.at[:, col:col + PAIR], dst_ref=dch.at[span(role, blk), j * PAIR:(j + 1) * PAIR],
            send_sem=dc_send.at[j * 4 + i], recv_sem=dc_recv.at[j * 4 + role], device_id=member[i], device_id_type=MESH)

    for j in range(2):
        for i in range(4):
            pl.when(role != i)(dc_copy(j, i).start)
    for i in range(4):
        @pl.when(role == i)
        def _():
            dch[i * blk:(i + 1) * blk, :] = dc_ref[:, i * head_cols:(i + 1) * head_cols]

    def dq_copy(j, i, t):
        col = t * head_cols + j * PAIR
        return pltpu.make_async_remote_copy(
            src_ref=d_heads.at[i * blk:(i + 1) * blk, col:col + PAIR],
            dst_ref=d_qkv.at[:, pl.ds(pl.multiple_of(role * 3 * head_cols + col, PAIR), PAIR)],
            send_sem=dq_send.at[(j * 4 + i) * 3 + t], recv_sem=dq_recv.at[(j * 4 + role) * 3 + t],
            device_id=member[i], device_id_type=MESH)

    def send_d_heads(j, ts):
        for i in range(4):
            @pl.when(role != i)
            def _():
                for t in ts:
                    dq_copy(j, i, t).start()

    shared_copies = [pltpu.make_async_remote_copy(
        src_ref=src, dst_ref=dst, send_sem=s_send.at[n], recv_sem=s_recv.at[n],
        device_id=here.device(c=1 - core), device_id_type=MESH) for n, (src, dst) in enumerate(zip(sources, shares))]

    steps = seq // BWD_ROWS
    p_cats, ds_cats = (p_cat, p_cat2), (ds_cat, ds_cat2)
    for j in range(2):
        for i in range(4):
            @pl.when(role != i)
            def _():
                pltpu.make_async_copy(dc_ref.at[:, :PAIR], dch.at[:blk, :PAIR], dc_recv.at[j * 4 + i]).wait()
        if j == 0:
            for copy in shared_copies:
                copy.start()
        k_view, v_view = qkv_ref.at[:, (2 + j) * PAIR:(3 + j) * PAIR], qkv_ref.at[:, (4 + j) * PAIR:(5 + j) * PAIR]
        k_t[...] = k_view[...].T
        dk_acc[...] = jnp.zeros_like(dk_acc)
        dv_acc[...] = jnp.zeros_like(dv_acc)

        cols = slice(j * PAIR, (j + 1) * PAIR)

        def scores_of(i, n):
            rows = span(i, BWD_ROWS)
            score_part(qkv_ref[rows, cols], dch[rows, cols], lse_ref[2 * j:2 * j + 2, rows], k_view, v_view, p_cats[n], ds_cats[n])

        def products_of(i, n):
            rows = span(i, BWD_ROWS)
            d_heads[rows, cols] = product_part(qkv_ref[rows, cols], dch[rows, cols], k_t, p_cats[n], ds_cats[n], dk_acc, dv_acc)

        def two_blocks(i, _):
            if j == 1:
                @pl.when(i == min(1, steps // 2 - 1))
                def _():
                    send_d_heads(0, (0, 1, 2))
            scores_of(2 * i + 1, 1)
            products_of(2 * i, 0)
            scores_of(2 * i + 2, 0)
            products_of(2 * i + 1, 1)
            return 0

        scores_of(0, 0)
        lax.fori_loop(0, steps // 2 - 1, two_blocks, 0)
        scores_of(steps - 1, 1)
        products_of(steps - 2, 0)
        if j == 1:
            for target in range(3):
                pl.when(role != target)(dq_copy(1, target, 0).start)
        products_of(steps - 1, 1)
        d_heads[:, head_cols + j * PAIR:head_cols + (j + 1) * PAIR] = (dk_acc[...] * SCALE).astype(BF16)
        d_heads[:, 2 * head_cols + j * PAIR:2 * head_cols + (j + 1) * PAIR] = dv_acc[...].astype(BF16)

    quarter = u_s.shape[2]
    pending = load(u_ref.at[:, :quarter], u_s.at[0], 0)
    for i in range(4):
        @pl.when(role == i)
        def _():
            d_qkv[:, i * 3 * head_cols:(i + 1) * 3 * head_cols] = d_heads[i * blk:(i + 1) * blk, :]
    pl.when(role != 3)(dq_copy(1, 3, 0).start)
    send_d_heads(1, (1, 2))
    stores = []
    count = u_ref.shape[1] // quarter
    for n in range(count):
        ahead = load(u_ref.at[:, (n + 1) * quarter:(n + 2) * quarter], u_s.at[(n + 1) % 2], (n + 1) % 2) if n + 1 < count else None
        pending.wait()
        if n >= 2:
            stores[n - 2].wait()
        g_s[n % 2] = dot_tn(u_s[n % 2], d_heads[...])
        stores.append(pltpu.make_async_copy(g_s.at[n % 2], g_ref.at[n * quarter:(n + 1) * quarter, :], out_sem.at[n % 2]))
        stores[n].start()
        pending = ahead
    w_rows = w_s.shape[1]
    chunks = wqkv_ref.shape[0] // w_rows
    w_load = load(wqkv_ref.at[:w_rows, :], w_s.at[0], 2)
    for j in range(2):
        for i in range(4):
            @pl.when(role != i)
            def _():
                for t in range(3):
                    pltpu.make_async_copy(d_heads.at[:blk, :PAIR], d_qkv.at[:, :PAIR], dq_recv.at[(j * 4 + i) * 3 + t]).wait()
    for n in range(chunks):
        ahead = load(wqkv_ref.at[(n + 1) * w_rows:(n + 2) * w_rows, :], w_s.at[(n + 1) % 2], 2 + (n + 1) % 2) if n + 1 < chunks else None
        w_load.wait()
        d_u[:, n * w_rows:(n + 1) * w_rows] = dot_nt(d_qkv[...], w_s[n % 2]).astype(BF16)
        w_load = ahead
    rows_each = min(128, blk)
    for n in range(blk // rows_each):
        rows = slice(n * rows_each, (n + 1) * rows_each)
        d_u[rows, :] = through_norm(x_ref[rows, :].astype(F32) + emb_row(emb_ref, 1), d_u[rows, :].astype(F32), dmid_ref[rows, :])
    keep = pltpu.make_async_copy(d_u, d_ref, out_sem.at[2])
    keep.start()
    stores[count - 2].wait()
    stores[count - 1].wait()
    give = pltpu.make_async_remote_copy(
        src_ref=d_u, dst_ref=other_ref, send_sem=d_send.at[0], recv_sem=d_recv.at[0],
        device_id=here.device(c=1 - core), device_id_type=MESH)
    give.start()
    for i in range(4):
        @pl.when(role != i)
        def _():
            for j in range(2):
                dc_copy(j, i).wait_send()
                for t in range(3):
                    dq_copy(j, i, t).wait_send()
    keep.wait()
    give.wait()
    for copy in shared_copies:
        copy.wait()


def backward_call(qkv, d_c, lse, d_mid, x, emb, w_qkv, u_seq, shared):
    seq, d_model = u_seq.shape
    blk, heads3 = seq // 4, qkv.shape[1]
    anywhere = pl.BlockSpec(memory_space=pl.ANY)
    in_vmem = pl.BlockSpec(memory_space=pltpu.VMEM)
    dma = pltpu.SemaphoreType.DMA
    quarter = d_model // 4
    return pl.pallas_call(
        functools.partial(backward_kernel, len(shared)),
        in_specs=[in_vmem] * 6 + [anywhere] * (2 + len(shared)),
        out_specs=[anywhere] * (3 + len(shared)),
        out_shape=[
            jax.ShapeDtypeStruct((blk, d_model), BF16),
            jax.ShapeDtypeStruct((blk, d_model), BF16),
            jax.ShapeDtypeStruct((d_model, heads3), F32),
        ] + [jax.ShapeDtypeStruct(value.shape, value.dtype) for value in shared],
        scratch_shapes=[
            pltpu.VMEM((seq, heads3 // 3), BF16),
            pltpu.VMEM((PAIR, seq), BF16),
            pltpu.VMEM((seq, PAIR), F32),
            pltpu.VMEM((seq, PAIR), F32),
            pltpu.VMEM((seq, 2 * BWD_ROWS), BF16),
            pltpu.VMEM((seq, 2 * BWD_ROWS), BF16),
            pltpu.VMEM((seq, 2 * BWD_ROWS), BF16),
            pltpu.VMEM((seq, 2 * BWD_ROWS), BF16),
            pltpu.VMEM((seq, heads3), BF16),
            pltpu.VMEM((blk, 4 * heads3), BF16),
            pltpu.VMEM((blk, d_model), BF16),
            pltpu.VMEM((2, quarter, 4 * heads3), BF16),
            pltpu.VMEM((2, seq, quarter), BF16),
            pltpu.VMEM((2, quarter, heads3), F32),
            dma((4,)), dma((3,)), dma((8,)), dma((8,)), dma((24,)), dma((24,)), dma((1,)), dma((1,)),
            dma((len(shared),)), dma((len(shared),)),
        ],
        compiler_params=pltpu.CompilerParams(vmem_limit_bytes=60 << 20, collective_id=3, has_side_effects=True),
        cost_estimate=pl.CostEstimate(
            flops=160 * seq * seq * PAIR, bytes_accessed=64 * seq * d_model, transcendentals=seq * seq * 4),
        name="backward",
    )(qkv, d_c, lse, d_mid, x, emb, w_qkv, u_seq, *shared)


def rms_rows(values):
    return values * lax.rsqrt(jnp.mean(values * values, axis=-1, keepdims=True) + EPS_NORM)


GELU_IN, GELU_CUBE = math.sqrt(2 / math.pi), 0.044715


def gelu_parts(z):
    square = z * z
    t = jnp.tanh(z * (GELU_IN + (GELU_IN * GELU_CUBE) * square))
    return 0.5 + 0.5 * t, t, square


def hidden_kernel(backward, forward, *refs):
    refs = list(refs)
    take = lambda: refs.pop(0)
    if forward:
        c_ref, x_ref, emb_ref, wo_ref = take(), take(), take(), take()
        w1_ref = take()
    else:
        h_ref, wo_ref, up_ref = take(), take(), take()
    w2_ref = take()
    both = forward and backward
    if backward:
        d_ref = take()
    if backward and not forward:
        w1b_ref = take()
    if forward:
        h_out, m_out = take(), take()
        up_out = None if both else take()
        act_out = take()
    if backward:
        dup_out, dmid_out, dc_out = take(), take(), take()
    else:
        x_out = take()
    if forward:
        h_s, m_s = take(), take()
    prev_s, acc = take(), take()
    step, last = pl.program_id(0), pl.num_programs(0) - 1

    if forward:
        @pl.when(step == 0)
        def _():
            h = (x_ref[...].astype(F32) + emb_row(emb_ref, 1) + dot_nn(c_ref[...], wo_ref[...])).astype(BF16)
            m = rms_rows(h.astype(F32)).astype(BF16)
            h_s[...], m_s[...] = h, m
            h_out[...], m_out[...] = h, m

    def both_parts():
        count = w1_ref.shape[1] // 2
        halves = [slice(n * count, (n + 1) * count) for n in range(2)]
        d_acts = [dot_nt(d_ref[...], w2_ref[half, :]).astype(BF16) for half in halves]
        ups = [dot_nn(m_s[...], w1_ref[:, half]).astype(BF16) for half in halves]
        total = None
        for half, d_act, up in zip(halves, d_acts, ups):
            z = up.astype(F32)
            factor, t, square = gelu_parts(z)
            act_out[:, half] = (z * factor).astype(BF16)
            slope = factor + z * ((1.0 - t * t) * (0.5 * GELU_IN + (1.5 * GELU_IN * GELU_CUBE) * square))
            d_up = (slope * d_act.astype(F32)).astype(BF16)
            dup_out[:, half] = d_up
            part = dot_nt(d_up, w1_ref[:, half])
            total = part if total is None else total + part
        return total

    def finish(total):
        h = (h_s if forward else h_ref)[...].astype(F32)
        d_mid = through_norm(h, total.astype(BF16).astype(F32), d_ref[...])
        dmid_out[...] = d_mid
        dc_out[...] = dot_nt(d_mid, wo_ref[...]).astype(BF16)

    if both:
        @pl.when(step == 0)
        def _():
            acc[...] = both_parts()

        @pl.when(step > 0)
        def _():
            acc[...] += both_parts()

        @pl.when(step == last)
        def _():
            finish(acc[...])
        return

    def first_part():
        slot = step % 2
        if backward:
            d_act = dot_nt(d_ref[...], w2_ref[...]).astype(BF16).astype(F32)
        if forward:
            up = dot_nn(m_s[...], w1_ref[...]).astype(BF16)
            up_out[...] = up
        else:
            up = up_ref[...]
        z = up.astype(F32)
        factor, t, square = gelu_parts(z)
        if forward:
            act = (z * factor).astype(BF16)
            act_out[...] = act
        if backward:
            slope = factor + z * ((1.0 - t * t) * (0.5 * GELU_IN + (1.5 * GELU_IN * GELU_CUBE) * square))
            d_up = (slope * d_act).astype(BF16)
            dup_out[...] = d_up
            prev_s[slot] = d_up
        else:
            prev_s[slot] = act

    def second_part():
        prev = prev_s[1 - step % 2]
        if backward:
            return dot_nt(prev, w1b_ref[...])
        return dot_nn(prev, w2_ref[...])

    pl.when(step == 0)(first_part)

    @pl.when(step == 1)
    def _():
        acc[...] = second_part()
        first_part()

    @pl.when(jnp.logical_and(step > 1, step < last))
    def _():
        acc[...] += second_part()
        first_part()

    @pl.when(step == last)
    def _():
        total = acc[...] + second_part()
        if backward:
            finish(total)
        else:
            x_out[...] = (h_s[...].astype(F32) + total).astype(BF16)


def hidden_call(forward, backward, w_o, w_1, w_2, context=None, x=None, emb=None, h=None, up=None, d_next=None):
    blk, d_model = (context if forward else h).shape
    hidden = w_1.shape[1]
    tile = HIDDEN
    steps = hidden // tile
    now, before = (lambda i: jnp.minimum(i, steps - 1)), (lambda i: jnp.maximum(i - 1, 0))
    whole = lambda rows, cols: pl.BlockSpec((rows, cols), lambda i: (0, 0))
    wide = pl.BlockSpec((blk, tile), lambda i: (0, now(i)))
    args, specs = [], []

    def add(value, spec):
        args.append(value)
        specs.append(spec)

    if forward:
        add(context, whole(blk, d_model))
        add(x, whole(blk, d_model))
        add(emb, whole(2, d_model))
        add(w_o, whole(d_model, d_model))
        add(w_1, pl.BlockSpec((d_model, tile), lambda i: (0, now(i))))
    else:
        add(h, whole(blk, d_model))
        add(w_o, whole(d_model, d_model))
        add(up, wide)
    add(w_2, pl.BlockSpec((tile, d_model), (lambda i: (now(i), 0)) if backward else (lambda i: (before(i), 0))))
    if backward:
        add(d_next, whole(blk, d_model))
    if backward and not forward:
        add(w_1, pl.BlockSpec((d_model, tile), lambda i: (0, before(i))))
    row = (whole(blk, d_model), jax.ShapeDtypeStruct((blk, d_model), BF16))
    big = (wide, jax.ShapeDtypeStruct((blk, hidden), BF16))
    outs = ([row, row] + [big] * (1 if backward else 2) if forward else []) + ([big, row, row] if backward else [row])
    return pl.pallas_call(
        functools.partial(hidden_kernel, backward, forward),
        grid=(steps + (0 if forward and backward else 1),),
        in_specs=specs,
        out_specs=[spec for spec, _ in outs],
        out_shape=[shape for _, shape in outs],
        scratch_shapes=([pltpu.VMEM((blk, d_model), BF16)] * 2 if forward else [])
        + [pltpu.VMEM((2, blk, tile), BF16), pltpu.VMEM((blk, d_model), F32)],
        compiler_params=pltpu.CompilerParams(vmem_limit_bytes=60 << 20),
        cost_estimate=pl.CostEstimate(
            flops=2 * blk * d_model * (hidden * (3 if forward and backward else 2) + 2 * d_model),
            bytes_accessed=4 * hidden * d_model + 8 * blk * hidden, transcendentals=blk * hidden),
        interpret=INTERPRET,
        name="hidden",
    )(*args)


def head_only(values, head):
    lane = lax.broadcasted_iota(jnp.int32, values.shape, 1)
    return jnp.where(lane // HEAD_DIM == head, values, jnp.zeros_like(values))


def score_part(q, d_out, lse, k_ref, v_ref, p_cat, ds_cat):
    block = q.shape[0]
    for head in range(2):
        scores = dot_nt(k_ref[...], head_only(q, head))
        probs = jnp.exp2(scores * EXP2_SCALE - lse[head:head + 1, :])
        d_probs = dot_nt(v_ref[...], head_only(d_out, head)).astype(BF16).astype(F32)
        inner = jnp.sum(probs * d_probs, axis=0, keepdims=True)
        cols = slice(head * block, (head + 1) * block)
        p_cat[:, cols] = probs.astype(BF16)
        ds_cat[:, cols] = (probs * (d_probs - inner)).astype(BF16)


def product_part(q, d_out, k_t, p_cat, ds_cat, dk_acc, dv_acc):
    block = q.shape[0]
    dqs = [dot_nn(k_t[head * HEAD_DIM:(head + 1) * HEAD_DIM, :], ds_cat[:, head * block:(head + 1) * block]) for head in range(2)]
    dv_acc[...] += dot_nn(p_cat[...], jnp.concatenate([head_only(d_out, head) for head in range(2)], axis=0))
    dk_acc[...] += dot_nn(ds_cat[...], jnp.concatenate([head_only(q, head) for head in range(2)], axis=0))
    return (jnp.concatenate(dqs, axis=0).T * SCALE).astype(BF16)


def backward_rows(q, d_out, lse, k_ref, v_ref, k_t, p_cat, ds_cat, dk_acc, dv_acc):
    score_part(q, d_out, lse, k_ref, v_ref, p_cat, ds_cat)
    return product_part(q, d_out, k_t, p_cat, ds_cat, dk_acc, dv_acc)


def last_kernel(qkv_ref, dc_ref, lse_ref, dmid_ref, x_ref, emb_ref, wqkv_ref, u_ref, gqkv2_ref,
                *refs):
    lefts = {'2': refs[:4], '1': refs[8:12], 'o': refs[15:18]}
    rights = {'2': refs[4:8], '1': refs[12:15], 'o': refs[18:22]}
    (dx_ref, g1_ref, g2_ref, go_ref, gq_ref, gk_ref, gv_ref, away2_ref, mid2_ref, keep2_ref,
     away1_ref, mid1_ref, keep1_ref, awayo_ref, mido_ref, keepo_ref, dup_other, dmid_other,
     dch, k_t, dk_acc, dv_acc, p_cat, ds_cat, d_heads, d_qkv, buf, buf_o, second, second_o, tmp, tmp_o,
     third, third_o, sum_1, sum_2, sum_o, qa, qb, q1, q2, q3, q4, d_1, w_s, u_s, g_s,
     left_t, stage,
     local_sem, load_sem, send_sem, recv_sem, dc_send, dc_recv, dq_send, dq_recv, z_send, z_recv, x_send, x_recv,
     p_send, p_recv) = refs[22:]
    seq = qkv_ref.shape[0]
    blk = seq // 4
    head_cols = 2 * PAIR
    here = Place()
    z, core, role, owner = here.z, here.c, here.role, here.owner
    here.meet()
    copies = Copies(send_sem, recv_sem)
    waits = []

    def span(index, count):
        return pl.ds(pl.multiple_of(index * count, count), count)

    def load(src, dst, n):
        copy = pltpu.make_async_copy(src, dst, load_sem.at[n])
        copy.start()
        return copy

    no = jnp.logical_not
    to_a, to_b = here.device(y=here.ya, x=here.xa), here.device(y=here.yb, x=here.xb)
    partner = here.device(c=1 - core)
    member = [here.device(z=z // 2 * 2 + i // 2, c=i % 2) for i in range(4)]
    piece = tmp.shape[1]

    def dc_copy(i):
        return pltpu.make_async_remote_copy(
            src_ref=dc_ref.at[:, i * head_cols:(i + 1) * head_cols], dst_ref=dch.at[span(role, blk), :],
            send_sem=dc_send.at[i], recv_sem=dc_recv.at[role], device_id=member[i], device_id_type=MESH)

    for i in range(4):
        pl.when(role != i)(dc_copy(i).start)

        @pl.when(role == i)
        def _():
            dch[i * blk:(i + 1) * blk, :] = dc_ref[:, i * head_cols:(i + 1) * head_cols]

    half = rights['1'][0].shape[1] // 8
    wide = 2 * half
    dmid_give = copies.start(lefts['o'][2], dmid_other, partner)
    dup_give = [copies.start(rights['1'][2].at[:, q * wide:(q + 1) * wide], dup_other.at[:, q * wide:(q + 1) * wide], partner)
                for q in range(4)]
    lefts['o'] = (*lefts['o'], dmid_other)
    rights['1'] = (*rights['1'], dup_other)
    firsts = {(w, q): [copies.make(ref.at[q, :, h * half:(h + 1) * half], buf.at[u + q, :, h * half:(h + 1) * half], to_a)
                       for h in range(2)] for w, ref, u in (('2', away2_ref, 0), ('1', away1_ref, 4)) for q in range(4)}
    firsts['o'] = [copies.make(awayo_ref.at[2 * h:2 * h + 2], buf_o.at[2 * h:2 * h + 2], to_a) for h in range(2)]
    seconds = {(w, q): copies.make(buf.at[u + q, piece:, :], second.at[u + q], to_b) for w, u in (('2', 0), ('1', 4)) for q in range(4)}
    seconds['o'] = copies.make(buf_o.at[:, piece:, :], second_o, to_b)

    def add_mid(unit):
        if unit == 'o':
            mid, keep, t, n = mido_ref, keepo_ref, tmp_o, 4
            bottom, top = buf_o.at[:, piece:, :], buf_o.at[:, :piece, :]
        else:
            w, q = unit
            mid, keep = (mid2_ref.at[q], keep2_ref.at[q]) if w == '2' else (mid1_ref.at[q], keep1_ref.at[q])
            u = q if w == '2' else 4 + q
            t, n, bottom, top = tmp, 6, buf.at[u, piece:, :], buf.at[u, :piece, :]
        loads = [load(mid, t.at[0], n), load(keep, t.at[1], n + 1)]
        for copy in firsts[unit]:
            copy.wait_recv()
        for copy in loads:
            copy.wait()
        bottom[...] += t[0]
        top[...] += t[1]
        seconds[unit].start()

    sums = {'2': (lambda q: buf.at[q, :piece, :], third.at[0], 0), '1': (lambda q: buf.at[4 + q, :piece, :], third.at[1], 1),
            'o': (lambda q: buf_o.at[q, :piece, :], third_o, 2)}
    far_q = here.z_by[2]

    def near_copy(w, q):
        part, got, n = sums[w]
        return pltpu.make_async_remote_copy(
            src_ref=part(q), dst_ref=got.at[q // 2], send_sem=z_send.at[n * 3 + q // 2], recv_sem=z_recv.at[n * 3 + q // 2],
            device_id=here.device(z=here.z_by[1]), device_id_type=MESH)

    def far_copy(w):
        part, got, n = sums[w]
        return pltpu.make_async_remote_copy(
            src_ref=part(far_q), dst_ref=got.at[2], send_sem=z_send.at[n * 3 + 2], recv_sem=z_recv.at[n * 3 + 2],
            device_id=here.device(z=far_q), device_id_type=MESH)

    def finish(unit):
        seconds[unit].wait_recv()
        if unit == 'o':
            buf_o[:, :piece, :] += second_o[...]
            w, qs = 'o', range(4)
        else:
            w, u = unit[0], unit[1] + (4 if unit[0] == '1' else 0)
            buf[u, :piece, :] += second[u]
            qs = (unit[1],)
        for q in qs:
            pl.when((z + q) % 2 == 1)(near_copy(w, q).start)

    def far(w):
        part, got, n = sums[w]
        for k in range(2):
            pltpu.make_async_copy(got.at[2], got.at[k], z_recv.at[n * 3 + k]).wait()
        theirs, ours = part(far_q), part(z)
        theirs[...] += got[far_q // 2]
        ours[...] += got[z // 2]
        far_copy(w).start()

    mine, by_a = here.piece(here.y, here.x), here.piece(here.ya, here.xa)
    by_b, by_ab = here.piece(here.yb, here.xb), here.piece(1 - here.y, 1 - here.x)
    gathers = {}

    def total(w):
        part, got, n = sums[w]
        out = {'2': sum_2, '1': sum_1, 'o': sum_o}[w]
        far_copy(w).wait_recv()
        out[...] = part(z)[...] + got[2]

    def gather_start(name, src, out, n):
        rows = lambda e: out.at[span(e, piece), :]
        keep = pltpu.make_async_copy(src, rows(mine), local_sem.at[n])
        keep.start()
        waits.append(keep)
        gathers[name] = dict(src=src, rows=rows, a=copies.start(src, rows(mine), to_a), b1=copies.start(src, rows(mine), to_b))

    def gather_second(name):
        g = gathers[name]
        g['a'].wait_recv()
        g['b2'] = copies.start(g['rows'](by_a), g['rows'](by_a), to_b)

    def gather_core(name):
        g = gathers[name]
        g['c'] = [copies.start(g['src'], g['rows'](mine), partner), copies.start(g['rows'](by_a), g['rows'](by_a), partner)]
        g['b1'].wait_recv()
        g['c'].append(copies.start(g['rows'](by_b), g['rows'](by_b), partner))
        g['b2'].wait_recv()
        g['c'].append(copies.start(g['rows'](by_ab), g['rows'](by_ab), partner))

    def dq_copy(j, i, t):
        col = t * head_cols + j * PAIR
        return pltpu.make_async_remote_copy(
            src_ref=d_heads.at[i * blk:(i + 1) * blk, col:col + PAIR],
            dst_ref=d_qkv.at[:, pl.ds(pl.multiple_of(role * 3 * head_cols + col, PAIR), PAIR)],
            send_sem=dq_send.at[(j * 4 + i) * 3 + t], recv_sem=dq_recv.at[(j * 4 + role) * 3 + t],
            device_id=member[i], device_id_type=MESH)

    def send_d_heads(j):
        for i in range(4):
            @pl.when(role != i)
            def _():
                for t in range(3):
                    dq_copy(j, i, t).start()

    index = [here.ya * 2 + here.xa, (1 - here.y) * 2 + 1 - here.x, here.yb * 2 + here.xb, here.y * 2 + here.x]
    spaces = (p_cat, ds_cat)
    parts = [('2', n) for n in range(8)] + [('1', n) for n in range(8)] + [('o', n) for n in range(2)]
    left_loads = [('2', q) for q in range(4)] + [('1', 0), ('o', 0)]

    def load_lefts(name, q):
        for n in range(16):
            pltpu.make_async_copy(
                lefts[name][n // 4].at[:, span(q * 8 + index[n % 4] * 2 + core, piece)],
                d_heads.at[n // 4 * blk:(n // 4 + 1) * blk, n % 4 * piece:(n % 4 + 1) * piece], load_sem.at[14]).start()

    def load_rights(s):
        name, n = parts[s]
        for i in range(4):
            pltpu.make_async_copy(
                rights[name][i].at[:, n * half:(n + 1) * half], spaces[s % 2].at[i * blk:(i + 1) * blk, :],
                load_sem.at[15 + s % 2]).start()

    def stored(s):
        pltpu.make_async_copy(stage.at[s % 2], stage.at[s % 2], load_sem.at[17 + s % 2]).wait()

    def send_part(s):
        name, n = parts[s]
        if name == 'o':
            firsts['o'][n].start()
        else:
            firsts[(name, n // 2)][n % 2].start()

    load_lefts(*left_loads[0])
    load_rights(0)
    load_rights(1)
    for s in range(len(parts)):
        name, n = parts[s]
        if n == 0 or name == '2' and n % 2 == 0:
            every = d_heads.at[:, :4 * piece]
            pltpu.make_async_copy(every, every, load_sem.at[14]).wait()
            left_t[...] = every[...].T
            left_loads.pop(0)
            if left_loads:
                if left_loads[0][0] == 'o':
                    dmid_give.wait_recv()
                load_lefts(*left_loads[0])
        if s + 1 < len(parts) and parts[s + 1][0] != '2':
            if parts[s + 1][0] == '1' and parts[s + 1][1] % 2 == 0:
                dup_give[parts[s + 1][1] // 2].wait_recv()
            load_rights(s + 1)
        space = spaces[s % 2]
        if name != '2' or n < 2:
            pltpu.make_async_copy(space, space, load_sem.at[15 + s % 2]).wait()
        if s >= 1:
            stored(s - 1)
            send_part(s - 1)
        stage[s % 2] = dot_nn(left_t[...], space[...])
        targets = {'2': (away2_ref, mid2_ref, keep2_ref), '1': (away1_ref, mid1_ref, keep1_ref),
                   'o': (awayo_ref, mido_ref, keepo_ref)}[name]
        for row, ref in zip((0, 2 * piece, 3 * piece), targets):
            rows = slice(row, row + (2 * piece if row == 0 else piece))
            if name == 'o':
                for k in range(2):
                    pltpu.make_async_copy(stage.at[s % 2, rows, k * (half // 2):(k + 1) * (half // 2)], ref.at[2 * n + k],
                                          load_sem.at[17 + s % 2]).start()
            else:
                pltpu.make_async_copy(stage.at[s % 2, rows, :], ref.at[n // 2, :, n % 2 * half:(n % 2 + 1) * half],
                                      load_sem.at[17 + s % 2]).start()
    stored(len(parts) - 1)
    send_part(len(parts) - 1)

    for i in range(4):
        @pl.when(role != i)
        def _():
            pltpu.make_async_copy(dc_ref.at[:, :head_cols], dch.at[:blk, :], dc_recv.at[i]).wait()

    moves = {(0, 0): [(add_mid, ('2', 0))], (0, 1): [(add_mid, ('2', 1))], (0, 4): [(finish, ('2', 0))],
             (0, 6): [(add_mid, ('2', 2)), (finish, ('2', 1))], (1, 0): [(send_d_heads, 0)],
             (1, 2): [(finish, ('2', 2)), (add_mid, ('2', 3))], (1, 6): [(finish, ('2', 3))], (1, 7): [(add_mid, ('1', 0))]}
    steps = seq // BWD_ROWS
    for j in range(2):
        k_view, v_view = qkv_ref.at[:, (2 + j) * PAIR:(3 + j) * PAIR], qkv_ref.at[:, (4 + j) * PAIR:(5 + j) * PAIR]
        k_t[...] = k_view[...].T
        dk_acc[...] = jnp.zeros_like(dk_acc)
        dv_acc[...] = jnp.zeros_like(dv_acc)

        def block(i, _):
            for n in range(8):
                if (j, n) in moves:
                    @pl.when(i == min(n, steps - 1))
                    def _():
                        for move, what in moves[(j, n)]:
                            move(what)
            rows = span(i, BWD_ROWS)
            cols = slice(j * PAIR, (j + 1) * PAIR)
            d_heads[rows, cols] = backward_rows(
                qkv_ref[rows, cols], dch[rows, cols], lse_ref[2 * j:2 * j + 2, rows], k_view, v_view,
                k_t, p_cat, ds_cat, dk_acc, dv_acc)
            return 0

        lax.fori_loop(0, steps, block, 0)
        d_heads[:, head_cols + j * PAIR:head_cols + (j + 1) * PAIR] = (dk_acc[...] * SCALE).astype(BF16)
        d_heads[:, 2 * head_cols + j * PAIR:2 * head_cols + (j + 1) * PAIR] = dv_acc[...].astype(BF16)

    quarter = 2 * piece

    def quarter_loads(n):
        return [load(u_ref.at[:, span(index[n], quarter)], u_s.at[n % 2], 8 + n % 2),
                load(gqkv2_ref.at[span(index[n], quarter), :], g_s.at[n % 2], 10 + n % 2)]

    pending = quarter_loads(0)
    for i in range(4):
        @pl.when(role == i)
        def _():
            d_qkv[:, i * 3 * head_cols:(i + 1) * 3 * head_cols] = d_heads[i * blk:(i + 1) * blk, :]
    send_d_heads(1)
    targets = [qa.at[0], qa.at[1], qb.at[0], qb.at[1]]
    first_q = copies.make(qa, q1, to_a)
    for n in range(4):
        ahead = quarter_loads(n + 1) if n < 3 else []
        for copy in pending:
            copy.wait()
        targets[n][...] = dot_tn(u_s[n % 2], d_heads[...]) + g_s[n % 2]
        pending = ahead
        if n == 0:
            far('2')
            add_mid(('1', 1))
            finish(('1', 0))
            finish(('1', 1))
        if n == 2:
            first_q.start()

    add_mid(('1', 2))
    w_rows = w_s.shape[1]
    chunks = wqkv_ref.shape[0] // w_rows
    w_load = load(wqkv_ref.at[:w_rows, :], w_s.at[0], 12)
    for j in range(2):
        for i in range(4):
            @pl.when(role != i)
            def _():
                for t in range(3):
                    pltpu.make_async_copy(d_heads.at[:blk, :PAIR], d_qkv.at[:, :PAIR], dq_recv.at[(j * 4 + i) * 3 + t]).wait()
    for n in range(chunks):
        ahead = load(wqkv_ref.at[(n + 1) * w_rows:(n + 2) * w_rows, :], w_s.at[(n + 1) % 2], 12 + (n + 1) % 2) if n + 1 < chunks else None
        w_load.wait()
        d_1[:, n * w_rows:(n + 1) * w_rows] = dot_nt(d_qkv[...], w_s[n % 2]).astype(BF16)
        w_load = ahead

    count = min(128, blk)
    for n in range(blk // count):
        rows = slice(n * count, (n + 1) * count)
        d_1[rows, :] = through_norm(x_ref[rows, :].astype(F32) + emb_row(emb_ref, 0), d_1[rows, :].astype(F32), dmid_ref[rows, :])

    own_seq, part_rows = z // 2, blk // 2

    def dx_rows(role, h):
        return pl.ds(pl.multiple_of(role * blk + h * part_rows, part_rows), part_rows)

    def dx_copy(n, h, device):
        slot = [0, 1 + core, 3 + core][n]
        return pltpu.make_async_remote_copy(
            src_ref=d_1.at[h * part_rows:(h + 1) * part_rows, :], dst_ref=dx_ref.at[dx_rows(role, h), :],
            send_sem=x_send.at[n * 2 + h], recv_sem=x_recv.at[slot * 2 + h], device_id=device, device_id_type=MESH)

    dx_side = [dx_copy(0, h, partner) for h in range(2)]
    dx_next = [dx_copy(1, h, here.device(z=here.z_by[1], c=own_seq)) for h in range(2)]
    dx_cross = [dx_copy(2, h, here.device(z=far_q, c=own_seq)) for h in range(2)]
    dx_keep = pltpu.make_async_copy(d_1, dx_ref.at[span(role, blk), :], local_sem.at[8])

    def dx_pass(cc, h):
        rows = dx_rows(z % 2 * 2 + cc, h)
        return pltpu.make_async_remote_copy(
            src_ref=dx_ref.at[rows, :], dst_ref=dx_ref.at[rows, :], send_sem=x_send.at[6 + cc * 2 + h],
            recv_sem=x_recv.at[(5 + cc) * 2 + h], device_id=here.device(z=here.z_by[1]), device_id_type=MESH)

    def dx_start(h):
        dx_cross[h].start()
        dx_next[h].start()
        pl.when(no(owner))(dx_side[h].start)

    def dx_got(slot, h):
        rows = d_1.at[:part_rows, :]
        pltpu.make_async_copy(rows, dx_ref.at[:part_rows, :], x_recv.at[slot * 2 + h]).wait()

    def dx_forward(h):
        @pl.when(no(owner))
        def _():
            for cc in range(2):
                dx_got(3 + cc, h)
                dx_pass(cc, h).start()

    finish(('1', 2))
    dx_start(0)
    pl.when(owner)(dx_keep.start)
    add_mid(('1', 3))
    finish(('1', 3))
    add_mid('o')
    dx_forward(0)
    far('1')
    first_q.wait_recv()
    qb[0] += q1[1]
    second_q = copies.start(qb.at[0], q2, to_b)
    qb[1] += q1[0]
    total('2')
    gather_start('2', sum_2, g2_ref, 0)
    second_q.wait_recv()
    qb[1] += q2[...]
    plane_stays = jnp.logical_and(2 * (z % 2) + core == z, z // 2 == core)
    plane_q = pltpu.make_async_remote_copy(
        src_ref=qb.at[1], dst_ref=q3, send_sem=p_send.at[0], recv_sem=p_recv.at[0],
        device_id=here.device(z=2 * (z % 2) + core, c=z // 2), device_id_type=MESH)

    @pl.when(plane_stays)
    def _():
        q3[...] = qb[1]

    pl.when(no(plane_stays))(plane_q.start)
    finish('o')
    total('1')
    gather_start('1', sum_1, g1_ref, 1)
    dx_start(1)
    gather_second('2')
    gather_second('1')
    pl.when(no(plane_stays))(plane_q.wait_recv)
    give_q = copies.start(q3.at[span(1 - core, piece), :], q4.at[0], partner)
    gather_core('2')
    give_q.wait_recv()
    q4[1] = q4[0] + q3[span(core, piece), :]
    far('o')
    for t, (name, out) in enumerate((('q', gq_ref), ('k', gk_ref), ('v', gv_ref))):
        gather_start(name, q4.at[1, :, t * head_cols:(t + 1) * head_cols], out, 3 + t)
    gather_core('1')
    for name in 'qkv':
        gather_second(name)
    for name in 'qkv':
        gather_core(name)
    dx_forward(1)
    total('o')
    gather_start('o', sum_o, go_ref, 2)
    gather_second('o')
    gather_core('o')

    @pl.when(owner)
    def _():
        for h in range(2):
            for slot in (0, 1, 2):
                dx_got(slot, h)
        dx_keep.wait()

    @pl.when(no(owner))
    def _():
        for h in range(2):
            dx_side[h].wait_send()
            for cc in range(2):
                dx_got(5 + cc, h)
                dx_pass(cc, h).wait_send()

    for g in gathers.values():
        for copy in g['c']:
            copy.wait_recv()
    for copy in waits:
        copy.wait()
    for copy in copies.sent:
        copy.wait_send()
    for h in range(2):
        dx_cross[h].wait_send()
        dx_next[h].wait_send()
    pl.when(no(plane_stays))(plane_q.wait_send)
    for i in range(4):
        @pl.when(role != i)
        def _():
            dc_copy(i).wait_send()
            for j in range(2):
                for t in range(3):
                    dq_copy(j, i, t).wait_send()
        for w in '21o':
            pl.when((z + i) % 2 == 1)(near_copy(w, i).wait_send)
    for w in '21o':
        far_copy(w).wait_send()


def last_call(qkv, d_c, lse, d_mid, x, emb, w_qkv, u_seq, g_qkv, w2_sides, w1_sides, wo_sides):
    seq, d_model = u_seq.shape
    blk, piece = seq // 4, d_model // 8
    n1, no = w1_sides[4].shape[1] // 4, wo_sides[3].shape[1] // 4
    assert n1 == d_model == 2 * 2 * BWD_ROWS and no * 2 == 2 * BWD_ROWS
    heads3 = qkv.shape[1]
    anywhere = pl.BlockSpec(memory_space=pl.ANY)
    in_vmem = pl.BlockSpec(memory_space=pltpu.VMEM)
    copies = 5 + 18 + 9 + 6 * 7 + 3
    dma = pltpu.SemaphoreType.DMA
    w_rows = min(128, d_model)
    return pl.pallas_call(
        last_kernel,
        in_specs=[in_vmem] * 6 + [anywhere] * 25,
        out_specs=[anywhere] * 18,
        out_shape=[
            jax.ShapeDtypeStruct((seq, d_model), BF16),
            jax.ShapeDtypeStruct((d_model, n1), F32),
            jax.ShapeDtypeStruct((8 * piece, n1), F32),
            jax.ShapeDtypeStruct((d_model, no), F32),
        ] + [jax.ShapeDtypeStruct((d_model, heads3 // 3), F32)] * 3
        + [jax.ShapeDtypeStruct((4, k * piece, n), F32) for n in (n1, n1, no) for k in (2, 1, 1)]
        + [jax.ShapeDtypeStruct((blk, n), BF16) for n in (4 * n1, d_model)],
        scratch_shapes=[
            pltpu.VMEM((seq, heads3 // 3), BF16),
            pltpu.VMEM((PAIR, seq), BF16),
            pltpu.VMEM((seq, PAIR), F32),
            pltpu.VMEM((seq, PAIR), F32),
            pltpu.VMEM((seq, 2 * BWD_ROWS), BF16),
            pltpu.VMEM((seq, 2 * BWD_ROWS), BF16),
            pltpu.VMEM((seq, heads3), BF16),
            pltpu.VMEM((blk, 4 * heads3), BF16),
            pltpu.VMEM((8, 2 * piece, n1), F32),
            pltpu.VMEM((4, 2 * piece, no), F32),
            pltpu.VMEM((8, piece, n1), F32),
            pltpu.VMEM((4, piece, no), F32),
            pltpu.VMEM((2, piece, n1), F32),
            pltpu.VMEM((2, 4, piece, no), F32),
            pltpu.VMEM((2, 3, piece, n1), F32),
            pltpu.VMEM((3, piece, no), F32),
            pltpu.VMEM((piece, n1), F32),
            pltpu.VMEM((piece, n1), F32),
            pltpu.VMEM((piece, no), F32),
            pltpu.VMEM((2, 2 * piece, heads3), F32),
            pltpu.VMEM((2, 2 * piece, heads3), F32),
            pltpu.VMEM((2, 2 * piece, heads3), F32),
            pltpu.VMEM((2 * piece, heads3), F32),
            pltpu.VMEM((2 * piece, heads3), F32),
            pltpu.VMEM((2, piece, heads3), F32),
            pltpu.VMEM((blk, d_model), BF16),
            pltpu.VMEM((2, w_rows, 4 * heads3), BF16),
            pltpu.VMEM((2, seq, 2 * piece), BF16),
            pltpu.VMEM((2, 2 * piece, heads3), F32),
            pltpu.VMEM((4 * piece, seq), BF16),
            pltpu.VMEM((2, 4 * piece, 2 * BWD_ROWS), F32),
            dma((9,)), dma((19,)), dma((copies,)), dma((copies,)),
            dma((4,)), dma((4,)), dma((24,)), dma((24,)), dma((9,)), dma((9,)), dma((10,)), dma((14,)), dma((1,)), dma((1,)),
        ],
        compiler_params=pltpu.CompilerParams(vmem_limit_bytes=63 << 20, collective_id=1, has_side_effects=True),
        cost_estimate=pl.CostEstimate(
            flops=160 * seq * seq * PAIR, bytes_accessed=128 * seq * d_model, transcendentals=seq * seq * 4),
        name="last",
    )(qkv, d_c, lse, d_mid, x, emb, w_qkv, u_seq, g_qkv, *w2_sides, *w1_sides, *wo_sides)[:7]


def solution(mesh):
    spec_col = P(None, 'model')
    spec_row = P('model', None)
    spec_act = P('data', None, None)
    spec_rep = P(None, None)

    def device_step(x_in, cot_out, step_emb, w_q, w_k, w_v, w_o, w_1, w_2):
        d_model = x_in.shape[2]
        c_1, lse_1, x_seq, cot, wo, w1, w2, w_qkv, x_1, h_1, m_1, up_1, act_1, x_2 = first_call(
            x_in[0], cot_out[0], step_emb, w_q, w_k, w_v, w_o, w_1, w_2)
        wo, w2 = wo.reshape(-1, d_model), w2.reshape(-1, d_model)

        c_2, lse_2, u_2_seq, qkv_2, u_1_seq, qkv_1 = forward_call(x_2, step_emb, x_seq, w_qkv)
        _, m_2, act_2, d_up_2, d_mid_2, d_c = hidden_call(True, True, wo, w1, w2, context=c_2, x=x_2, emb=step_emb, d_next=cot)
        shared = (act_2, act_1, cot, m_2, m_1, d_up_2, d_mid_2, c_2, c_1)
        d_2, d_2_other, g_qkv_2, *others = backward_call(
            qkv_2, d_c, lse_2, d_mid_2, x_2, step_emb, w_qkv, u_2_seq, shared)
        act_2o, act_1o, cot_o, m_2o, m_1o, d_up_2o, d_mid_2o, c_2o, c_1o = others
        d_up_1, d_mid_1, d_c = hidden_call(False, True, wo, w1, w2, h=h_1, up=up_1, d_next=d_2)
        w2_parts = (act_2, act_2o, act_1, act_1o, cot, cot_o, d_2, d_2_other)
        w1_sides = (m_2, m_2o, m_1, m_1o, d_up_2, d_up_2o, d_up_1)
        wo_sides = (d_mid_2, d_mid_2o, d_mid_1, c_2, c_2o, c_1, c_1o)
        d_x, g_w1, g_w2, g_wo, g_q, g_k, g_v = last_call(
            qkv_1, d_c, lse_1, d_mid_1, x_1, step_emb, w_qkv, u_1_seq, g_qkv_2, w2_parts, w1_sides, wo_sides)
        return g_q, g_k, g_v, g_wo.T, g_w1, g_w2, d_x[None]

    return jax.shard_map(device_step, mesh=mesh,
                         in_specs=(spec_act, spec_act, spec_rep, spec_col, spec_col, spec_col, spec_row, spec_col, spec_row),
                         out_specs=(spec_col, spec_col, spec_col, spec_row, spec_col, spec_row, spec_act),
                         check_vma=False)
```

```python
import functools
import math

import jax
import jax.numpy as jnp
from jax import lax
from jax.experimental import pallas as pl
from jax.experimental.pallas import tpu as pltpu
from jax.sharding import PartitionSpec as P


HEAD_DIM = 64
EPS_NORM = 1e-6
SCALE = HEAD_DIM ** -0.5
EXP2_SCALE = SCALE * math.log2(math.e)
PAIR = 2 * HEAD_DIM
FWD_ROWS = 512
BWD_ROWS = 256
KEYS = 256
HIDDEN = 1024
HIDDEN_FIRST = 512
INTERPRET = False
AXES = ('model', 'data')
BF16 = jnp.bfloat16
F32 = jnp.float32
MESH = pl.DeviceIdType.MESH

def rms_norm(values):
    return values * lax.rsqrt(jnp.mean(values * values, axis=-1, keepdims=True) + EPS_NORM)


def dot_nt(a, b):
    return lax.dot_general(a, b, (((1,), (1,)), ((), ())), preferred_element_type=F32)


def dot_nn(a, b):
    return lax.dot_general(a, b, (((1,), (0,)), ((), ())), preferred_element_type=F32)


def dot_tn(a, b):
    return lax.dot_general(a, b, (((0,), (0,)), ((), ())), preferred_element_type=F32)


def attend_rows(q, k_ref, v_t, e_refs):
    count = k_ref.shape[0] // KEYS
    lane = lax.broadcasted_iota(jnp.int32, q.shape, 1)
    q_heads = [jnp.where(lane // HEAD_DIM == head, q, jnp.zeros_like(q)) for head in range(2)]
    tops, run, total, outs, sums = [[], []], [None, None], [None, None], [], []
    for j in range(count):
        keys = slice(j * KEYS, (j + 1) * KEYS)
        for head in range(2):
            scores = dot_nt(k_ref[keys, :], q_heads[head])
            top = jnp.max(scores, axis=0, keepdims=True) * EXP2_SCALE
            if j:
                top = jnp.maximum(top, run[head])
            weights = jnp.exp2(scores * EXP2_SCALE - top)
            part = jnp.sum(weights, axis=0, keepdims=True)
            total[head] = total[head] * jnp.exp2(run[head] - top) + part if j else part
            run[head] = top
            tops[head].append(top)
            e_refs[head][keys, :] = weights
    for head in range(2):
        inverse = 1.0 / total[head]
        out = None
        for j in range(count):
            keys = slice(j * KEYS, (j + 1) * KEYS)
            factor = inverse * jnp.exp2(tops[head][j] - run[head])
            probs = (e_refs[head][keys, :] * factor).astype(BF16)
            part = dot_nn(v_t[head * HEAD_DIM:(head + 1) * HEAD_DIM, keys], probs)
            out = out + part if j else part
        sums.append(run[head] + jnp.log2(total[head]))
        outs.append(out)
    return outs, sums


class Place:
    def __init__(self):
        self.z = lax.axis_index('model')
        d = lax.axis_index('data')
        self.y, self.x, self.c = d // 4, d // 2 % 2, d % 2
        z = self.z
        self.z_by = {1: z + 1 - 2 * (z % 2), 2: (z + 2) % 4, 3: 3 - z}
        x, y, c = self.x, self.y, self.c
        self.xa, self.ya = x + (1 - c) * (1 - 2 * x), y + c * (1 - 2 * y)
        self.xb, self.yb = x + c * (1 - 2 * x), y + (1 - c) * (1 - 2 * y)
        self.role = z % 2 * 2 + c
        self.owner = c == z // 2

    def piece(self, y, x, c=None):
        return y * 4 + x * 2 + (self.c if c is None else c)

    def device(self, z=None, y=None, x=None, c=None):
        z, y, x, c = (own if given is None else given for given, own in zip((z, y, x, c), (self.z, self.y, self.x, self.c)))
        return {'model': z, 'data': y * 4 + x * 2 + c}

    def peers(self):
        column = [self.device(z=z, c=c) for z in (self.z, *self.z_by.values()) for c in (self.c, 1 - self.c)][1:]
        return column + [self.device(x=1 - self.x), self.device(y=1 - self.y)]

    def meet(self):
        barrier = pltpu.get_barrier_semaphore()
        peers = self.peers()
        for peer in peers:
            pl.semaphore_signal(barrier, inc=1, device_id=peer, device_id_type=MESH)
        pl.semaphore_wait(barrier, len(peers))


class Copies:
    def __init__(self, send_sem, recv_sem):
        self.send_sem, self.recv_sem, self.used, self.sent = send_sem, recv_sem, 0, []

    def make(self, src, dst, device):
        n, self.used = self.used, self.used + 1
        copy = pltpu.make_async_remote_copy(
            src_ref=src, dst_ref=dst, send_sem=self.send_sem.at[n], recv_sem=self.recv_sem.at[n],
            device_id=device, device_id_type=MESH)
        self.sent.append(copy)
        return copy

    def start(self, src, dst, device):
        copy = self.make(src, dst, device)
        copy.start()
        return copy


def first_kernel(x_ref, cot_ref, emb_ref, wq_ref, wk_ref, wv_ref, wo_ref, w1_ref, w2_ref,
                 c1_ref, lse_ref, xs_ref, cot_loc_ref, full_o, full_1, full_2, full_qkv,
                 x1_ref, h_ref, m_ref, up_ref, act_ref, x2_ref,
                 qkv_s, vt_s, e_a, e_b, c_buf, lse_s, cot_s, x1_s, c1_s, h_s, m_s, wo_s, w1_s, w2_s, up_s, act_s, acc,
                 local_sem, send_sem, recv_sem, c_send, c_recv, one_send, one_recv, load_sem, out_sem, z_send, z_recv):
    seq, d_model = x_ref.shape
    blk = seq // 4
    head_cols = wq_ref.shape[1]
    here = Place()
    z, core, role, owner = here.z, here.c, here.role, here.owner
    here.meet()
    copies = Copies(send_sem, recv_sem)

    def span(index, count):
        return pl.ds(pl.multiple_of(index * count, count), count)

    ff_cols, out_rows, piece = w1_ref.shape[1], wo_ref.shape[0] // 8, d_model // 8
    hidden = w2_ref.shape[0] // 8

    def block_qkv(zz, e):
        return full_qkv.at[span(e, piece), span(zz, 3 * head_cols)]

    units = {
        'o': lambda zz, e: full_o.at[zz, span(e, out_rows), :],
        '1': lambda zz, e: full_1.at[span(e, piece), span(zz, ff_cols)],
        '2': lambda zz, e: full_2.at[zz, span(e, hidden), :],
        'qkv': block_qkv,
    }

    def own_parts(name, e):
        if name == 'o':
            return [(wo_ref.at[span(e, out_rows), :], units[name](z, e))]
        if name == '1':
            return [(w1_ref.at[span(e, piece), :], units[name](z, e))]
        if name == '2':
            return [(w2_ref.at[span(e, hidden), :], units[name](z, e))]
        return [(ref.at[span(e, piece), :],
                 full_qkv.at[span(e, piece), pl.ds(pl.multiple_of((z * 3 + t) * head_cols, head_cols), head_cols)])
                for t, ref in enumerate((wq_ref, wk_ref, wv_ref))]

    mine = here.piece(here.y, here.x)
    by_a = here.piece(here.ya, here.xa)
    by_b = here.piece(here.yb, here.xb)
    by_ab = here.piece(1 - here.y, 1 - here.x)
    to_a, to_b = here.device(y=here.ya, x=here.xa), here.device(y=here.yb, x=here.xb)
    partner = here.device(c=1 - core)
    names = ('o', '1', '2', 'qkv')
    right, left = here.device(z=(z + 1) % 4), here.device(z=(z + 3) % 4)

    def piece_copy(name, src, dst, n, zz, device):
        return pltpu.make_async_remote_copy(
            src_ref=src, dst_ref=dst, send_sem=z_send.at[n], recv_sem=z_recv.at[names.index(name) * 4 + zz],
            device_id=device, device_id_type=MESH)

    owns, passes, stage_a, stage_b1, stage_b2, stage_c = {}, {}, {}, {}, {}, {}
    used = 0
    for name in names:
        parts = own_parts(name, mine)
        owns[name] = []
        for device, there in ((right, z < 3), (left, z > 0)):
            owns[name].append((there, [piece_copy(name, src, dst, used + i, z, device) for i, (src, dst) in enumerate(parts)]))
            used += len(parts)
        passes[name] = []
        for zz in range(4):
            block = units[name](zz, mine)
            passes[name].append([piece_copy(name, block, block, used, zz, device) for device in (right, left)])
            used += 1
        make = lambda zz, e, device: copies.make(units[name](zz, e), units[name](zz, e), device)
        stage_a[name] = [make(zz, mine, to_a) for zz in range(4)]
        stage_b1[name] = [make(zz, mine, to_b) for zz in range(4)]
        stage_b2[name] = [make(zz, by_a, to_b) for zz in range(4)]
        stage_c[name] = [[make(zz, e, partner) for e in (mine, by_a, by_b, by_ab)] for zz in range(4)]

    def begin_z(name):
        for there, group in owns[name]:
            @pl.when(there)
            def _():
                for copy in group:
                    copy.start()

    def arrived(name, distance):
        for zz in range(4):
            @pl.when(jnp.logical_or(z == zz + distance, z == zz - distance))
            def _():
                block = units[name](zz, mine)
                pltpu.make_async_copy(block, block, z_recv.at[names.index(name) * 4 + zz]).wait()
                if zz + distance < 3:
                    pl.when(z == zz + distance)(passes[name][zz][0].start)
                if zz - distance > 0:
                    pl.when(z == zz - distance)(passes[name][zz][1].start)
                stage_a[name][zz].start()
                stage_b1[name][zz].start()

    def others(act):
        for zz in range(4):
            @pl.when(z != zz)
            def _():
                act(zz)

    def forward_a(name):
        def act(zz):
            stage_a[name][zz].wait_recv()
            stage_b2[name][zz].start()
        others(act)

    def forward_b(name):
        def act(zz):
            stage_b1[name][zz].wait_recv()
            stage_b2[name][zz].wait_recv()
            for copy in stage_c[name][zz]:
                copy.start()
        others(act)

    def gathered(name):
        def act(zz):
            for copy in stage_c[name][zz]:
                copy.wait_recv()
        others(act)

    begin_z('o')
    begin_z('1')

    locals_ = []

    def copy_local(src, dst):
        copy = pltpu.make_async_copy(src, dst, local_sem.at[len(locals_)])
        locals_.append(copy)
        copy.start()

    copy_local(w1_ref, full_1.at[:, span(z, ff_cols)])
    copy_local(w2_ref, full_2.at[z])
    copy_local(wo_ref, full_o.at[z])
    for t, ref in enumerate((wq_ref, wk_ref, wv_ref)):
        copy_local(ref, full_qkv.at[:, pl.ds(pl.multiple_of((z * 3 + t) * head_cols, head_cols), head_cols)])
    other_role = z % 2 * 2 + 1 - core
    give_x = pltpu.make_async_remote_copy(
        src_ref=x_ref, dst_ref=xs_ref, send_sem=one_send.at[0], recv_sem=one_recv.at[0], device_id=partner, device_id_type=MESH)
    give_cot = pltpu.make_async_remote_copy(
        src_ref=cot_ref.at[span(other_role, blk), :], dst_ref=cot_loc_ref, send_sem=one_send.at[1], recv_sem=one_recv.at[1],
        device_id=partner, device_id_type=MESH)
    keep_x = pltpu.make_async_copy(x_ref, xs_ref, local_sem.at[6])
    take_cot = pltpu.make_async_copy(cot_ref.at[span(role, blk), :], cot_s, local_sem.at[7])
    keep_cot = pltpu.make_async_copy(cot_s, cot_loc_ref, local_sem.at[8])

    @pl.when(owner)
    def _():
        give_x.start()
        give_cot.start()
        keep_x.start()
        take_cot.start()

    def project(i):
        rows = span(i, blk)
        unit = unit_rows(x_ref[rows, :], emb_row(emb_ref, 0))
        for t, ref in enumerate((wq_ref, wk_ref, wv_ref)):
            qkv_s[rows, t * head_cols:(t + 1) * head_cols] = dot_nn(unit, ref[...]).astype(BF16)

    for i in range(4):
        if i == 2:
            arrived('o', 1)
        project(i)

    def context_copy(j, i):
        src = c_buf.at[j, span(i, blk), :]
        dst = c1_ref.at[:, pl.ds(pl.multiple_of((z * 2 + j) * PAIR, PAIR), PAIR)]
        target_z, target_c = 2 * core + i // 2, i % 2
        remote = pltpu.make_async_remote_copy(
            src_ref=src, dst_ref=dst, send_sem=c_send.at[j * 4 + i], recv_sem=c_recv.at[j * 4 + z],
            device_id=here.device(z=target_z, c=target_c), device_id_type=MESH)
        local = pltpu.make_async_copy(src, dst, c_recv.at[j * 4 + z])
        return remote, local, jnp.logical_and(target_z == z, target_c == core)

    def send_context(j, i):
        remote, local, to_self = context_copy(j, i)
        pl.when(to_self)(local.start)
        pl.when(jnp.logical_not(to_self))(remote.start)

    moves = {(0, 0): [(arrived, 'o', 2)], (0, 1): [(arrived, '1', 1), (begin_z, '2'), (arrived, 'o', 3)],
             (0, 3): [(arrived, '1', 2)], (1, 1): [(arrived, '2', 1), (begin_z, 'qkv')],
             (1, 2): [(arrived, '1', 3), (forward_a, 'o')], (1, 3): [(arrived, '2', 2), (forward_b, 'o')]}
    for j in range(2):
        vt_s[...] = qkv_s[:, (4 + j) * PAIR:(5 + j) * PAIR].T
        k_view = qkv_s.at[:, (2 + j) * PAIR:(3 + j) * PAIR]
        for i in range(4):
            if i or j:
                send_context(j if i else 0, i - 1 if i else 3)
            for move, *what in moves.get((j, i), ()):
                move(*what)
            rows = slice(i * blk, (i + 1) * blk)
            outs, sums = attend_rows(qkv_s[rows, j * PAIR:(j + 1) * PAIR], k_view, vt_s, (e_a, e_b))
            c_buf[j, rows, :] = jnp.concatenate(outs, axis=0).T.astype(BF16)
            for head in range(2):
                lse_s[2 * j + head:2 * j + head + 1, rows] = sums[head]

    @pl.when(owner)
    def _():
        take_cot.wait()
        keep_cot.start()

    forward_a('1')
    arrived('qkv', 1)
    send_context(1, 3)
    give_lse = pltpu.make_async_remote_copy(
        src_ref=lse_s, dst_ref=lse_ref, send_sem=one_send.at[2], recv_sem=one_recv.at[2],
        device_id=here.device(z=2 * core + z // 2, c=z % 2), device_id_type=MESH)
    keep_lse = pltpu.make_async_copy(lse_s, lse_ref, local_sem.at[9])
    lse_stays = jnp.logical_and(2 * core + z // 2 == z, z % 2 == core)
    pl.when(lse_stays)(keep_lse.start)
    pl.when(jnp.logical_not(lse_stays))(give_lse.start)
    arrived('2', 3)
    forward_b('1')
    arrived('qkv', 2)
    arrived('qkv', 3)

    @pl.when(owner)
    def _():
        keep_x.wait()

    @pl.when(jnp.logical_not(owner))
    def _():
        give_x.wait_recv()

    for j in range(2):
        for zz in range(4):
            pltpu.make_async_copy(c_buf.at[j, :blk, :], c1_ref.at[:, :PAIR], c_recv.at[j * 4 + zz]).wait()

    def load(src, dst, n):
        copy = pltpu.make_async_copy(src, dst, load_sem.at[n])
        copy.start()
        return copy

    loads = [load(xs_ref.at[span(role, blk), :], x1_s, 0), load(c1_ref, c1_s, 1)]
    for copy in locals_:
        copy.wait()
    gathered('o')
    loads += [load(full_o.at[zz], wo_s.at[zz * wo_ref.shape[0]:(zz + 1) * wo_ref.shape[0], :], 2 + zz) for zz in range(4)]
    for copy in loads:
        copy.wait()
    h = (x1_s[...].astype(F32) + emb_row(emb_ref, 0) + dot_nn(c1_s[...], wo_s[...])).astype(BF16)
    m = rms_rows(h.astype(F32)).astype(BF16)
    h_s[...], m_s[...] = h, m
    gathered('1')
    tile = w1_s.shape[2]
    steps = full_1.shape[1] // tile
    per_plane = full_2.shape[1] // tile

    def w1_load(n):
        return pltpu.make_async_copy(full_1.at[:, span(n, tile)], w1_s.at[n % 2], load_sem.at[6 + n % 2])

    def w2_load(n):
        return pltpu.make_async_copy(full_2.at[n // per_plane, span(n % per_plane, tile), :], w2_s.at[n % 2], load_sem.at[8 + n % 2])

    def up_store(n):
        return pltpu.make_async_copy(up_s.at[n % 2], up_ref.at[:, span(n, tile)], out_sem.at[n % 2])

    w1_load(0).start()

    def up_part(n, _):
        @pl.when(n + 1 < steps)
        def _():
            w1_load(n + 1).start()

        @pl.when(n == steps // 8)
        def _():
            forward_a('2')

        @pl.when(n == steps * 5 // 8)
        def _():
            forward_a('qkv')

        w1_load(n).wait()

        @pl.when(n >= 2)
        def _():
            up_store(n - 2).wait()

        up = dot_nn(m_s[...], w1_s[n % 2]).astype(BF16)
        up_s[n % 2] = up
        factor = gelu_parts(up.astype(F32))[0]
        act_s[:, span(n, tile)] = (up.astype(F32) * factor).astype(BF16)
        up_store(n).start()
        return 0

    lax.fori_loop(0, steps, up_part, 0)
    forward_b('2')
    outs = [pltpu.make_async_copy(src, dst, out_sem.at[2 + n]) for n, (src, dst) in enumerate(
        ((x1_s, x1_ref), (h_s, h_ref), (m_s, m_ref), (act_s, act_ref)))]
    for copy in outs:
        copy.start()
    gathered('2')
    w2_load(0).start()
    acc[...] = jnp.zeros_like(acc)

    def down_part(n, _):
        @pl.when(n + 1 < steps)
        def _():
            w2_load(n + 1).start()

        @pl.when(n == steps // 2)
        def _():
            forward_b('qkv')

        w2_load(n).wait()
        acc[...] += dot_nn(act_s[:, span(n, tile)], w2_s[n % 2])
        return 0

    lax.fori_loop(0, steps, down_part, 0)
    c1_s[...] = (h_s[...].astype(F32) + acc[...]).astype(BF16)
    out_x2 = pltpu.make_async_copy(c1_s, x2_ref, out_sem.at[6])
    for j in range(2):
        for i in range(4):
            remote, _, to_self = context_copy(j, i)
            pl.when(jnp.logical_not(to_self))(remote.wait_send)
    pl.when(lse_stays)(keep_lse.wait)

    @pl.when(jnp.logical_not(lse_stays))
    def _():
        give_lse.wait_send()
        give_lse.wait_recv()

    out_x2.start()

    @pl.when(owner)
    def _():
        give_x.wait_send()
        give_cot.wait_send()
        keep_cot.wait()

    @pl.when(jnp.logical_not(owner))
    def _():
        give_cot.wait_recv()

    for n in range(steps - 2, steps):
        up_store(n).wait()
    for copy in outs:
        copy.wait()
    out_x2.wait()
    gathered('qkv')
    for name in names:
        for there, group in owns[name]:
            @pl.when(there)
            def _():
                for copy in group:
                    copy.wait_send()

        def sent(zz):
            for copy in (stage_a[name][zz], stage_b1[name][zz], stage_b2[name][zz], *stage_c[name][zz]):
                copy.wait_send()
        others(sent)
        for zz in range(4):
            pl.when(jnp.logical_and(z > zz, z < 3))(passes[name][zz][0].wait_send)
            pl.when(jnp.logical_and(z < zz, z > 0))(passes[name][zz][1].wait_send)


def first_call(x, cot, emb, w_q, w_k, w_v, w_o, w_1, w_2):
    seq, d_model = x.shape
    head_cols, ff_cols, blk = w_q.shape[1], w_1.shape[1], seq // 4
    anywhere = pl.BlockSpec(memory_space=pl.ANY)
    in_vmem = pl.BlockSpec(memory_space=pltpu.VMEM)
    copies = 4 * (3 * 4 + 16)
    hidden, tile = 4 * ff_cols, min(HIDDEN_FIRST, ff_cols)
    shape = jax.ShapeDtypeStruct
    dma = pltpu.SemaphoreType.DMA
    return pl.pallas_call(
        first_kernel,
        in_specs=[in_vmem, anywhere] + [in_vmem] * 7,
        out_specs=[anywhere] * 14,
        out_shape=[
            shape((blk, d_model), BF16),
            shape((4, seq), F32),
            shape((seq, d_model), BF16),
            shape((blk, d_model), BF16),
            shape((4, *w_o.shape), BF16),
            shape((d_model, hidden), BF16),
            shape((4, *w_2.shape), BF16),
            shape((d_model, 12 * head_cols), BF16),
            shape((blk, d_model), BF16),
            shape((blk, d_model), BF16),
            shape((blk, d_model), BF16),
            shape((blk, hidden), BF16),
            shape((blk, hidden), BF16),
            shape((blk, d_model), BF16),
        ],
        scratch_shapes=[
            pltpu.VMEM((seq, 3 * head_cols), BF16),
            pltpu.VMEM((PAIR, seq), BF16),
            pltpu.VMEM((seq, blk), F32),
            pltpu.VMEM((seq, blk), F32),
            pltpu.VMEM((2, seq, PAIR), BF16),
            pltpu.VMEM((4, seq), F32),
            pltpu.VMEM((blk, d_model), BF16),
            pltpu.VMEM((blk, d_model), BF16),
            pltpu.VMEM((blk, d_model), BF16),
            pltpu.VMEM((blk, d_model), BF16),
            pltpu.VMEM((blk, d_model), BF16),
            pltpu.VMEM((d_model, d_model), BF16),
            pltpu.VMEM((2, d_model, tile), BF16),
            pltpu.VMEM((2, tile, d_model), BF16),
            pltpu.VMEM((2, blk, tile), BF16),
            pltpu.VMEM((blk, hidden), BF16),
            pltpu.VMEM((blk, d_model), F32),
            dma((10,)), dma((copies,)), dma((copies,)), dma((8,)), dma((8,)), dma((3,)), dma((3,)), dma((10,)), dma((7,)), dma((28,)), dma((16,)),
        ],
        compiler_params=pltpu.CompilerParams(vmem_limit_bytes=60 << 20, collective_id=0, has_side_effects=True),
        cost_estimate=pl.CostEstimate(
            flops=64 * seq * seq * PAIR, bytes_accessed=64 * seq * d_model, transcendentals=seq * seq * 4),
        name="first",
    )(x, cot, emb, w_q, w_k, w_v, w_o, w_1, w_2)


def emb_row(emb_ref, row):
    return emb_ref[...].astype(F32)[row:row + 1, :]


def unit_rows(values, emb):
    values = values.astype(F32) + emb
    return (values * lax.rsqrt(jnp.mean(values * values, axis=-1, keepdims=True) + EPS_NORM)).astype(BF16)


def forward_kernel(x_ref, emb_ref, xs1_ref, wqkv_ref,
                   c_ref, lse_ref, u2_ref, qkv2_ref, u1_ref, qkv1_ref,
                   w_s, blocks, u_s, qkv_s, x1_s, u1_s, qkv1_s, v_t, e_a, e_b, c_buf, lse_s,
                   local_sem, first_sem, out_sem, x_send, x_recv, c_send, c_recv):
    seq = xs1_ref.shape[0]
    blk = seq // 4
    head_cols = 2 * PAIR
    here = Place()
    z, core, role = here.z, here.c, here.role

    def span(index, count):
        return pl.ds(pl.multiple_of(index * count, count), count)

    w_load = pltpu.make_async_copy(wqkv_ref.at[:, span(role, 3 * head_cols)], w_s, local_sem.at[0])
    w_load.start()
    x1_load = [pltpu.make_async_copy(xs1_ref.at[i * blk:(i + 1) * blk, :], x1_s.at[i % 2], first_sem.at[i % 2]) for i in range(4)]
    x1_load[0].start()
    here.meet()
    partner, across = here.device(c=1 - core), here.device(z=here.z_by[1])
    role_side, role_over = z % 2 * 2 + 1 - core, (1 - z % 2) * 2 + core
    role_last = (1 - z % 2) * 2 + 1 - core

    def x_copy(n, src, slot, device):
        return pltpu.make_async_remote_copy(
            src_ref=src, dst_ref=blocks.at[slot], send_sem=x_send.at[n], recv_sem=x_recv.at[n],
            device_id=device, device_id_type=MESH)

    over, side = x_copy(0, x_ref, 0, across), x_copy(1, x_ref, 1, partner)
    last = x_copy(2, blocks.at[0], 2, partner)
    over.start()
    side.start()

    def project(src, at_role):
        rows = span(at_role, blk)
        unit = unit_rows(src, emb_row(emb_ref, 1))
        u_s[rows, :] = unit
        qkv_s[rows, :] = dot_nn(unit, w_s[...]).astype(BF16)

    w_load.wait()
    project(x_ref[...], role)
    side.wait_recv()
    project(blocks[1], role_side)

    stores = []
    for i in range(4):
        if i < 3:
            x1_load[i + 1].start()
        x1_load[i].wait()
        if i >= 2:
            for copy in stores[i - 2]:
                copy.wait()
        unit = unit_rows(x1_s[i % 2], emb_row(emb_ref, 0))
        u1_s[i % 2] = unit
        qkv1_s[i % 2] = dot_nn(unit, w_s[...]).astype(BF16)
        stores.append([pltpu.make_async_copy(u1_s.at[i % 2], u1_ref.at[i * blk:(i + 1) * blk, :], out_sem.at[i % 2]),
                       pltpu.make_async_copy(qkv1_s.at[i % 2], qkv1_ref.at[i * blk:(i + 1) * blk, :], out_sem.at[2 + i % 2])])
        for copy in stores[i]:
            copy.start()

    over.wait_recv()
    last.start()
    project(blocks[0], role_over)
    last.wait_recv()
    project(blocks[2], role_last)
    keep_u = pltpu.make_async_copy(u_s, u2_ref, local_sem.at[1])
    keep_qkv = pltpu.make_async_copy(qkv_s, qkv2_ref, local_sem.at[2])
    keep_u.start()
    keep_qkv.start()

    member = [here.device(z=z // 2 * 2 + i // 2, c=i % 2) for i in range(4)]

    def c_copy(j, i):
        src = c_buf.at[j, i * blk:(i + 1) * blk, :]
        dst = c_ref.at[:, pl.ds(pl.multiple_of((role * 2 + j) * PAIR, PAIR), PAIR)]
        remote = pltpu.make_async_remote_copy(
            src_ref=src, dst_ref=dst, send_sem=c_send.at[j * 4 + i], recv_sem=c_recv.at[j * 4 + role],
            device_id=member[i], device_id_type=MESH)
        return remote, pltpu.make_async_copy(src, dst, c_recv.at[j * 4 + role])

    def send_context(j, i):
        remote, local = c_copy(j, i)
        pl.when(role == i)(local.start)
        pl.when(role != i)(remote.start)

    for j in range(2):
        v_t[...] = qkv_s[:, (4 + j) * PAIR:(5 + j) * PAIR].T
        k_view = qkv_s.at[:, (2 + j) * PAIR:(3 + j) * PAIR]
        for i in range(4):
            if i or j:
                send_context(j if i else 0, i - 1 if i else 3)
            rows = slice(i * blk, (i + 1) * blk)
            outs, sums = attend_rows(qkv_s[rows, j * PAIR:(j + 1) * PAIR], k_view, v_t, (e_a, e_b))
            c_buf[j, rows, :] = jnp.concatenate(outs, axis=0).T.astype(BF16)
            for head in range(2):
                lse_s[2 * j + head:2 * j + head + 1, rows] = sums[head]
    lse_ref[...] = lse_s[...]
    send_context(1, 3)
    for j in range(2):
        for i in range(4):
            pltpu.make_async_copy(c_buf.at[j, :blk, :], c_ref.at[:, :PAIR], c_recv.at[j * 4 + i]).wait()
            pl.when(role != i)(c_copy(j, i)[0].wait_send)
    for copy in (over, side, last):
        copy.wait_send()
    for group in stores[2:]:
        for copy in group:
            copy.wait()
    keep_u.wait()
    keep_qkv.wait()


def forward_call(x, emb, xs_1, w_qkv):
    blk, d_model = x.shape
    seq, head_cols = 4 * blk, 2 * PAIR
    anywhere = pl.BlockSpec(memory_space=pl.ANY)
    in_vmem = pl.BlockSpec(memory_space=pltpu.VMEM)
    dma = pltpu.SemaphoreType.DMA
    return pl.pallas_call(
        forward_kernel,
        in_specs=[in_vmem, in_vmem, anywhere, anywhere],
        out_specs=[anywhere, in_vmem] + [anywhere] * 4,
        out_shape=[
            jax.ShapeDtypeStruct((blk, d_model), BF16),
            jax.ShapeDtypeStruct((4, seq), F32),
        ] + [jax.ShapeDtypeStruct((seq, n), BF16) for n in (d_model, 3 * head_cols)] * 2,
        scratch_shapes=[
            pltpu.VMEM((d_model, 3 * head_cols), BF16),
            pltpu.VMEM((3, blk, d_model), BF16),
            pltpu.VMEM((seq, d_model), BF16),
            pltpu.VMEM((seq, 3 * head_cols), BF16),
            pltpu.VMEM((2, blk, d_model), BF16),
            pltpu.VMEM((2, blk, d_model), BF16),
            pltpu.VMEM((2, blk, 3 * head_cols), BF16),
            pltpu.VMEM((PAIR, seq), BF16),
            pltpu.VMEM((seq, blk), F32),
            pltpu.VMEM((seq, blk), F32),
            pltpu.VMEM((2, seq, PAIR), BF16),
            pltpu.VMEM((4, seq), F32),
            dma((3,)), dma((2,)), dma((4,)), dma((3,)), dma((3,)), dma((8,)), dma((8,)),
        ],
        compiler_params=pltpu.CompilerParams(vmem_limit_bytes=60 << 20, collective_id=2, has_side_effects=True),
        cost_estimate=pl.CostEstimate(
            flops=64 * seq * seq * PAIR, bytes_accessed=32 * seq * d_model, transcendentals=seq * seq * 4),
        name="forward",
    )(x, emb, xs_1, w_qkv)


def through_norm(values, up, d_mid):
    inverse = lax.rsqrt(jnp.mean(values * values, axis=-1, keepdims=True) + EPS_NORM)
    inner = jnp.mean(values * up, axis=-1, keepdims=True)
    return (d_mid.astype(F32) + inverse * up - values * (inverse * inverse * inverse * inner)).astype(BF16)


def backward_kernel(shared, qkv_ref, dc_ref, lse_ref, dmid_ref, x_ref, emb_ref, wqkv_ref, u_ref, *refs):
    sources, (d_ref, other_ref, g_ref), shares = refs[:shared], refs[shared:shared + 3], refs[shared + 3:2 * shared + 3]
    (dch, k_t, dk_acc, dv_acc, p_cat, ds_cat, p_cat2, ds_cat2, d_heads, d_qkv, d_u, w_s, u_s, g_s,
     load_sem, out_sem, dc_send, dc_recv, dq_send, dq_recv, d_send, d_recv, s_send, s_recv) = refs[2 * shared + 3:]
    seq = qkv_ref.shape[0]
    blk = seq // 4
    head_cols = 2 * PAIR
    here = Place()
    z, core, role = here.z, here.c, here.role
    here.meet()
    member = [here.device(z=z // 2 * 2 + i // 2, c=i % 2) for i in range(4)]

    def span(index, count):
        return pl.ds(pl.multiple_of(index * count, count), count)

    def load(src, dst, n):
        copy = pltpu.make_async_copy(src, dst, load_sem.at[n])
        copy.start()
        return copy

    def dc_copy(j, i):
        col = i * head_cols + j * PAIR
        return pltpu.make_async_remote_copy(
            src_ref=dc_ref.at[:, col:col + PAIR], dst_ref=dch.at[span(role, blk), j * PAIR:(j + 1) * PAIR],
            send_sem=dc_send.at[j * 4 + i], recv_sem=dc_recv.at[j * 4 + role], device_id=member[i], device_id_type=MESH)

    for j in range(2):
        for i in range(4):
            pl.when(role != i)(dc_copy(j, i).start)
    for i in range(4):
        @pl.when(role == i)
        def _():
            dch[i * blk:(i + 1) * blk, :] = dc_ref[:, i * head_cols:(i + 1) * head_cols]

    def dq_copy(j, i, t):
        col = t * head_cols + j * PAIR
        return pltpu.make_async_remote_copy(
            src_ref=d_heads.at[i * blk:(i + 1) * blk, col:col + PAIR],
            dst_ref=d_qkv.at[:, pl.ds(pl.multiple_of(role * 3 * head_cols + col, PAIR), PAIR)],
            send_sem=dq_send.at[(j * 4 + i) * 3 + t], recv_sem=dq_recv.at[(j * 4 + role) * 3 + t],
            device_id=member[i], device_id_type=MESH)

    def send_d_heads(j, ts):
        for i in range(4):
            @pl.when(role != i)
            def _():
                for t in ts:
                    dq_copy(j, i, t).start()

    shared_copies = [pltpu.make_async_remote_copy(
        src_ref=src, dst_ref=dst, send_sem=s_send.at[n], recv_sem=s_recv.at[n],
        device_id=here.device(c=1 - core), device_id_type=MESH) for n, (src, dst) in enumerate(zip(sources, shares))]

    steps = seq // BWD_ROWS
    p_cats, ds_cats = (p_cat, p_cat2), (ds_cat, ds_cat2)
    for j in range(2):
        for i in range(4):
            @pl.when(role != i)
            def _():
                pltpu.make_async_copy(dc_ref.at[:, :PAIR], dch.at[:blk, :PAIR], dc_recv.at[j * 4 + i]).wait()
        if j == 0:
            for copy in shared_copies:
                copy.start()
        k_view, v_view = qkv_ref.at[:, (2 + j) * PAIR:(3 + j) * PAIR], qkv_ref.at[:, (4 + j) * PAIR:(5 + j) * PAIR]
        k_t[...] = k_view[...].T
        dk_acc[...] = jnp.zeros_like(dk_acc)
        dv_acc[...] = jnp.zeros_like(dv_acc)

        cols = slice(j * PAIR, (j + 1) * PAIR)

        def scores_of(i, n):
            rows = span(i, BWD_ROWS)
            score_part(qkv_ref[rows, cols], dch[rows, cols], lse_ref[2 * j:2 * j + 2, rows], k_view, v_view, p_cats[n], ds_cats[n])

        def products_of(i, n):
            rows = span(i, BWD_ROWS)
            d_heads[rows, cols] = product_part(qkv_ref[rows, cols], dch[rows, cols], k_t, p_cats[n], ds_cats[n], dk_acc, dv_acc)

        def two_blocks(i, _):
            if j == 1:
                @pl.when(i == min(1, steps // 2 - 1))
                def _():
                    send_d_heads(0, (0, 1, 2))
            scores_of(2 * i + 1, 1)
            products_of(2 * i, 0)
            scores_of(2 * i + 2, 0)
            products_of(2 * i + 1, 1)
            return 0

        scores_of(0, 0)
        lax.fori_loop(0, steps // 2 - 1, two_blocks, 0)
        scores_of(steps - 1, 1)
        products_of(steps - 2, 0)
        if j == 1:
            for target in range(3):
                pl.when(role != target)(dq_copy(1, target, 0).start)
        products_of(steps - 1, 1)
        d_heads[:, head_cols + j * PAIR:head_cols + (j + 1) * PAIR] = (dk_acc[...] * SCALE).astype(BF16)
        d_heads[:, 2 * head_cols + j * PAIR:2 * head_cols + (j + 1) * PAIR] = dv_acc[...].astype(BF16)

    quarter = u_s.shape[2]
    pending = load(u_ref.at[:, :quarter], u_s.at[0], 0)
    for i in range(4):
        @pl.when(role == i)
        def _():
            d_qkv[:, i * 3 * head_cols:(i + 1) * 3 * head_cols] = d_heads[i * blk:(i + 1) * blk, :]
    pl.when(role != 3)(dq_copy(1, 3, 0).start)
    send_d_heads(1, (1, 2))
    stores = []
    count = u_ref.shape[1] // quarter
    for n in range(count):
        ahead = load(u_ref.at[:, (n + 1) * quarter:(n + 2) * quarter], u_s.at[(n + 1) % 2], (n + 1) % 2) if n + 1 < count else None
        pending.wait()
        if n >= 2:
            stores[n - 2].wait()
        g_s[n % 2] = dot_tn(u_s[n % 2], d_heads[...])
        stores.append(pltpu.make_async_copy(g_s.at[n % 2], g_ref.at[n * quarter:(n + 1) * quarter, :], out_sem.at[n % 2]))
        stores[n].start()
        pending = ahead
    w_rows = w_s.shape[1]
    chunks = wqkv_ref.shape[0] // w_rows
    w_load = load(wqkv_ref.at[:w_rows, :], w_s.at[0], 2)
    for j in range(2):
        for i in range(4):
            @pl.when(role != i)
            def _():
                for t in range(3):
                    pltpu.make_async_copy(d_heads.at[:blk, :PAIR], d_qkv.at[:, :PAIR], dq_recv.at[(j * 4 + i) * 3 + t]).wait()
    for n in range(chunks):
        ahead = load(wqkv_ref.at[(n + 1) * w_rows:(n + 2) * w_rows, :], w_s.at[(n + 1) % 2], 2 + (n + 1) % 2) if n + 1 < chunks else None
        w_load.wait()
        d_u[:, n * w_rows:(n + 1) * w_rows] = dot_nt(d_qkv[...], w_s[n % 2]).astype(BF16)
        w_load = ahead
    rows_each = min(128, blk)
    for n in range(blk // rows_each):
        rows = slice(n * rows_each, (n + 1) * rows_each)
        d_u[rows, :] = through_norm(x_ref[rows, :].astype(F32) + emb_row(emb_ref, 1), d_u[rows, :].astype(F32), dmid_ref[rows, :])
    keep = pltpu.make_async_copy(d_u, d_ref, out_sem.at[2])
    keep.start()
    stores[count - 2].wait()
    stores[count - 1].wait()
    give = pltpu.make_async_remote_copy(
        src_ref=d_u, dst_ref=other_ref, send_sem=d_send.at[0], recv_sem=d_recv.at[0],
        device_id=here.device(c=1 - core), device_id_type=MESH)
    give.start()
    for i in range(4):
        @pl.when(role != i)
        def _():
            for j in range(2):
                dc_copy(j, i).wait_send()
                for t in range(3):
                    dq_copy(j, i, t).wait_send()
    keep.wait()
    give.wait()
    for copy in shared_copies:
        copy.wait()


def backward_call(qkv, d_c, lse, d_mid, x, emb, w_qkv, u_seq, shared):
    seq, d_model = u_seq.shape
    blk, heads3 = seq // 4, qkv.shape[1]
    anywhere = pl.BlockSpec(memory_space=pl.ANY)
    in_vmem = pl.BlockSpec(memory_space=pltpu.VMEM)
    dma = pltpu.SemaphoreType.DMA
    quarter = d_model // 4
    return pl.pallas_call(
        functools.partial(backward_kernel, len(shared)),
        in_specs=[in_vmem] * 6 + [anywhere] * (2 + len(shared)),
        out_specs=[anywhere] * (3 + len(shared)),
        out_shape=[
            jax.ShapeDtypeStruct((blk, d_model), BF16),
            jax.ShapeDtypeStruct((blk, d_model), BF16),
            jax.ShapeDtypeStruct((d_model, heads3), F32),
        ] + [jax.ShapeDtypeStruct(value.shape, value.dtype) for value in shared],
        scratch_shapes=[
            pltpu.VMEM((seq, heads3 // 3), BF16),
            pltpu.VMEM((PAIR, seq), BF16),
            pltpu.VMEM((seq, PAIR), F32),
            pltpu.VMEM((seq, PAIR), F32),
            pltpu.VMEM((seq, 2 * BWD_ROWS), BF16),
            pltpu.VMEM((seq, 2 * BWD_ROWS), BF16),
            pltpu.VMEM((seq, 2 * BWD_ROWS), BF16),
            pltpu.VMEM((seq, 2 * BWD_ROWS), BF16),
            pltpu.VMEM((seq, heads3), BF16),
            pltpu.VMEM((blk, 4 * heads3), BF16),
            pltpu.VMEM((blk, d_model), BF16),
            pltpu.VMEM((2, quarter, 4 * heads3), BF16),
            pltpu.VMEM((2, seq, quarter), BF16),
            pltpu.VMEM((2, quarter, heads3), F32),
            dma((4,)), dma((3,)), dma((8,)), dma((8,)), dma((24,)), dma((24,)), dma((1,)), dma((1,)),
            dma((len(shared),)), dma((len(shared),)),
        ],
        compiler_params=pltpu.CompilerParams(vmem_limit_bytes=60 << 20, collective_id=3, has_side_effects=True),
        cost_estimate=pl.CostEstimate(
            flops=160 * seq * seq * PAIR, bytes_accessed=64 * seq * d_model, transcendentals=seq * seq * 4),
        name="backward",
    )(qkv, d_c, lse, d_mid, x, emb, w_qkv, u_seq, *shared)


def rms_rows(values):
    return values * lax.rsqrt(jnp.mean(values * values, axis=-1, keepdims=True) + EPS_NORM)


GELU_IN, GELU_CUBE = math.sqrt(2 / math.pi), 0.044715


def gelu_parts(z):
    square = z * z
    t = jnp.tanh(z * (GELU_IN + (GELU_IN * GELU_CUBE) * square))
    return 0.5 + 0.5 * t, t, square


def hidden_kernel(backward, forward, *refs):
    refs = list(refs)
    take = lambda: refs.pop(0)
    if forward:
        c_ref, x_ref, emb_ref, wo_ref = take(), take(), take(), take()
        w1_ref = take()
    else:
        h_ref, wo_ref, up_ref = take(), take(), take()
    w2_ref = take()
    both = forward and backward
    if backward:
        d_ref = take()
    if backward and not forward:
        w1b_ref = take()
    if forward:
        h_out, m_out = take(), take()
        up_out = None if both else take()
        act_out = take()
    if backward:
        dup_out, dmid_out, dc_out = take(), take(), take()
    else:
        x_out = take()
    if forward:
        h_s, m_s = take(), take()
    prev_s, acc = take(), take()
    step, last = pl.program_id(0), pl.num_programs(0) - 1

    if forward:
        @pl.when(step == 0)
        def _():
            h = (x_ref[...].astype(F32) + emb_row(emb_ref, 1) + dot_nn(c_ref[...], wo_ref[...])).astype(BF16)
            m = rms_rows(h.astype(F32)).astype(BF16)
            h_s[...], m_s[...] = h, m
            h_out[...], m_out[...] = h, m

    def both_parts():
        count = w1_ref.shape[1] // 2
        halves = [slice(n * count, (n + 1) * count) for n in range(2)]
        d_acts = [dot_nt(d_ref[...], w2_ref[half, :]).astype(BF16) for half in halves]
        ups = [dot_nn(m_s[...], w1_ref[:, half]).astype(BF16) for half in halves]
        total = None
        for half, d_act, up in zip(halves, d_acts, ups):
            z = up.astype(F32)
            factor, t, square = gelu_parts(z)
            act_out[:, half] = (z * factor).astype(BF16)
            slope = factor + z * ((1.0 - t * t) * (0.5 * GELU_IN + (1.5 * GELU_IN * GELU_CUBE) * square))
            d_up = (slope * d_act.astype(F32)).astype(BF16)
            dup_out[:, half] = d_up
            part = dot_nt(d_up, w1_ref[:, half])
            total = part if total is None else total + part
        return total

    def finish(total):
        h = (h_s if forward else h_ref)[...].astype(F32)
        d_mid = through_norm(h, total.astype(BF16).astype(F32), d_ref[...])
        dmid_out[...] = d_mid
        dc_out[...] = dot_nt(d_mid, wo_ref[...]).astype(BF16)

    if both:
        @pl.when(step == 0)
        def _():
            acc[...] = both_parts()

        @pl.when(step > 0)
        def _():
            acc[...] += both_parts()

        @pl.when(step == last)
        def _():
            finish(acc[...])
        return

    def first_part():
        slot = step % 2
        if backward:
            d_act = dot_nt(d_ref[...], w2_ref[...]).astype(BF16).astype(F32)
        if forward:
            up = dot_nn(m_s[...], w1_ref[...]).astype(BF16)
            up_out[...] = up
        else:
            up = up_ref[...]
        z = up.astype(F32)
        factor, t, square = gelu_parts(z)
        if forward:
            act = (z * factor).astype(BF16)
            act_out[...] = act
        if backward:
            slope = factor + z * ((1.0 - t * t) * (0.5 * GELU_IN + (1.5 * GELU_IN * GELU_CUBE) * square))
            d_up = (slope * d_act).astype(BF16)
            dup_out[...] = d_up
            prev_s[slot] = d_up
        else:
            prev_s[slot] = act

    def second_part():
        prev = prev_s[1 - step % 2]
        if backward:
            return dot_nt(prev, w1b_ref[...])
        return dot_nn(prev, w2_ref[...])

    pl.when(step == 0)(first_part)

    @pl.when(step == 1)
    def _():
        acc[...] = second_part()
        first_part()

    @pl.when(jnp.logical_and(step > 1, step < last))
    def _():
        acc[...] += second_part()
        first_part()

    @pl.when(step == last)
    def _():
        total = acc[...] + second_part()
        if backward:
            finish(total)
        else:
            x_out[...] = (h_s[...].astype(F32) + total).astype(BF16)


def hidden_call(forward, backward, w_o, w_1, w_2, context=None, x=None, emb=None, h=None, up=None, d_next=None):
    blk, d_model = (context if forward else h).shape
    hidden = w_1.shape[1]
    tile = HIDDEN
    steps = hidden // tile
    now, before = (lambda i: jnp.minimum(i, steps - 1)), (lambda i: jnp.maximum(i - 1, 0))
    whole = lambda rows, cols: pl.BlockSpec((rows, cols), lambda i: (0, 0))
    wide = pl.BlockSpec((blk, tile), lambda i: (0, now(i)))
    args, specs = [], []

    def add(value, spec):
        args.append(value)
        specs.append(spec)

    if forward:
        add(context, whole(blk, d_model))
        add(x, whole(blk, d_model))
        add(emb, whole(2, d_model))
        add(w_o, whole(d_model, d_model))
        add(w_1, pl.BlockSpec((d_model, tile), lambda i: (0, now(i))))
    else:
        add(h, whole(blk, d_model))
        add(w_o, whole(d_model, d_model))
        add(up, wide)
    add(w_2, pl.BlockSpec((tile, d_model), (lambda i: (now(i), 0)) if backward else (lambda i: (before(i), 0))))
    if backward:
        add(d_next, whole(blk, d_model))
    if backward and not forward:
        add(w_1, pl.BlockSpec((d_model, tile), lambda i: (0, before(i))))
    row = (whole(blk, d_model), jax.ShapeDtypeStruct((blk, d_model), BF16))
    big = (wide, jax.ShapeDtypeStruct((blk, hidden), BF16))
    outs = ([row, row] + [big] * (1 if backward else 2) if forward else []) + ([big, row, row] if backward else [row])
    return pl.pallas_call(
        functools.partial(hidden_kernel, backward, forward),
        grid=(steps + (0 if forward and backward else 1),),
        in_specs=specs,
        out_specs=[spec for spec, _ in outs],
        out_shape=[shape for _, shape in outs],
        scratch_shapes=([pltpu.VMEM((blk, d_model), BF16)] * 2 if forward else [])
        + [pltpu.VMEM((2, blk, tile), BF16), pltpu.VMEM((blk, d_model), F32)],
        compiler_params=pltpu.CompilerParams(vmem_limit_bytes=60 << 20),
        cost_estimate=pl.CostEstimate(
            flops=2 * blk * d_model * (hidden * (3 if forward and backward else 2) + 2 * d_model),
            bytes_accessed=4 * hidden * d_model + 8 * blk * hidden, transcendentals=blk * hidden),
        interpret=INTERPRET,
        name="hidden",
    )(*args)


def head_only(values, head):
    lane = lax.broadcasted_iota(jnp.int32, values.shape, 1)
    return jnp.where(lane // HEAD_DIM == head, values, jnp.zeros_like(values))


def score_part(q, d_out, lse, k_ref, v_ref, p_cat, ds_cat):
    block = q.shape[0]
    for head in range(2):
        scores = dot_nt(k_ref[...], head_only(q, head))
        probs = jnp.exp2(scores * EXP2_SCALE - lse[head:head + 1, :])
        d_probs = dot_nt(v_ref[...], head_only(d_out, head)).astype(BF16).astype(F32)
        inner = jnp.sum(probs * d_probs, axis=0, keepdims=True)
        cols = slice(head * block, (head + 1) * block)
        p_cat[:, cols] = probs.astype(BF16)
        ds_cat[:, cols] = (probs * (d_probs - inner)).astype(BF16)


def product_part(q, d_out, k_t, p_cat, ds_cat, dk_acc, dv_acc):
    block = q.shape[0]
    dqs = [dot_nn(k_t[head * HEAD_DIM:(head + 1) * HEAD_DIM, :], ds_cat[:, head * block:(head + 1) * block]) for head in range(2)]
    dv_acc[...] += dot_nn(p_cat[...], jnp.concatenate([head_only(d_out, head) for head in range(2)], axis=0))
    dk_acc[...] += dot_nn(ds_cat[...], jnp.concatenate([head_only(q, head) for head in range(2)], axis=0))
    return (jnp.concatenate(dqs, axis=0).T * SCALE).astype(BF16)


def backward_rows(q, d_out, lse, k_ref, v_ref, k_t, p_cat, ds_cat, dk_acc, dv_acc):
    score_part(q, d_out, lse, k_ref, v_ref, p_cat, ds_cat)
    return product_part(q, d_out, k_t, p_cat, ds_cat, dk_acc, dv_acc)


def last_kernel(qkv_ref, dc_ref, lse_ref, dmid_ref, x_ref, emb_ref, wqkv_ref, u_ref, gqkv2_ref,
                *refs):
    lefts = {'2': refs[:4], '1': refs[8:12], 'o': refs[15:18]}
    rights = {'2': refs[4:8], '1': refs[12:15], 'o': refs[18:22]}
    (dx_ref, g1_ref, g2_ref, go_ref, gq_ref, gk_ref, gv_ref, away2_ref, mid2_ref, keep2_ref,
     away1_ref, mid1_ref, keep1_ref, awayo_ref, mido_ref, keepo_ref, dup_other, dmid_other,
     dch, k_t, dk_acc, dv_acc, p_cat, ds_cat, d_heads, d_qkv, buf, buf_o, second, second_o, tmp, tmp_o,
     third, third_o, sum_1, sum_2, sum_o, qa, qb, q1, q2, q3, q4, d_1, w_s, u_s, g_s,
     left_t, stage,
     local_sem, load_sem, send_sem, recv_sem, dc_send, dc_recv, dq_send, dq_recv, z_send, z_recv, x_send, x_recv,
     p_send, p_recv) = refs[22:]
    seq = qkv_ref.shape[0]
    blk = seq // 4
    head_cols = 2 * PAIR
    here = Place()
    z, core, role, owner = here.z, here.c, here.role, here.owner
    here.meet()
    copies = Copies(send_sem, recv_sem)
    waits = []

    def span(index, count):
        return pl.ds(pl.multiple_of(index * count, count), count)

    def load(src, dst, n):
        copy = pltpu.make_async_copy(src, dst, load_sem.at[n])
        copy.start()
        return copy

    no = jnp.logical_not
    to_a, to_b = here.device(y=here.ya, x=here.xa), here.device(y=here.yb, x=here.xb)
    partner = here.device(c=1 - core)
    member = [here.device(z=z // 2 * 2 + i // 2, c=i % 2) for i in range(4)]
    piece = tmp.shape[1]

    def dc_copy(i):
        return pltpu.make_async_remote_copy(
            src_ref=dc_ref.at[:, i * head_cols:(i + 1) * head_cols], dst_ref=dch.at[span(role, blk), :],
            send_sem=dc_send.at[i], recv_sem=dc_recv.at[role], device_id=member[i], device_id_type=MESH)

    for i in range(4):
        pl.when(role != i)(dc_copy(i).start)

        @pl.when(role == i)
        def _():
            dch[i * blk:(i + 1) * blk, :] = dc_ref[:, i * head_cols:(i + 1) * head_cols]

    half = rights['1'][0].shape[1] // 8
    wide = 2 * half
    dmid_give = copies.start(lefts['o'][2], dmid_other, partner)
    dup_give = [copies.start(rights['1'][2].at[:, q * wide:(q + 1) * wide], dup_other.at[:, q * wide:(q + 1) * wide], partner)
                for q in range(4)]
    lefts['o'] = (*lefts['o'], dmid_other)
    rights['1'] = (*rights['1'], dup_other)
    firsts = {(w, q): [copies.make(ref.at[q, :, h * half:(h + 1) * half], buf.at[u + q, :, h * half:(h + 1) * half], to_a)
                       for h in range(2)] for w, ref, u in (('2', away2_ref, 0), ('1', away1_ref, 4)) for q in range(4)}
    firsts['o'] = [copies.make(awayo_ref.at[2 * h:2 * h + 2], buf_o.at[2 * h:2 * h + 2], to_a) for h in range(2)]
    seconds = {(w, q): copies.make(buf.at[u + q, piece:, :], second.at[u + q], to_b) for w, u in (('2', 0), ('1', 4)) for q in range(4)}
    seconds['o'] = copies.make(buf_o.at[:, piece:, :], second_o, to_b)

    def add_mid(unit):
        if unit == 'o':
            mid, keep, t, n = mido_ref, keepo_ref, tmp_o, 4
            bottom, top = buf_o.at[:, piece:, :], buf_o.at[:, :piece, :]
        else:
            w, q = unit
            mid, keep = (mid2_ref.at[q], keep2_ref.at[q]) if w == '2' else (mid1_ref.at[q], keep1_ref.at[q])
            u = q if w == '2' else 4 + q
            t, n, bottom, top = tmp, 6, buf.at[u, piece:, :], buf.at[u, :piece, :]
        loads = [load(mid, t.at[0], n), load(keep, t.at[1], n + 1)]
        for copy in firsts[unit]:
            copy.wait_recv()
        for copy in loads:
            copy.wait()
        bottom[...] += t[0]
        top[...] += t[1]
        seconds[unit].start()

    sums = {'2': (lambda q: buf.at[q, :piece, :], third.at[0], 0), '1': (lambda q: buf.at[4 + q, :piece, :], third.at[1], 1),
            'o': (lambda q: buf_o.at[q, :piece, :], third_o, 2)}
    far_q = here.z_by[2]

    def near_copy(w, q):
        part, got, n = sums[w]
        return pltpu.make_async_remote_copy(
            src_ref=part(q), dst_ref=got.at[q // 2], send_sem=z_send.at[n * 3 + q // 2], recv_sem=z_recv.at[n * 3 + q // 2],
            device_id=here.device(z=here.z_by[1]), device_id_type=MESH)

    def far_copy(w):
        part, got, n = sums[w]
        return pltpu.make_async_remote_copy(
            src_ref=part(far_q), dst_ref=got.at[2], send_sem=z_send.at[n * 3 + 2], recv_sem=z_recv.at[n * 3 + 2],
            device_id=here.device(z=far_q), device_id_type=MESH)

    def finish(unit):
        seconds[unit].wait_recv()
        if unit == 'o':
            buf_o[:, :piece, :] += second_o[...]
            w, qs = 'o', range(4)
        else:
            w, u = unit[0], unit[1] + (4 if unit[0] == '1' else 0)
            buf[u, :piece, :] += second[u]
            qs = (unit[1],)
        for q in qs:
            pl.when((z + q) % 2 == 1)(near_copy(w, q).start)

    def far(w):
        part, got, n = sums[w]
        for k in range(2):
            pltpu.make_async_copy(got.at[2], got.at[k], z_recv.at[n * 3 + k]).wait()
        theirs, ours = part(far_q), part(z)
        theirs[...] += got[far_q // 2]
        ours[...] += got[z // 2]
        far_copy(w).start()

    mine, by_a = here.piece(here.y, here.x), here.piece(here.ya, here.xa)
    by_b, by_ab = here.piece(here.yb, here.xb), here.piece(1 - here.y, 1 - here.x)
    gathers = {}

    def total(w):
        part, got, n = sums[w]
        out = {'2': sum_2, '1': sum_1, 'o': sum_o}[w]
        far_copy(w).wait_recv()
        out[...] = part(z)[...] + got[2]

    def gather_start(name, src, out, n):
        rows = lambda e: out.at[span(e, piece), :]
        keep = pltpu.make_async_copy(src, rows(mine), local_sem.at[n])
        keep.start()
        waits.append(keep)
        gathers[name] = dict(src=src, rows=rows, a=copies.start(src, rows(mine), to_a), b1=copies.start(src, rows(mine), to_b))

    def gather_second(name):
        g = gathers[name]
        g['a'].wait_recv()
        g['b2'] = copies.start(g['rows'](by_a), g['rows'](by_a), to_b)

    def gather_core(name):
        g = gathers[name]
        g['c'] = [copies.start(g['src'], g['rows'](mine), partner), copies.start(g['rows'](by_a), g['rows'](by_a), partner)]
        g['b1'].wait_recv()
        g['c'].append(copies.start(g['rows'](by_b), g['rows'](by_b), partner))
        g['b2'].wait_recv()
        g['c'].append(copies.start(g['rows'](by_ab), g['rows'](by_ab), partner))

    def dq_copy(j, i, t):
        col = t * head_cols + j * PAIR
        return pltpu.make_async_remote_copy(
            src_ref=d_heads.at[i * blk:(i + 1) * blk, col:col + PAIR],
            dst_ref=d_qkv.at[:, pl.ds(pl.multiple_of(role * 3 * head_cols + col, PAIR), PAIR)],
            send_sem=dq_send.at[(j * 4 + i) * 3 + t], recv_sem=dq_recv.at[(j * 4 + role) * 3 + t],
            device_id=member[i], device_id_type=MESH)

    def send_d_heads(j):
        for i in range(4):
            @pl.when(role != i)
            def _():
                for t in range(3):
                    dq_copy(j, i, t).start()

    index = [here.ya * 2 + here.xa, (1 - here.y) * 2 + 1 - here.x, here.yb * 2 + here.xb, here.y * 2 + here.x]
    spaces = (p_cat, ds_cat)
    parts = [('2', n) for n in range(8)] + [('1', n) for n in range(8)] + [('o', n) for n in range(2)]
    left_loads = [('2', q) for q in range(4)] + [('1', 0), ('o', 0)]

    def load_lefts(name, q):
        for n in range(16):
            pltpu.make_async_copy(
                lefts[name][n // 4].at[:, span(q * 8 + index[n % 4] * 2 + core, piece)],
                d_heads.at[n // 4 * blk:(n // 4 + 1) * blk, n % 4 * piece:(n % 4 + 1) * piece], load_sem.at[14]).start()

    def load_rights(s):
        name, n = parts[s]
        for i in range(4):
            pltpu.make_async_copy(
                rights[name][i].at[:, n * half:(n + 1) * half], spaces[s % 2].at[i * blk:(i + 1) * blk, :],
                load_sem.at[15 + s % 2]).start()

    def stored(s):
        pltpu.make_async_copy(stage.at[s % 2], stage.at[s % 2], load_sem.at[17 + s % 2]).wait()

    def send_part(s):
        name, n = parts[s]
        if name == 'o':
            firsts['o'][n].start()
        else:
            firsts[(name, n // 2)][n % 2].start()

    load_lefts(*left_loads[0])
    load_rights(0)
    load_rights(1)
    for s in range(len(parts)):
        name, n = parts[s]
        if n == 0 or name == '2' and n % 2 == 0:
            every = d_heads.at[:, :4 * piece]
            pltpu.make_async_copy(every, every, load_sem.at[14]).wait()
            left_t[...] = every[...].T
            left_loads.pop(0)
            if left_loads:
                if left_loads[0][0] == 'o':
                    dmid_give.wait_recv()
                load_lefts(*left_loads[0])
        if s + 1 < len(parts) and parts[s + 1][0] != '2':
            if parts[s + 1][0] == '1' and parts[s + 1][1] % 2 == 0:
                dup_give[parts[s + 1][1] // 2].wait_recv()
            load_rights(s + 1)
        space = spaces[s % 2]
        if name != '2' or n < 2:
            pltpu.make_async_copy(space, space, load_sem.at[15 + s % 2]).wait()
        if s >= 1:
            stored(s - 1)
            send_part(s - 1)
        stage[s % 2] = dot_nn(left_t[...], space[...])
        targets = {'2': (away2_ref, mid2_ref, keep2_ref), '1': (away1_ref, mid1_ref, keep1_ref),
                   'o': (awayo_ref, mido_ref, keepo_ref)}[name]
        for row, ref in zip((0, 2 * piece, 3 * piece), targets):
            rows = slice(row, row + (2 * piece if row == 0 else piece))
            if name == 'o':
                for k in range(2):
                    pltpu.make_async_copy(stage.at[s % 2, rows, k * (half // 2):(k + 1) * (half // 2)], ref.at[2 * n + k],
                                          load_sem.at[17 + s % 2]).start()
            else:
                pltpu.make_async_copy(stage.at[s % 2, rows, :], ref.at[n // 2, :, n % 2 * half:(n % 2 + 1) * half],
                                      load_sem.at[17 + s % 2]).start()
    stored(len(parts) - 1)
    send_part(len(parts) - 1)

    for i in range(4):
        @pl.when(role != i)
        def _():
            pltpu.make_async_copy(dc_ref.at[:, :head_cols], dch.at[:blk, :], dc_recv.at[i]).wait()

    moves = {(0, 0): [(add_mid, ('2', 0))], (0, 1): [(add_mid, ('2', 1))], (0, 4): [(finish, ('2', 0))],
             (0, 6): [(add_mid, ('2', 2)), (finish, ('2', 1))], (1, 0): [(send_d_heads, 0)],
             (1, 2): [(finish, ('2', 2)), (add_mid, ('2', 3))], (1, 6): [(finish, ('2', 3))], (1, 7): [(add_mid, ('1', 0))]}
    steps = seq // BWD_ROWS
    for j in range(2):
        k_view, v_view = qkv_ref.at[:, (2 + j) * PAIR:(3 + j) * PAIR], qkv_ref.at[:, (4 + j) * PAIR:(5 + j) * PAIR]
        k_t[...] = k_view[...].T
        dk_acc[...] = jnp.zeros_like(dk_acc)
        dv_acc[...] = jnp.zeros_like(dv_acc)

        def block(i, _):
            for n in range(8):
                if (j, n) in moves:
                    @pl.when(i == min(n, steps - 1))
                    def _():
                        for move, what in moves[(j, n)]:
                            move(what)
            rows = span(i, BWD_ROWS)
            cols = slice(j * PAIR, (j + 1) * PAIR)
            d_heads[rows, cols] = backward_rows(
                qkv_ref[rows, cols], dch[rows, cols], lse_ref[2 * j:2 * j + 2, rows], k_view, v_view,
                k_t, p_cat, ds_cat, dk_acc, dv_acc)
            return 0

        lax.fori_loop(0, steps, block, 0)
        d_heads[:, head_cols + j * PAIR:head_cols + (j + 1) * PAIR] = (dk_acc[...] * SCALE).astype(BF16)
        d_heads[:, 2 * head_cols + j * PAIR:2 * head_cols + (j + 1) * PAIR] = dv_acc[...].astype(BF16)

    quarter = 2 * piece

    def quarter_loads(n):
        return [load(u_ref.at[:, span(index[n], quarter)], u_s.at[n % 2], 8 + n % 2),
                load(gqkv2_ref.at[span(index[n], quarter), :], g_s.at[n % 2], 10 + n % 2)]

    pending = quarter_loads(0)
    for i in range(4):
        @pl.when(role == i)
        def _():
            d_qkv[:, i * 3 * head_cols:(i + 1) * 3 * head_cols] = d_heads[i * blk:(i + 1) * blk, :]
    send_d_heads(1)
    targets = [qa.at[0], qa.at[1], qb.at[0], qb.at[1]]
    first_q = copies.make(qa, q1, to_a)
    for n in range(4):
        ahead = quarter_loads(n + 1) if n < 3 else []
        for copy in pending:
            copy.wait()
        targets[n][...] = dot_tn(u_s[n % 2], d_heads[...]) + g_s[n % 2]
        pending = ahead
        if n == 0:
            far('2')
            add_mid(('1', 1))
            finish(('1', 0))
            finish(('1', 1))
        if n == 2:
            first_q.start()

    add_mid(('1', 2))
    w_rows = w_s.shape[1]
    chunks = wqkv_ref.shape[0] // w_rows
    w_load = load(wqkv_ref.at[:w_rows, :], w_s.at[0], 12)
    for j in range(2):
        for i in range(4):
            @pl.when(role != i)
            def _():
                for t in range(3):
                    pltpu.make_async_copy(d_heads.at[:blk, :PAIR], d_qkv.at[:, :PAIR], dq_recv.at[(j * 4 + i) * 3 + t]).wait()
    for n in range(chunks):
        ahead = load(wqkv_ref.at[(n + 1) * w_rows:(n + 2) * w_rows, :], w_s.at[(n + 1) % 2], 12 + (n + 1) % 2) if n + 1 < chunks else None
        w_load.wait()
        d_1[:, n * w_rows:(n + 1) * w_rows] = dot_nt(d_qkv[...], w_s[n % 2]).astype(BF16)
        w_load = ahead

    count = min(128, blk)
    for n in range(blk // count):
        rows = slice(n * count, (n + 1) * count)
        d_1[rows, :] = through_norm(x_ref[rows, :].astype(F32) + emb_row(emb_ref, 0), d_1[rows, :].astype(F32), dmid_ref[rows, :])

    own_seq, part_rows = z // 2, blk // 2

    def dx_rows(role, h):
        return pl.ds(pl.multiple_of(role * blk + h * part_rows, part_rows), part_rows)

    def dx_copy(n, h, device):
        slot = [0, 1 + core, 3 + core][n]
        return pltpu.make_async_remote_copy(
            src_ref=d_1.at[h * part_rows:(h + 1) * part_rows, :], dst_ref=dx_ref.at[dx_rows(role, h), :],
            send_sem=x_send.at[n * 2 + h], recv_sem=x_recv.at[slot * 2 + h], device_id=device, device_id_type=MESH)

    dx_side = [dx_copy(0, h, partner) for h in range(2)]
    dx_next = [dx_copy(1, h, here.device(z=here.z_by[1], c=own_seq)) for h in range(2)]
    dx_cross = [dx_copy(2, h, here.device(z=far_q, c=own_seq)) for h in range(2)]
    dx_keep = pltpu.make_async_copy(d_1, dx_ref.at[span(role, blk), :], local_sem.at[8])

    def dx_pass(cc, h):
        rows = dx_rows(z % 2 * 2 + cc, h)
        return pltpu.make_async_remote_copy(
            src_ref=dx_ref.at[rows, :], dst_ref=dx_ref.at[rows, :], send_sem=x_send.at[6 + cc * 2 + h],
            recv_sem=x_recv.at[(5 + cc) * 2 + h], device_id=here.device(z=here.z_by[1]), device_id_type=MESH)

    def dx_start(h):
        dx_cross[h].start()
        dx_next[h].start()
        pl.when(no(owner))(dx_side[h].start)

    def dx_got(slot, h):
        rows = d_1.at[:part_rows, :]
        pltpu.make_async_copy(rows, dx_ref.at[:part_rows, :], x_recv.at[slot * 2 + h]).wait()

    def dx_forward(h):
        @pl.when(no(owner))
        def _():
            for cc in range(2):
                dx_got(3 + cc, h)
                dx_pass(cc, h).start()

    finish(('1', 2))
    dx_start(0)
    pl.when(owner)(dx_keep.start)
    add_mid(('1', 3))
    finish(('1', 3))
    add_mid('o')
    dx_forward(0)
    far('1')
    first_q.wait_recv()
    qb[0] += q1[1]
    second_q = copies.start(qb.at[0], q2, to_b)
    qb[1] += q1[0]
    total('2')
    gather_start('2', sum_2, g2_ref, 0)
    second_q.wait_recv()
    qb[1] += q2[...]
    plane_stays = jnp.logical_and(2 * (z % 2) + core == z, z // 2 == core)
    plane_q = pltpu.make_async_remote_copy(
        src_ref=qb.at[1], dst_ref=q3, send_sem=p_send.at[0], recv_sem=p_recv.at[0],
        device_id=here.device(z=2 * (z % 2) + core, c=z // 2), device_id_type=MESH)

    @pl.when(plane_stays)
    def _():
        q3[...] = qb[1]

    pl.when(no(plane_stays))(plane_q.start)
    finish('o')
    total('1')
    gather_start('1', sum_1, g1_ref, 1)
    dx_start(1)
    gather_second('2')
    gather_second('1')
    pl.when(no(plane_stays))(plane_q.wait_recv)
    give_q = copies.start(q3.at[span(1 - core, piece), :], q4.at[0], partner)
    gather_core('2')
    give_q.wait_recv()
    q4[1] = q4[0] + q3[span(core, piece), :]
    far('o')
    for t, (name, out) in enumerate((('q', gq_ref), ('k', gk_ref), ('v', gv_ref))):
        gather_start(name, q4.at[1, :, t * head_cols:(t + 1) * head_cols], out, 3 + t)
    gather_core('1')
    for name in 'qkv':
        gather_second(name)
    for name in 'qkv':
        gather_core(name)
    dx_forward(1)
    total('o')
    gather_start('o', sum_o, go_ref, 2)
    gather_second('o')
    gather_core('o')

    @pl.when(owner)
    def _():
        for h in range(2):
            for slot in (0, 1, 2):
                dx_got(slot, h)
        dx_keep.wait()

    @pl.when(no(owner))
    def _():
        for h in range(2):
            dx_side[h].wait_send()
            for cc in range(2):
                dx_got(5 + cc, h)
                dx_pass(cc, h).wait_send()

    for g in gathers.values():
        for copy in g['c']:
            copy.wait_recv()
    for copy in waits:
        copy.wait()
    for copy in copies.sent:
        copy.wait_send()
    for h in range(2):
        dx_cross[h].wait_send()
        dx_next[h].wait_send()
    pl.when(no(plane_stays))(plane_q.wait_send)
    for i in range(4):
        @pl.when(role != i)
        def _():
            dc_copy(i).wait_send()
            for j in range(2):
                for t in range(3):
                    dq_copy(j, i, t).wait_send()
        for w in '21o':
            pl.when((z + i) % 2 == 1)(near_copy(w, i).wait_send)
    for w in '21o':
        far_copy(w).wait_send()


def last_call(qkv, d_c, lse, d_mid, x, emb, w_qkv, u_seq, g_qkv, w2_sides, w1_sides, wo_sides):
    seq, d_model = u_seq.shape
    blk, piece = seq // 4, d_model // 8
    n1, no = w1_sides[4].shape[1] // 4, wo_sides[3].shape[1] // 4
    assert n1 == d_model == 2 * 2 * BWD_ROWS and no * 2 == 2 * BWD_ROWS
    heads3 = qkv.shape[1]
    anywhere = pl.BlockSpec(memory_space=pl.ANY)
    in_vmem = pl.BlockSpec(memory_space=pltpu.VMEM)
    copies = 5 + 18 + 9 + 6 * 7 + 3
    dma = pltpu.SemaphoreType.DMA
    w_rows = min(128, d_model)
    return pl.pallas_call(
        last_kernel,
        in_specs=[in_vmem] * 6 + [anywhere] * 25,
        out_specs=[anywhere] * 18,
        out_shape=[
            jax.ShapeDtypeStruct((seq, d_model), BF16),
            jax.ShapeDtypeStruct((d_model, n1), F32),
            jax.ShapeDtypeStruct((8 * piece, n1), F32),
            jax.ShapeDtypeStruct((d_model, no), F32),
        ] + [jax.ShapeDtypeStruct((d_model, heads3 // 3), F32)] * 3
        + [jax.ShapeDtypeStruct((4, k * piece, n), F32) for n in (n1, n1, no) for k in (2, 1, 1)]
        + [jax.ShapeDtypeStruct((blk, n), BF16) for n in (4 * n1, d_model)],
        scratch_shapes=[
            pltpu.VMEM((seq, heads3 // 3), BF16),
            pltpu.VMEM((PAIR, seq), BF16),
            pltpu.VMEM((seq, PAIR), F32),
            pltpu.VMEM((seq, PAIR), F32),
            pltpu.VMEM((seq, 2 * BWD_ROWS), BF16),
            pltpu.VMEM((seq, 2 * BWD_ROWS), BF16),
            pltpu.VMEM((seq, heads3), BF16),
            pltpu.VMEM((blk, 4 * heads3), BF16),
            pltpu.VMEM((8, 2 * piece, n1), F32),
            pltpu.VMEM((4, 2 * piece, no), F32),
            pltpu.VMEM((8, piece, n1), F32),
            pltpu.VMEM((4, piece, no), F32),
            pltpu.VMEM((2, piece, n1), F32),
            pltpu.VMEM((2, 4, piece, no), F32),
            pltpu.VMEM((2, 3, piece, n1), F32),
            pltpu.VMEM((3, piece, no), F32),
            pltpu.VMEM((piece, n1), F32),
            pltpu.VMEM((piece, n1), F32),
            pltpu.VMEM((piece, no), F32),
            pltpu.VMEM((2, 2 * piece, heads3), F32),
            pltpu.VMEM((2, 2 * piece, heads3), F32),
            pltpu.VMEM((2, 2 * piece, heads3), F32),
            pltpu.VMEM((2 * piece, heads3), F32),
            pltpu.VMEM((2 * piece, heads3), F32),
            pltpu.VMEM((2, piece, heads3), F32),
            pltpu.VMEM((blk, d_model), BF16),
            pltpu.VMEM((2, w_rows, 4 * heads3), BF16),
            pltpu.VMEM((2, seq, 2 * piece), BF16),
            pltpu.VMEM((2, 2 * piece, heads3), F32),
            pltpu.VMEM((4 * piece, seq), BF16),
            pltpu.VMEM((2, 4 * piece, 2 * BWD_ROWS), F32),
            dma((9,)), dma((19,)), dma((copies,)), dma((copies,)),
            dma((4,)), dma((4,)), dma((24,)), dma((24,)), dma((9,)), dma((9,)), dma((10,)), dma((14,)), dma((1,)), dma((1,)),
        ],
        compiler_params=pltpu.CompilerParams(vmem_limit_bytes=63 << 20, collective_id=1, has_side_effects=True),
        cost_estimate=pl.CostEstimate(
            flops=160 * seq * seq * PAIR, bytes_accessed=128 * seq * d_model, transcendentals=seq * seq * 4),
        name="last",
    )(qkv, d_c, lse, d_mid, x, emb, w_qkv, u_seq, g_qkv, *w2_sides, *w1_sides, *wo_sides)[:7]


def solution(mesh):
    spec_col = P(None, 'model')
    spec_row = P('model', None)
    spec_act = P('data', None, None)
    spec_rep = P(None, None)

    def device_step(x_in, cot_out, step_emb, w_q, w_k, w_v, w_o, w_1, w_2):
        d_model = x_in.shape[2]
        c_1, lse_1, x_seq, cot, wo, w1, w2, w_qkv, x_1, h_1, m_1, up_1, act_1, x_2 = first_call(
            x_in[0], cot_out[0], step_emb, w_q, w_k, w_v, w_o, w_1, w_2)
        wo, w2 = wo.reshape(-1, d_model), w2.reshape(-1, d_model)

        c_2, lse_2, u_2_seq, qkv_2, u_1_seq, qkv_1 = forward_call(x_2, step_emb, x_seq, w_qkv)
        _, m_2, act_2, d_up_2, d_mid_2, d_c = hidden_call(True, True, wo, w1, w2, context=c_2, x=x_2, emb=step_emb, d_next=cot)
        shared = (act_2, act_1, cot, m_2, m_1, d_up_2, d_mid_2, c_2, c_1)
        d_2, d_2_other, g_qkv_2, *others = backward_call(
            qkv_2, d_c, lse_2, d_mid_2, x_2, step_emb, w_qkv, u_2_seq, shared)
        act_2o, act_1o, cot_o, m_2o, m_1o, d_up_2o, d_mid_2o, c_2o, c_1o = others
        d_up_1, d_mid_1, d_c = hidden_call(False, True, wo, w1, w2, h=h_1, up=up_1, d_next=d_2)
        w2_parts = (act_2, act_2o, act_1, act_1o, cot, cot_o, d_2, d_2_other)
        w1_sides = (m_2, m_2o, m_1, m_1o, d_up_2, d_up_2o, d_up_1)
        wo_sides = (d_mid_2, d_mid_2o, d_mid_1, c_2, c_2o, c_1, c_1o)
        d_x, g_w1, g_w2, g_wo, g_q, g_k, g_v = last_call(
            qkv_1, d_c, lse_1, d_mid_1, x_1, step_emb, w_qkv, u_1_seq, g_qkv_2, w2_parts, w1_sides, wo_sides)
        return g_q, g_k, g_v, g_wo.T, g_w1, g_w2, d_x[None]

    return jax.shard_map(device_step, mesh=mesh,
                         in_specs=(spec_act, spec_act, spec_rep, spec_col, spec_col, spec_col, spec_row, spec_col, spec_row),
                         out_specs=(spec_col, spec_col, spec_col, spec_row, spec_col, spec_row, spec_act),
                         check_vma=False)
```

```python
import functools
import math

import jax
import jax.numpy as jnp
from jax import lax
from jax.experimental import pallas as pl
from jax.experimental.pallas import tpu as pltpu
from jax.sharding import PartitionSpec as P


HEAD_DIM = 64
EPS_NORM = 1e-6
SCALE = HEAD_DIM ** -0.5
EXP2_SCALE = SCALE * math.log2(math.e)
PAIR = 2 * HEAD_DIM
FWD_ROWS = 512
BWD_ROWS = 256
KEYS = 256
HIDDEN = 1024
HIDDEN_FIRST = 512
INTERPRET = False
AXES = ('model', 'data')
BF16 = jnp.bfloat16
F32 = jnp.float32
MESH = pl.DeviceIdType.MESH

def rms_norm(values):
    return values * lax.rsqrt(jnp.mean(values * values, axis=-1, keepdims=True) + EPS_NORM)


def dot_nt(a, b):
    return lax.dot_general(a, b, (((1,), (1,)), ((), ())), preferred_element_type=F32)


def dot_nn(a, b):
    return lax.dot_general(a, b, (((1,), (0,)), ((), ())), preferred_element_type=F32)


def dot_tn(a, b):
    return lax.dot_general(a, b, (((0,), (0,)), ((), ())), preferred_element_type=F32)


def attend_rows(q, k_ref, v_t, e_refs):
    count = k_ref.shape[0] // KEYS
    lane = lax.broadcasted_iota(jnp.int32, q.shape, 1)
    q_heads = [jnp.where(lane // HEAD_DIM == head, q, jnp.zeros_like(q)) for head in range(2)]
    tops, run, total, outs, sums = [[], []], [None, None], [None, None], [], []
    for j in range(count):
        keys = slice(j * KEYS, (j + 1) * KEYS)
        for head in range(2):
            scores = dot_nt(k_ref[keys, :], q_heads[head])
            top = jnp.max(scores, axis=0, keepdims=True) * EXP2_SCALE
            if j:
                top = jnp.maximum(top, run[head])
            weights = jnp.exp2(scores * EXP2_SCALE - top)
            part = jnp.sum(weights, axis=0, keepdims=True)
            total[head] = total[head] * jnp.exp2(run[head] - top) + part if j else part
            run[head] = top
            tops[head].append(top)
            e_refs[head][keys, :] = weights
    for head in range(2):
        inverse = 1.0 / total[head]
        out = None
        for j in range(count):
            keys = slice(j * KEYS, (j + 1) * KEYS)
            factor = inverse * jnp.exp2(tops[head][j] - run[head])
            probs = (e_refs[head][keys, :] * factor).astype(BF16)
            part = dot_nn(v_t[head * HEAD_DIM:(head + 1) * HEAD_DIM, keys], probs)
            out = out + part if j else part
        sums.append(run[head] + jnp.log2(total[head]))
        outs.append(out)
    return outs, sums


class Place:
    def __init__(self):
        self.z = lax.axis_index('model')
        d = lax.axis_index('data')
        self.y, self.x, self.c = d // 4, d // 2 % 2, d % 2
        z = self.z
        self.z_by = {1: z + 1 - 2 * (z % 2), 2: (z + 2) % 4, 3: 3 - z}
        x, y, c = self.x, self.y, self.c
        self.xa, self.ya = x + (1 - c) * (1 - 2 * x), y + c * (1 - 2 * y)
        self.xb, self.yb = x + c * (1 - 2 * x), y + (1 - c) * (1 - 2 * y)
        self.role = z % 2 * 2 + c
        self.owner = c == z // 2

    def piece(self, y, x, c=None):
        return y * 4 + x * 2 + (self.c if c is None else c)

    def device(self, z=None, y=None, x=None, c=None):
        z, y, x, c = (own if given is None else given for given, own in zip((z, y, x, c), (self.z, self.y, self.x, self.c)))
        return {'model': z, 'data': y * 4 + x * 2 + c}

    def peers(self):
        column = [self.device(z=z, c=c) for z in (self.z, *self.z_by.values()) for c in (self.c, 1 - self.c)][1:]
        return column + [self.device(x=1 - self.x), self.device(y=1 - self.y)]

    def meet(self):
        barrier = pltpu.get_barrier_semaphore()
        peers = self.peers()
        for peer in peers:
            pl.semaphore_signal(barrier, inc=1, device_id=peer, device_id_type=MESH)
        pl.semaphore_wait(barrier, len(peers))


class Copies:
    def __init__(self, send_sem, recv_sem):
        self.send_sem, self.recv_sem, self.used, self.sent = send_sem, recv_sem, 0, []

    def make(self, src, dst, device):
        n, self.used = self.used, self.used + 1
        copy = pltpu.make_async_remote_copy(
            src_ref=src, dst_ref=dst, send_sem=self.send_sem.at[n], recv_sem=self.recv_sem.at[n],
            device_id=device, device_id_type=MESH)
        self.sent.append(copy)
        return copy

    def start(self, src, dst, device):
        copy = self.make(src, dst, device)
        copy.start()
        return copy


def first_kernel(x_ref, cot_ref, emb_ref, wq_ref, wk_ref, wv_ref, wo_ref, w1_ref, w2_ref,
                 c1_ref, lse_ref, xs_ref, cot_loc_ref, full_o, full_1, full_2, full_qkv,
                 x1_ref, h_ref, m_ref, up_ref, act_ref, x2_ref,
                 qkv_s, vt_s, e_a, e_b, c_buf, lse_s, cot_s, x1_s, c1_s, h_s, m_s, wo_s, w1_s, w2_s, up_s, act_s, acc,
                 local_sem, send_sem, recv_sem, c_send, c_recv, one_send, one_recv, load_sem, out_sem, z_send, z_recv):
    seq, d_model = x_ref.shape
    blk = seq // 4
    head_cols = wq_ref.shape[1]
    here = Place()
    z, core, role, owner = here.z, here.c, here.role, here.owner
    here.meet()
    copies = Copies(send_sem, recv_sem)

    def span(index, count):
        return pl.ds(pl.multiple_of(index * count, count), count)

    ff_cols, out_rows, piece = w1_ref.shape[1], wo_ref.shape[0] // 8, d_model // 8
    hidden = w2_ref.shape[0] // 8

    def block_qkv(zz, e):
        return full_qkv.at[span(e, piece), span(zz, 3 * head_cols)]

    units = {
        'o': lambda zz, e: full_o.at[zz, span(e, out_rows), :],
        '1': lambda zz, e: full_1.at[span(e, piece), span(zz, ff_cols)],
        '2': lambda zz, e: full_2.at[zz, span(e, hidden), :],
        'qkv': block_qkv,
    }

    def own_parts(name, e):
        if name == 'o':
            return [(wo_ref.at[span(e, out_rows), :], units[name](z, e))]
        if name == '1':
            return [(w1_ref.at[span(e, piece), :], units[name](z, e))]
        if name == '2':
            return [(w2_ref.at[span(e, hidden), :], units[name](z, e))]
        return [(ref.at[span(e, piece), :],
                 full_qkv.at[span(e, piece), pl.ds(pl.multiple_of((z * 3 + t) * head_cols, head_cols), head_cols)])
                for t, ref in enumerate((wq_ref, wk_ref, wv_ref))]

    mine = here.piece(here.y, here.x)
    by_a = here.piece(here.ya, here.xa)
    by_b = here.piece(here.yb, here.xb)
    by_ab = here.piece(1 - here.y, 1 - here.x)
    to_a, to_b = here.device(y=here.ya, x=here.xa), here.device(y=here.yb, x=here.xb)
    partner = here.device(c=1 - core)
    names = ('o', '1', '2', 'qkv')
    right, left = here.device(z=(z + 1) % 4), here.device(z=(z + 3) % 4)

    def piece_copy(name, src, dst, n, zz, device):
        return pltpu.make_async_remote_copy(
            src_ref=src, dst_ref=dst, send_sem=z_send.at[n], recv_sem=z_recv.at[names.index(name) * 4 + zz],
            device_id=device, device_id_type=MESH)

    owns, passes, stage_a, stage_b1, stage_b2, stage_c = {}, {}, {}, {}, {}, {}
    used = 0
    for name in names:
        parts = own_parts(name, mine)
        owns[name] = []
        for device, there in ((right, z < 3), (left, z > 0)):
            owns[name].append((there, [piece_copy(name, src, dst, used + i, z, device) for i, (src, dst) in enumerate(parts)]))
            used += len(parts)
        passes[name] = []
        for zz in range(4):
            block = units[name](zz, mine)
            passes[name].append([piece_copy(name, block, block, used, zz, device) for device in (right, left)])
            used += 1
        make = lambda zz, e, device: copies.make(units[name](zz, e), units[name](zz, e), device)
        stage_a[name] = [make(zz, mine, to_a) for zz in range(4)]
        stage_b1[name] = [make(zz, mine, to_b) for zz in range(4)]
        stage_b2[name] = [make(zz, by_a, to_b) for zz in range(4)]
        stage_c[name] = [[make(zz, e, partner) for e in (mine, by_a, by_b, by_ab)] for zz in range(4)]

    def begin_z(name):
        for there, group in owns[name]:
            @pl.when(there)
            def _():
                for copy in group:
                    copy.start()

    def arrived(name, distance):
        for zz in range(4):
            @pl.when(jnp.logical_or(z == zz + distance, z == zz - distance))
            def _():
                block = units[name](zz, mine)
                pltpu.make_async_copy(block, block, z_recv.at[names.index(name) * 4 + zz]).wait()
                if zz + distance < 3:
                    pl.when(z == zz + distance)(passes[name][zz][0].start)
                if zz - distance > 0:
                    pl.when(z == zz - distance)(passes[name][zz][1].start)
                stage_a[name][zz].start()
                stage_b1[name][zz].start()

    def others(act):
        for zz in range(4):
            @pl.when(z != zz)
            def _():
                act(zz)

    def forward_a(name):
        def act(zz):
            stage_a[name][zz].wait_recv()
            stage_b2[name][zz].start()
        others(act)

    def forward_b(name):
        def act(zz):
            stage_b1[name][zz].wait_recv()
            stage_b2[name][zz].wait_recv()
            for copy in stage_c[name][zz]:
                copy.start()
        others(act)

    def gathered(name):
        def act(zz):
            for copy in stage_c[name][zz]:
                copy.wait_recv()
        others(act)

    begin_z('o')
    begin_z('1')

    locals_ = []

    def copy_local(src, dst):
        copy = pltpu.make_async_copy(src, dst, local_sem.at[len(locals_)])
        locals_.append(copy)
        copy.start()

    copy_local(w1_ref, full_1.at[:, span(z, ff_cols)])
    copy_local(w2_ref, full_2.at[z])
    copy_local(wo_ref, full_o.at[z])
    for t, ref in enumerate((wq_ref, wk_ref, wv_ref)):
        copy_local(ref, full_qkv.at[:, pl.ds(pl.multiple_of((z * 3 + t) * head_cols, head_cols), head_cols)])
    other_role = z % 2 * 2 + 1 - core
    give_x = pltpu.make_async_remote_copy(
        src_ref=x_ref, dst_ref=xs_ref, send_sem=one_send.at[0], recv_sem=one_recv.at[0], device_id=partner, device_id_type=MESH)
    give_cot = pltpu.make_async_remote_copy(
        src_ref=cot_ref.at[span(other_role, blk), :], dst_ref=cot_loc_ref, send_sem=one_send.at[1], recv_sem=one_recv.at[1],
        device_id=partner, device_id_type=MESH)
    keep_x = pltpu.make_async_copy(x_ref, xs_ref, local_sem.at[6])
    take_cot = pltpu.make_async_copy(cot_ref.at[span(role, blk), :], cot_s, local_sem.at[7])
    keep_cot = pltpu.make_async_copy(cot_s, cot_loc_ref, local_sem.at[8])

    @pl.when(owner)
    def _():
        give_x.start()
        give_cot.start()
        keep_x.start()
        take_cot.start()

    def project(i):
        rows = span(i, blk)
        unit = unit_rows(x_ref[rows, :], emb_row(emb_ref, 0))
        for t, ref in enumerate((wq_ref, wk_ref, wv_ref)):
            qkv_s[rows, t * head_cols:(t + 1) * head_cols] = dot_nn(unit, ref[...]).astype(BF16)

    for i in range(4):
        if i == 2:
            arrived('o', 1)
        project(i)

    def context_copy(j, i):
        src = c_buf.at[j, span(i, blk), :]
        dst = c1_ref.at[:, pl.ds(pl.multiple_of((z * 2 + j) * PAIR, PAIR), PAIR)]
        target_z, target_c = 2 * core + i // 2, i % 2
        remote = pltpu.make_async_remote_copy(
            src_ref=src, dst_ref=dst, send_sem=c_send.at[j * 4 + i], recv_sem=c_recv.at[j * 4 + z],
            device_id=here.device(z=target_z, c=target_c), device_id_type=MESH)
        local = pltpu.make_async_copy(src, dst, c_recv.at[j * 4 + z])
        return remote, local, jnp.logical_and(target_z == z, target_c == core)

    def send_context(j, i):
        remote, local, to_self = context_copy(j, i)
        pl.when(to_self)(local.start)
        pl.when(jnp.logical_not(to_self))(remote.start)

    moves = {(0, 0): [(arrived, 'o', 2), (begin_z, '2')], (0, 1): [(arrived, '1', 1), (arrived, 'o', 3)],
             (0, 2): [(begin_z, 'qkv')], (0, 3): [(arrived, '1', 2)], (1, 0): [(arrived, '2', 1)],
             (1, 2): [(arrived, '1', 3), (forward_a, 'o')], (1, 3): [(arrived, '2', 2), (forward_b, 'o')]}
    for j in range(2):
        vt_s[...] = qkv_s[:, (4 + j) * PAIR:(5 + j) * PAIR].T
        k_view = qkv_s.at[:, (2 + j) * PAIR:(3 + j) * PAIR]
        for i in range(4):
            if i or j:
                send_context(j if i else 0, i - 1 if i else 3)
            for move, *what in moves.get((j, i), ()):
                move(*what)
            rows = slice(i * blk, (i + 1) * blk)
            outs, sums = attend_rows(qkv_s[rows, j * PAIR:(j + 1) * PAIR], k_view, vt_s, (e_a, e_b))
            c_buf[j, rows, :] = jnp.concatenate(outs, axis=0).T.astype(BF16)
            for head in range(2):
                lse_s[2 * j + head:2 * j + head + 1, rows] = sums[head]

    @pl.when(owner)
    def _():
        take_cot.wait()
        keep_cot.start()

    forward_a('1')
    arrived('qkv', 1)
    send_context(1, 3)
    give_lse = pltpu.make_async_remote_copy(
        src_ref=lse_s, dst_ref=lse_ref, send_sem=one_send.at[2], recv_sem=one_recv.at[2],
        device_id=here.device(z=2 * core + z // 2, c=z % 2), device_id_type=MESH)
    keep_lse = pltpu.make_async_copy(lse_s, lse_ref, local_sem.at[9])
    lse_stays = jnp.logical_and(2 * core + z // 2 == z, z % 2 == core)
    pl.when(lse_stays)(keep_lse.start)
    pl.when(jnp.logical_not(lse_stays))(give_lse.start)
    arrived('2', 3)
    forward_b('1')
    arrived('qkv', 2)
    arrived('qkv', 3)

    @pl.when(owner)
    def _():
        keep_x.wait()

    @pl.when(jnp.logical_not(owner))
    def _():
        give_x.wait_recv()

    for j in range(2):
        for zz in range(4):
            pltpu.make_async_copy(c_buf.at[j, :blk, :], c1_ref.at[:, :PAIR], c_recv.at[j * 4 + zz]).wait()

    def load(src, dst, n):
        copy = pltpu.make_async_copy(src, dst, load_sem.at[n])
        copy.start()
        return copy

    loads = [load(xs_ref.at[span(role, blk), :], x1_s, 0), load(c1_ref, c1_s, 1)]
    for copy in locals_:
        copy.wait()
    gathered('o')
    loads += [load(full_o.at[zz], wo_s.at[zz * wo_ref.shape[0]:(zz + 1) * wo_ref.shape[0], :], 2 + zz) for zz in range(4)]
    for copy in loads:
        copy.wait()
    h = (x1_s[...].astype(F32) + emb_row(emb_ref, 0) + dot_nn(c1_s[...], wo_s[...])).astype(BF16)
    m = rms_rows(h.astype(F32)).astype(BF16)
    h_s[...], m_s[...] = h, m
    gathered('1')
    tile = w1_s.shape[2]
    steps = full_1.shape[1] // tile
    per_plane = full_2.shape[1] // tile

    def w1_load(n):
        return pltpu.make_async_copy(full_1.at[:, span(n, tile)], w1_s.at[n % 2], load_sem.at[6 + n % 2])

    def w2_load(n):
        return pltpu.make_async_copy(full_2.at[n // per_plane, span(n % per_plane, tile), :], w2_s.at[n % 2], load_sem.at[8 + n % 2])

    def up_store(n):
        return pltpu.make_async_copy(up_s.at[n % 2], up_ref.at[:, span(n, tile)], out_sem.at[n % 2])

    w1_load(0).start()

    def up_part(n, _):
        @pl.when(n + 1 < steps)
        def _():
            w1_load(n + 1).start()

        @pl.when(n == steps // 8)
        def _():
            forward_a('2')

        @pl.when(n == steps * 5 // 8)
        def _():
            forward_a('qkv')

        w1_load(n).wait()

        @pl.when(n >= 2)
        def _():
            up_store(n - 2).wait()

        up = dot_nn(m_s[...], w1_s[n % 2]).astype(BF16)
        up_s[n % 2] = up
        factor = gelu_parts(up.astype(F32))[0]
        act_s[:, span(n, tile)] = (up.astype(F32) * factor).astype(BF16)
        up_store(n).start()
        return 0

    lax.fori_loop(0, steps, up_part, 0)
    forward_b('2')
    outs = [pltpu.make_async_copy(src, dst, out_sem.at[2 + n]) for n, (src, dst) in enumerate(
        ((x1_s, x1_ref), (h_s, h_ref), (m_s, m_ref), (act_s, act_ref)))]
    for copy in outs:
        copy.start()
    gathered('2')
    w2_load(0).start()
    acc[...] = jnp.zeros_like(acc)

    def down_part(n, _):
        @pl.when(n + 1 < steps)
        def _():
            w2_load(n + 1).start()

        @pl.when(n == steps // 2)
        def _():
            forward_b('qkv')

        w2_load(n).wait()
        acc[...] += dot_nn(act_s[:, span(n, tile)], w2_s[n % 2])
        return 0

    lax.fori_loop(0, steps, down_part, 0)
    c1_s[...] = (h_s[...].astype(F32) + acc[...]).astype(BF16)
    out_x2 = pltpu.make_async_copy(c1_s, x2_ref, out_sem.at[6])
    for j in range(2):
        for i in range(4):
            remote, _, to_self = context_copy(j, i)
            pl.when(jnp.logical_not(to_self))(remote.wait_send)
    pl.when(lse_stays)(keep_lse.wait)

    @pl.when(jnp.logical_not(lse_stays))
    def _():
        give_lse.wait_send()
        give_lse.wait_recv()

    out_x2.start()

    @pl.when(owner)
    def _():
        give_x.wait_send()
        give_cot.wait_send()
        keep_cot.wait()

    @pl.when(jnp.logical_not(owner))
    def _():
        give_cot.wait_recv()

    for n in range(steps - 2, steps):
        up_store(n).wait()
    for copy in outs:
        copy.wait()
    out_x2.wait()
    gathered('qkv')
    for name in names:
        for there, group in owns[name]:
            @pl.when(there)
            def _():
                for copy in group:
                    copy.wait_send()

        def sent(zz):
            for copy in (stage_a[name][zz], stage_b1[name][zz], stage_b2[name][zz], *stage_c[name][zz]):
                copy.wait_send()
        others(sent)
        for zz in range(4):
            pl.when(jnp.logical_and(z > zz, z < 3))(passes[name][zz][0].wait_send)
            pl.when(jnp.logical_and(z < zz, z > 0))(passes[name][zz][1].wait_send)


def first_call(x, cot, emb, w_q, w_k, w_v, w_o, w_1, w_2):
    seq, d_model = x.shape
    head_cols, ff_cols, blk = w_q.shape[1], w_1.shape[1], seq // 4
    anywhere = pl.BlockSpec(memory_space=pl.ANY)
    in_vmem = pl.BlockSpec(memory_space=pltpu.VMEM)
    copies = 4 * (3 * 4 + 16)
    hidden, tile = 4 * ff_cols, min(HIDDEN_FIRST, ff_cols)
    shape = jax.ShapeDtypeStruct
    dma = pltpu.SemaphoreType.DMA
    return pl.pallas_call(
        first_kernel,
        in_specs=[in_vmem, anywhere] + [in_vmem] * 7,
        out_specs=[anywhere] * 14,
        out_shape=[
            shape((blk, d_model), BF16),
            shape((4, seq), F32),
            shape((seq, d_model), BF16),
            shape((blk, d_model), BF16),
            shape((4, *w_o.shape), BF16),
            shape((d_model, hidden), BF16),
            shape((4, *w_2.shape), BF16),
            shape((d_model, 12 * head_cols), BF16),
            shape((blk, d_model), BF16),
            shape((blk, d_model), BF16),
            shape((blk, d_model), BF16),
            shape((blk, hidden), BF16),
            shape((blk, hidden), BF16),
            shape((blk, d_model), BF16),
        ],
        scratch_shapes=[
            pltpu.VMEM((seq, 3 * head_cols), BF16),
            pltpu.VMEM((PAIR, seq), BF16),
            pltpu.VMEM((seq, blk), F32),
            pltpu.VMEM((seq, blk), F32),
            pltpu.VMEM((2, seq, PAIR), BF16),
            pltpu.VMEM((4, seq), F32),
            pltpu.VMEM((blk, d_model), BF16),
            pltpu.VMEM((blk, d_model), BF16),
            pltpu.VMEM((blk, d_model), BF16),
            pltpu.VMEM((blk, d_model), BF16),
            pltpu.VMEM((blk, d_model), BF16),
            pltpu.VMEM((d_model, d_model), BF16),
            pltpu.VMEM((2, d_model, tile), BF16),
            pltpu.VMEM((2, tile, d_model), BF16),
            pltpu.VMEM((2, blk, tile), BF16),
            pltpu.VMEM((blk, hidden), BF16),
            pltpu.VMEM((blk, d_model), F32),
            dma((10,)), dma((copies,)), dma((copies,)), dma((8,)), dma((8,)), dma((3,)), dma((3,)), dma((10,)), dma((7,)), dma((28,)), dma((16,)),
        ],
        compiler_params=pltpu.CompilerParams(vmem_limit_bytes=60 << 20, collective_id=0, has_side_effects=True),
        cost_estimate=pl.CostEstimate(
            flops=64 * seq * seq * PAIR, bytes_accessed=64 * seq * d_model, transcendentals=seq * seq * 4),
        name="first",
    )(x, cot, emb, w_q, w_k, w_v, w_o, w_1, w_2)


def emb_row(emb_ref, row):
    return emb_ref[...].astype(F32)[row:row + 1, :]


def unit_rows(values, emb):
    values = values.astype(F32) + emb
    return (values * lax.rsqrt(jnp.mean(values * values, axis=-1, keepdims=True) + EPS_NORM)).astype(BF16)


def forward_kernel(x_ref, emb_ref, xs1_ref, wqkv_ref,
                   c_ref, lse_ref, u2_ref, qkv2_ref, u1_ref, qkv1_ref,
                   w_s, blocks, u_s, qkv_s, x1_s, u1_s, qkv1_s, v_t, e_a, e_b, c_buf, lse_s,
                   local_sem, first_sem, out_sem, x_send, x_recv, c_send, c_recv):
    seq = xs1_ref.shape[0]
    blk = seq // 4
    head_cols = 2 * PAIR
    here = Place()
    z, core, role = here.z, here.c, here.role

    def span(index, count):
        return pl.ds(pl.multiple_of(index * count, count), count)

    w_load = pltpu.make_async_copy(wqkv_ref.at[:, span(role, 3 * head_cols)], w_s, local_sem.at[0])
    w_load.start()
    x1_load = [pltpu.make_async_copy(xs1_ref.at[i * blk:(i + 1) * blk, :], x1_s.at[i % 2], first_sem.at[i % 2]) for i in range(4)]
    x1_load[0].start()
    here.meet()
    partner, across = here.device(c=1 - core), here.device(z=here.z_by[1])
    role_side, role_over = z % 2 * 2 + 1 - core, (1 - z % 2) * 2 + core
    role_last = (1 - z % 2) * 2 + 1 - core

    def x_copy(n, src, slot, device):
        return pltpu.make_async_remote_copy(
            src_ref=src, dst_ref=blocks.at[slot], send_sem=x_send.at[n], recv_sem=x_recv.at[n],
            device_id=device, device_id_type=MESH)

    over, side = x_copy(0, x_ref, 0, across), x_copy(1, x_ref, 1, partner)
    last = x_copy(2, blocks.at[0], 2, partner)
    over.start()
    side.start()

    def project(src, at_role):
        rows = span(at_role, blk)
        unit = unit_rows(src, emb_row(emb_ref, 1))
        u_s[rows, :] = unit
        qkv_s[rows, :] = dot_nn(unit, w_s[...]).astype(BF16)

    w_load.wait()
    project(x_ref[...], role)
    side.wait_recv()
    project(blocks[1], role_side)

    stores = []
    for i in range(4):
        if i < 3:
            x1_load[i + 1].start()
        x1_load[i].wait()
        if i >= 2:
            for copy in stores[i - 2]:
                copy.wait()
        unit = unit_rows(x1_s[i % 2], emb_row(emb_ref, 0))
        u1_s[i % 2] = unit
        qkv1_s[i % 2] = dot_nn(unit, w_s[...]).astype(BF16)
        stores.append([pltpu.make_async_copy(u1_s.at[i % 2], u1_ref.at[i * blk:(i + 1) * blk, :], out_sem.at[i % 2]),
                       pltpu.make_async_copy(qkv1_s.at[i % 2], qkv1_ref.at[i * blk:(i + 1) * blk, :], out_sem.at[2 + i % 2])])
        for copy in stores[i]:
            copy.start()

    over.wait_recv()
    last.start()
    project(blocks[0], role_over)
    last.wait_recv()
    project(blocks[2], role_last)
    keep_u = pltpu.make_async_copy(u_s, u2_ref, local_sem.at[1])
    keep_qkv = pltpu.make_async_copy(qkv_s, qkv2_ref, local_sem.at[2])
    keep_u.start()
    keep_qkv.start()

    member = [here.device(z=z // 2 * 2 + i // 2, c=i % 2) for i in range(4)]

    def c_copy(j, i):
        src = c_buf.at[j, i * blk:(i + 1) * blk, :]
        dst = c_ref.at[:, pl.ds(pl.multiple_of((role * 2 + j) * PAIR, PAIR), PAIR)]
        remote = pltpu.make_async_remote_copy(
            src_ref=src, dst_ref=dst, send_sem=c_send.at[j * 4 + i], recv_sem=c_recv.at[j * 4 + role],
            device_id=member[i], device_id_type=MESH)
        return remote, pltpu.make_async_copy(src, dst, c_recv.at[j * 4 + role])

    def send_context(j, i):
        remote, local = c_copy(j, i)
        pl.when(role == i)(local.start)
        pl.when(role != i)(remote.start)

    for j in range(2):
        v_t[...] = qkv_s[:, (4 + j) * PAIR:(5 + j) * PAIR].T
        k_view = qkv_s.at[:, (2 + j) * PAIR:(3 + j) * PAIR]
        for i in range(4):
            if i or j:
                send_context(j if i else 0, i - 1 if i else 3)
            rows = slice(i * blk, (i + 1) * blk)
            outs, sums = attend_rows(qkv_s[rows, j * PAIR:(j + 1) * PAIR], k_view, v_t, (e_a, e_b))
            c_buf[j, rows, :] = jnp.concatenate(outs, axis=0).T.astype(BF16)
            for head in range(2):
                lse_s[2 * j + head:2 * j + head + 1, rows] = sums[head]
    lse_ref[...] = lse_s[...]
    send_context(1, 3)
    for j in range(2):
        for i in range(4):
            pltpu.make_async_copy(c_buf.at[j, :blk, :], c_ref.at[:, :PAIR], c_recv.at[j * 4 + i]).wait()
            pl.when(role != i)(c_copy(j, i)[0].wait_send)
    for copy in (over, side, last):
        copy.wait_send()
    for group in stores[2:]:
        for copy in group:
            copy.wait()
    keep_u.wait()
    keep_qkv.wait()


def forward_call(x, emb, xs_1, w_qkv):
    blk, d_model = x.shape
    seq, head_cols = 4 * blk, 2 * PAIR
    anywhere = pl.BlockSpec(memory_space=pl.ANY)
    in_vmem = pl.BlockSpec(memory_space=pltpu.VMEM)
    dma = pltpu.SemaphoreType.DMA
    return pl.pallas_call(
        forward_kernel,
        in_specs=[in_vmem, in_vmem, anywhere, anywhere],
        out_specs=[anywhere, in_vmem] + [anywhere] * 4,
        out_shape=[
            jax.ShapeDtypeStruct((blk, d_model), BF16),
            jax.ShapeDtypeStruct((4, seq), F32),
        ] + [jax.ShapeDtypeStruct((seq, n), BF16) for n in (d_model, 3 * head_cols)] * 2,
        scratch_shapes=[
            pltpu.VMEM((d_model, 3 * head_cols), BF16),
            pltpu.VMEM((3, blk, d_model), BF16),
            pltpu.VMEM((seq, d_model), BF16),
            pltpu.VMEM((seq, 3 * head_cols), BF16),
            pltpu.VMEM((2, blk, d_model), BF16),
            pltpu.VMEM((2, blk, d_model), BF16),
            pltpu.VMEM((2, blk, 3 * head_cols), BF16),
            pltpu.VMEM((PAIR, seq), BF16),
            pltpu.VMEM((seq, blk), F32),
            pltpu.VMEM((seq, blk), F32),
            pltpu.VMEM((2, seq, PAIR), BF16),
            pltpu.VMEM((4, seq), F32),
            dma((3,)), dma((2,)), dma((4,)), dma((3,)), dma((3,)), dma((8,)), dma((8,)),
        ],
        compiler_params=pltpu.CompilerParams(vmem_limit_bytes=60 << 20, collective_id=2, has_side_effects=True),
        cost_estimate=pl.CostEstimate(
            flops=64 * seq * seq * PAIR, bytes_accessed=32 * seq * d_model, transcendentals=seq * seq * 4),
        name="forward",
    )(x, emb, xs_1, w_qkv)


def through_norm(values, up, d_mid):
    inverse = lax.rsqrt(jnp.mean(values * values, axis=-1, keepdims=True) + EPS_NORM)
    inner = jnp.mean(values * up, axis=-1, keepdims=True)
    return (d_mid.astype(F32) + inverse * up - values * (inverse * inverse * inverse * inner)).astype(BF16)


def backward_kernel(shared, qkv_ref, dc_ref, lse_ref, dmid_ref, x_ref, emb_ref, wqkv_ref, u_ref, *refs):
    sources, (d_ref, other_ref, g_ref), shares = refs[:shared], refs[shared:shared + 3], refs[shared + 3:2 * shared + 3]
    (dch, k_t, dk_acc, dv_acc, p_cat, ds_cat, p_cat2, ds_cat2, d_heads, d_qkv, d_u, w_s, u_s, g_s,
     load_sem, out_sem, dc_send, dc_recv, dq_send, dq_recv, d_send, d_recv, s_send, s_recv) = refs[2 * shared + 3:]
    seq = qkv_ref.shape[0]
    blk = seq // 4
    head_cols = 2 * PAIR
    here = Place()
    z, core, role = here.z, here.c, here.role
    here.meet()
    member = [here.device(z=z // 2 * 2 + i // 2, c=i % 2) for i in range(4)]

    def span(index, count):
        return pl.ds(pl.multiple_of(index * count, count), count)

    def load(src, dst, n):
        copy = pltpu.make_async_copy(src, dst, load_sem.at[n])
        copy.start()
        return copy

    def dc_copy(j, i):
        col = i * head_cols + j * PAIR
        return pltpu.make_async_remote_copy(
            src_ref=dc_ref.at[:, col:col + PAIR], dst_ref=dch.at[span(role, blk), j * PAIR:(j + 1) * PAIR],
            send_sem=dc_send.at[j * 4 + i], recv_sem=dc_recv.at[j * 4 + role], device_id=member[i], device_id_type=MESH)

    for j in range(2):
        for i in range(4):
            pl.when(role != i)(dc_copy(j, i).start)
    for i in range(4):
        @pl.when(role == i)
        def _():
            dch[i * blk:(i + 1) * blk, :] = dc_ref[:, i * head_cols:(i + 1) * head_cols]

    def dq_copy(j, i, t):
        col = t * head_cols + j * PAIR
        return pltpu.make_async_remote_copy(
            src_ref=d_heads.at[i * blk:(i + 1) * blk, col:col + PAIR],
            dst_ref=d_qkv.at[:, pl.ds(pl.multiple_of(role * 3 * head_cols + col, PAIR), PAIR)],
            send_sem=dq_send.at[(j * 4 + i) * 3 + t], recv_sem=dq_recv.at[(j * 4 + role) * 3 + t],
            device_id=member[i], device_id_type=MESH)

    def send_d_heads(j, ts):
        for i in range(4):
            @pl.when(role != i)
            def _():
                for t in ts:
                    dq_copy(j, i, t).start()

    shared_copies = [pltpu.make_async_remote_copy(
        src_ref=src, dst_ref=dst, send_sem=s_send.at[n], recv_sem=s_recv.at[n],
        device_id=here.device(c=1 - core), device_id_type=MESH) for n, (src, dst) in enumerate(zip(sources, shares))]

    steps = seq // BWD_ROWS
    p_cats, ds_cats = (p_cat, p_cat2), (ds_cat, ds_cat2)
    for j in range(2):
        for i in range(4):
            @pl.when(role != i)
            def _():
                pltpu.make_async_copy(dc_ref.at[:, :PAIR], dch.at[:blk, :PAIR], dc_recv.at[j * 4 + i]).wait()
        if j == 0:
            for copy in shared_copies:
                copy.start()
        k_view, v_view = qkv_ref.at[:, (2 + j) * PAIR:(3 + j) * PAIR], qkv_ref.at[:, (4 + j) * PAIR:(5 + j) * PAIR]
        k_t[...] = k_view[...].T
        dk_acc[...] = jnp.zeros_like(dk_acc)
        dv_acc[...] = jnp.zeros_like(dv_acc)

        cols = slice(j * PAIR, (j + 1) * PAIR)

        def scores_of(i, n):
            rows = span(i, BWD_ROWS)
            score_part(qkv_ref[rows, cols], dch[rows, cols], lse_ref[2 * j:2 * j + 2, rows], k_view, v_view, p_cats[n], ds_cats[n])

        def products_of(i, n):
            rows = span(i, BWD_ROWS)
            d_heads[rows, cols] = product_part(qkv_ref[rows, cols], dch[rows, cols], k_t, p_cats[n], ds_cats[n], dk_acc, dv_acc)

        def two_blocks(i, _):
            if j == 1:
                @pl.when(i == min(1, steps // 2 - 1))
                def _():
                    send_d_heads(0, (0, 1, 2))
            scores_of(2 * i + 1, 1)
            products_of(2 * i, 0)
            scores_of(2 * i + 2, 0)
            products_of(2 * i + 1, 1)
            return 0

        scores_of(0, 0)
        lax.fori_loop(0, steps // 2 - 1, two_blocks, 0)
        scores_of(steps - 1, 1)
        products_of(steps - 2, 0)
        if j == 1:
            for target in range(3):
                pl.when(role != target)(dq_copy(1, target, 0).start)
        products_of(steps - 1, 1)
        d_heads[:, head_cols + j * PAIR:head_cols + (j + 1) * PAIR] = (dk_acc[...] * SCALE).astype(BF16)
        d_heads[:, 2 * head_cols + j * PAIR:2 * head_cols + (j + 1) * PAIR] = dv_acc[...].astype(BF16)

    quarter = u_s.shape[2]
    pending = load(u_ref.at[:, :quarter], u_s.at[0], 0)
    for i in range(4):
        @pl.when(role == i)
        def _():
            d_qkv[:, i * 3 * head_cols:(i + 1) * 3 * head_cols] = d_heads[i * blk:(i + 1) * blk, :]
    pl.when(role != 3)(dq_copy(1, 3, 0).start)
    send_d_heads(1, (1, 2))
    stores = []
    count = u_ref.shape[1] // quarter
    for n in range(count):
        ahead = load(u_ref.at[:, (n + 1) * quarter:(n + 2) * quarter], u_s.at[(n + 1) % 2], (n + 1) % 2) if n + 1 < count else None
        pending.wait()
        if n >= 2:
            stores[n - 2].wait()
        g_s[n % 2] = dot_tn(u_s[n % 2], d_heads[...])
        stores.append(pltpu.make_async_copy(g_s.at[n % 2], g_ref.at[n * quarter:(n + 1) * quarter, :], out_sem.at[n % 2]))
        stores[n].start()
        pending = ahead
    w_rows = w_s.shape[1]
    chunks = wqkv_ref.shape[0] // w_rows
    w_load = load(wqkv_ref.at[:w_rows, :], w_s.at[0], 2)
    for j in range(2):
        for i in range(4):
            @pl.when(role != i)
            def _():
                for t in range(3):
                    pltpu.make_async_copy(d_heads.at[:blk, :PAIR], d_qkv.at[:, :PAIR], dq_recv.at[(j * 4 + i) * 3 + t]).wait()
    for n in range(chunks):
        ahead = load(wqkv_ref.at[(n + 1) * w_rows:(n + 2) * w_rows, :], w_s.at[(n + 1) % 2], 2 + (n + 1) % 2) if n + 1 < chunks else None
        w_load.wait()
        d_u[:, n * w_rows:(n + 1) * w_rows] = dot_nt(d_qkv[...], w_s[n % 2]).astype(BF16)
        w_load = ahead
    rows_each = min(128, blk)
    for n in range(blk // rows_each):
        rows = slice(n * rows_each, (n + 1) * rows_each)
        d_u[rows, :] = through_norm(x_ref[rows, :].astype(F32) + emb_row(emb_ref, 1), d_u[rows, :].astype(F32), dmid_ref[rows, :])
    keep = pltpu.make_async_copy(d_u, d_ref, out_sem.at[2])
    keep.start()
    stores[count - 2].wait()
    stores[count - 1].wait()
    give = pltpu.make_async_remote_copy(
        src_ref=d_u, dst_ref=other_ref, send_sem=d_send.at[0], recv_sem=d_recv.at[0],
        device_id=here.device(c=1 - core), device_id_type=MESH)
    give.start()
    for i in range(4):
        @pl.when(role != i)
        def _():
            for j in range(2):
                dc_copy(j, i).wait_send()
                for t in range(3):
                    dq_copy(j, i, t).wait_send()
    keep.wait()
    give.wait()
    for copy in shared_copies:
        copy.wait()


def backward_call(qkv, d_c, lse, d_mid, x, emb, w_qkv, u_seq, shared):
    seq, d_model = u_seq.shape
    blk, heads3 = seq // 4, qkv.shape[1]
    anywhere = pl.BlockSpec(memory_space=pl.ANY)
    in_vmem = pl.BlockSpec(memory_space=pltpu.VMEM)
    dma = pltpu.SemaphoreType.DMA
    quarter = d_model // 4
    return pl.pallas_call(
        functools.partial(backward_kernel, len(shared)),
        in_specs=[in_vmem] * 6 + [anywhere] * (2 + len(shared)),
        out_specs=[anywhere] * (3 + len(shared)),
        out_shape=[
            jax.ShapeDtypeStruct((blk, d_model), BF16),
            jax.ShapeDtypeStruct((blk, d_model), BF16),
            jax.ShapeDtypeStruct((d_model, heads3), F32),
        ] + [jax.ShapeDtypeStruct(value.shape, value.dtype) for value in shared],
        scratch_shapes=[
            pltpu.VMEM((seq, heads3 // 3), BF16),
            pltpu.VMEM((PAIR, seq), BF16),
            pltpu.VMEM((seq, PAIR), F32),
            pltpu.VMEM((seq, PAIR), F32),
            pltpu.VMEM((seq, 2 * BWD_ROWS), BF16),
            pltpu.VMEM((seq, 2 * BWD_ROWS), BF16),
            pltpu.VMEM((seq, 2 * BWD_ROWS), BF16),
            pltpu.VMEM((seq, 2 * BWD_ROWS), BF16),
            pltpu.VMEM((seq, heads3), BF16),
            pltpu.VMEM((blk, 4 * heads3), BF16),
            pltpu.VMEM((blk, d_model), BF16),
            pltpu.VMEM((2, quarter, 4 * heads3), BF16),
            pltpu.VMEM((2, seq, quarter), BF16),
            pltpu.VMEM((2, quarter, heads3), F32),
            dma((4,)), dma((3,)), dma((8,)), dma((8,)), dma((24,)), dma((24,)), dma((1,)), dma((1,)),
            dma((len(shared),)), dma((len(shared),)),
        ],
        compiler_params=pltpu.CompilerParams(vmem_limit_bytes=60 << 20, collective_id=3, has_side_effects=True),
        cost_estimate=pl.CostEstimate(
            flops=160 * seq * seq * PAIR, bytes_accessed=64 * seq * d_model, transcendentals=seq * seq * 4),
        name="backward",
    )(qkv, d_c, lse, d_mid, x, emb, w_qkv, u_seq, *shared)


def rms_rows(values):
    return values * lax.rsqrt(jnp.mean(values * values, axis=-1, keepdims=True) + EPS_NORM)


GELU_IN, GELU_CUBE = math.sqrt(2 / math.pi), 0.044715


def gelu_parts(z):
    square = z * z
    t = jnp.tanh(z * (GELU_IN + (GELU_IN * GELU_CUBE) * square))
    return 0.5 + 0.5 * t, t, square


def hidden_kernel(backward, forward, *refs):
    refs = list(refs)
    take = lambda: refs.pop(0)
    if forward:
        c_ref, x_ref, emb_ref, wo_ref = take(), take(), take(), take()
        w1_ref = take()
    else:
        h_ref, wo_ref, up_ref = take(), take(), take()
    w2_ref = take()
    both = forward and backward
    if backward:
        d_ref = take()
    if backward and not forward:
        w1b_ref = take()
    if forward:
        h_out, m_out = take(), take()
        up_out = None if both else take()
        act_out = take()
    if backward:
        dup_out, dmid_out, dc_out = take(), take(), take()
    else:
        x_out = take()
    if forward:
        h_s, m_s = take(), take()
    prev_s, acc = take(), take()
    step, last = pl.program_id(0), pl.num_programs(0) - 1

    if forward:
        @pl.when(step == 0)
        def _():
            h = (x_ref[...].astype(F32) + emb_row(emb_ref, 1) + dot_nn(c_ref[...], wo_ref[...])).astype(BF16)
            m = rms_rows(h.astype(F32)).astype(BF16)
            h_s[...], m_s[...] = h, m
            h_out[...], m_out[...] = h, m

    def both_parts():
        count = w1_ref.shape[1] // 2
        halves = [slice(n * count, (n + 1) * count) for n in range(2)]
        d_acts = [dot_nt(d_ref[...], w2_ref[half, :]).astype(BF16) for half in halves]
        ups = [dot_nn(m_s[...], w1_ref[:, half]).astype(BF16) for half in halves]
        total = None
        for half, d_act, up in zip(halves, d_acts, ups):
            z = up.astype(F32)
            factor, t, square = gelu_parts(z)
            act_out[:, half] = (z * factor).astype(BF16)
            slope = factor + z * ((1.0 - t * t) * (0.5 * GELU_IN + (1.5 * GELU_IN * GELU_CUBE) * square))
            d_up = (slope * d_act.astype(F32)).astype(BF16)
            dup_out[:, half] = d_up
            part = dot_nt(d_up, w1_ref[:, half])
            total = part if total is None else total + part
        return total

    def finish(total):
        h = (h_s if forward else h_ref)[...].astype(F32)
        d_mid = through_norm(h, total.astype(BF16).astype(F32), d_ref[...])
        dmid_out[...] = d_mid
        dc_out[...] = dot_nt(d_mid, wo_ref[...]).astype(BF16)

    if both:
        @pl.when(step == 0)
        def _():
            acc[...] = both_parts()

        @pl.when(step > 0)
        def _():
            acc[...] += both_parts()

        @pl.when(step == last)
        def _():
            finish(acc[...])
        return

    def first_part():
        slot = step % 2
        if backward:
            d_act = dot_nt(d_ref[...], w2_ref[...]).astype(BF16).astype(F32)
        if forward:
            up = dot_nn(m_s[...], w1_ref[...]).astype(BF16)
            up_out[...] = up
        else:
            up = up_ref[...]
        z = up.astype(F32)
        factor, t, square = gelu_parts(z)
        if forward:
            act = (z * factor).astype(BF16)
            act_out[...] = act
        if backward:
            slope = factor + z * ((1.0 - t * t) * (0.5 * GELU_IN + (1.5 * GELU_IN * GELU_CUBE) * square))
            d_up = (slope * d_act).astype(BF16)
            dup_out[...] = d_up
            prev_s[slot] = d_up
        else:
            prev_s[slot] = act

    def second_part():
        prev = prev_s[1 - step % 2]
        if backward:
            return dot_nt(prev, w1b_ref[...])
        return dot_nn(prev, w2_ref[...])

    pl.when(step == 0)(first_part)

    @pl.when(step == 1)
    def _():
        acc[...] = second_part()
        first_part()

    @pl.when(jnp.logical_and(step > 1, step < last))
    def _():
        acc[...] += second_part()
        first_part()

    @pl.when(step == last)
    def _():
        total = acc[...] + second_part()
        if backward:
            finish(total)
        else:
            x_out[...] = (h_s[...].astype(F32) + total).astype(BF16)


def hidden_call(forward, backward, w_o, w_1, w_2, context=None, x=None, emb=None, h=None, up=None, d_next=None):
    blk, d_model = (context if forward else h).shape
    hidden = w_1.shape[1]
    tile = HIDDEN
    steps = hidden // tile
    now, before = (lambda i: jnp.minimum(i, steps - 1)), (lambda i: jnp.maximum(i - 1, 0))
    whole = lambda rows, cols: pl.BlockSpec((rows, cols), lambda i: (0, 0))
    wide = pl.BlockSpec((blk, tile), lambda i: (0, now(i)))
    args, specs = [], []

    def add(value, spec):
        args.append(value)
        specs.append(spec)

    if forward:
        add(context, whole(blk, d_model))
        add(x, whole(blk, d_model))
        add(emb, whole(2, d_model))
        add(w_o, whole(d_model, d_model))
        add(w_1, pl.BlockSpec((d_model, tile), lambda i: (0, now(i))))
    else:
        add(h, whole(blk, d_model))
        add(w_o, whole(d_model, d_model))
        add(up, wide)
    add(w_2, pl.BlockSpec((tile, d_model), (lambda i: (now(i), 0)) if backward else (lambda i: (before(i), 0))))
    if backward:
        add(d_next, whole(blk, d_model))
    if backward and not forward:
        add(w_1, pl.BlockSpec((d_model, tile), lambda i: (0, before(i))))
    row = (whole(blk, d_model), jax.ShapeDtypeStruct((blk, d_model), BF16))
    big = (wide, jax.ShapeDtypeStruct((blk, hidden), BF16))
    outs = ([row, row] + [big] * (1 if backward else 2) if forward else []) + ([big, row, row] if backward else [row])
    return pl.pallas_call(
        functools.partial(hidden_kernel, backward, forward),
        grid=(steps + (0 if forward and backward else 1),),
        in_specs=specs,
        out_specs=[spec for spec, _ in outs],
        out_shape=[shape for _, shape in outs],
        scratch_shapes=([pltpu.VMEM((blk, d_model), BF16)] * 2 if forward else [])
        + [pltpu.VMEM((2, blk, tile), BF16), pltpu.VMEM((blk, d_model), F32)],
        compiler_params=pltpu.CompilerParams(vmem_limit_bytes=60 << 20),
        cost_estimate=pl.CostEstimate(
            flops=2 * blk * d_model * (hidden * (3 if forward and backward else 2) + 2 * d_model),
            bytes_accessed=4 * hidden * d_model + 8 * blk * hidden, transcendentals=blk * hidden),
        interpret=INTERPRET,
        name="hidden",
    )(*args)


def head_only(values, head):
    lane = lax.broadcasted_iota(jnp.int32, values.shape, 1)
    return jnp.where(lane // HEAD_DIM == head, values, jnp.zeros_like(values))


def score_part(q, d_out, lse, k_ref, v_ref, p_cat, ds_cat):
    block = q.shape[0]
    for head in range(2):
        scores = dot_nt(k_ref[...], head_only(q, head))
        probs = jnp.exp2(scores * EXP2_SCALE - lse[head:head + 1, :])
        d_probs = dot_nt(v_ref[...], head_only(d_out, head)).astype(BF16).astype(F32)
        inner = jnp.sum(probs * d_probs, axis=0, keepdims=True)
        cols = slice(head * block, (head + 1) * block)
        p_cat[:, cols] = probs.astype(BF16)
        ds_cat[:, cols] = (probs * (d_probs - inner)).astype(BF16)


def product_part(q, d_out, k_t, p_cat, ds_cat, dk_acc, dv_acc):
    block = q.shape[0]
    dqs = [dot_nn(k_t[head * HEAD_DIM:(head + 1) * HEAD_DIM, :], ds_cat[:, head * block:(head + 1) * block]) for head in range(2)]
    dv_acc[...] += dot_nn(p_cat[...], jnp.concatenate([head_only(d_out, head) for head in range(2)], axis=0))
    dk_acc[...] += dot_nn(ds_cat[...], jnp.concatenate([head_only(q, head) for head in range(2)], axis=0))
    return (jnp.concatenate(dqs, axis=0).T * SCALE).astype(BF16)


def backward_rows(q, d_out, lse, k_ref, v_ref, k_t, p_cat, ds_cat, dk_acc, dv_acc):
    score_part(q, d_out, lse, k_ref, v_ref, p_cat, ds_cat)
    return product_part(q, d_out, k_t, p_cat, ds_cat, dk_acc, dv_acc)


def last_kernel(qkv_ref, dc_ref, lse_ref, dmid_ref, x_ref, emb_ref, wqkv_ref, u_ref, gqkv2_ref,
                *refs):
    lefts = {'2': refs[:4], '1': refs[8:12], 'o': refs[15:18]}
    rights = {'2': refs[4:8], '1': refs[12:15], 'o': refs[18:22]}
    (dx_ref, g1_ref, g2_ref, go_ref, gq_ref, gk_ref, gv_ref, away2_ref, mid2_ref, keep2_ref,
     away1_ref, mid1_ref, keep1_ref, awayo_ref, mido_ref, keepo_ref, dup_other, dmid_other,
     dch, k_t, dk_acc, dv_acc, p_cat, ds_cat, d_heads, d_qkv, buf, buf_o, second, second_o, tmp, tmp_o,
     third, third_o, sum_1, sum_2, sum_o, qa, qb, q1, q2, q3, q4, d_1, w_s, u_s, g_s,
     left_t, stage,
     local_sem, load_sem, send_sem, recv_sem, dc_send, dc_recv, dq_send, dq_recv, z_send, z_recv, x_send, x_recv,
     p_send, p_recv) = refs[22:]
    seq = qkv_ref.shape[0]
    blk = seq // 4
    head_cols = 2 * PAIR
    here = Place()
    z, core, role, owner = here.z, here.c, here.role, here.owner
    here.meet()
    copies = Copies(send_sem, recv_sem)
    waits = []

    def span(index, count):
        return pl.ds(pl.multiple_of(index * count, count), count)

    def load(src, dst, n):
        copy = pltpu.make_async_copy(src, dst, load_sem.at[n])
        copy.start()
        return copy

    no = jnp.logical_not
    to_a, to_b = here.device(y=here.ya, x=here.xa), here.device(y=here.yb, x=here.xb)
    partner = here.device(c=1 - core)
    member = [here.device(z=z // 2 * 2 + i // 2, c=i % 2) for i in range(4)]
    piece = tmp.shape[1]

    def dc_copy(i):
        return pltpu.make_async_remote_copy(
            src_ref=dc_ref.at[:, i * head_cols:(i + 1) * head_cols], dst_ref=dch.at[span(role, blk), :],
            send_sem=dc_send.at[i], recv_sem=dc_recv.at[role], device_id=member[i], device_id_type=MESH)

    for i in range(4):
        pl.when(role != i)(dc_copy(i).start)

        @pl.when(role == i)
        def _():
            dch[i * blk:(i + 1) * blk, :] = dc_ref[:, i * head_cols:(i + 1) * head_cols]

    half = rights['1'][0].shape[1] // 8
    wide = 2 * half
    dmid_give = copies.start(lefts['o'][2], dmid_other, partner)
    dup_give = [copies.start(rights['1'][2].at[:, q * wide:(q + 1) * wide], dup_other.at[:, q * wide:(q + 1) * wide], partner)
                for q in range(4)]
    lefts['o'] = (*lefts['o'], dmid_other)
    rights['1'] = (*rights['1'], dup_other)
    firsts = {(w, q): [copies.make(ref.at[q, :, h * half:(h + 1) * half], buf.at[u + q, :, h * half:(h + 1) * half], to_a)
                       for h in range(2)] for w, ref, u in (('2', away2_ref, 0), ('1', away1_ref, 4)) for q in range(4)}
    firsts['o'] = [copies.make(awayo_ref.at[2 * h:2 * h + 2], buf_o.at[2 * h:2 * h + 2], to_a) for h in range(2)]
    seconds = {(w, q): copies.make(buf.at[u + q, piece:, :], second.at[u + q], to_b) for w, u in (('2', 0), ('1', 4)) for q in range(4)}
    seconds['o'] = copies.make(buf_o.at[:, piece:, :], second_o, to_b)

    def add_mid(unit):
        if unit == 'o':
            mid, keep, t, n = mido_ref, keepo_ref, tmp_o, 4
            bottom, top = buf_o.at[:, piece:, :], buf_o.at[:, :piece, :]
        else:
            w, q = unit
            mid, keep = (mid2_ref.at[q], keep2_ref.at[q]) if w == '2' else (mid1_ref.at[q], keep1_ref.at[q])
            u = q if w == '2' else 4 + q
            t, n, bottom, top = tmp, 6, buf.at[u, piece:, :], buf.at[u, :piece, :]
        loads = [load(mid, t.at[0], n), load(keep, t.at[1], n + 1)]
        for copy in firsts[unit]:
            copy.wait_recv()
        for copy in loads:
            copy.wait()
        bottom[...] += t[0]
        top[...] += t[1]
        seconds[unit].start()

    sums = {'2': (lambda q: buf.at[q, :piece, :], third.at[0], 0), '1': (lambda q: buf.at[4 + q, :piece, :], third.at[1], 1),
            'o': (lambda q: buf_o.at[q, :piece, :], third_o, 2)}
    far_q = here.z_by[2]

    def near_copy(w, q):
        part, got, n = sums[w]
        return pltpu.make_async_remote_copy(
            src_ref=part(q), dst_ref=got.at[q // 2], send_sem=z_send.at[n * 3 + q // 2], recv_sem=z_recv.at[n * 3 + q // 2],
            device_id=here.device(z=here.z_by[1]), device_id_type=MESH)

    def far_copy(w):
        part, got, n = sums[w]
        return pltpu.make_async_remote_copy(
            src_ref=part(far_q), dst_ref=got.at[2], send_sem=z_send.at[n * 3 + 2], recv_sem=z_recv.at[n * 3 + 2],
            device_id=here.device(z=far_q), device_id_type=MESH)

    def finish(unit):
        seconds[unit].wait_recv()
        if unit == 'o':
            buf_o[:, :piece, :] += second_o[...]
            w, qs = 'o', range(4)
        else:
            w, u = unit[0], unit[1] + (4 if unit[0] == '1' else 0)
            buf[u, :piece, :] += second[u]
            qs = (unit[1],)
        for q in qs:
            pl.when((z + q) % 2 == 1)(near_copy(w, q).start)

    def far(w):
        part, got, n = sums[w]
        for k in range(2):
            pltpu.make_async_copy(got.at[2], got.at[k], z_recv.at[n * 3 + k]).wait()
        theirs, ours = part(far_q), part(z)
        theirs[...] += got[far_q // 2]
        ours[...] += got[z // 2]
        far_copy(w).start()

    mine, by_a = here.piece(here.y, here.x), here.piece(here.ya, here.xa)
    by_b, by_ab = here.piece(here.yb, here.xb), here.piece(1 - here.y, 1 - here.x)
    gathers = {}

    def total(w):
        part, got, n = sums[w]
        out = {'2': sum_2, '1': sum_1, 'o': sum_o}[w]
        far_copy(w).wait_recv()
        out[...] = part(z)[...] + got[2]

    def gather_start(name, src, out, n):
        rows = lambda e: out.at[span(e, piece), :]
        keep = pltpu.make_async_copy(src, rows(mine), local_sem.at[n])
        keep.start()
        waits.append(keep)
        gathers[name] = dict(src=src, rows=rows, a=copies.start(src, rows(mine), to_a), b1=copies.start(src, rows(mine), to_b))

    def gather_second(name):
        g = gathers[name]
        g['a'].wait_recv()
        g['b2'] = copies.start(g['rows'](by_a), g['rows'](by_a), to_b)

    def gather_core(name):
        g = gathers[name]
        g['c'] = [copies.start(g['src'], g['rows'](mine), partner), copies.start(g['rows'](by_a), g['rows'](by_a), partner)]
        g['b1'].wait_recv()
        g['c'].append(copies.start(g['rows'](by_b), g['rows'](by_b), partner))
        g['b2'].wait_recv()
        g['c'].append(copies.start(g['rows'](by_ab), g['rows'](by_ab), partner))

    def dq_copy(j, i, t):
        col = t * head_cols + j * PAIR
        return pltpu.make_async_remote_copy(
            src_ref=d_heads.at[i * blk:(i + 1) * blk, col:col + PAIR],
            dst_ref=d_qkv.at[:, pl.ds(pl.multiple_of(role * 3 * head_cols + col, PAIR), PAIR)],
            send_sem=dq_send.at[(j * 4 + i) * 3 + t], recv_sem=dq_recv.at[(j * 4 + role) * 3 + t],
            device_id=member[i], device_id_type=MESH)

    def send_d_heads(j):
        for i in range(4):
            @pl.when(role != i)
            def _():
                for t in range(3):
                    dq_copy(j, i, t).start()

    index = [here.ya * 2 + here.xa, (1 - here.y) * 2 + 1 - here.x, here.yb * 2 + here.xb, here.y * 2 + here.x]
    spaces = (p_cat, ds_cat)
    parts = [('2', n) for n in range(8)] + [('1', n) for n in range(8)] + [('o', n) for n in range(2)]
    left_loads = [('2', q) for q in range(4)] + [('1', 0), ('o', 0)]

    def load_lefts(name, q):
        for n in range(16):
            pltpu.make_async_copy(
                lefts[name][n // 4].at[:, span(q * 8 + index[n % 4] * 2 + core, piece)],
                d_heads.at[n // 4 * blk:(n // 4 + 1) * blk, n % 4 * piece:(n % 4 + 1) * piece], load_sem.at[14]).start()

    def load_rights(s):
        name, n = parts[s]
        for i in range(4):
            pltpu.make_async_copy(
                rights[name][i].at[:, n * half:(n + 1) * half], spaces[s % 2].at[i * blk:(i + 1) * blk, :],
                load_sem.at[15 + s % 2]).start()

    def stored(s):
        pltpu.make_async_copy(stage.at[s % 2], stage.at[s % 2], load_sem.at[17 + s % 2]).wait()

    def send_part(s):
        name, n = parts[s]
        if name == 'o':
            firsts['o'][n].start()
        else:
            firsts[(name, n // 2)][n % 2].start()

    load_lefts(*left_loads[0])
    load_rights(0)
    load_rights(1)
    for s in range(len(parts)):
        name, n = parts[s]
        if n == 0 or name == '2' and n % 2 == 0:
            every = d_heads.at[:, :4 * piece]
            pltpu.make_async_copy(every, every, load_sem.at[14]).wait()
            left_t[...] = every[...].T
            left_loads.pop(0)
            if left_loads:
                if left_loads[0][0] == 'o':
                    dmid_give.wait_recv()
                load_lefts(*left_loads[0])
        if s + 1 < len(parts) and parts[s + 1][0] != '2':
            if parts[s + 1][0] == '1' and parts[s + 1][1] % 2 == 0:
                dup_give[parts[s + 1][1] // 2].wait_recv()
            load_rights(s + 1)
        space = spaces[s % 2]
        if name != '2' or n < 2:
            pltpu.make_async_copy(space, space, load_sem.at[15 + s % 2]).wait()
        if s >= 1:
            stored(s - 1)
            send_part(s - 1)
        stage[s % 2] = dot_nn(left_t[...], space[...])
        targets = {'2': (away2_ref, mid2_ref, keep2_ref), '1': (away1_ref, mid1_ref, keep1_ref),
                   'o': (awayo_ref, mido_ref, keepo_ref)}[name]
        for row, ref in zip((0, 2 * piece, 3 * piece), targets):
            rows = slice(row, row + (2 * piece if row == 0 else piece))
            if name == 'o':
                for k in range(2):
                    pltpu.make_async_copy(stage.at[s % 2, rows, k * (half // 2):(k + 1) * (half // 2)], ref.at[2 * n + k],
                                          load_sem.at[17 + s % 2]).start()
            else:
                pltpu.make_async_copy(stage.at[s % 2, rows, :], ref.at[n // 2, :, n % 2 * half:(n % 2 + 1) * half],
                                      load_sem.at[17 + s % 2]).start()
    stored(len(parts) - 1)
    send_part(len(parts) - 1)

    for i in range(4):
        @pl.when(role != i)
        def _():
            pltpu.make_async_copy(dc_ref.at[:, :head_cols], dch.at[:blk, :], dc_recv.at[i]).wait()

    moves = {(0, 0): [(add_mid, ('2', 0))], (0, 1): [(add_mid, ('2', 1))], (0, 4): [(finish, ('2', 0))],
             (0, 6): [(add_mid, ('2', 2)), (finish, ('2', 1))], (1, 0): [(send_d_heads, 0)],
             (1, 2): [(finish, ('2', 2)), (add_mid, ('2', 3))], (1, 6): [(finish, ('2', 3))], (1, 7): [(add_mid, ('1', 0))]}
    steps = seq // BWD_ROWS
    for j in range(2):
        k_view, v_view = qkv_ref.at[:, (2 + j) * PAIR:(3 + j) * PAIR], qkv_ref.at[:, (4 + j) * PAIR:(5 + j) * PAIR]
        k_t[...] = k_view[...].T
        dk_acc[...] = jnp.zeros_like(dk_acc)
        dv_acc[...] = jnp.zeros_like(dv_acc)

        def block(i, _):
            for n in range(8):
                if (j, n) in moves:
                    @pl.when(i == min(n, steps - 1))
                    def _():
                        for move, what in moves[(j, n)]:
                            move(what)
            rows = span(i, BWD_ROWS)
            cols = slice(j * PAIR, (j + 1) * PAIR)
            d_heads[rows, cols] = backward_rows(
                qkv_ref[rows, cols], dch[rows, cols], lse_ref[2 * j:2 * j + 2, rows], k_view, v_view,
                k_t, p_cat, ds_cat, dk_acc, dv_acc)
            return 0

        lax.fori_loop(0, steps, block, 0)
        d_heads[:, head_cols + j * PAIR:head_cols + (j + 1) * PAIR] = (dk_acc[...] * SCALE).astype(BF16)
        d_heads[:, 2 * head_cols + j * PAIR:2 * head_cols + (j + 1) * PAIR] = dv_acc[...].astype(BF16)

    quarter = 2 * piece

    def quarter_loads(n):
        return [load(u_ref.at[:, span(index[n], quarter)], u_s.at[n % 2], 8 + n % 2),
                load(gqkv2_ref.at[span(index[n], quarter), :], g_s.at[n % 2], 10 + n % 2)]

    pending = quarter_loads(0)
    for i in range(4):
        @pl.when(role == i)
        def _():
            d_qkv[:, i * 3 * head_cols:(i + 1) * 3 * head_cols] = d_heads[i * blk:(i + 1) * blk, :]
    send_d_heads(1)
    targets = [qa.at[0], qa.at[1], qb.at[0], qb.at[1]]
    first_q = copies.make(qa, q1, to_a)
    for n in range(4):
        ahead = quarter_loads(n + 1) if n < 3 else []
        for copy in pending:
            copy.wait()
        targets[n][...] = dot_tn(u_s[n % 2], d_heads[...]) + g_s[n % 2]
        pending = ahead
        if n == 0:
            far('2')
            add_mid(('1', 1))
            finish(('1', 0))
            finish(('1', 1))
        if n == 2:
            first_q.start()

    add_mid(('1', 2))
    w_rows = w_s.shape[1]
    chunks = wqkv_ref.shape[0] // w_rows
    w_load = load(wqkv_ref.at[:w_rows, :], w_s.at[0], 12)
    for j in range(2):
        for i in range(4):
            @pl.when(role != i)
            def _():
                for t in range(3):
                    pltpu.make_async_copy(d_heads.at[:blk, :PAIR], d_qkv.at[:, :PAIR], dq_recv.at[(j * 4 + i) * 3 + t]).wait()
    for n in range(chunks):
        ahead = load(wqkv_ref.at[(n + 1) * w_rows:(n + 2) * w_rows, :], w_s.at[(n + 1) % 2], 12 + (n + 1) % 2) if n + 1 < chunks else None
        w_load.wait()
        d_1[:, n * w_rows:(n + 1) * w_rows] = dot_nt(d_qkv[...], w_s[n % 2]).astype(BF16)
        w_load = ahead

    count = min(128, blk)
    for n in range(blk // count):
        rows = slice(n * count, (n + 1) * count)
        d_1[rows, :] = through_norm(x_ref[rows, :].astype(F32) + emb_row(emb_ref, 0), d_1[rows, :].astype(F32), dmid_ref[rows, :])

    own_seq, part_rows = z // 2, blk // 2

    def dx_rows(role, h):
        return pl.ds(pl.multiple_of(role * blk + h * part_rows, part_rows), part_rows)

    def dx_copy(n, h, device):
        slot = [0, 1 + core, 3 + core][n]
        return pltpu.make_async_remote_copy(
            src_ref=d_1.at[h * part_rows:(h + 1) * part_rows, :], dst_ref=dx_ref.at[dx_rows(role, h), :],
            send_sem=x_send.at[n * 2 + h], recv_sem=x_recv.at[slot * 2 + h], device_id=device, device_id_type=MESH)

    dx_side = [dx_copy(0, h, partner) for h in range(2)]
    dx_next = [dx_copy(1, h, here.device(z=here.z_by[1], c=own_seq)) for h in range(2)]
    dx_cross = [dx_copy(2, h, here.device(z=far_q, c=own_seq)) for h in range(2)]
    dx_keep = pltpu.make_async_copy(d_1, dx_ref.at[span(role, blk), :], local_sem.at[8])

    def dx_pass(cc, h):
        rows = dx_rows(z % 2 * 2 + cc, h)
        return pltpu.make_async_remote_copy(
            src_ref=dx_ref.at[rows, :], dst_ref=dx_ref.at[rows, :], send_sem=x_send.at[6 + cc * 2 + h],
            recv_sem=x_recv.at[(5 + cc) * 2 + h], device_id=here.device(z=here.z_by[1]), device_id_type=MESH)

    def dx_start(h):
        dx_cross[h].start()
        dx_next[h].start()
        pl.when(no(owner))(dx_side[h].start)

    def dx_got(slot, h):
        rows = d_1.at[:part_rows, :]
        pltpu.make_async_copy(rows, dx_ref.at[:part_rows, :], x_recv.at[slot * 2 + h]).wait()

    def dx_forward(h):
        @pl.when(no(owner))
        def _():
            for cc in range(2):
                dx_got(3 + cc, h)
                dx_pass(cc, h).start()

    finish(('1', 2))
    dx_start(0)
    pl.when(owner)(dx_keep.start)
    add_mid(('1', 3))
    finish(('1', 3))
    add_mid('o')
    dx_forward(0)
    far('1')
    first_q.wait_recv()
    qb[0] += q1[1]
    second_q = copies.start(qb.at[0], q2, to_b)
    qb[1] += q1[0]
    total('2')
    gather_start('2', sum_2, g2_ref, 0)
    second_q.wait_recv()
    qb[1] += q2[...]
    plane_stays = jnp.logical_and(2 * (z % 2) + core == z, z // 2 == core)
    plane_q = pltpu.make_async_remote_copy(
        src_ref=qb.at[1], dst_ref=q3, send_sem=p_send.at[0], recv_sem=p_recv.at[0],
        device_id=here.device(z=2 * (z % 2) + core, c=z // 2), device_id_type=MESH)

    @pl.when(plane_stays)
    def _():
        q3[...] = qb[1]

    pl.when(no(plane_stays))(plane_q.start)
    finish('o')
    total('1')
    gather_start('1', sum_1, g1_ref, 1)
    dx_start(1)
    gather_second('2')
    gather_second('1')
    pl.when(no(plane_stays))(plane_q.wait_recv)
    give_q = copies.start(q3.at[span(1 - core, piece), :], q4.at[0], partner)
    gather_core('2')
    give_q.wait_recv()
    q4[1] = q4[0] + q3[span(core, piece), :]
    far('o')
    for t, (name, out) in enumerate((('q', gq_ref), ('k', gk_ref), ('v', gv_ref))):
        gather_start(name, q4.at[1, :, t * head_cols:(t + 1) * head_cols], out, 3 + t)
    gather_core('1')
    for name in 'qkv':
        gather_second(name)
    for name in 'qkv':
        gather_core(name)
    dx_forward(1)
    total('o')
    gather_start('o', sum_o, go_ref, 2)
    gather_second('o')
    gather_core('o')

    @pl.when(owner)
    def _():
        for h in range(2):
            for slot in (0, 1, 2):
                dx_got(slot, h)
        dx_keep.wait()

    @pl.when(no(owner))
    def _():
        for h in range(2):
            dx_side[h].wait_send()
            for cc in range(2):
                dx_got(5 + cc, h)
                dx_pass(cc, h).wait_send()

    for g in gathers.values():
        for copy in g['c']:
            copy.wait_recv()
    for copy in waits:
        copy.wait()
    for copy in copies.sent:
        copy.wait_send()
    for h in range(2):
        dx_cross[h].wait_send()
        dx_next[h].wait_send()
    pl.when(no(plane_stays))(plane_q.wait_send)
    for i in range(4):
        @pl.when(role != i)
        def _():
            dc_copy(i).wait_send()
            for j in range(2):
                for t in range(3):
                    dq_copy(j, i, t).wait_send()
        for w in '21o':
            pl.when((z + i) % 2 == 1)(near_copy(w, i).wait_send)
    for w in '21o':
        far_copy(w).wait_send()


def last_call(qkv, d_c, lse, d_mid, x, emb, w_qkv, u_seq, g_qkv, w2_sides, w1_sides, wo_sides):
    seq, d_model = u_seq.shape
    blk, piece = seq // 4, d_model // 8
    n1, no = w1_sides[4].shape[1] // 4, wo_sides[3].shape[1] // 4
    assert n1 == d_model == 2 * 2 * BWD_ROWS and no * 2 == 2 * BWD_ROWS
    heads3 = qkv.shape[1]
    anywhere = pl.BlockSpec(memory_space=pl.ANY)
    in_vmem = pl.BlockSpec(memory_space=pltpu.VMEM)
    copies = 5 + 18 + 9 + 6 * 7 + 3
    dma = pltpu.SemaphoreType.DMA
    w_rows = min(128, d_model)
    return pl.pallas_call(
        last_kernel,
        in_specs=[in_vmem] * 6 + [anywhere] * 25,
        out_specs=[anywhere] * 18,
        out_shape=[
            jax.ShapeDtypeStruct((seq, d_model), BF16),
            jax.ShapeDtypeStruct((d_model, n1), F32),
            jax.ShapeDtypeStruct((8 * piece, n1), F32),
            jax.ShapeDtypeStruct((d_model, no), F32),
        ] + [jax.ShapeDtypeStruct((d_model, heads3 // 3), F32)] * 3
        + [jax.ShapeDtypeStruct((4, k * piece, n), F32) for n in (n1, n1, no) for k in (2, 1, 1)]
        + [jax.ShapeDtypeStruct((blk, n), BF16) for n in (4 * n1, d_model)],
        scratch_shapes=[
            pltpu.VMEM((seq, heads3 // 3), BF16),
            pltpu.VMEM((PAIR, seq), BF16),
            pltpu.VMEM((seq, PAIR), F32),
            pltpu.VMEM((seq, PAIR), F32),
            pltpu.VMEM((seq, 2 * BWD_ROWS), BF16),
            pltpu.VMEM((seq, 2 * BWD_ROWS), BF16),
            pltpu.VMEM((seq, heads3), BF16),
            pltpu.VMEM((blk, 4 * heads3), BF16),
            pltpu.VMEM((8, 2 * piece, n1), F32),
            pltpu.VMEM((4, 2 * piece, no), F32),
            pltpu.VMEM((8, piece, n1), F32),
            pltpu.VMEM((4, piece, no), F32),
            pltpu.VMEM((2, piece, n1), F32),
            pltpu.VMEM((2, 4, piece, no), F32),
            pltpu.VMEM((2, 3, piece, n1), F32),
            pltpu.VMEM((3, piece, no), F32),
            pltpu.VMEM((piece, n1), F32),
            pltpu.VMEM((piece, n1), F32),
            pltpu.VMEM((piece, no), F32),
            pltpu.VMEM((2, 2 * piece, heads3), F32),
            pltpu.VMEM((2, 2 * piece, heads3), F32),
            pltpu.VMEM((2, 2 * piece, heads3), F32),
            pltpu.VMEM((2 * piece, heads3), F32),
            pltpu.VMEM((2 * piece, heads3), F32),
            pltpu.VMEM((2, piece, heads3), F32),
            pltpu.VMEM((blk, d_model), BF16),
            pltpu.VMEM((2, w_rows, 4 * heads3), BF16),
            pltpu.VMEM((2, seq, 2 * piece), BF16),
            pltpu.VMEM((2, 2 * piece, heads3), F32),
            pltpu.VMEM((4 * piece, seq), BF16),
            pltpu.VMEM((2, 4 * piece, 2 * BWD_ROWS), F32),
            dma((9,)), dma((19,)), dma((copies,)), dma((copies,)),
            dma((4,)), dma((4,)), dma((24,)), dma((24,)), dma((9,)), dma((9,)), dma((10,)), dma((14,)), dma((1,)), dma((1,)),
        ],
        compiler_params=pltpu.CompilerParams(vmem_limit_bytes=63 << 20, collective_id=1, has_side_effects=True),
        cost_estimate=pl.CostEstimate(
            flops=160 * seq * seq * PAIR, bytes_accessed=128 * seq * d_model, transcendentals=seq * seq * 4),
        name="last",
    )(qkv, d_c, lse, d_mid, x, emb, w_qkv, u_seq, g_qkv, *w2_sides, *w1_sides, *wo_sides)[:7]


def solution(mesh):
    spec_col = P(None, 'model')
    spec_row = P('model', None)
    spec_act = P('data', None, None)
    spec_rep = P(None, None)

    def device_step(x_in, cot_out, step_emb, w_q, w_k, w_v, w_o, w_1, w_2):
        d_model = x_in.shape[2]
        c_1, lse_1, x_seq, cot, wo, w1, w2, w_qkv, x_1, h_1, m_1, up_1, act_1, x_2 = first_call(
            x_in[0], cot_out[0], step_emb, w_q, w_k, w_v, w_o, w_1, w_2)
        wo, w2 = wo.reshape(-1, d_model), w2.reshape(-1, d_model)

        c_2, lse_2, u_2_seq, qkv_2, u_1_seq, qkv_1 = forward_call(x_2, step_emb, x_seq, w_qkv)
        _, m_2, act_2, d_up_2, d_mid_2, d_c = hidden_call(True, True, wo, w1, w2, context=c_2, x=x_2, emb=step_emb, d_next=cot)
        shared = (act_2, act_1, cot, m_2, m_1, d_up_2, d_mid_2, c_2, c_1)
        d_2, d_2_other, g_qkv_2, *others = backward_call(
            qkv_2, d_c, lse_2, d_mid_2, x_2, step_emb, w_qkv, u_2_seq, shared)
        act_2o, act_1o, cot_o, m_2o, m_1o, d_up_2o, d_mid_2o, c_2o, c_1o = others
        d_up_1, d_mid_1, d_c = hidden_call(False, True, wo, w1, w2, h=h_1, up=up_1, d_next=d_2)
        w2_parts = (act_2, act_2o, act_1, act_1o, cot, cot_o, d_2, d_2_other)
        w1_sides = (m_2, m_2o, m_1, m_1o, d_up_2, d_up_2o, d_up_1)
        wo_sides = (d_mid_2, d_mid_2o, d_mid_1, c_2, c_2o, c_1, c_1o)
        d_x, g_w1, g_w2, g_wo, g_q, g_k, g_v = last_call(
            qkv_1, d_c, lse_1, d_mid_1, x_1, step_emb, w_qkv, u_1_seq, g_qkv_2, w2_parts, w1_sides, wo_sides)
        return g_q, g_k, g_v, g_wo.T, g_w1, g_w2, d_x[None]

    return jax.shard_map(device_step, mesh=mesh,
                         in_specs=(spec_act, spec_act, spec_rep, spec_col, spec_col, spec_col, spec_row, spec_col, spec_row),
                         out_specs=(spec_col, spec_col, spec_col, spec_row, spec_col, spec_row, spec_act),
                         check_vma=False)
```
